32 devices in a mesh: dp: 8 (over z, x), head: 4 (over y, core).
Axes of the slice: x: 2, y: 2, z: 4, core: 2. Of those that a mesh axis runs over, the one named last changes fastest.
Arguments:
- inputs: bfloat16 [16384, 1024], P(('dp', 'head')), may hold values from -6 to 6
- lengths: int32 [8, 4], P('dp'), may hold values from 1 to 1024, 2048 in all within a row
- attn_gain: bfloat16 [1024], replicated, may hold values from 0.5 to 1.5
- attn_shift: bfloat16 [1024], replicated, may hold values from -3 to 3
- mlp_gain: bfloat16 [1024], replicated, may hold values from 0.5 to 1.5
- mlp_shift: bfloat16 [1024], replicated, may hold values from -3 to 3
- w_qkv: bfloat16 [1024, 3072], replicated, may hold values from -0.1875 to 0.1875
- b_qkv: bfloat16 [3072], replicated, may hold values from -3 to 3
- w_out: bfloat16 [1024, 1024], replicated, may hold values from -1.5 to 1.5
- b_out: bfloat16 [1024], replicated, may hold values from -3 to 3
- w_up: bfloat16 [1024, 4096], replicated, may hold values from -0.1875 to 0.1875
- b_up: bfloat16 [4096], replicated, may hold values from -3 to 3
- w_down: bfloat16 [4096, 1024], replicated, may hold values from -0.09375 to 0.09375
- b_down: bfloat16 [1024], replicated, may hold values from -3 to 3
- cotangent: bfloat16 [16384, 1024], P(('dp', 'head')), may hold values from -6 to 6
Outputs:
- output: bfloat16 [16384, 1024], P(('dp', 'head'))
- grad_inputs: float32 [16384, 1024], P(('dp', 'head'))
- grad_attn_gain: float32 [1024], replicated
- grad_attn_shift: float32 [1024], replicated
- grad_mlp_gain: float32 [1024], replicated
- grad_mlp_shift: float32 [1024], replicated
- grad_w_qkv: float32 [1024, 3072], P('dp', 'head')
- grad_b_qkv: float32 [3072], replicated
- grad_w_out: float32 [1024, 1024], P('dp', 'head')
- grad_b_out: float32 [1024], replicated
- grad_w_up: float32 [1024, 4096], P('dp', 'head')
- grad_b_up: float32 [4096], replicated
- grad_w_down: float32 [4096, 1024], P('dp', 'head')
- grad_b_down: float32 [1024], replicated
The draws below stay inside these ranges and needn't reach their ends.
Inputs may be any that keep to these rules, and one draw needn't show every extreme that they name: Each row lists the lengths of the 4 sequences packed in order into one group of 2048 tokens; a row sums to 2048 and its longest sequence has 1024 tokens.
All inputs are finite; a program needn't handle non-finite values.
Results may differ from the reference program's by a relative error of at most 0.012.
Values may be sent and summed in bfloat16 or wider, within the bound.
A program may use at most 192 MiB of HBM per device.

```python
import math
import jax
import jax.numpy as jnp
import numpy as np
from jax import lax

D = 1024
HEADS = 16
HD = 64
ROT = 16
FF = 4096
SEQS = 4
GROUP_TOK = 2048
MAXLEN = 1024
GROUPS = 8
TOKENS = 16384


def strengthened(entries, own_key, source, target, shards_of, factor):
    owner, partner = [(jnp.arange(entries.shape[axis_at]) // (entries.shape[axis_at] // shards_of)).reshape([-1 if axis == axis_at else 1 for axis in range(entries.ndim)]) for axis_at in (source, target)]
    chosen = jax.random.permutation(own_key, shards_of)[partner]
    strong = (owner == chosen) | (owner == (partner + shards_of // 2) % shards_of)
    return jnp.where(strong, factor * entries, entries)


def level_of(key, extent, cuts, low, high):
    level = 1.0
    for dim, parts in cuts:
        steps = jax.random.uniform(jax.random.fold_in(jax.random.fold_in(key, 6), dim), (parts,), jnp.float32, low / len(cuts), high / len(cuts))
        level = level * jnp.repeat(jnp.exp(steps), extent[dim] // parts).reshape((-1,) + (1,) * (len(extent) - 1 - dim))
    return level


def length_profile(count, total, bound, slope):
    portions = [(1 << 20) // math.isqrt(rank ** slope) + 1 for rank in range(2, count + 1)]
    spare, counts = total - bound - (count - 1), [1] * (count - 1)
    while spare > 0:
        free = [i for i in range(count - 1) if counts[i] < bound]
        pool, left = sum([portions[i] for i in free]), spare
        for i in free:
            addition = min(bound - counts[i], max(1, left * portions[i] // pool), spare)
            counts[i] = counts[i] + addition
            spare = spare - addition
    return np.array([bound] + counts)


def uneven(key, amount, total, bound, skew):
    if amount == 2:
        one = jax.random.randint(key, (), max(1, total - bound), min(bound, total - 1) + 1)
        return jnp.stack([one, total - one])
    tallies = jnp.asarray(length_profile(amount, total, bound, skew), jnp.int32)
    couples = (amount - 1) // 2
    giver, taker = tallies[1:1 + 2 * couples:2], tallies[2:2 + 2 * couples:2]
    margin = jnp.minimum(giver - 1, bound - taker)
    shifted = jax.random.randint(jax.random.fold_in(key, 1), (couples,), 0, 1 << 20) % (margin + 1)
    tallies = tallies.at[1:1 + 2 * couples:2].set(giver - shifted).at[2:2 + 2 * couples:2].set(taker + shifted)
    return tallies[jax.random.permutation(jax.random.fold_in(key, 2), amount)]


def noise(own_key, dims, width, limit, split=(), kind=jnp.bfloat16):
    values = width * jax.random.normal(own_key, dims, jnp.float32)
    if split:
        values = values * level_of(own_key, dims, split, -0.22, 0.18)
    return jnp.clip(values, -limit, limit).astype(kind)


def bell_draw_with(key, shape, spread, most, pieces, heavy, kind=jnp.bfloat16):
    values = spread * jax.random.normal(key, shape, jnp.float32)
    if pieces:
        values = values * level_of(key, shape, pieces, -0.22, 0.18)
    return jnp.clip(strengthened(values, jax.random.fold_in(key, 3), *heavy), -most, most).astype(kind)


def setup_inputs(seed: int = 0) -> dict:
    streams_of = jax.random.split(jax.random.key(seed), 16)
    inputs = noise(streams_of[0], (TOKENS, D), 1.0, 6.0, ((0, 32),))
    lengths = jax.vmap(lambda own: uneven(own, SEQS, GROUP_TOK, MAXLEN, 2))(jax.random.split(streams_of[1], GROUPS)).reshape((GROUPS, SEQS)).astype(jnp.int32)
    attn_gain = jnp.clip(1.0 + 0.1 * jax.random.normal(streams_of[2], (D,), jnp.float32), 0.5, 1.5).astype(jnp.bfloat16)
    attn_shift = noise(streams_of[3], (D,), 0.5, 3.0)
    mlp_gain = jnp.clip(1.0 + 0.1 * jax.random.normal(streams_of[4], (D,), jnp.float32), 0.5, 1.5).astype(jnp.bfloat16)
    mlp_shift = noise(streams_of[5], (D,), 0.5, 3.0)
    w_qkv = noise(streams_of[6], (D, 3 * D), D ** -0.5, 0.1875)
    b_qkv = noise(streams_of[7], (3 * D,), 0.5, 3.0)
    w_out = noise(streams_of[8], (D, D), (D // 64) ** -0.5, 1.5)
    b_out = noise(streams_of[9], (D,), 0.5, 3.0)
    w_up = noise(streams_of[10], (D, FF), D ** -0.5, 0.1875)
    b_up = noise(streams_of[11], (FF,), 0.5, 3.0)
    w_down = noise(streams_of[12], (FF, D), FF ** -0.5, 0.09375)
    b_down = noise(streams_of[13], (D,), 0.5, 3.0)
    cotangent = bell_draw_with(streams_of[14], (TOKENS, D), 1.0, 6.0, ((0, 32),), (0, 1, 32, 2.75))
    return dict(inputs=inputs, lengths=lengths, attn_gain=attn_gain, attn_shift=attn_shift, mlp_gain=mlp_gain, mlp_shift=mlp_shift, w_qkv=w_qkv, b_qkv=b_qkv, w_out=w_out, b_out=b_out, w_up=w_up, b_up=b_up, w_down=w_down, b_down=b_down, cotangent=cotangent)


@jax.custom_vjp
def low(v):
    return lax.optimization_barrier(v.astype(jnp.bfloat16)).astype(jnp.float32)

@jax.custom_vjp
def low_back(v):
    return v

def low_keep(v):
    return (low(v), None)

def low_pass(kept, grad):
    return (grad,)

def back_keep(v):
    return (v, None)

def back_low(kept, grad):
    return (low(grad),)
low.defvjp(low_keep, low_pass)
low_back.defvjp(back_keep, back_low)

def matmul(left, right):
    return jnp.dot(left, right, precision=lax.Precision.HIGHEST, preferred_element_type=jnp.float32)

def layer_norm(value, gain, shift):
    center = value - lax.optimization_barrier(jnp.mean(value, axis=-1, keepdims=True))
    scale_inv = lax.rsqrt(lax.optimization_barrier(jnp.mean(center * center, axis=-1, keepdims=True)) + 1e-05)
    normed = center * scale_inv
    return normed * gain + shift

def group_layout(seq_lens, total_len):
    seq_ends = jnp.cumsum(seq_lens, dtype=jnp.int32)
    starts = seq_ends - seq_lens
    index = jnp.arange(total_len, dtype=jnp.int32)
    segment = lax.optimization_barrier(jnp.sum((index[:, None] >= seq_ends[None, :]).astype(jnp.int32), axis=1, dtype=jnp.int32))
    chosen = segment[:, None] == jnp.arange(seq_lens.shape[0], dtype=jnp.int32)[None, :]
    offset = lax.optimization_barrier(jnp.sum(jnp.where(chosen, starts[None, :], 0), axis=1, dtype=jnp.int32))
    return (segment, index - offset)

def rotate(value, position, sign):
    half_rot = ROT // 2
    freqs = 10000.0 ** (-(2.0 * jnp.arange(half_rot, dtype=jnp.float32)) / ROT)
    angles = position.astype(jnp.float32)[:, None] * freqs[None, :]
    cosine = jnp.cos(angles)[:, None, :]
    sine = jnp.sin(angles)[:, None, :]
    first = value[..., :half_rot]
    second = value[..., half_rot:ROT]
    return jnp.concatenate([first * cosine - sign * second * sine, second * cosine + sign * first * sine, value[..., ROT:]], axis=-1)

def group_forward(params, group_in, seq_lens):
    attn_gain, attn_shift, mlp_gain, mlp_shift, w_qkv, b_qkv, w_out, b_out, w_up, b_up, w_down, b_down = params
    rows = group_in.shape[0]
    norm_attn = low(layer_norm(group_in, attn_gain, attn_shift))
    norm_mlp = low(layer_norm(group_in, mlp_gain, mlp_shift))
    triple = low(low_back(matmul(norm_attn, w_qkv) + b_qkv)).reshape(rows, 3, HEADS, HD)
    segment, position = group_layout(seq_lens, rows)
    queries = low(rotate(triple[:, 0], position, 1.0))
    keys_rot = low(rotate(triple[:, 1], position, 1.0))
    values = triple[:, 2]
    block = min(512, rows)
    key_index = jnp.arange(rows, dtype=jnp.int32)

    def one_block(block_id):
        start = block_id * block
        query_blk = lax.dynamic_slice_in_dim(queries, start, block, 0)
        row_index = start + jnp.arange(block, dtype=jnp.int32)
        row_seg = lax.dynamic_slice_in_dim(segment, start, block, 0)
        scores = jnp.einsum('qhd,khd->hqk', query_blk, keys_rot, precision=lax.Precision.HIGHEST) * HD ** (-0.5)
        scores = low_back(scores)
        allowed = (row_seg[:, None] == segment[None, :]) & (key_index[None, :] <= row_index[:, None])
        scores = jnp.where(allowed[None], scores, -1e+30)
        peak = lax.optimization_barrier(jnp.max(scores, axis=-1, keepdims=True))
        weights = jnp.exp(scores - peak)
        weights = low(weights / lax.optimization_barrier(jnp.sum(weights, axis=-1, keepdims=True)))
        return jnp.einsum('hqk,khd->qhd', weights, values, precision=lax.Precision.HIGHEST)
    context = lax.map(jax.checkpoint(one_block), jnp.arange(rows // block, dtype=jnp.int32))
    context = low(low_back(context.reshape(rows, D)))
    attn_part = matmul(context, w_out) + b_out
    pre_act = low_back(matmul(norm_mlp, w_up) + b_up)
    hidden = low(jax.nn.gelu(pre_act, approximate=False))
    mlp_part = matmul(hidden, w_down) + b_down
    return group_in + attn_part + mlp_part

def reference(inputs, lengths, attn_gain, attn_shift, mlp_gain, mlp_shift, w_qkv, b_qkv, w_out, b_out, w_up, b_up, w_down, b_down, cotangent):
    params = tuple([tensor.astype(jnp.float32) for tensor in (attn_gain, attn_shift, mlp_gain, mlp_shift, w_qkv, b_qkv, w_out, b_out, w_up, b_up, w_down, b_down)])
    grouped = inputs.astype(jnp.float32).reshape(GROUPS, GROUP_TOK, D)
    checked = jax.checkpoint(group_forward)

    def forward(grouped_in, weights):

        def step(carry, item):
            return (carry, checked(weights, item[0], item[1]))
        unused, outputs = lax.scan(step, jnp.zeros((), jnp.float32), (grouped_in, lengths))
        return outputs
    result, pullback = jax.vjp(forward, grouped, params)
    grad_in, grads = pullback(cotangent.astype(jnp.float32).reshape(GROUPS, GROUP_TOK, D))
    return (result.reshape(TOKENS, D).astype(jnp.bfloat16), grad_in.reshape(TOKENS, D), grads[0], grads[1], grads[2], grads[3], grads[4], grads[5], grads[6], grads[7], grads[8], grads[9], grads[10], grads[11])
```

```python
import functools

import jax
import jax.numpy as jnp
from jax import lax
from jax.experimental import pallas as pl
from jax.experimental.pallas import tpu as pltpu
from jax.sharding import PartitionSpec as P

HD = 64
ROT = 16
HALF = ROT // 2
NN = (((1,), (0,)), ((), ()))
NT = (((1,), (1,)), ((), ()))
TN = (((0,), (0,)), ((), ()))
BF = jnp.bfloat16
F32 = jnp.float32
VMEM_LIMIT = 62 * 1024 * 1024


def mm(a, b, dims=NN):
    return lax.dot_general(a, b, dims, preferred_element_type=F32)


def norm_parts(x):
    v = x.astype(F32)
    center = v - jnp.mean(v, axis=-1, keepdims=True)
    inv = lax.rsqrt(jnp.mean(center * center, axis=-1, keepdims=True) + 1e-5)
    return center * inv, inv


def mlp_kernel(prev, final, pos, *refs):
    x_ref, dy_ref, wu, wd, bu, gain, shift = refs[:7]
    refs = refs[7:]
    if prev:
        pwu, pwd, psmall, psmallf = refs[:4]
        refs = refs[4:]
    part_ref, g_ref, out_wu, out_wd, small, smallf = refs[:6]
    if final:
        dwu, dwd = refs[6:8]
    else:
        dwu, dwd = out_wu, out_wd
    step = pl.program_id(0)

    @pl.when(step == 0)
    def _():
        if prev:
            dwu[...] = pwu[...]
            dwd[...] = pwd[...]
            small[...] = psmall[...]
            smallf[...] = psmallf[...]
        else:
            dwu[...] = jnp.zeros_like(dwu)
            dwd[...] = jnp.zeros_like(dwd)
            small[...] = jnp.zeros_like(small)
            smallf[...] = jnp.zeros_like(smallf)

    normed, _unused = norm_parts(x_ref[...])
    scale = gain[...].astype(F32)
    nm = (normed * scale + shift[...].astype(F32)).astype(BF)
    dy = dy_ref[...]
    pre = mm(nm, wu[...]) + bu[...].astype(F32)
    cdf = 0.5 + 0.5 * lax.erf(pre * (0.5**0.5))
    hid = (pre * cdf).astype(BF)
    slope = cdf + pre * (jnp.exp(-0.5 * pre * pre) * 0.3989422804014327)
    gp = (mm(dy, wd[...], NT) * slope).astype(BF)
    part_ref[...] = mm(hid, wd[...]).astype(BF)
    r = mm(gp, wu[...], NT)
    g_ref[...] = (r * scale).astype(BF)
    smallf[0:1, :] += jnp.sum(gp.astype(F32), axis=0, keepdims=True)
    small[0:1, :] += jnp.sum(r * normed, axis=0, keepdims=True)
    small[1:2, :] += jnp.sum(r, axis=0, keepdims=True)
    small[2:3, :] += jnp.sum(dy.astype(F32), axis=0, keepdims=True)
    dwd[...] += mm(hid, dy, TN)
    dwu[...] += mm(nm, gp, TN)

    if final:

        @pl.when(step == pl.num_programs(0) - 1)
        def _():
            out_wu[...] = dwu[...].astype(BF)
            out_wd[...] = dwd[...].astype(BF)


def mlp(pos, x, dy, wu, wd, bu, gain, shift, n, prev=None, final=True, tt=512):
    tok, d = x.shape
    f = wu.shape[1] // n
    row = lambda i, p: (i, 0)
    zero = lambda i, p: (0, 0)
    one = pl.Buffered(1)
    const = lambda shape: pl.BlockSpec(shape, zero, pipeline_mode=one)
    accs = [const((d, f)), const((f, d)), const((8, d)), const((8, f))]
    kind = BF if final else F32
    grid_spec = pltpu.PrefetchScalarGridSpec(
        num_scalar_prefetch=1,
        grid=(tok // tt,),
        in_specs=[
            pl.BlockSpec((tt, d), row),
            pl.BlockSpec((tt, d), row),
            pl.BlockSpec((d, f), lambda i, p: (0, p[0]), pipeline_mode=one),
            pl.BlockSpec((f, d), lambda i, p: (p[0], 0), pipeline_mode=one),
            pl.BlockSpec((1, f), lambda i, p: (0, p[0])),
            const((1, d)),
            const((1, d)),
        ]
        + (accs if prev is not None else []),
        out_specs=[pl.BlockSpec((tt, d), row), pl.BlockSpec((tt, d), row)] + accs,
        scratch_shapes=[pltpu.VMEM((d, f), F32), pltpu.VMEM((f, d), F32)] if final else [],
    )
    return pl.pallas_call(
        functools.partial(mlp_kernel, prev is not None, final),
        grid_spec=grid_spec,
        out_shape=(
            jax.ShapeDtypeStruct((tok, d), BF),
            jax.ShapeDtypeStruct((tok, d), BF),
            jax.ShapeDtypeStruct((d, f), kind),
            jax.ShapeDtypeStruct((f, d), kind),
            jax.ShapeDtypeStruct((8, d), F32),
            jax.ShapeDtypeStruct((8, f), F32),
        ),
        compiler_params=pltpu.CompilerParams(vmem_limit_bytes=VMEM_LIMIT),
        cost_estimate=pl.CostEstimate(
            flops=12 * tok * d * f, bytes_accessed=8 * tok * d + 12 * d * f, transcendentals=2 * tok * f
        ),
        name="mlp",
    )(pos, x, dy, wu, wd, bu, gain, shift, *(prev or ()))


def proj_kernel(nh, prev, pos, *refs):
    x_ref, dy_ref, wq, wk, wv, bq, bk, bv, wo, gain, shift, cos, sin = refs[:13]
    qt, kt, vt, dot, kn, vn, na_ref = refs[13 + (7 if prev else 0) :]
    normed, _unused = norm_parts(x_ref[...])
    na = (normed * gain[...].astype(F32) + shift[...].astype(F32)).astype(BF)
    na_ref[...] = na
    co = cos[...]
    si = sin[...]

    def rotated(t, scale):
        rows = []
        for h in range(nh):
            u = t[h * HD : (h + 1) * HD]
            u1 = u[:HALF]
            u2 = u[HALF:ROT]
            rows += [u1 * co - u2 * si, u2 * co + u1 * si, u[ROT:]]
        out = jnp.concatenate(rows, axis=0).astype(BF)
        return out if scale is None else out * jnp.asarray(scale, BF)

    def triple(w, b):
        return (mm(na, w[...]) + b[...].astype(F32)).astype(BF)

    qt[...] = rotated(triple(wq, bq).astype(F32).T, HD**-0.5)
    keys = rotated(triple(wk, bk).astype(F32).T, None)
    kt[...] = keys
    kn[...] = keys.T
    values = triple(wv, bv)
    vn[...] = values
    vt[...] = values.T
    dot[...] = mm(wo[...], dy_ref[...], NT).astype(BF)


def proj(pos, x, dy, w_qkv, b_qkv, w_out, gain, shift, cos, sin, n, total, first, prev=None, tt=512):
    tok, d = x.shape
    w = d // n
    nh = w // HD
    off = first // tt
    row = lambda i, p: (i, 0)
    zero = lambda i, p: (0, 0)
    one = pl.Buffered(1)
    wspec = lambda k: pl.BlockSpec((d, w), lambda i, p: (0, k * n + p[0]), pipeline_mode=one)
    bspec = lambda k: pl.BlockSpec((1, w), lambda i, p: (0, k * n + p[0]))
    lane = lambda rows: pl.BlockSpec((rows, tt), lambda i, p: (0, off + i))
    nat = lambda cols: pl.BlockSpec((tt, cols), lambda i, p: (off + i, 0))
    shapes = [(w, total)] * 4 + [(total, w)] * 2 + [(total, d)]
    grid_spec = pltpu.PrefetchScalarGridSpec(
        num_scalar_prefetch=1,
        grid=(tok // tt,),
        in_specs=[pl.BlockSpec((tt, d), row), pl.BlockSpec((tt, d), row)]
        + [wspec(0), wspec(1), wspec(2), bspec(0), bspec(1), bspec(2)]
        + [pl.BlockSpec((w, d), lambda i, p: (p[0], 0), pipeline_mode=one)]
        + [pl.BlockSpec((1, d), zero), pl.BlockSpec((1, d), zero), lane(HALF), lane(HALF)]
        + ([pl.BlockSpec(memory_space=pl.ANY)] * 7 if prev is not None else []),
        out_specs=[lane(w)] * 4 + [nat(w)] * 2 + [nat(d)],
    )
    return pl.pallas_call(
        functools.partial(proj_kernel, nh, prev is not None),
        grid_spec=grid_spec,
        out_shape=tuple(jax.ShapeDtypeStruct(s, BF) for s in shapes),
        input_output_aliases={14 + k: k for k in range(7)} if prev is not None else {},
        compiler_params=pltpu.CompilerParams(vmem_limit_bytes=VMEM_LIMIT),
        cost_estimate=pl.CostEstimate(
            flops=8 * tok * d * w, bytes_accessed=6 * tok * d + 12 * tok * w + 8 * d * w, transcendentals=0
        ),
        name="proj",
    )(pos, x, dy, w_qkv, w_qkv, w_qkv, b_qkv, b_qkv, b_qkv, w_out, gain, shift, cos, sin, *(prev or ()))


def attn_kernel(nh, tok, blk, per, lens, rel, cos, sin, seg_start, qt, kt, vt, dot, kn, vn,
                gt_ref, ctx_ref, exps, peaks, dk, dv, oacc, dqacc, mrow, lrow, drow, qpad, dopad):
    nseq = lens.shape[0]
    nblk = tok // blk
    shift = rel[0]

    def place(b):
        return pl.multiple_of(((b // per) ^ shift) * (per * blk) + (b % per) * blk, blk)

    dk[...] = jnp.zeros_like(dk)
    dv[...] = jnp.zeros_like(dv)
    qpad[...] = jnp.zeros_like(qpad)
    dopad[...] = jnp.zeros_like(dopad)
    rows_iota = lax.broadcasted_iota(jnp.int32, (blk, blk), 0)
    cols_iota = lax.broadcasted_iota(jnp.int32, (1, blk), 1)

    def one_block(i, carry):
        first_tok = i * blk
        begin = jnp.int32(0)
        total = jnp.int32(0)
        for s in range(nseq - 1):
            total = total + lens[s]
            begin = jnp.where(total <= first_tok, total, begin)
        low = begin // blk
        cols = pl.ds(place(i), blk)
        start_row = seg_start[:, cols]
        query_idx = cols_iota + first_tok
        for h in range(nh):
            half = (h % 2) * HD
            qpad[h, half : half + HD, :] = qt[h * HD : (h + 1) * HD, cols]
            dopad[h, half : half + HD, :] = dot[h * HD : (h + 1) * HD, cols]
        mrow[...] = jnp.full_like(mrow, -1e30)
        lrow[...] = jnp.zeros_like(lrow)
        oacc[...] = jnp.zeros_like(oacc)
        dqacc[...] = jnp.zeros_like(dqacc)

        def forward(step, c):
            b = i - step
            krow = place(b)
            kidx = rows_iota + b * blk
            allowed = (kidx >= start_row) & (kidx <= query_idx)
            for h in range(nh):
                pair = (h // 2) * 128
                s = mm(kn[pl.ds(krow, blk), pair : pair + 128], qpad[h])
                s = jnp.where(allowed, s, -1e30)
                old = mrow[h : h + 1, :]
                new = jnp.maximum(old, jnp.max(s, axis=0, keepdims=True))
                e = jnp.exp(s - new)
                alpha = jnp.exp(old - new)
                lrow[h : h + 1, :] = lrow[h : h + 1, :] * alpha + jnp.sum(e, axis=0, keepdims=True)
                mrow[h : h + 1, :] = new
                peaks[step, h : h + 1, :] = new
                exps[h, step] = e
                oacc[h] = oacc[h] * alpha + mm(vt[h * HD : (h + 1) * HD, pl.ds(krow, blk)], e.astype(BF))
            return c

        lax.fori_loop(0, i - low + 1, forward, 0)
        for h in range(nh):
            hs = slice(h * HD, (h + 1) * HD)
            inv = 1.0 / lrow[h : h + 1, :]
            o = oacc[h] * inv
            drow[h : h + 1, :] = jnp.sum(o * dot[hs, cols].astype(F32), axis=0, keepdims=True)
            lrow[h : h + 1, :] = inv
            ctx_ref[hs, cols] = o.astype(BF)

        def backward(step, c):
            kcols = pl.ds(place(i - step), blk)
            for h in range(nh):
                pair = (h // 2) * 128
                hs = slice(h * HD, (h + 1) * HD)
                factor = jnp.exp(peaks[step, h : h + 1, :] - mrow[h : h + 1, :]) * lrow[h : h + 1, :]
                p = exps[h, step] * factor
                dp = mm(vn[kcols, pair : pair + 128], dopad[h])
                ds = (p * (dp - drow[h : h + 1, :])).astype(BF)
                dv[hs, kcols] += mm(dot[hs, cols], p.astype(BF), NT)
                dk[hs, kcols] += mm(qt[hs, cols], ds, NT)
                dqacc[hs, :] += mm(kt[hs, kcols], ds)
            return c

        lax.fori_loop(0, i - low + 1, backward, 0)
        co = cos[:, cols]
        si = sin[:, cols]
        for h in range(nh):
            base = h * HD
            g = dqacc[base : base + HD, :] * (HD**-0.5)
            g1 = g[:HALF]
            g2 = g[HALF:ROT]
            gt_ref[base : base + HD, cols] = jnp.concatenate(
                [g1 * co + g2 * si, g2 * co - g1 * si, g[ROT:]], axis=0
            ).astype(BF)
        return carry

    lax.fori_loop(0, nblk, one_block, 0)

    def finish(i, carry):
        cols = pl.ds(pl.multiple_of(i * blk, blk), blk)
        co = cos[:, cols]
        si = sin[:, cols]
        for h in range(nh):
            base = h * HD
            g = dk[base : base + HD, cols]
            g1 = g[:HALF]
            g2 = g[HALF:ROT]
            gt_ref[nh * HD + base : nh * HD + base + HD, cols] = jnp.concatenate(
                [g1 * co + g2 * si, g2 * co - g1 * si, g[ROT:]], axis=0
            ).astype(BF)
        gt_ref[2 * nh * HD :, cols] = dv[:, cols].astype(BF)
        return carry

    lax.fori_loop(0, nblk, finish, 0)


def attention(lens, rel, cos, sin, seg_start, qt, kt, vt, dot, kn, vn, chunk, maxlen, blk=256):
    width, tok = qt.shape
    nh = width // HD
    wb = maxlen // blk + 1
    vm = pl.BlockSpec(memory_space=pltpu.VMEM)
    sm = pl.BlockSpec(memory_space=pltpu.SMEM)
    return pl.pallas_call(
        functools.partial(attn_kernel, nh, tok, blk, chunk // blk),
        out_shape=(jax.ShapeDtypeStruct((3 * width, tok), BF), jax.ShapeDtypeStruct((width, tok), BF)),
        in_specs=[sm, sm] + [vm] * 9,
        out_specs=(vm, vm),
        scratch_shapes=[
            pltpu.VMEM((nh, wb, blk, blk), F32),
            pltpu.VMEM((wb, 8, blk), F32),
            pltpu.VMEM((width, tok), F32),
            pltpu.VMEM((width, tok), F32),
            pltpu.VMEM((nh, HD, blk), F32),
            pltpu.VMEM((width, blk), F32),
            pltpu.VMEM((8, blk), F32),
            pltpu.VMEM((8, blk), F32),
            pltpu.VMEM((8, blk), F32),
            pltpu.VMEM((nh, 128, blk), BF),
            pltpu.VMEM((nh, 128, blk), BF),
        ],
        compiler_params=pltpu.CompilerParams(vmem_limit_bytes=VMEM_LIMIT),
        cost_estimate=pl.CostEstimate(
            flops=20 * width * tok * maxlen, bytes_accessed=20 * width * tok, transcendentals=nh * tok * maxlen
        ),
        name="attention",
    )(lens, rel, cos, sin, seg_start, qt, kt, vt, dot, kn, vn)


def post_kernel(prev, final, pos, *refs):
    gt_ref, na_ref, x_ref, gm_ref, wq, wk, wv, gain = refs[:8]
    refs = refs[8:]
    if prev:
        pw, pb, psmall = refs[:3]
        refs = refs[3:]
    g_ref, out_w, bias, small = refs[:4]
    dw = refs[4] if final else out_w
    step = pl.program_id(0)

    @pl.when(step == 0)
    def _():
        if prev:
            dw[...] = pw[...]
            bias[...] = pb[...]
            small[...] = psmall[...]
        else:
            dw[...] = jnp.zeros_like(dw)
            bias[...] = jnp.zeros_like(bias)
            small[...] = jnp.zeros_like(small)

    gt = gt_ref[...]
    w = wq.shape[1]
    normed, _unused = norm_parts(x_ref[...])
    scale = gain[...].astype(F32)
    gn = gt.T
    r = mm(gn[:, :w], wq[...], NT) + mm(gn[:, w : 2 * w], wk[...], NT) + mm(gn[:, 2 * w :], wv[...], NT)
    g_ref[...] = (r * scale + gm_ref[...].astype(F32)).astype(BF)
    small[0:1, :] += jnp.sum(r * normed, axis=0, keepdims=True)
    small[1:2, :] += jnp.sum(r, axis=0, keepdims=True)
    bias[0:1, :] += jnp.sum(gn.astype(F32), axis=0, keepdims=True)
    dw[...] += mm(gt, na_ref[...])

    if final:

        @pl.when(step == pl.num_programs(0) - 1)
        def _():
            for b in range(dw.shape[1] // 128):
                out_w[b] = dw[:, b * 128 : (b + 1) * 128].astype(BF)


def post(pos, gt, na, x, gm, w_qkv, gain, n, first, prev=None, final=True, tt=512):
    tok, d = x.shape
    w = d // n
    off = first // tt
    row = lambda i, p: (i, 0)
    zero = lambda i, p: (0, 0)
    one = pl.Buffered(1)
    const = lambda shape: pl.BlockSpec(shape, zero, pipeline_mode=one)
    wspec = lambda k: pl.BlockSpec((d, w), lambda i, p: (0, k * n + p[0]), pipeline_mode=one)
    tail = [const((8, 3 * w)), const((8, d))]
    wout = pl.BlockSpec((d // 128, 3 * w, 128), lambda i, p: (0, 0, 0), pipeline_mode=one) if final else const((3 * w, d))
    grid_spec = pltpu.PrefetchScalarGridSpec(
        num_scalar_prefetch=1,
        grid=(tok // tt,),
        in_specs=[
            pl.BlockSpec((3 * w, tt), lambda i, p: (0, off + i)),
            pl.BlockSpec((tt, d), lambda i, p: (off + i, 0)),
            pl.BlockSpec((tt, d), row),
            pl.BlockSpec((tt, d), row),
            wspec(0),
            wspec(1),
            wspec(2),
            const((1, d)),
        ]
        + ([const((3 * w, d))] + tail if prev is not None else []),
        out_specs=[pl.BlockSpec((tt, d), row), wout] + tail,
        scratch_shapes=[pltpu.VMEM((3 * w, d), F32)] if final else [],
    )
    return pl.pallas_call(
        functools.partial(post_kernel, prev is not None, final),
        grid_spec=grid_spec,
        out_shape=(
            jax.ShapeDtypeStruct((tok, d), BF),
            jax.ShapeDtypeStruct((d // 128, 3 * w, 128), BF) if final else jax.ShapeDtypeStruct((3 * w, d), F32),
            jax.ShapeDtypeStruct((8, 3 * w), F32),
            jax.ShapeDtypeStruct((8, d), F32),
        ),
        compiler_params=pltpu.CompilerParams(vmem_limit_bytes=VMEM_LIMIT),
        cost_estimate=pl.CostEstimate(
            flops=12 * tok * d * w, bytes_accessed=8 * tok * d + 6 * tok * w + 18 * d * w, transcendentals=0
        ),
        name="post",
    )(pos, gt, na, x, gm, w_qkv, w_qkv, w_qkv, gain, *(prev or ()))


def layout(seq_lens, index):
    ends = jnp.cumsum(seq_lens, dtype=jnp.int32)
    starts = ends - seq_lens
    first = jnp.zeros_like(index)
    for s in range(1, seq_lens.shape[0]):
        first = jnp.where(index >= starts[s], starts[s], first)
    return first, index - first


def swap_bits(parts, j):
    low = (j & 1) == 1
    high = (j & 2) == 2
    a, b, c, d = parts
    a, b, c, d = jnp.where(low, b, a), jnp.where(low, a, b), jnp.where(low, d, c), jnp.where(low, c, d)
    return [jnp.where(high, c, a), jnp.where(high, d, b), jnp.where(high, a, c), jnp.where(high, b, d)]


def head_perm(v, bit):
    return lax.ppermute(v, "head", [(k, k ^ bit) for k in range(4)])


def dp_perm(v, bit):
    return lax.ppermute(v, "dp", [(k, k ^ bit) for k in range(8)])


def pick(v, index, axis=0):
    return lax.dynamic_index_in_dim(v, index, axis, keepdims=False)


def dp_scatter(blocks, i):
    x = i & 1
    z = i >> 1
    pairs = blocks.reshape((4, 2) + blocks.shape[1:])
    other = dp_perm(pick(pairs, 1 - x, 1), 1)
    mine = pick(pairs, x, 1).astype(F32) + other.astype(F32)
    low = mine.astype(BF)
    result = pick(mine, z)
    for s in (1, 2, 3):
        result = result + dp_perm(pick(low, z ^ s), 2 * s).astype(F32)
    return result


def sum_all(v):
    for bit in (1, 2):
        v = v + head_perm(v, bit)
    for bit in (1, 2, 4):
        v = v + dp_perm(v, bit)
    return v


def to_owner(v, i, j):
    cols = v.reshape(v.shape[0], 4, v.shape[1] // 4)
    got = []
    for r in range(4):
        pairs = []
        for si in range(8):
            for sj in range(4):
                pairs.append((si * 4 + sj, (2 * sj + si // 4) * 4 + ((si % 4) ^ r)))
        got.append(lax.ppermute(pick(cols, (i % 4) ^ r, 1), ("dp", "head"), pairs))
    return jnp.concatenate(swap_bits(got, j), axis=0)


def qkv_owner(v, j):
    got = []
    for t in range(3):
        pairs = [((3 * dst + t) % 4, dst) for dst in range(4)]
        slot = jnp.int32(0)
        for src, dst in pairs:
            slot = jnp.where(j == src, (3 * dst + t) // 4, slot)
        got.append(lax.ppermute(pick(v, slot), "head", pairs))
    return jnp.concatenate(got, axis=0)


def fast_body(inputs, lengths, attn_gain, attn_shift, mlp_gain, mlp_shift, w_qkv, b_qkv, w_out, b_out,
              w_up, b_up, w_down, b_down, cotangent):
    own, d = inputs.shape
    n = 4
    tok = own * n
    w = d // n
    i = lax.axis_index("dp")
    j = lax.axis_index("head")
    pos = j.astype(jnp.int32).reshape(1)
    rows = lambda v: v.reshape(1, -1)
    ga, sa, gm, sm = rows(attn_gain), rows(attn_shift), rows(mlp_gain), rows(mlp_shift)
    bq, bu = rows(b_qkv), rows(b_up)
    lens = lengths[0]

    x_y = head_perm(inputs, 2)
    x_c = head_perm(inputs, 1)
    dy_c = head_perm(cotangent, 1)
    dy_y = head_perm(cotangent, 2)
    x_a = jnp.concatenate([inputs, x_c], axis=0)
    dy_a = jnp.concatenate([cotangent, dy_c], axis=0)

    lane = jnp.arange(tok, dtype=jnp.int32)
    index = ((lane // own) ^ j) * own + lane % own
    first, position = layout(lens, index)
    freqs = 10000.0 ** (-(2.0 * jnp.arange(HALF, dtype=F32)) / ROT)
    angle = freqs[:, None] * position.astype(F32)[None, :]
    cos, sin = jnp.cos(angle), jnp.sin(angle)
    seg_start = first[None, :]

    part_a, gm_a, *acc_a = mlp(pos, x_a, dy_a, w_up, w_down, bu, gm, sm, n, final=False)
    pre_a = proj(pos, x_a, dy_a, w_qkv, bq, w_out, ga, sa, cos, sin, n, tok, 0)

    x_b = jnp.concatenate([x_y, head_perm(x_y, 1)], axis=0)
    dy_b = jnp.concatenate([dy_y, head_perm(dy_y, 1)], axis=0)
    part_b, gm_b, dwu, dwd, small, smallf = mlp(pos, x_b, dy_b, w_up, w_down, bu, gm, sm, n, prev=tuple(acc_a))
    qt, kt, vt, dot, kn, vn, na = proj(
        pos, x_b, dy_b, w_qkv, bq, w_out, ga, sa, cos, sin, n, tok, 2 * own, prev=tuple(pre_a)
    )

    part_y = part_b[:own].astype(F32) + head_perm(part_b[own:], 1).astype(F32)
    part_0 = part_a[:own].astype(F32) + head_perm(part_a[own:], 1).astype(F32)
    mlp_sum = part_0 + head_perm(part_y.astype(BF), 2).astype(F32)

    up_down = jnp.concatenate([dwu.reshape(8, 128, d), dwd.reshape(8, 128, d)], axis=1)
    up_down = dp_scatter(up_down, i)
    grad_w_up = up_down[:128]
    grad_w_down = to_owner(up_down[128:].astype(BF), i, j).astype(F32)
    slots = jnp.where(jnp.arange(4)[:, None] == j, smallf[0:1], 0.0)
    early = sum_all(jnp.concatenate([small[:2], small[2:3] * 0.25, slots, jnp.zeros((1, d), F32)], axis=0))

    gt, ctx = attention(lens, pos, cos, sin, seg_start, qt, kt, vt, dot, kn, vn, own, tok // 2)

    got = [ctx[:, :own]] + [head_perm(ctx[:, r * own : (r + 1) * own], r) for r in (1, 2, 3)]
    w_rel = w_out.reshape(n, w, d)
    attn_part = mm(jnp.concatenate(got, axis=0), jnp.concatenate([pick(w_rel, j ^ r) for r in range(n)], axis=0), TN)
    bias = b_out.astype(F32) + b_down.astype(F32)
    output = (inputs.astype(F32) + attn_part + mlp_sum + bias).astype(BF)

    dw_out = mm(ctx[:, : 2 * own], dy_a) + mm(ctx[:, 2 * own :], dy_b)

    g_b, dwq, bias_b, small_b = post(pos, gt, na, x_b, gm_b, w_qkv, ga, n, 2 * own, final=False)
    g_y = g_b[:own].astype(F32) + head_perm(g_b[own:], 1).astype(F32)
    g_y = head_perm(g_y.astype(BF), 2)
    g_a, dwq, bias_q, small_q = post(pos, gt, na, x_a, gm_a, w_qkv, ga, n, 0, prev=(dwq, bias_b, small_b))
    g_sum = g_a[:own].astype(F32) + head_perm(g_a[own:], 1).astype(F32) + g_y.astype(F32)

    qkv = dp_scatter(dwq, i)
    grad_w_qkv = qkv_owner(qkv.astype(BF).reshape(3, w, 128), j).astype(F32).T
    out_sum = dp_scatter(dw_out.astype(BF).reshape(8, w // 8, d), i)
    grad_w_out = to_owner(out_sum.astype(BF), i, j).astype(F32)

    slots = jnp.where(jnp.arange(4)[None, :, None] == j, bias_q[0].reshape(3, 1, w), 0.0).reshape(3, d)
    late = sum_all(jnp.concatenate([small_q[:2], slots, jnp.zeros((3, d), F32)], axis=0))

    normed, inv = norm_parts(inputs)
    grad_inputs = cotangent.astype(F32) + inv * (
        g_sum - jnp.mean(g_sum, axis=-1, keepdims=True) - normed * jnp.mean(g_sum * normed, axis=-1, keepdims=True)
    )
    return (output, grad_inputs, late[0], late[1], early[0], early[1], grad_w_qkv, late[2:5].reshape(-1),
            grad_w_out, early[2], grad_w_up, early[3:7].reshape(-1), grad_w_down, early[2])


def general_body(inputs, lengths, attn_gain, attn_shift, mlp_gain, mlp_shift, w_qkv, b_qkv, w_out, b_out,
                 w_up, b_up, w_down, b_down, cotangent):
    own, d = inputs.shape
    n = lax.axis_size("head")
    n_dp = lax.axis_size("dp")
    tok = own * n
    w = d // n
    f = w_up.shape[1] // n
    j = lax.axis_index("head")
    pos = j.astype(jnp.int32).reshape(1)
    rows = lambda v: v.reshape(1, -1)
    ga, sa, gm, sm = rows(attn_gain), rows(attn_shift), rows(mlp_gain), rows(mlp_shift)
    bq, bu = rows(b_qkv), rows(b_up)
    lens = lengths[0]
    gather = lambda v: lax.all_gather(v, "head", axis=0, tiled=True)
    over_dp = lambda v, axis: lax.psum_scatter(v, "dp", scatter_dimension=axis, tiled=True)
    over_head = lambda v: lax.psum_scatter(v, "head", scatter_dimension=0, tiled=True)
    x_all = gather(inputs)
    dy_all = gather(cotangent)
    first, position = layout(lens, jnp.arange(tok, dtype=jnp.int32))
    freqs = 10000.0 ** (-(2.0 * jnp.arange(HALF, dtype=F32)) / ROT)
    angle = freqs[:, None] * position.astype(F32)[None, :]
    cos, sin = jnp.cos(angle), jnp.sin(angle)
    part, g_mlp, dwu, dwd, small, smallf = mlp(pos, x_all, dy_all, w_up, w_down, bu, gm, sm, n)
    qt, kt, vt, dot, kn, vn, na = proj(pos, x_all, dy_all, w_qkv, bq, w_out, ga, sa, cos, sin, n, tok, 0)
    gt, ctx = attention(
        lens, jnp.zeros((1,), jnp.int32), cos, sin, first[None, :], qt, kt, vt, dot, kn, vn, own, tok // 2
    )
    total, dwq, bias_q, small_q = post(pos, gt, na, x_all, g_mlp, w_qkv, ga, n, 0)
    attn_part = mm(ctx, lax.dynamic_slice_in_dim(w_out, j * w, w, 0), TN)
    bias = b_out.astype(F32) + b_down.astype(F32)
    output = inputs.astype(F32) + over_head((attn_part + part.astype(F32)).astype(BF)).astype(F32) + bias
    g_sum = over_head(total).astype(F32)
    normed, inv = norm_parts(inputs)
    grad_inputs = cotangent.astype(F32) + inv * (
        g_sum - jnp.mean(g_sum, axis=-1, keepdims=True) - normed * jnp.mean(g_sum * normed, axis=-1, keepdims=True)
    )
    dw_out = mm(ctx, dy_all).astype(BF)
    spread = lambda v: lax.all_to_all(v, "head", split_axis=1, concat_axis=0, tiled=True)
    grad_w_up = over_dp(dwu, 0).astype(F32)
    grad_w_down = over_dp(spread(dwd), 0).astype(F32)
    grad_w_out = over_dp(spread(dw_out), 0).astype(F32)
    qkv = over_dp(jnp.transpose(dwq, (0, 2, 1)).reshape(d, 3 * w), 0)
    qkv = lax.all_gather(qkv.reshape(d // n_dp, 3, w), "head", axis=2, tiled=True).reshape(d // n_dp, 3 * d)
    grad_w_qkv = lax.dynamic_slice_in_dim(qkv, j * 3 * w, 3 * w, 1).astype(F32)
    slots = jnp.where(jnp.arange(n)[:, None] == j, smallf[0:1], 0.0).reshape(-1)
    slots_q = jnp.where(jnp.arange(n)[None, :, None] == j, bias_q[0].reshape(3, 1, w), 0.0).reshape(-1)
    sums = lax.psum((small_q[0], small_q[1], small[0], small[1], slots_q, small[2] / n, slots), ("dp", "head"))
    return (output.astype(BF), grad_inputs, sums[0], sums[1], sums[2], sums[3], grad_w_qkv, sums[4],
            grad_w_out, sums[5], grad_w_up, sums[6], grad_w_down, sums[5])


def solution(mesh):
    fast = mesh.shape["dp"] == 8 and mesh.shape["head"] == 4
    whole = P(("dp", "head"), None)
    weight = P("dp", "head")
    return jax.shard_map(
        fast_body if fast else general_body,
        mesh=mesh,
        in_specs=(whole, P("dp", None)) + (P(),) * 12 + (whole,),
        out_specs=(whole, whole, P(), P(), P(), P(), weight, P(), weight, P(), weight, P(), weight, P()),
        check_vma=False,
    )
```

```python
import functools

import jax
import jax.numpy as jnp
from jax import lax
from jax.experimental import pallas as pl
from jax.experimental.pallas import tpu as pltpu
from jax.sharding import PartitionSpec as P

HD = 64
ROT = 16
HALF = ROT // 2
NN = (((1,), (0,)), ((), ()))
NT = (((1,), (1,)), ((), ()))
TN = (((0,), (0,)), ((), ()))
BF = jnp.bfloat16
F32 = jnp.float32
VMEM_LIMIT = 62 * 1024 * 1024


def mm(a, b, dims=NN):
    return lax.dot_general(a, b, dims, preferred_element_type=F32)


def norm_parts(x):
    v = x.astype(F32)
    center = v - jnp.mean(v, axis=-1, keepdims=True)
    inv = lax.rsqrt(jnp.mean(center * center, axis=-1, keepdims=True) + 1e-5)
    return center * inv, inv


def mlp_kernel(prev, final, pos, *refs):
    x_ref, dy_ref, wu, wd, bu, gain, shift = refs[:7]
    refs = refs[7:]
    if prev:
        pwu, pwd, psmall, psmallf = refs[:4]
        refs = refs[4:]
    part_ref, g_ref, out_wu, out_wd, small, smallf = refs[:6]
    if final:
        dwu, dwd = refs[6:8]
    else:
        dwu, dwd = out_wu, out_wd
    step = pl.program_id(0)

    @pl.when(step == 0)
    def _():
        if prev:
            dwu[...] = pwu[...]
            dwd[...] = pwd[...]
            small[...] = psmall[...]
            smallf[...] = psmallf[...]
        else:
            dwu[...] = jnp.zeros_like(dwu)
            dwd[...] = jnp.zeros_like(dwd)
            small[...] = jnp.zeros_like(small)
            smallf[...] = jnp.zeros_like(smallf)

    normed, _unused = norm_parts(x_ref[...])
    scale = gain[...].astype(F32)
    nm = (normed * scale + shift[...].astype(F32)).astype(BF)
    dy = dy_ref[...]
    pre = mm(nm, wu[...]) + bu[...].astype(F32)
    cdf = 0.5 + 0.5 * lax.erf(pre * (0.5**0.5))
    hid = (pre * cdf).astype(BF)
    slope = cdf + pre * (jnp.exp(-0.5 * pre * pre) * 0.3989422804014327)
    gp = (mm(dy, wd[...], NT) * slope).astype(BF)
    part_ref[...] = mm(hid, wd[...]).astype(BF)
    r = mm(gp, wu[...], NT)
    g_ref[...] = (r * scale).astype(BF)
    smallf[0:1, :] += jnp.sum(gp.astype(F32), axis=0, keepdims=True)
    small[0:1, :] += jnp.sum(r * normed, axis=0, keepdims=True)
    small[1:2, :] += jnp.sum(r, axis=0, keepdims=True)
    small[2:3, :] += jnp.sum(dy.astype(F32), axis=0, keepdims=True)
    dwd[...] += mm(hid, dy, TN)
    dwu[...] += mm(nm, gp, TN)

    if final:

        @pl.when(step == pl.num_programs(0) - 1)
        def _():
            out_wu[...] = dwu[...].astype(BF)
            out_wd[...] = dwd[...].astype(BF)


def mlp(pos, x, dy, wu, wd, bu, gain, shift, n, prev=None, final=True, tt=512):
    tok, d = x.shape
    f = wu.shape[1] // n
    row = lambda i, p: (i, 0)
    zero = lambda i, p: (0, 0)
    one = pl.Buffered(1)
    const = lambda shape: pl.BlockSpec(shape, zero, pipeline_mode=one)
    accs = [const((d, f)), const((f, d)), const((8, d)), const((8, f))]
    kind = BF if final else F32
    grid_spec = pltpu.PrefetchScalarGridSpec(
        num_scalar_prefetch=1,
        grid=(tok // tt,),
        in_specs=[
            pl.BlockSpec((tt, d), row),
            pl.BlockSpec((tt, d), row),
            pl.BlockSpec((d, f), lambda i, p: (0, p[0]), pipeline_mode=one),
            pl.BlockSpec((f, d), lambda i, p: (p[0], 0), pipeline_mode=one),
            pl.BlockSpec((1, f), lambda i, p: (0, p[0])),
            const((1, d)),
            const((1, d)),
        ]
        + (accs if prev is not None else []),
        out_specs=[pl.BlockSpec((tt, d), row), pl.BlockSpec((tt, d), row)] + accs,
        scratch_shapes=[pltpu.VMEM((d, f), F32), pltpu.VMEM((f, d), F32)] if final else [],
    )
    return pl.pallas_call(
        functools.partial(mlp_kernel, prev is not None, final),
        grid_spec=grid_spec,
        out_shape=(
            jax.ShapeDtypeStruct((tok, d), BF),
            jax.ShapeDtypeStruct((tok, d), BF),
            jax.ShapeDtypeStruct((d, f), kind),
            jax.ShapeDtypeStruct((f, d), kind),
            jax.ShapeDtypeStruct((8, d), F32),
            jax.ShapeDtypeStruct((8, f), F32),
        ),
        compiler_params=pltpu.CompilerParams(vmem_limit_bytes=VMEM_LIMIT),
        cost_estimate=pl.CostEstimate(
            flops=12 * tok * d * f, bytes_accessed=8 * tok * d + 12 * d * f, transcendentals=2 * tok * f
        ),
        name="mlp",
    )(pos, x, dy, wu, wd, bu, gain, shift, *(prev or ()))


def proj_kernel(nh, prev, pos, *refs):
    x_ref, dy_ref, wq, wk, wv, bq, bk, bv, wo, gain, shift, cos, sin = refs[:13]
    qt, kt, vt, dot, kn, vn, na_ref = refs[13 + (7 if prev else 0) :]
    normed, _unused = norm_parts(x_ref[...])
    na = (normed * gain[...].astype(F32) + shift[...].astype(F32)).astype(BF)
    na_ref[...] = na
    co = cos[...]
    si = sin[...]

    def rotated(t, scale):
        rows = []
        for h in range(nh):
            u = t[h * HD : (h + 1) * HD]
            u1 = u[:HALF]
            u2 = u[HALF:ROT]
            rows += [u1 * co - u2 * si, u2 * co + u1 * si, u[ROT:]]
        out = jnp.concatenate(rows, axis=0).astype(BF)
        return out if scale is None else out * jnp.asarray(scale, BF)

    def triple(w, b):
        return (mm(na, w[...]) + b[...].astype(F32)).astype(BF)

    qt[...] = rotated(triple(wq, bq).astype(F32).T, HD**-0.5)
    keys = rotated(triple(wk, bk).astype(F32).T, None)
    kt[...] = keys
    kn[...] = keys.T
    values = triple(wv, bv)
    vn[...] = values
    vt[...] = values.T
    dot[...] = mm(wo[...], dy_ref[...], NT).astype(BF)


def proj(pos, x, dy, w_qkv, b_qkv, w_out, gain, shift, cos, sin, n, total, first, prev=None, tt=512):
    tok, d = x.shape
    w = d // n
    nh = w // HD
    off = first // tt
    row = lambda i, p: (i, 0)
    zero = lambda i, p: (0, 0)
    one = pl.Buffered(1)
    wspec = lambda k: pl.BlockSpec((d, w), lambda i, p: (0, k * n + p[0]), pipeline_mode=one)
    bspec = lambda k: pl.BlockSpec((1, w), lambda i, p: (0, k * n + p[0]))
    lane = lambda rows: pl.BlockSpec((rows, tt), lambda i, p: (0, off + i))
    nat = lambda cols: pl.BlockSpec((tt, cols), lambda i, p: (off + i, 0))
    shapes = [(w, total)] * 4 + [(total, w)] * 2 + [(total, d)]
    grid_spec = pltpu.PrefetchScalarGridSpec(
        num_scalar_prefetch=1,
        grid=(tok // tt,),
        in_specs=[pl.BlockSpec((tt, d), row), pl.BlockSpec((tt, d), row)]
        + [wspec(0), wspec(1), wspec(2), bspec(0), bspec(1), bspec(2)]
        + [pl.BlockSpec((w, d), lambda i, p: (p[0], 0), pipeline_mode=one)]
        + [pl.BlockSpec((1, d), zero), pl.BlockSpec((1, d), zero), lane(HALF), lane(HALF)]
        + ([pl.BlockSpec(memory_space=pl.ANY)] * 7 if prev is not None else []),
        out_specs=[lane(w)] * 4 + [nat(w)] * 2 + [nat(d)],
    )
    return pl.pallas_call(
        functools.partial(proj_kernel, nh, prev is not None),
        grid_spec=grid_spec,
        out_shape=tuple(jax.ShapeDtypeStruct(s, BF) for s in shapes),
        input_output_aliases={14 + k: k for k in range(7)} if prev is not None else {},
        compiler_params=pltpu.CompilerParams(vmem_limit_bytes=VMEM_LIMIT),
        cost_estimate=pl.CostEstimate(
            flops=8 * tok * d * w, bytes_accessed=6 * tok * d + 12 * tok * w + 8 * d * w, transcendentals=0
        ),
        name="proj",
    )(pos, x, dy, w_qkv, w_qkv, w_qkv, b_qkv, b_qkv, b_qkv, w_out, gain, shift, cos, sin, *(prev or ()))


def head_kernel(nh, x_hbm, dy_hbm, wu_hbm, wd_hbm, wqkv_hbm, wo_hbm, bu, bq, gain_m, shift_m, gain_a, shift_a, cos, sin,
                g_out, na_out, dy_out, qt, kt, vt, dot, kn, vn, p_own, p_far, out_wu, out_wd, small, smallf,
                xs, dys, wu, wd, wqkv, wt, wo, bias_t, parts, far_in, near_in, dwu, dwd, load, send, recv):
    step = pl.program_id(0)
    j = lax.axis_index("head")
    own, d = x_hbm.shape
    f = wu.shape[1]
    w = wo.shape[0]
    half = own // 2
    core = {"head": j ^ 1}
    across = {"head": j ^ 2}

    def remote(src, dst, k, to):
        return pltpu.make_async_remote_copy(
            src_ref=src, dst_ref=dst, send_sem=send.at[k], recv_sem=recv.at[k], device_id=to,
            device_id_type=pl.DeviceIdType.MESH)

    lo, hi = pl.ds(0, half), pl.ds(half, half)
    copies = [
        remote(x_hbm, xs.at[1], 0, core),
        remote(dy_hbm, dys.at[1], 1, core),
        remote(x_hbm.at[lo], xs.at[2, lo], 2, across),
        remote(dy_hbm.at[lo], dys.at[2, lo], 3, across),
        remote(x_hbm.at[hi], xs.at[3, lo], 4, across),
        remote(dy_hbm.at[hi], dys.at[3, lo], 5, across),
        remote(xs.at[2, lo], xs.at[2, hi], 6, core),
        remote(dys.at[2, lo], dys.at[2, hi], 7, core),
        remote(xs.at[3, lo], xs.at[3, hi], 8, core),
        remote(dys.at[3, lo], dys.at[3, hi], 9, core),
        remote(parts.at[1], near_in, 10, core),
        remote(parts.at[2, hi], far_in.at[lo], 11, core),
        remote(parts.at[3, hi], far_in.at[hi], 12, core),
    ]
    locals_ = [
        pltpu.make_async_copy(x_hbm, xs.at[0], load.at[0]),
        pltpu.make_async_copy(dy_hbm, dys.at[0], load.at[1]),
        pltpu.make_async_copy(wu_hbm.at[:, pl.ds(j * f, f)], wu, load.at[2]),
        pltpu.make_async_copy(wd_hbm.at[pl.ds(j * f, f)], wd, load.at[3]),
        pltpu.make_async_copy(wo_hbm.at[pl.ds(j * w, w)], wo, load.at[4]),
    ] + [
        pltpu.make_async_copy(wqkv_hbm.at[:, pl.ds(k * d + j * w, w)], wqkv.at[:, pl.ds(k * w, w)], load.at[5 + k])
        for k in range(3)
    ]

    @pl.when(step == 0)
    def _():
        barrier = pltpu.get_barrier_semaphore()
        for to in (core, across):
            pl.semaphore_signal(barrier, inc=1, device_id=to, device_id_type=pl.DeviceIdType.MESH)
        for c in locals_:
            c.start()
        pl.semaphore_wait(barrier, 2)
        for c in copies[:6]:
            c.start()
        dwu[...] = jnp.zeros_like(dwu)
        dwd[...] = jnp.zeros_like(dwd)
        small[...] = jnp.zeros_like(small)
        smallf[...] = jnp.zeros_like(smallf)
        for c in locals_:
            c.wait()
        for k in range(3):
            wt[k * w : (k + 1) * w, :] = wqkv[:, k * w : (k + 1) * w].T
            row = bq[:, pl.ds(pl.multiple_of(k * d + j * w, 128), w)].astype(F32)
            bias_t[k * w : (k + 1) * w, :] = jnp.broadcast_to(row, (128, w)).T

    @pl.when(step == 1)
    def _():
        copies[0].wait_recv()
        copies[1].wait_recv()

    @pl.when(step == 2)
    def _():
        copies[6].wait_recv()
        copies[7].wait_recv()

    @pl.when(step == 3)
    def _():
        copies[8].wait_recv()
        copies[9].wait_recv()

    normed, _unused = norm_parts(xs[step])
    scale = gain_m[...].astype(F32)
    nm = (normed * scale + shift_m[...].astype(F32)).astype(BF)
    na = (normed * gain_a[...].astype(F32) + shift_a[...].astype(F32)).astype(BF)
    dy = dys[step]
    na_out[...] = na
    dy_out[...] = dy
    pre = mm(nm, wu[...]) + bu[:, pl.ds(pl.multiple_of(j * f, 128), f)].astype(F32)
    cdf = 0.5 + 0.5 * lax.erf(pre * (0.5**0.5))
    hid = (pre * cdf).astype(BF)
    slope = cdf + pre * (jnp.exp(-0.5 * pre * pre) * 0.3989422804014327)
    gp = (mm(dy, wd[...], NT) * slope).astype(BF)
    parts[step] = mm(hid, wd[...]).astype(BF)
    r = mm(gp, wu[...], NT)
    g_out[...] = (r * scale).astype(BF)
    smallf[0:1, :] += jnp.sum(gp.astype(F32), axis=0, keepdims=True)
    small[0:1, :] += jnp.sum(r * normed, axis=0, keepdims=True)
    small[1:2, :] += jnp.sum(r, axis=0, keepdims=True)
    small[2:3, :] += jnp.sum(dy.astype(F32), axis=0, keepdims=True)
    dwd[...] += mm(hid, dy, TN)
    dwu[...] += mm(nm, gp, TN)

    @pl.when(step == 1)
    def _():
        for k in (2, 3):
            copies[k].wait_recv()
            copies[k + 4].start()
        copies[10].start()

    @pl.when(step == 2)
    def _():
        for k in (4, 5):
            copies[k].wait_recv()
            copies[k + 4].start()
        copies[11].start()

    @pl.when(step == 3)
    def _():
        copies[12].start()
        for b in range(out_wu.shape[0]):
            rows = out_wu.shape[1]
            out_wu[b] = dwu[b * rows : (b + 1) * rows, :].astype(BF)
        for b in range(out_wd.shape[0]):
            rows = out_wd.shape[1]
            out_wd[b] = dwd[b * rows : (b + 1) * rows, :].astype(BF)

    co = cos[...]
    si = sin[...]

    def projected(k):
        b = bias_t[k * w : (k + 1) * w, :]
        t = mm(wt[k * w : (k + 1) * w, :], na, NT)
        return (t + jnp.concatenate([b] * (own // 128), axis=1)).astype(BF)

    def rotated(t, factor):
        rows = []
        for h in range(nh):
            u = t[h * HD : (h + 1) * HD].astype(F32)
            u1 = u[:HALF]
            u2 = u[HALF:ROT]
            rows += [u1 * co - u2 * si, u2 * co + u1 * si, u[ROT:]]
        out = jnp.concatenate(rows, axis=0)
        return (out if factor is None else out * factor).astype(BF)

    qt[...] = rotated(projected(0), HD**-0.5)
    keys = rotated(projected(1), None)
    kt[...] = keys
    kn[...] = keys.T
    values = projected(2)
    vt[...] = values
    vn[...] = values.T
    dot[...] = mm(wo[...], dy, NT).astype(BF)

    @pl.when(step == 3)
    def _():
        copies[10].wait_recv()
        p_own[...] = (parts[0].astype(F32) + near_in[...].astype(F32)).astype(BF)
        copies[11].wait_recv()
        p_far[lo] = (parts[2, lo].astype(F32) + far_in[lo].astype(F32)).astype(BF)
        copies[12].wait_recv()
        p_far[hi] = (parts[3, lo].astype(F32) + far_in[hi].astype(F32)).astype(BF)
        for c in copies:
            c.wait_send()


def head_stage(x, dy, w_up, w_down, w_qkv, w_out, bu, bq, gm, sm, ga, sa, cos, sin, n, cid):
    own, d = x.shape
    tok = own * n
    w = d // n
    f = w_up.shape[1] // n
    row = lambda i: (i, 0)
    lane = lambda rows: pl.BlockSpec((rows, own), lambda i: (0, i))
    nat = lambda cols: pl.BlockSpec((own, cols), row)
    one = pl.Buffered(1)
    const = lambda shape: pl.BlockSpec(shape, lambda i: (0,) * len(shape), pipeline_mode=one)
    hbm = pl.BlockSpec(memory_space=pl.ANY)
    sds = jax.ShapeDtypeStruct
    return pl.pallas_call(
        functools.partial(head_kernel, w // HD),
        grid=(n,),
        in_specs=[hbm] * 6
        + [const((1, w_up.shape[1])), const((1, 3 * d))]
        + [const((1, d))] * 4
        + [lane(HALF), lane(HALF)],
        out_specs=[nat(d)] * 3
        + [lane(w)] * 4
        + [nat(w)] * 2
        + [const((own, d))] * 2
        + [const((8, d // 8, f)), const((8, f // 8, d)), const((8, d)), const((8, f))],
        out_shape=tuple(
            [sds((tok, d), BF)] * 3
            + [sds((w, tok), BF)] * 4
            + [sds((tok, w), BF)] * 2
            + [sds((own, d), BF)] * 2
            + [sds((8, d // 8, f), BF), sds((8, f // 8, d), BF), sds((8, d), F32), sds((8, f), F32)]
        ),
        scratch_shapes=[
            pltpu.VMEM((4, own, d), BF),
            pltpu.VMEM((4, own, d), BF),
            pltpu.VMEM((d, f), BF),
            pltpu.VMEM((f, d), BF),
            pltpu.VMEM((d, 3 * w), BF),
            pltpu.VMEM((3 * w, d), BF),
            pltpu.VMEM((w, d), BF),
            pltpu.VMEM((3 * w, 128), F32),
            pltpu.VMEM((4, own, d), BF),
            pltpu.VMEM((own, d), BF),
            pltpu.VMEM((own, d), BF),
            pltpu.VMEM((d, f), F32),
            pltpu.VMEM((f, d), F32),
            pltpu.SemaphoreType.DMA((8,)),
            pltpu.SemaphoreType.DMA((13,)),
            pltpu.SemaphoreType.DMA((13,)),
        ],
        compiler_params=pltpu.CompilerParams(
            vmem_limit_bytes=VMEM_LIMIT, collective_id=cid, has_side_effects=True
        ),
        cost_estimate=pl.CostEstimate(
            flops=12 * tok * d * f + 10 * tok * d * w, bytes_accessed=12 * tok * d + 8 * d * f, transcendentals=2 * tok * f
        ),
        name="head_stage",
    )(x, dy, w_up, w_down, w_qkv, w_out, bu, bq, gm, sm, ga, sa, cos, sin)


def attn_kernel(nh, tok, blk, per, halved, lens, rel, cos, sin, seg_start, qt, kt, vt, dot, kn, vn,
                gt_ref, ctx_ref, exps, peaks, dk, dv, oacc, dqacc, mrow, lrow, drow, qpad, dopad):
    nseq = lens.shape[0]
    nblk = tok // blk
    shift = rel[0]

    def place(b):
        chunk = (b // per) ^ shift
        half = b % per
        at = chunk * per + half
        if halved:
            at = jnp.where(chunk < 2, at, 4 + (chunk - 2) + 2 * half)
        return pl.multiple_of(at * blk, blk)

    dk[...] = jnp.zeros_like(dk)
    dv[...] = jnp.zeros_like(dv)
    qpad[...] = jnp.zeros_like(qpad)
    dopad[...] = jnp.zeros_like(dopad)
    rows_iota = lax.broadcasted_iota(jnp.int32, (blk, blk), 0)
    cols_iota = lax.broadcasted_iota(jnp.int32, (1, blk), 1)

    def one_block(i, carry):
        first_tok = i * blk
        begin = jnp.int32(0)
        total = jnp.int32(0)
        for s in range(nseq - 1):
            total = total + lens[s]
            begin = jnp.where(total <= first_tok, total, begin)
        low = begin // blk
        cols = pl.ds(place(i), blk)
        start_row = seg_start[:, cols]
        query_idx = cols_iota + first_tok
        for h in range(nh):
            half = (h % 2) * HD
            qpad[h, half : half + HD, :] = qt[h * HD : (h + 1) * HD, cols]
            dopad[h, half : half + HD, :] = dot[h * HD : (h + 1) * HD, cols]
        mrow[...] = jnp.full_like(mrow, -1e30)
        lrow[...] = jnp.zeros_like(lrow)
        oacc[...] = jnp.zeros_like(oacc)
        dqacc[...] = jnp.zeros_like(dqacc)

        def forward(step, c):
            b = i - step
            krow = place(b)
            kidx = rows_iota + b * blk
            allowed = (kidx >= start_row) & (kidx <= query_idx)
            for h in range(nh):
                pair = (h // 2) * 128
                s = mm(kn[pl.ds(krow, blk), pair : pair + 128], qpad[h])
                s = jnp.where(allowed, s, -1e30)
                old = mrow[h : h + 1, :]
                new = jnp.maximum(old, jnp.max(s, axis=0, keepdims=True))
                e = jnp.exp(s - new)
                alpha = jnp.exp(old - new)
                lrow[h : h + 1, :] = lrow[h : h + 1, :] * alpha + jnp.sum(e, axis=0, keepdims=True)
                mrow[h : h + 1, :] = new
                peaks[step, h : h + 1, :] = new
                exps[h, step] = e
                oacc[h] = oacc[h] * alpha + mm(vt[h * HD : (h + 1) * HD, pl.ds(krow, blk)], e.astype(BF))
            return c

        lax.fori_loop(0, i - low + 1, forward, 0)
        for h in range(nh):
            hs = slice(h * HD, (h + 1) * HD)
            inv = 1.0 / lrow[h : h + 1, :]
            o = oacc[h] * inv
            drow[h : h + 1, :] = jnp.sum(o * dot[hs, cols].astype(F32), axis=0, keepdims=True)
            lrow[h : h + 1, :] = inv
            ctx_ref[hs, cols] = o.astype(BF)

        def backward(step, c):
            kcols = pl.ds(place(i - step), blk)
            for h in range(nh):
                pair = (h // 2) * 128
                hs = slice(h * HD, (h + 1) * HD)
                factor = jnp.exp(peaks[step, h : h + 1, :] - mrow[h : h + 1, :]) * lrow[h : h + 1, :]
                p = exps[h, step] * factor
                dp = mm(vn[kcols, pair : pair + 128], dopad[h])
                ds = (p * (dp - drow[h : h + 1, :])).astype(BF)
                dv[hs, kcols] += mm(dot[hs, cols], p.astype(BF), NT)
                dk[hs, kcols] += mm(qt[hs, cols], ds, NT)
                dqacc[hs, :] += mm(kt[hs, kcols], ds)
            return c

        lax.fori_loop(0, i - low + 1, backward, 0)
        co = cos[:, cols]
        si = sin[:, cols]
        for h in range(nh):
            base = h * HD
            g = dqacc[base : base + HD, :] * (HD**-0.5)
            g1 = g[:HALF]
            g2 = g[HALF:ROT]
            gt_ref[base : base + HD, cols] = jnp.concatenate(
                [g1 * co + g2 * si, g2 * co - g1 * si, g[ROT:]], axis=0
            ).astype(BF)
        return carry

    lax.fori_loop(0, nblk, one_block, 0)

    def finish(i, carry):
        cols = pl.ds(pl.multiple_of(i * blk, blk), blk)
        co = cos[:, cols]
        si = sin[:, cols]
        for h in range(nh):
            base = h * HD
            g = dk[base : base + HD, cols]
            g1 = g[:HALF]
            g2 = g[HALF:ROT]
            gt_ref[nh * HD + base : nh * HD + base + HD, cols] = jnp.concatenate(
                [g1 * co + g2 * si, g2 * co - g1 * si, g[ROT:]], axis=0
            ).astype(BF)
        gt_ref[2 * nh * HD :, cols] = dv[:, cols].astype(BF)
        return carry

    lax.fori_loop(0, nblk, finish, 0)


def attention(lens, rel, cos, sin, seg_start, qt, kt, vt, dot, kn, vn, chunk, maxlen, halved=False, blk=256):
    width, tok = qt.shape
    nh = width // HD
    wb = maxlen // blk + 1
    vm = pl.BlockSpec(memory_space=pltpu.VMEM)
    sm = pl.BlockSpec(memory_space=pltpu.SMEM)
    return pl.pallas_call(
        functools.partial(attn_kernel, nh, tok, blk, chunk // blk, halved),
        out_shape=(jax.ShapeDtypeStruct((3 * width, tok), BF), jax.ShapeDtypeStruct((width, tok), BF)),
        in_specs=[sm, sm] + [vm] * 9,
        out_specs=(vm, vm),
        scratch_shapes=[
            pltpu.VMEM((nh, wb, blk, blk), F32),
            pltpu.VMEM((wb, 8, blk), F32),
            pltpu.VMEM((width, tok), F32),
            pltpu.VMEM((width, tok), F32),
            pltpu.VMEM((nh, HD, blk), F32),
            pltpu.VMEM((width, blk), F32),
            pltpu.VMEM((8, blk), F32),
            pltpu.VMEM((8, blk), F32),
            pltpu.VMEM((8, blk), F32),
            pltpu.VMEM((nh, 128, blk), BF),
            pltpu.VMEM((nh, 128, blk), BF),
        ],
        compiler_params=pltpu.CompilerParams(vmem_limit_bytes=VMEM_LIMIT),
        cost_estimate=pl.CostEstimate(
            flops=20 * width * tok * maxlen, bytes_accessed=20 * width * tok, transcendentals=nh * tok * maxlen
        ),
        name="attention",
    )(lens, rel, cos, sin, seg_start, qt, kt, vt, dot, kn, vn)


def post_kernel(pos, gt_ref, na_ref, gm_ref, wq, wk, wv, gain, shift, g_ref, out_w, bias, small, dw):
    step = pl.program_id(0)

    @pl.when(step == 0)
    def _():
        dw[...] = jnp.zeros_like(dw)
        bias[...] = jnp.zeros_like(bias)
        small[...] = jnp.zeros_like(small)

    gt = gt_ref[...]
    na = na_ref[...]
    w = wq.shape[1]
    scale = gain[...].astype(F32)
    gn = gt.T
    r = mm(gn[:, :w], wq[...], NT) + mm(gn[:, w : 2 * w], wk[...], NT) + mm(gn[:, 2 * w :], wv[...], NT)
    g_ref[...] = (r * scale + gm_ref[...].astype(F32)).astype(BF)
    small[0:1, :] += jnp.sum(r * na.astype(F32), axis=0, keepdims=True)
    small[1:2, :] += jnp.sum(r, axis=0, keepdims=True)
    bias[0:1, :] += jnp.sum(gn.astype(F32), axis=0, keepdims=True)
    dw[...] += mm(gt, na)

    @pl.when(step == pl.num_programs(0) - 1)
    def _():
        for b in range(dw.shape[1] // 128):
            out_w[b] = dw[:, b * 128 : (b + 1) * 128].astype(BF)
        small[0:1, :] = (small[0:1, :] - shift[...].astype(F32) * small[1:2, :]) / scale


def post(pos, gt, na, gm, w_qkv, gain, shift, n, tt=512):
    tok, d = na.shape
    w = d // n
    row = lambda i, p: (i, 0)
    zero = lambda i, p: (0, 0)
    one = pl.Buffered(1)
    const = lambda shape: pl.BlockSpec(shape, zero, pipeline_mode=one)
    wspec = lambda k: pl.BlockSpec((d, w), lambda i, p: (0, k * n + p[0]), pipeline_mode=one)
    grid_spec = pltpu.PrefetchScalarGridSpec(
        num_scalar_prefetch=1,
        grid=(tok // tt,),
        in_specs=[
            pl.BlockSpec((3 * w, tt), lambda i, p: (0, i)),
            pl.BlockSpec((tt, d), row),
            pl.BlockSpec((tt, d), row),
            wspec(0),
            wspec(1),
            wspec(2),
            const((1, d)),
            const((1, d)),
        ],
        out_specs=[
            pl.BlockSpec((tt, d), row),
            pl.BlockSpec((d // 128, 3 * w, 128), lambda i, p: (0, 0, 0), pipeline_mode=one),
            const((8, 3 * w)),
            const((8, d)),
        ],
        scratch_shapes=[pltpu.VMEM((3 * w, d), F32)],
    )
    return pl.pallas_call(
        post_kernel,
        grid_spec=grid_spec,
        out_shape=(
            jax.ShapeDtypeStruct((tok, d), BF),
            jax.ShapeDtypeStruct((d // 128, 3 * w, 128), BF),
            jax.ShapeDtypeStruct((8, 3 * w), F32),
            jax.ShapeDtypeStruct((8, d), F32),
        ),
        compiler_params=pltpu.CompilerParams(vmem_limit_bytes=VMEM_LIMIT),
        cost_estimate=pl.CostEstimate(
            flops=12 * tok * d * w, bytes_accessed=8 * tok * d + 6 * tok * w + 18 * d * w, transcendentals=0
        ),
        name="post",
    )(pos, gt, na, gm, w_qkv, w_qkv, w_qkv, gain, shift)


def layout(seq_lens, index):
    ends = jnp.cumsum(seq_lens, dtype=jnp.int32)
    starts = ends - seq_lens
    first = jnp.zeros_like(index)
    for s in range(1, seq_lens.shape[0]):
        first = jnp.where(index >= starts[s], starts[s], first)
    return first, index - first


def swap_bits(parts, j):
    low = (j & 1) == 1
    high = (j & 2) == 2
    a, b, c, d = parts
    a, b, c, d = jnp.where(low, b, a), jnp.where(low, a, b), jnp.where(low, d, c), jnp.where(low, c, d)
    return [jnp.where(high, c, a), jnp.where(high, d, b), jnp.where(high, a, c), jnp.where(high, b, d)]


def head_perm(v, bit):
    return lax.ppermute(v, "head", [(k, k ^ bit) for k in range(4)])


def dp_perm(v, bit):
    return lax.ppermute(v, "dp", [(k, k ^ bit) for k in range(8)])


def pick(v, index, axis=0):
    return lax.dynamic_index_in_dim(v, index, axis, keepdims=False)


def dp_scatter(blocks, i):
    x = i & 1
    z = i >> 1
    pairs = blocks.reshape((4, 2) + blocks.shape[1:])
    other = dp_perm(pick(pairs, 1 - x, 1), 1)
    mine = pick(pairs, x, 1).astype(F32) + other.astype(F32)
    low = mine.astype(BF)
    result = pick(mine, z)
    for s in (1, 2, 3):
        result = result + dp_perm(pick(low, z ^ s), 2 * s).astype(F32)
    return result


def sum_all(v):
    for bit in (1, 2):
        v = v + head_perm(v, bit)
    for bit in (1, 2, 4):
        v = v + dp_perm(v, bit)
    return v


def to_owner(v, i, j):
    cols = v.reshape(v.shape[0], 4, v.shape[1] // 4)
    got = []
    for r in range(4):
        pairs = []
        for si in range(8):
            for sj in range(4):
                pairs.append((si * 4 + sj, (2 * sj + si // 4) * 4 + ((si % 4) ^ r)))
        got.append(lax.ppermute(pick(cols, (i % 4) ^ r, 1), ("dp", "head"), pairs))
    return jnp.concatenate(swap_bits(got, j), axis=0)


def qkv_owner(v, j):
    got = []
    for t in range(3):
        pairs = [((3 * dst + t) % 4, dst) for dst in range(4)]
        slot = jnp.int32(0)
        for src, dst in pairs:
            slot = jnp.where(j == src, (3 * dst + t) // 4, slot)
        got.append(lax.ppermute(pick(v, slot), "head", pairs))
    return jnp.concatenate(got, axis=0)


def fast_body(inputs, lengths, attn_gain, attn_shift, mlp_gain, mlp_shift, w_qkv, b_qkv, w_out, b_out,
              w_up, b_up, w_down, b_down, cotangent):
    own, d = inputs.shape
    n = 4
    tok = own * n
    w = d // n
    i = lax.axis_index("dp")
    j = lax.axis_index("head")
    pos = j.astype(jnp.int32).reshape(1)
    rows = lambda v: v.reshape(1, -1)
    ga, sa, gm, sm = rows(attn_gain), rows(attn_shift), rows(mlp_gain), rows(mlp_shift)
    bq, bu = rows(b_qkv), rows(b_up)
    lens = lengths[0]

    lane = jnp.arange(tok, dtype=jnp.int32)
    half = own // 2
    far = (lane - 2 * own) // half
    chunk = jnp.where(lane < 2 * own, lane // own, 2 + (far & 1))
    offset = jnp.where(lane < 2 * own, lane % own, (far >> 1) * half + lane % half)
    index = (chunk ^ j) * own + offset
    first, position = layout(lens, index)
    freqs = 10000.0 ** (-(2.0 * jnp.arange(HALF, dtype=F32)) / ROT)
    angle = freqs[:, None] * position.astype(F32)[None, :]
    cos, sin = jnp.cos(angle), jnp.sin(angle)
    seg_start = first[None, :]

    g_mlp, na, dy_all, qt, kt, vt, dot, kn, vn, p_own, p_far, dwu, dwd, small, smallf = head_stage(
        inputs, cotangent, w_up, w_down, w_qkv, w_out, bu, bq, gm, sm, ga, sa, cos, sin, n, 0
    )
    mlp_sum = p_own.astype(F32) + head_perm(p_far, 2).astype(F32)

    up_down = jnp.concatenate([dwu, dwd], axis=1)
    up_down = dp_scatter(up_down, i)
    grad_w_up = up_down[:128]
    grad_w_down = to_owner(up_down[128:].astype(BF), i, j).astype(F32)
    slots = jnp.where(jnp.arange(4)[:, None] == j, smallf[0:1], 0.0)
    early = sum_all(jnp.concatenate([small[:2], small[2:3] * 0.25, slots, jnp.zeros((1, d), F32)], axis=0))

    gt, ctx = attention(lens, pos, cos, sin, seg_start, qt, kt, vt, dot, kn, vn, own, tok // 2, halved=True)

    far_y = [ctx[:, 2 * own : 2 * own + half], ctx[:, 3 * own : 3 * own + half]]
    far_d = [ctx[:, 2 * own + half : 3 * own], ctx[:, 3 * own + half :]]
    got = [
        ctx[:, :own],
        head_perm(ctx[:, own : 2 * own], 1),
        head_perm(jnp.concatenate(far_y, axis=1), 2),
        head_perm(jnp.concatenate(far_d, axis=1), 3),
    ]
    w_rel = w_out.reshape(n, w, d)
    attn_part = mm(jnp.concatenate(got, axis=0), jnp.concatenate([pick(w_rel, j ^ r) for r in range(n)], axis=0), TN)
    bias = b_out.astype(F32) + b_down.astype(F32)
    output = (inputs.astype(F32) + attn_part + mlp_sum + bias).astype(BF)

    dw_out = mm(ctx, dy_all)

    g, dwq, bias_q, small_q = post(pos, gt, na, g_mlp, w_qkv, ga, sa, n)
    g_far = jnp.concatenate([g[2 * own : 2 * own + half], g[3 * own : 3 * own + half]], axis=0).astype(F32)
    g_dia = jnp.concatenate([g[2 * own + half : 3 * own], g[3 * own + half :]], axis=0)
    g_y = head_perm((g_far + head_perm(g_dia, 1).astype(F32)).astype(BF), 2)
    g_sum = g[:own].astype(F32) + head_perm(g[own : 2 * own], 1).astype(F32) + g_y.astype(F32)

    qkv = dp_scatter(dwq, i)
    grad_w_qkv = qkv_owner(qkv.astype(BF).reshape(3, w, 128), j).astype(F32).T
    out_sum = dp_scatter(dw_out.astype(BF).reshape(8, w // 8, d), i)
    grad_w_out = to_owner(out_sum.astype(BF), i, j).astype(F32)

    slots = jnp.where(jnp.arange(4)[None, :, None] == j, bias_q[0].reshape(3, 1, w), 0.0).reshape(3, d)
    late = sum_all(jnp.concatenate([small_q[:2], slots, jnp.zeros((3, d), F32)], axis=0))

    normed, inv = norm_parts(inputs)
    grad_inputs = cotangent.astype(F32) + inv * (
        g_sum - jnp.mean(g_sum, axis=-1, keepdims=True) - normed * jnp.mean(g_sum * normed, axis=-1, keepdims=True)
    )
    return (output, grad_inputs, late[0], late[1], early[0], early[1], grad_w_qkv, late[2:5].reshape(-1),
            grad_w_out, early[2], grad_w_up, early[3:7].reshape(-1), grad_w_down, early[2])


def general_body(inputs, lengths, attn_gain, attn_shift, mlp_gain, mlp_shift, w_qkv, b_qkv, w_out, b_out,
                 w_up, b_up, w_down, b_down, cotangent):
    own, d = inputs.shape
    n = lax.axis_size("head")
    n_dp = lax.axis_size("dp")
    tok = own * n
    w = d // n
    f = w_up.shape[1] // n
    j = lax.axis_index("head")
    pos = j.astype(jnp.int32).reshape(1)
    rows = lambda v: v.reshape(1, -1)
    ga, sa, gm, sm = rows(attn_gain), rows(attn_shift), rows(mlp_gain), rows(mlp_shift)
    bq, bu = rows(b_qkv), rows(b_up)
    lens = lengths[0]
    gather = lambda v: lax.all_gather(v, "head", axis=0, tiled=True)
    over_dp = lambda v, axis: lax.psum_scatter(v, "dp", scatter_dimension=axis, tiled=True)
    over_head = lambda v: lax.psum_scatter(v, "head", scatter_dimension=0, tiled=True)
    x_all = gather(inputs)
    dy_all = gather(cotangent)
    first, position = layout(lens, jnp.arange(tok, dtype=jnp.int32))
    freqs = 10000.0 ** (-(2.0 * jnp.arange(HALF, dtype=F32)) / ROT)
    angle = freqs[:, None] * position.astype(F32)[None, :]
    cos, sin = jnp.cos(angle), jnp.sin(angle)
    part, g_mlp, dwu, dwd, small, smallf = mlp(pos, x_all, dy_all, w_up, w_down, bu, gm, sm, n)
    qt, kt, vt, dot, kn, vn, na = proj(pos, x_all, dy_all, w_qkv, bq, w_out, ga, sa, cos, sin, n, tok, 0)
    gt, ctx = attention(
        lens, jnp.zeros((1,), jnp.int32), cos, sin, first[None, :], qt, kt, vt, dot, kn, vn, own, tok // 2
    )
    total, dwq, bias_q, small_q = post(pos, gt, na, g_mlp, w_qkv, ga, sa, n)
    attn_part = mm(ctx, lax.dynamic_slice_in_dim(w_out, j * w, w, 0), TN)
    bias = b_out.astype(F32) + b_down.astype(F32)
    output = inputs.astype(F32) + over_head((attn_part + part.astype(F32)).astype(BF)).astype(F32) + bias
    g_sum = over_head(total).astype(F32)
    normed, inv = norm_parts(inputs)
    grad_inputs = cotangent.astype(F32) + inv * (
        g_sum - jnp.mean(g_sum, axis=-1, keepdims=True) - normed * jnp.mean(g_sum * normed, axis=-1, keepdims=True)
    )
    dw_out = mm(ctx, dy_all).astype(BF)
    spread = lambda v: lax.all_to_all(v, "head", split_axis=1, concat_axis=0, tiled=True)
    grad_w_up = over_dp(dwu, 0).astype(F32)
    grad_w_down = over_dp(spread(dwd), 0).astype(F32)
    grad_w_out = over_dp(spread(dw_out), 0).astype(F32)
    qkv = over_dp(jnp.transpose(dwq, (0, 2, 1)).reshape(d, 3 * w), 0)
    qkv = lax.all_gather(qkv.reshape(d // n_dp, 3, w), "head", axis=2, tiled=True).reshape(d // n_dp, 3 * d)
    grad_w_qkv = lax.dynamic_slice_in_dim(qkv, j * 3 * w, 3 * w, 1).astype(F32)
    slots = jnp.where(jnp.arange(n)[:, None] == j, smallf[0:1], 0.0).reshape(-1)
    slots_q = jnp.where(jnp.arange(n)[None, :, None] == j, bias_q[0].reshape(3, 1, w), 0.0).reshape(-1)
    sums = lax.psum((small_q[0], small_q[1], small[0], small[1], slots_q, small[2] / n, slots), ("dp", "head"))
    return (output.astype(BF), grad_inputs, sums[0], sums[1], sums[2], sums[3], grad_w_qkv, sums[4],
            grad_w_out, sums[5], grad_w_up, sums[6], grad_w_down, sums[5])


def solution(mesh):
    fast = mesh.shape["dp"] == 8 and mesh.shape["head"] == 4
    whole = P(("dp", "head"), None)
    weight = P("dp", "head")
    return jax.shard_map(
        fast_body if fast else general_body,
        mesh=mesh,
        in_specs=(whole, P("dp", None)) + (P(),) * 12 + (whole,),
        out_specs=(whole, whole, P(), P(), P(), P(), weight, P(), weight, P(), weight, P(), weight, P()),
        check_vma=False,
    )
```

```python
import functools

import jax
import jax.numpy as jnp
import numpy as np
from jax import lax
from jax.experimental import pallas as pl
from jax.experimental.pallas import tpu as pltpu
from jax.sharding import PartitionSpec as P

HD = 64
ROT = 16
HALF = ROT // 2
NN = (((1,), (0,)), ((), ()))
NT = (((1,), (1,)), ((), ()))
TN = (((0,), (0,)), ((), ()))
FREQS = (10000.0 ** (-(2.0 * np.arange(HALF)) / ROT)).astype(np.float32)
BF = jnp.bfloat16
F32 = jnp.float32
VMEM_LIMIT = 62 * 1024 * 1024


def mm(a, b, dims=NN):
    return lax.dot_general(a, b, dims, preferred_element_type=F32)


def norm_parts(x):
    v = x.astype(F32)
    center = v - jnp.mean(v, axis=-1, keepdims=True)
    inv = lax.rsqrt(jnp.mean(center * center, axis=-1, keepdims=True) + 1e-5)
    return center * inv, inv


def mlp_kernel(prev, final, pos, *refs):
    x_ref, dy_ref, wu, wd, bu, gain, shift = refs[:7]
    refs = refs[7:]
    if prev:
        pwu, pwd, psmall, psmallf = refs[:4]
        refs = refs[4:]
    part_ref, g_ref, out_wu, out_wd, small, smallf = refs[:6]
    if final:
        dwu, dwd = refs[6:8]
    else:
        dwu, dwd = out_wu, out_wd
    step = pl.program_id(0)

    @pl.when(step == 0)
    def _():
        if prev:
            dwu[...] = pwu[...]
            dwd[...] = pwd[...]
            small[...] = psmall[...]
            smallf[...] = psmallf[...]
        else:
            dwu[...] = jnp.zeros_like(dwu)
            dwd[...] = jnp.zeros_like(dwd)
            small[...] = jnp.zeros_like(small)
            smallf[...] = jnp.zeros_like(smallf)

    normed, _ = norm_parts(x_ref[...])
    scale = gain[...].astype(F32)
    nm = (normed * scale + shift[...].astype(F32)).astype(BF)
    dy = dy_ref[...]
    pre = mm(nm, wu[...]) + bu[...].astype(F32)
    cdf = 0.5 + 0.5 * lax.erf(pre * (0.5**0.5))
    hid = (pre * cdf).astype(BF)
    slope = cdf + pre * (jnp.exp(-0.5 * pre * pre) * 0.3989422804014327)
    gp = (mm(dy, wd[...], NT) * slope).astype(BF)
    part_ref[...] = mm(hid, wd[...]).astype(BF)
    r = mm(gp, wu[...], NT)
    g_ref[...] = (r * scale).astype(BF)
    smallf[0:1, :] += jnp.sum(gp.astype(F32), axis=0, keepdims=True)
    small[0:1, :] += jnp.sum(r * normed, axis=0, keepdims=True)
    small[1:2, :] += jnp.sum(r, axis=0, keepdims=True)
    small[2:3, :] += jnp.sum(dy.astype(F32), axis=0, keepdims=True)
    dwd[...] += mm(hid, dy, TN)
    dwu[...] += mm(nm, gp, TN)

    if final:

        @pl.when(step == pl.num_programs(0) - 1)
        def _():
            out_wu[...] = dwu[...].astype(BF)
            out_wd[...] = dwd[...].astype(BF)


def mlp(pos, x, dy, wu, wd, bu, gain, shift, n, prev=None, final=True, tt=512):
    tok, d = x.shape
    f = wu.shape[1] // n
    row = lambda i, p: (i, 0)
    zero = lambda i, p: (0, 0)
    one = pl.Buffered(1)
    const = lambda shape: pl.BlockSpec(shape, zero, pipeline_mode=one)
    accs = [const((d, f)), const((f, d)), const((8, d)), const((8, f))]
    kind = BF if final else F32
    grid_spec = pltpu.PrefetchScalarGridSpec(
        num_scalar_prefetch=1,
        grid=(tok // tt,),
        in_specs=[
            pl.BlockSpec((tt, d), row),
            pl.BlockSpec((tt, d), row),
            pl.BlockSpec((d, f), lambda i, p: (0, p[0]), pipeline_mode=one),
            pl.BlockSpec((f, d), lambda i, p: (p[0], 0), pipeline_mode=one),
            pl.BlockSpec((1, f), lambda i, p: (0, p[0])),
            const((1, d)),
            const((1, d)),
        ]
        + (accs if prev is not None else []),
        out_specs=[pl.BlockSpec((tt, d), row), pl.BlockSpec((tt, d), row)] + accs,
        scratch_shapes=[pltpu.VMEM((d, f), F32), pltpu.VMEM((f, d), F32)] if final else [],
    )
    return pl.pallas_call(
        functools.partial(mlp_kernel, prev is not None, final),
        grid_spec=grid_spec,
        out_shape=(
            jax.ShapeDtypeStruct((tok, d), BF),
            jax.ShapeDtypeStruct((tok, d), BF),
            jax.ShapeDtypeStruct((d, f), kind),
            jax.ShapeDtypeStruct((f, d), kind),
            jax.ShapeDtypeStruct((8, d), F32),
            jax.ShapeDtypeStruct((8, f), F32),
        ),
        compiler_params=pltpu.CompilerParams(vmem_limit_bytes=VMEM_LIMIT),
        cost_estimate=pl.CostEstimate(
            flops=12 * tok * d * f, bytes_accessed=8 * tok * d + 12 * d * f, transcendentals=2 * tok * f
        ),
        name="mlp",
    )(pos, x, dy, wu, wd, bu, gain, shift, *(prev or ()))


def proj_kernel(nh, prev, pos, *refs):
    x_ref, dy_ref, wq, wk, wv, bq, bk, bv, wo, gain, shift, cos, sin = refs[:13]
    qt, kt, vt, dot, kn, vn, na_ref = refs[13 + (7 if prev else 0) :]
    normed, _ = norm_parts(x_ref[...])
    na = (normed * gain[...].astype(F32) + shift[...].astype(F32)).astype(BF)
    na_ref[...] = na
    co = cos[...]
    si = sin[...]

    def rotated(t, scale):
        rows = []
        for h in range(nh):
            u = t[h * HD : (h + 1) * HD]
            u1 = u[:HALF]
            u2 = u[HALF:ROT]
            rows += [u1 * co - u2 * si, u2 * co + u1 * si, u[ROT:]]
        out = jnp.concatenate(rows, axis=0).astype(BF)
        return out if scale is None else out * jnp.asarray(scale, BF)

    def triple(w, b):
        return (mm(na, w[...]) + b[...].astype(F32)).astype(BF)

    qt[...] = rotated(triple(wq, bq).astype(F32).T, HD**-0.5)
    keys = rotated(triple(wk, bk).astype(F32).T, None)
    kt[...] = keys
    kn[...] = keys.T
    values = triple(wv, bv)
    vn[...] = values
    vt[...] = values.T
    dot[...] = mm(wo[...], dy_ref[...], NT).astype(BF)


def proj(pos, x, dy, w_qkv, b_qkv, w_out, gain, shift, cos, sin, n, total, first, prev=None, tt=512):
    tok, d = x.shape
    w = d // n
    nh = w // HD
    off = first // tt
    row = lambda i, p: (i, 0)
    zero = lambda i, p: (0, 0)
    one = pl.Buffered(1)
    wspec = lambda k: pl.BlockSpec((d, w), lambda i, p: (0, k * n + p[0]), pipeline_mode=one)
    bspec = lambda k: pl.BlockSpec((1, w), lambda i, p: (0, k * n + p[0]))
    lane = lambda rows: pl.BlockSpec((rows, tt), lambda i, p: (0, off + i))
    nat = lambda cols: pl.BlockSpec((tt, cols), lambda i, p: (off + i, 0))
    shapes = [(w, total)] * 4 + [(total, w)] * 2 + [(total, d)]
    grid_spec = pltpu.PrefetchScalarGridSpec(
        num_scalar_prefetch=1,
        grid=(tok // tt,),
        in_specs=[pl.BlockSpec((tt, d), row), pl.BlockSpec((tt, d), row)]
        + [wspec(0), wspec(1), wspec(2), bspec(0), bspec(1), bspec(2)]
        + [pl.BlockSpec((w, d), lambda i, p: (p[0], 0), pipeline_mode=one)]
        + [pl.BlockSpec((1, d), zero), pl.BlockSpec((1, d), zero), lane(HALF), lane(HALF)]
        + ([pl.BlockSpec(memory_space=pl.ANY)] * 7 if prev is not None else []),
        out_specs=[lane(w)] * 4 + [nat(w)] * 2 + [nat(d)],
    )
    return pl.pallas_call(
        functools.partial(proj_kernel, nh, prev is not None),
        grid_spec=grid_spec,
        out_shape=tuple(jax.ShapeDtypeStruct(s, BF) for s in shapes),
        input_output_aliases={14 + k: k for k in range(7)} if prev is not None else {},
        compiler_params=pltpu.CompilerParams(vmem_limit_bytes=VMEM_LIMIT),
        cost_estimate=pl.CostEstimate(
            flops=8 * tok * d * w, bytes_accessed=6 * tok * d + 12 * tok * w + 8 * d * w, transcendentals=0
        ),
        name="proj",
    )(pos, x, dy, w_qkv, w_qkv, w_qkv, b_qkv, b_qkv, b_qkv, w_out, gain, shift, cos, sin, *(prev or ()))


def head_kernel(nh, x_hbm, dy_hbm, wu_hbm, wd_hbm, wqkv_hbm, wo_hbm, bu, bq, gain_m, shift_m, gain_a, shift_a, freqs, lens,
                g_out, na_out, dy_out, qt, kt, vt, dot, kn, vn, cos, sin, p_own, p_far, up_keep, up_send, dn_keep, dn_send,
                small, smallf,
                xs, dys, wu, wd, wqkv, wt, wo, bias_t, parts, far_in, near_in, dwu, dwd, load, send, recv):
    step = pl.program_id(0)
    i = lax.axis_index("dp")
    j = lax.axis_index("head")
    own, d = x_hbm.shape
    f = wu.shape[1]
    w = wo.shape[0]
    half = own // 2
    core = {"head": j ^ 1}
    across = {"head": j ^ 2}

    def remote(src, dst, k, to):
        return pltpu.make_async_remote_copy(
            src_ref=src, dst_ref=dst, send_sem=send.at[k], recv_sem=recv.at[k], device_id=to,
            device_id_type=pl.DeviceIdType.MESH)

    lo, hi = pl.ds(0, half), pl.ds(half, half)
    copies = [
        remote(x_hbm, xs.at[1], 0, core),
        remote(dy_hbm, dys.at[1], 1, core),
        remote(x_hbm.at[lo], xs.at[2, lo], 2, across),
        remote(dy_hbm.at[lo], dys.at[2, lo], 3, across),
        remote(x_hbm.at[hi], xs.at[3, lo], 4, across),
        remote(dy_hbm.at[hi], dys.at[3, lo], 5, across),
        remote(xs.at[2, lo], xs.at[2, hi], 6, core),
        remote(dys.at[2, lo], dys.at[2, hi], 7, core),
        remote(xs.at[3, lo], xs.at[3, hi], 8, core),
        remote(dys.at[3, lo], dys.at[3, hi], 9, core),
        remote(parts.at[1], near_in, 10, core),
        remote(parts.at[2, hi], far_in.at[lo], 11, core),
        remote(parts.at[3, hi], far_in.at[hi], 12, core),
    ]
    locals_ = [
        pltpu.make_async_copy(x_hbm, xs.at[0], load.at[0]),
        pltpu.make_async_copy(dy_hbm, dys.at[0], load.at[1]),
        pltpu.make_async_copy(wu_hbm.at[:, pl.ds(j * f, f)], wu, load.at[2]),
        pltpu.make_async_copy(wd_hbm.at[pl.ds(j * f, f)], wd, load.at[3]),
        pltpu.make_async_copy(wo_hbm.at[pl.ds(j * w, w)], wo, load.at[4]),
    ] + [
        pltpu.make_async_copy(wqkv_hbm.at[:, pl.ds(k * d + j * w, w)], wqkv.at[:, pl.ds(k * w, w)], load.at[5 + k])
        for k in range(3)
    ]

    @pl.when(step == 0)
    def _():
        barrier = pltpu.get_barrier_semaphore()
        for to in (core, across):
            pl.semaphore_signal(barrier, inc=1, device_id=to, device_id_type=pl.DeviceIdType.MESH)
        for c in locals_:
            c.start()
        pl.semaphore_wait(barrier, 2)
        for c in copies[:6]:
            c.start()
        dwu[...] = jnp.zeros_like(dwu)
        dwd[...] = jnp.zeros_like(dwd)
        small[...] = jnp.zeros_like(small)
        smallf[...] = jnp.zeros_like(smallf)
        for c in locals_:
            c.wait()
        for k in range(3):
            wt[k * w : (k + 1) * w, :] = wqkv[:, k * w : (k + 1) * w].T
            row = bq[:, pl.ds(pl.multiple_of(k * d + j * w, 128), w)].astype(F32)
            bias_t[k * w : (k + 1) * w, :] = jnp.broadcast_to(row, (128, w)).T

    @pl.when(step == 1)
    def _():
        copies[0].wait_recv()
        copies[1].wait_recv()

    @pl.when(step == 2)
    def _():
        copies[6].wait_recv()
        copies[7].wait_recv()

    @pl.when(step == 3)
    def _():
        copies[8].wait_recv()
        copies[9].wait_recv()

    normed, _ = norm_parts(xs[step])
    scale = gain_m[...].astype(F32)
    nm = (normed * scale + shift_m[...].astype(F32)).astype(BF)
    na = (normed * gain_a[...].astype(F32) + shift_a[...].astype(F32)).astype(BF)
    dy = dys[step]
    na_out[...] = na
    dy_out[...] = dy
    pre = mm(nm, wu[...]) + bu[:, pl.ds(pl.multiple_of(j * f, 128), f)].astype(F32)
    cdf = 0.5 + 0.5 * lax.erf(pre * (0.5**0.5))
    hid = (pre * cdf).astype(BF)
    slope = cdf + pre * (jnp.exp(-0.5 * pre * pre) * 0.3989422804014327)
    gp = (mm(dy, wd[...], NT) * slope).astype(BF)
    parts[step] = mm(hid, wd[...]).astype(BF)
    r = mm(gp, wu[...], NT)
    g_out[...] = (r * scale).astype(BF)
    smallf[0:1, :] += jnp.sum(gp.astype(F32), axis=0, keepdims=True)
    small[0:1, :] += jnp.sum(r * normed, axis=0, keepdims=True)
    small[1:2, :] += jnp.sum(r, axis=0, keepdims=True)
    small[2:3, :] += jnp.sum(dy.astype(F32), axis=0, keepdims=True)
    dwd[...] += mm(hid, dy, TN)
    dwu[...] += mm(nm, gp, TN)

    @pl.when(step == 1)
    def _():
        for k in (2, 3):
            copies[k].wait_recv()
            copies[k + 4].start()
        copies[10].start()

    @pl.when(step == 2)
    def _():
        for k in (4, 5):
            copies[k].wait_recv()
            copies[k + 4].start()
        copies[11].start()

    @pl.when(step == 3)
    def _():
        copies[12].start()
        rows = up_keep.shape[1]
        for b in range(4):
            for ref, acc, at in (
                (up_keep, dwu, 2 * b + i % 2),
                (up_send, dwu, 2 * b + 1 - i % 2),
                (dn_keep, dwd, 4 * (b // 2) + 2 * ((i // 2) % 2) + b % 2),
                (dn_send, dwd, 4 * (b // 2) + 2 * (1 - (i // 2) % 2) + b % 2),
            ):
                ref[b] = acc[pl.ds(pl.multiple_of(at * rows, rows), rows), :].astype(BF)

    lane = lax.broadcasted_iota(jnp.int32, (1, own), 1)
    far = jnp.where(lane < half, j ^ 2, j ^ 3) * own + (step - 2) * half + lane % half
    index = jnp.where(step == 0, j * own + lane, jnp.where(step == 1, (j ^ 1) * own + lane, far))
    begin = jnp.zeros_like(index)
    total = jnp.int32(0)
    for s in range(lens.shape[0] - 1):
        total = total + lens[s]
        begin = jnp.where(index >= total, total, begin)
    angle = jnp.concatenate([freqs[...]] * (own // 128), axis=1) * (index - begin).astype(F32)
    co = jnp.cos(angle)
    si = jnp.sin(angle)
    cos[...] = co
    sin[...] = si

    def projected(k):
        b = bias_t[k * w : (k + 1) * w, :]
        t = mm(wt[k * w : (k + 1) * w, :], na, NT)
        return (t + jnp.concatenate([b] * (own // 128), axis=1)).astype(BF)

    def rotated(t, factor):
        rows = []
        for h in range(nh):
            u = t[h * HD : (h + 1) * HD].astype(F32)
            u1 = u[:HALF]
            u2 = u[HALF:ROT]
            rows += [u1 * co - u2 * si, u2 * co + u1 * si, u[ROT:]]
        out = jnp.concatenate(rows, axis=0)
        return (out if factor is None else out * factor).astype(BF)

    qt[...] = rotated(projected(0), HD**-0.5)
    keys = rotated(projected(1), None)
    kt[...] = keys
    kn[...] = keys.T
    values = projected(2)
    vt[...] = values
    vn[...] = values.T
    dot[...] = mm(wo[...], dy, NT).astype(BF)

    @pl.when(step == 3)
    def _():
        copies[10].wait_recv()
        p_own[...] = (parts[0].astype(F32) + near_in[...].astype(F32)).astype(BF)
        copies[11].wait_recv()
        p_far[lo] = (parts[2, lo].astype(F32) + far_in[lo].astype(F32)).astype(BF)
        copies[12].wait_recv()
        p_far[hi] = (parts[3, lo].astype(F32) + far_in[hi].astype(F32)).astype(BF)
        for c in copies:
            c.wait_send()


def head_stage(x, dy, w_up, w_down, w_qkv, w_out, bu, bq, gm, sm, ga, sa, freqs, lens, n, cid):
    own, d = x.shape
    tok = own * n
    w = d // n
    f = w_up.shape[1] // n
    row = lambda i: (i, 0)
    lane = lambda rows: pl.BlockSpec((rows, own), lambda i: (0, i))
    nat = lambda cols: pl.BlockSpec((own, cols), row)
    one = pl.Buffered(1)
    const = lambda shape: pl.BlockSpec(shape, lambda i: (0,) * len(shape), pipeline_mode=one)
    hbm = pl.BlockSpec(memory_space=pl.ANY)
    sds = jax.ShapeDtypeStruct
    return pl.pallas_call(
        functools.partial(head_kernel, w // HD),
        grid=(n,),
        in_specs=[hbm] * 6
        + [const((1, w_up.shape[1])), const((1, 3 * d))]
        + [const((1, d))] * 4
        + [const((HALF, 128)), pl.BlockSpec(memory_space=pltpu.SMEM)],
        out_specs=[nat(d)] * 3
        + [lane(w)] * 4
        + [nat(w)] * 2
        + [lane(HALF)] * 2
        + [const((own, d))] * 2
        + [const((4, d // 8, f))] * 2
        + [const((4, f // 8, d))] * 2
        + [const((8, d)), const((8, f))],
        out_shape=tuple(
            [sds((tok, d), BF)] * 3
            + [sds((w, tok), BF)] * 4
            + [sds((tok, w), BF)] * 2
            + [sds((HALF, tok), F32)] * 2
            + [sds((own, d), BF)] * 2
            + [sds((4, d // 8, f), BF)] * 2
            + [sds((4, f // 8, d), BF)] * 2
            + [sds((8, d), F32), sds((8, f), F32)]
        ),
        scratch_shapes=[
            pltpu.VMEM((4, own, d), BF),
            pltpu.VMEM((4, own, d), BF),
            pltpu.VMEM((d, f), BF),
            pltpu.VMEM((f, d), BF),
            pltpu.VMEM((d, 3 * w), BF),
            pltpu.VMEM((3 * w, d), BF),
            pltpu.VMEM((w, d), BF),
            pltpu.VMEM((3 * w, 128), F32),
            pltpu.VMEM((4, own, d), BF),
            pltpu.VMEM((own, d), BF),
            pltpu.VMEM((own, d), BF),
            pltpu.VMEM((d, f), F32),
            pltpu.VMEM((f, d), F32),
            pltpu.SemaphoreType.DMA((8,)),
            pltpu.SemaphoreType.DMA((13,)),
            pltpu.SemaphoreType.DMA((13,)),
        ],
        compiler_params=pltpu.CompilerParams(
            vmem_limit_bytes=VMEM_LIMIT, collective_id=cid, has_side_effects=True
        ),
        cost_estimate=pl.CostEstimate(
            flops=12 * tok * d * f + 10 * tok * d * w, bytes_accessed=12 * tok * d + 8 * d * f, transcendentals=2 * tok * f
        ),
        name="head_stage",
    )(x, dy, w_up, w_down, w_qkv, w_out, bu, bq, gm, sm, ga, sa, freqs, lens)


def attn_kernel(nh, tok, blk, per, halved, lens, rel, cos, sin, qt, kt, vt, dot, kn, vn,
                gt_ref, ctx_ref, exps, peaks, dk, dv, oacc, dqacc, mrow, lrow, drow, qpad, dopad):
    nseq = lens.shape[0]
    nblk = tok // blk
    shift = rel[0]

    def place(b):
        chunk = (b // per) ^ shift
        half = b % per
        at = chunk * per + half
        if halved:
            at = jnp.where(chunk < 2, at, 4 + (chunk - 2) + 2 * half)
        return pl.multiple_of(at * blk, blk)

    dk[...] = jnp.zeros_like(dk)
    dv[...] = jnp.zeros_like(dv)
    qpad[...] = jnp.zeros_like(qpad)
    dopad[...] = jnp.zeros_like(dopad)
    rows_iota = lax.broadcasted_iota(jnp.int32, (blk, blk), 0)
    cols_iota = lax.broadcasted_iota(jnp.int32, (1, blk), 1)

    def one_block(i, carry):
        first_tok = i * blk
        begin = jnp.int32(0)
        total = jnp.int32(0)
        for s in range(nseq - 1):
            total = total + lens[s]
            begin = jnp.where(total <= first_tok, total, begin)
        low = begin // blk
        cols = pl.ds(place(i), blk)
        query_idx = cols_iota + first_tok
        start_row = jnp.zeros_like(query_idx)
        total = jnp.int32(0)
        for s in range(nseq - 1):
            total = total + lens[s]
            start_row = jnp.where(query_idx >= total, total, start_row)
        for h in range(nh):
            half = (h % 2) * HD
            qpad[h, half : half + HD, :] = qt[h * HD : (h + 1) * HD, cols]
            dopad[h, half : half + HD, :] = dot[h * HD : (h + 1) * HD, cols]
        mrow[...] = jnp.full_like(mrow, -1e30)
        lrow[...] = jnp.zeros_like(lrow)
        oacc[...] = jnp.zeros_like(oacc)
        dqacc[...] = jnp.zeros_like(dqacc)

        def forward(step, c):
            b = i - step
            krow = place(b)
            kidx = rows_iota + b * blk
            allowed = (kidx >= start_row) & (kidx <= query_idx)
            for h in range(nh):
                pair = (h // 2) * 128
                s = mm(kn[pl.ds(krow, blk), pair : pair + 128], qpad[h])
                s = jnp.where(allowed, s, -1e30)
                old = mrow[h : h + 1, :]
                new = jnp.maximum(old, jnp.max(s, axis=0, keepdims=True))
                e = jnp.exp(s - new)
                alpha = jnp.exp(old - new)
                lrow[h : h + 1, :] = lrow[h : h + 1, :] * alpha + jnp.sum(e, axis=0, keepdims=True)
                mrow[h : h + 1, :] = new
                peaks[step, h : h + 1, :] = new
                exps[h, step] = e
                oacc[h] = oacc[h] * alpha + mm(vt[h * HD : (h + 1) * HD, pl.ds(krow, blk)], e.astype(BF))
            return c

        lax.fori_loop(0, i - low + 1, forward, 0)
        for h in range(nh):
            hs = slice(h * HD, (h + 1) * HD)
            inv = 1.0 / lrow[h : h + 1, :]
            o = oacc[h] * inv
            drow[h : h + 1, :] = jnp.sum(o * dot[hs, cols].astype(F32), axis=0, keepdims=True)
            lrow[h : h + 1, :] = inv
            ctx_ref[hs, cols] = o.astype(BF)

        def backward(step, c):
            kcols = pl.ds(place(i - step), blk)
            for h in range(nh):
                pair = (h // 2) * 128
                hs = slice(h * HD, (h + 1) * HD)
                factor = jnp.exp(peaks[step, h : h + 1, :] - mrow[h : h + 1, :]) * lrow[h : h + 1, :]
                p = exps[h, step] * factor
                dp = mm(vn[kcols, pair : pair + 128], dopad[h])
                ds = (p * (dp - drow[h : h + 1, :])).astype(BF)
                dv[hs, kcols] += mm(dot[hs, cols], p.astype(BF), NT)
                dk[hs, kcols] += mm(qt[hs, cols], ds, NT)
                dqacc[hs, :] += mm(kt[hs, kcols], ds)
            return c

        lax.fori_loop(0, i - low + 1, backward, 0)
        co = cos[:, cols]
        si = sin[:, cols]
        for h in range(nh):
            base = h * HD
            g = dqacc[base : base + HD, :] * (HD**-0.5)
            g1 = g[:HALF]
            g2 = g[HALF:ROT]
            gt_ref[base : base + HD, cols] = jnp.concatenate(
                [g1 * co + g2 * si, g2 * co - g1 * si, g[ROT:]], axis=0
            ).astype(BF)
        return carry

    lax.fori_loop(0, nblk, one_block, 0)

    def finish(i, carry):
        cols = pl.ds(pl.multiple_of(i * blk, blk), blk)
        co = cos[:, cols]
        si = sin[:, cols]
        for h in range(nh):
            base = h * HD
            g = dk[base : base + HD, cols]
            g1 = g[:HALF]
            g2 = g[HALF:ROT]
            gt_ref[nh * HD + base : nh * HD + base + HD, cols] = jnp.concatenate(
                [g1 * co + g2 * si, g2 * co - g1 * si, g[ROT:]], axis=0
            ).astype(BF)
        gt_ref[2 * nh * HD :, cols] = dv[:, cols].astype(BF)
        return carry

    lax.fori_loop(0, nblk, finish, 0)


def attention(lens, rel, cos, sin, qt, kt, vt, dot, kn, vn, chunk, maxlen, halved=False, blk=256):
    width, tok = qt.shape
    nh = width // HD
    wb = maxlen // blk + 1
    vm = pl.BlockSpec(memory_space=pltpu.VMEM)
    sm = pl.BlockSpec(memory_space=pltpu.SMEM)
    return pl.pallas_call(
        functools.partial(attn_kernel, nh, tok, blk, chunk // blk, halved),
        out_shape=(jax.ShapeDtypeStruct((3 * width, tok), BF), jax.ShapeDtypeStruct((width, tok), BF)),
        in_specs=[sm, sm] + [vm] * 8,
        out_specs=(vm, vm),
        scratch_shapes=[
            pltpu.VMEM((nh, wb, blk, blk), F32),
            pltpu.VMEM((wb, 8, blk), F32),
            pltpu.VMEM((width, tok), F32),
            pltpu.VMEM((width, tok), F32),
            pltpu.VMEM((nh, HD, blk), F32),
            pltpu.VMEM((width, blk), F32),
            pltpu.VMEM((8, blk), F32),
            pltpu.VMEM((8, blk), F32),
            pltpu.VMEM((8, blk), F32),
            pltpu.VMEM((nh, 128, blk), BF),
            pltpu.VMEM((nh, 128, blk), BF),
        ],
        compiler_params=pltpu.CompilerParams(vmem_limit_bytes=VMEM_LIMIT),
        cost_estimate=pl.CostEstimate(
            flops=20 * width * tok * maxlen, bytes_accessed=20 * width * tok, transcendentals=nh * tok * maxlen
        ),
        name="attention",
    )(lens, rel, cos, sin, qt, kt, vt, dot, kn, vn)


def post_kernel(pos, gt_ref, na_ref, gm_ref, wq, wk, wv, gain, shift, g_ref, out_w, bias, small, dw):
    step = pl.program_id(0)

    @pl.when(step == 0)
    def _():
        dw[...] = jnp.zeros_like(dw)
        bias[...] = jnp.zeros_like(bias)
        small[...] = jnp.zeros_like(small)

    gt = gt_ref[...]
    na = na_ref[...]
    w = wq.shape[1]
    scale = gain[...].astype(F32)
    gn = gt.T
    r = mm(gn[:, :w], wq[...], NT) + mm(gn[:, w : 2 * w], wk[...], NT) + mm(gn[:, 2 * w :], wv[...], NT)
    g_ref[...] = (r * scale + gm_ref[...].astype(F32)).astype(BF)
    small[0:1, :] += jnp.sum(r * na.astype(F32), axis=0, keepdims=True)
    small[1:2, :] += jnp.sum(r, axis=0, keepdims=True)
    bias[0:1, :] += jnp.sum(gn.astype(F32), axis=0, keepdims=True)
    dw[...] += mm(gt, na)

    @pl.when(step == pl.num_programs(0) - 1)
    def _():
        for b in range(dw.shape[1] // 128):
            out_w[b] = dw[:, b * 128 : (b + 1) * 128].astype(BF)
        small[0:1, :] = (small[0:1, :] - shift[...].astype(F32) * small[1:2, :]) / scale


def post(pos, gt, na, gm, w_qkv, gain, shift, n, tt=512):
    tok, d = na.shape
    w = d // n
    row = lambda i, p: (i, 0)
    zero = lambda i, p: (0, 0)
    one = pl.Buffered(1)
    const = lambda shape: pl.BlockSpec(shape, zero, pipeline_mode=one)
    wspec = lambda k: pl.BlockSpec((d, w), lambda i, p: (0, k * n + p[0]), pipeline_mode=one)
    grid_spec = pltpu.PrefetchScalarGridSpec(
        num_scalar_prefetch=1,
        grid=(tok // tt,),
        in_specs=[
            pl.BlockSpec((3 * w, tt), lambda i, p: (0, i)),
            pl.BlockSpec((tt, d), row),
            pl.BlockSpec((tt, d), row),
            wspec(0),
            wspec(1),
            wspec(2),
            const((1, d)),
            const((1, d)),
        ],
        out_specs=[
            pl.BlockSpec((tt, d), row),
            pl.BlockSpec((d // 128, 3 * w, 128), lambda i, p: (0, 0, 0), pipeline_mode=one),
            const((8, 3 * w)),
            const((8, d)),
        ],
        scratch_shapes=[pltpu.VMEM((3 * w, d), F32)],
    )
    return pl.pallas_call(
        post_kernel,
        grid_spec=grid_spec,
        out_shape=(
            jax.ShapeDtypeStruct((tok, d), BF),
            jax.ShapeDtypeStruct((d // 128, 3 * w, 128), BF),
            jax.ShapeDtypeStruct((8, 3 * w), F32),
            jax.ShapeDtypeStruct((8, d), F32),
        ),
        compiler_params=pltpu.CompilerParams(vmem_limit_bytes=VMEM_LIMIT),
        cost_estimate=pl.CostEstimate(
            flops=12 * tok * d * w, bytes_accessed=8 * tok * d + 6 * tok * w + 18 * d * w, transcendentals=0
        ),
        name="post",
    )(pos, gt, na, gm, w_qkv, w_qkv, w_qkv, gain, shift)


def tail_kernel(gt_h, na_h, gm_h, ctx_h, dya_h, wqkv_h, wo_h, upk_h, upo_h, dnk_h, dno_h, x_h, dyo_h, pown_h, py_h,
                ga, sa, bo, bd, small, smallf,
                out_ref, gin_ref, wup_ref, wdn_ref, wq_ref, wout_ref, sums_ref,
                gt, na, gm, ctx, dya, wqkv, wo, upk, upo, dnk, dno, xo, dyo, pown, py,
                ctx_in, up4, dn4, up_in, dn_in, up2, dn2, up_in2, dn_in2,
                dwq, qa_in, qb_in, qa4, qb4, qa_in2, qb_in2, qa2, qb2, qa_in3, qb_in3, qfin, q_own,
                dwo, wo_in, wo4, wo_in2, wo2, wo_in3, piece, owner_in,
                far_in, near_in, far_sum, y_in, sm, sm_in, load, send, recv):
    i = lax.axis_index("dp")
    j = lax.axis_index("head")
    own, d = x_h.shape
    w = wqkv.shape[1] // 3
    half = own // 2
    bx = i % 2
    b0 = (i // 2) % 2
    b1 = i // 4
    mesh_id = pl.DeviceIdType.MESH
    core, across, diag = {"head": j ^ 1}, {"head": j ^ 2}, {"head": j ^ 3}
    px, p0, p1 = {"dp": i ^ 1}, {"dp": i ^ 2}, {"dp": i ^ 4}
    lo, hi = pl.ds(0, half), pl.ds(half, half)
    count = [0]

    def remote(src, dst, to):
        k = count[0]
        count[0] += 1
        return pltpu.make_async_remote_copy(
            src_ref=src, dst_ref=dst, send_sem=send.at[k], recv_sem=recv.at[k], device_id=to, device_id_type=mesh_id)

    def local(src, dst, k):
        return pltpu.make_async_copy(src, dst, load.at[k])

    loads = [
        local(upk_h, upk, 0), local(upo_h, upo, 1), local(dnk_h, dnk, 2), local(dno_h, dno, 3),
        local(gt_h, gt, 4), local(na_h, na, 5), local(ctx_h, ctx, 6), local(dya_h, dya, 7), local(gm_h, gm, 8),
        local(wqkv_h.at[:, pl.ds(j * w, w)], wqkv.at[:, pl.ds(0, w)], 9),
        local(wqkv_h.at[:, pl.ds(d + j * w, w)], wqkv.at[:, pl.ds(w, w)], 10),
        local(wqkv_h.at[:, pl.ds(2 * d + j * w, w)], wqkv.at[:, pl.ds(2 * w, w)], 11),
        local(wo_h, wo, 12), local(x_h, xo, 13), local(dyo_h, dyo, 14), local(pown_h, pown, 15), local(py_h, py, 16),
    ]
    c_ctx = [
        remote(ctx_h.at[:, pl.ds(2 * own, half)], ctx_in.at[1, :, lo], across),
        remote(ctx_h.at[:, pl.ds(3 * own, half)], ctx_in.at[1, :, hi], across),
        remote(ctx_h.at[:, pl.ds(2 * own + half, half)], ctx_in.at[2, :, lo], diag),
        remote(ctx_h.at[:, pl.ds(3 * own + half, half)], ctx_in.at[2, :, hi], diag),
        remote(ctx_h.at[:, pl.ds(own, own)], ctx_in.at[0], core),
    ]
    c_up0 = remote(up4.at[:, 1 - b0], up_in, p0)
    c_dnx = remote(dn4.at[:, 1 - bx], dn_in, px)
    c_up1 = remote(up2.at[1 - b1], up_in2, p1)
    c_dn1 = remote(dn2.at[1 - b1], dn_in2, p1)
    rows = dwq.shape[3] // 2
    ra, rb = pl.ds(0, rows), pl.ds(rows, rows)
    c_qa = remote(dwq.at[:, :, 1 - bx, ra], qa_in, px)
    c_qb = remote(dwq.at[:, 1 - b0, :, rb], qb_in, p0)
    c_qa0 = remote(qa4.at[:, 1 - b0], qa_in2, p0)
    c_qbx = remote(qb4.at[:, 1 - bx], qb_in2, px)
    c_qa1 = remote(qa2.at[1 - b1], qa_in3, p1)
    c_qb1 = remote(qb2.at[1 - b1], qb_in3, p1)
    c_wox = remote(dwo.at[:, :, 1 - bx], wo_in, px)
    c_wo0 = remote(wo4.at[:, 1 - b0], wo_in2, p0)
    c_wo1 = remote(wo2.at[1 - b1], wo_in3, p1)
    c_g = [
        remote(gm.at[pl.ds(2 * own + half, half)], far_in.at[lo], core),
        remote(gm.at[pl.ds(3 * own + half, half)], far_in.at[hi], core),
        remote(gm.at[pl.ds(own, own)], near_in, core),
    ]
    c_y = [remote(far_sum.at[lo], y_in.at[lo], across), remote(far_sum.at[hi], y_in.at[hi], across)]
    c_sm = [remote(sm.at[s], sm_in.at[s], to) for s, to in enumerate((core, across, px, p0, p1))]
    dests = []
    c_own = []
    for r in range(4):
        di, dj = 2 * j + i // 4, (i % 4) ^ r
        dests.append((di, dj))
        c_own.append(remote(piece.at[:, pl.ds(pl.multiple_of(dj * w, 128), w)], owner_in.at[i % 4], {"dp": di, "head": dj}))
    c_q = []
    q_dst = []
    for t in range(3):
        dst = (t - j + 4) % 4
        q_dst.append(dst)
        c_q.append(remote(qfin.at[(3 * dst + t) // 4], q_own.at[t], {"head": dst}))

    barrier = pltpu.get_barrier_semaphore()
    for to in (core, across, diag, px, p0, p1):
        pl.semaphore_signal(barrier, inc=1, device_id=to, device_id_type=mesh_id)
    for c in loads:
        c.start()
    for r in range(4):
        si, sj = 4 * (i % 2) + (j ^ r), i // 2

        @pl.when((si != i) | (sj != j))
        def _():
            pl.semaphore_signal(barrier, inc=1, device_id={"dp": si, "head": sj}, device_id_type=mesh_id)

    to_self = jnp.where(2 * j + i // 4 == i, 1, 0)
    pl.semaphore_wait(barrier, 10 - to_self)

    for c in c_ctx:
        c.start()

    def added(a, b):
        return a.astype(F32) + b.astype(F32)

    for k in range(4):
        loads[k].wait()
    up4[:, 1 - b0] = added(upk[:, 1 - b0], upo[:, 1 - b0]).astype(BF)
    c_up0.start()
    dn4[:, 1 - bx] = added(dnk[:, 1 - bx], dno[:, 1 - bx]).astype(BF)
    c_dnx.start()

    loads[4].wait()
    loads[5].wait()
    for k in range(4):
        t = mm(gt[...], na[:, 256 * k : 256 * (k + 1)]).astype(BF)
        dwq[k // 2, k % 2, 0] = t[:, :128]
        dwq[k // 2, k % 2, 1] = t[:, 128:]
    c_qa.start()
    c_qb.start()
    loads[6].wait()
    loads[7].wait()
    t = mm(ctx[...], dya[...]).astype(BF)
    for b in range(8):
        dwo[b // 4, (b // 2) % 2, b % 2] = t[32 * b : 32 * (b + 1)]
    c_wox.start()

    for k in range(8, 12):
        loads[k].wait()
    scale = ga[...].astype(F32)
    ones = jnp.zeros((1, d), F32)
    s_gain, s_shift, s_bias = ones, ones, jnp.zeros((1, 3 * w), F32)

    def tile(at, size, sums):
        ts = slice(at, at + size)
        gn = gt[:, ts].T
        r = mm(gn, wqkv[...], NT)
        gm[ts, :] = (r * scale + gm[ts, :].astype(F32)).astype(BF)
        return (
            sums[0] + jnp.sum(r * na[ts, :].astype(F32), axis=0, keepdims=True),
            sums[1] + jnp.sum(r, axis=0, keepdims=True),
            sums[2] + jnp.sum(gn.astype(F32), axis=0, keepdims=True),
        )

    sums = (s_gain, s_shift, s_bias)
    sums = tile(2 * own, own, sums)
    c_g[0].start()
    sums = tile(3 * own, own, sums)
    c_g[1].start()
    c_up0.wait_recv()
    mine = added(upk[:, b0], upo[:, b0]) + up_in[...].astype(F32)
    up2[...] = mine.astype(BF)
    c_up1.start()
    c_g[0].wait_recv()
    far_sum[lo] = added(gm[2 * own : 2 * own + half], far_in[lo]).astype(BF)
    c_y[0].start()
    c_dnx.wait_recv()
    mine = added(dnk[:, bx], dno[:, bx]) + dn_in[...].astype(F32)
    dn2[...] = mine.astype(BF)
    c_dn1.start()
    c_g[1].wait_recv()
    far_sum[hi] = added(gm[3 * own : 3 * own + half], far_in[hi]).astype(BF)
    c_y[1].start()
    sums = tile(own, own, sums)
    c_g[2].start()
    sums = tile(0, own, sums)

    sm[0] = jnp.zeros((16, d), F32)
    shift = sa[...].astype(F32)
    sm[0, 0:1, :] = (sums[0] - shift * sums[1]) / scale
    sm[0, 1:2, :] = sums[1]
    for k in range(3):
        sm[0, 2 + k : 3 + k, pl.ds(pl.multiple_of(j * w, 128), w)] = sums[2][:, k * w : (k + 1) * w]
    sm[0, 5:7, :] = small[0:2, :]
    sm[0, 7:8, :] = small[2:3, :] * 0.25
    sm[0, pl.ds(8 + j, 1), :] = smallf[0:1, :]
    c_sm[0].start()

    c_qa.wait_recv()
    qa4[...] = added(dwq[:, :, bx, ra], qa_in[...]).astype(BF)
    c_qa0.start()
    c_qb.wait_recv()
    qb4[...] = added(dwq[:, b0, :, rb], qb_in[...]).astype(BF)
    c_qbx.start()
    c_wox.wait_recv()
    wo4[...] = added(dwo[:, :, bx], wo_in[...]).astype(BF)
    c_wo0.start()

    def small_step(s):
        c_sm[s].wait_recv()
        sm[s + 1] = sm[s] + sm_in[s]
        if s < 4:
            c_sm[s + 1].start()

    small_step(0)
    for k in range(12, 17):
        loads[k].wait()
    attn = mm(ctx[:, :own], wo[pl.ds(pl.multiple_of(j * w, 128), w), :], TN)
    c_ctx[4].wait_recv()
    attn += mm(ctx_in[0], wo[pl.ds(pl.multiple_of((j ^ 1) * w, 128), w), :], TN)
    for k in range(4):
        c_ctx[k].wait_recv()
    attn += mm(ctx_in[1], wo[pl.ds(pl.multiple_of((j ^ 2) * w, 128), w), :], TN)
    attn += mm(ctx_in[2], wo[pl.ds(pl.multiple_of((j ^ 3) * w, 128), w), :], TN)
    out_ref[...] = (
        xo[...].astype(F32) + attn + added(pown[...], py[...]) + (bo[...].astype(F32) + bd[...].astype(F32))
    ).astype(BF)
    small_step(1)

    c_qa0.wait_recv()
    qa2[...] = added(qa4[:, b0], qa_in2[...]).astype(BF)
    c_qa1.start()
    c_qbx.wait_recv()
    qb2[...] = added(qb4[:, bx], qb_in2[...]).astype(BF)
    c_qb1.start()
    c_wo0.wait_recv()
    wo2[...] = added(wo4[:, b0], wo_in2[...]).astype(BF)
    c_wo1.start()
    small_step(2)
    c_up1.wait_recv()
    wup_ref[...] = added(up2[b1], up_in2[...])
    c_dn1.wait_recv()
    piece[: dn2.shape[1], :] = added(dn2[b1], dn_in2[...]).astype(BF)
    small_step(3)
    c_qa1.wait_recv()
    c_qb1.wait_recv()
    done = jnp.concatenate([added(qa2[b1], qa_in3[...]), added(qb2[b1], qb_in3[...])], axis=0).astype(BF)
    for k in range(3):
        qfin[k] = done[k * w : (k + 1) * w]
    for t in range(3):

        @pl.when(q_dst[t] != j)
        def _():
            c_q[t].start()

        @pl.when(q_dst[t] == j)
        def _():
            q_own[t] = qfin[(3 * j + t) // 4]

    c_wo1.wait_recv()
    piece[dn2.shape[1] :, :] = added(wo2[b1], wo_in3[...]).astype(BF)
    for r in range(4):
        di, dj = dests[r]

        @pl.when((di != i) | (dj != j))
        def _():
            c_own[r].start()

        @pl.when((di == i) & (dj == j))
        def _():
            owner_in[i % 4] = piece[:, pl.ds(pl.multiple_of(dj * w, 128), w)]

    small_step(4)
    sums_ref[...] = sm[5]

    c_g[2].wait_recv()
    near = added(gm[0:own], near_in[...])
    normed, inv = norm_parts(xo[...])
    c_y[0].wait_recv()
    c_y[1].wait_recv()
    g = near + y_in[...].astype(F32)
    gin_ref[...] = dyo[...].astype(F32) + inv * (
        g - jnp.mean(g, axis=-1, keepdims=True) - normed * jnp.mean(g * normed, axis=-1, keepdims=True)
    )

    for t in range(3):

        @pl.when(q_dst[t] != j)
        def _():
            c_q[t].wait_recv()

        wq_ref[:, t * w : (t + 1) * w] = q_own[t].astype(F32).T
    for r in range(4):
        di, dj = dests[r]

        @pl.when((di != i) | (dj != j))
        def _():
            c_own[r].wait_recv()

    nd = dn2.shape[1]
    no = wo2.shape[1]
    for a in range(4):
        wdn_ref[a * nd : (a + 1) * nd, :] = owner_in[a, :nd].astype(F32)
        wout_ref[a * no : (a + 1) * no, :] = owner_in[a, nd:].astype(F32)

    for c in c_ctx + [c_up0, c_dnx, c_up1, c_dn1, c_qa, c_qb, c_qa0, c_qbx, c_qa1, c_qb1, c_wox, c_wo0, c_wo1] + c_g + c_y + c_sm:
        c.wait_send()
    for t in range(3):

        @pl.when(q_dst[t] != j)
        def _():
            c_q[t].wait_send()

    for r in range(4):
        di, dj = dests[r]

        @pl.when((di != i) | (dj != j))
        def _():
            c_own[r].wait_send()


def tail_stage(gt, na, gm, ctx, dya, w_qkv, w_out, upk, upo, dnk, dno, x, dy, pown, py, ga, sa, bo, bd, small, smallf, cid):
    own, d = x.shape
    tok = na.shape[0]
    w = d // 4
    vm = pl.BlockSpec(memory_space=pltpu.VMEM)
    hbm = pl.BlockSpec(memory_space=pl.ANY)
    sds = jax.ShapeDtypeStruct
    big = lambda *s: pltpu.VMEM(s, BF)
    nb = d // 8
    no = w // 8
    r2 = 3 * w // 2
    return pl.pallas_call(
        tail_kernel,
        in_specs=[hbm] * 15 + [vm] * 6,
        out_specs=[vm] * 7,
        out_shape=(
            sds((own, d), BF), sds((own, d), F32), sds((nb, d), F32), sds((4 * nb, w), F32),
            sds((nb, 3 * w), F32), sds((4 * no, w), F32), sds((16, d), F32),
        ),
        scratch_shapes=[
            big(3 * w, tok), big(tok, d), big(tok, d), big(w, tok), big(tok, d), big(d, 3 * w), big(d, d),
            big(2, 2, nb, d), big(2, 2, nb, d), big(2, 2, nb, d), big(2, 2, nb, d),
            big(own, d), big(own, d), big(own, d), big(own, d),
            big(3, w, own), big(2, 2, nb, d), big(2, 2, nb, d), big(2, nb, d), big(2, nb, d),
            big(2, nb, d), big(2, nb, d), big(nb, d), big(nb, d),
            big(2, 2, 2, 3 * w, 128), big(2, 2, r2, 128), big(2, 2, r2, 128), big(2, 2, r2, 128), big(2, 2, r2, 128),
            big(2, r2, 128), big(2, r2, 128), big(2, r2, 128), big(2, r2, 128), big(r2, 128), big(r2, 128),
            big(3, w, 128), big(3, w, 128),
            big(2, 2, 2, no, d), big(2, 2, no, d), big(2, 2, no, d), big(2, no, d), big(2, no, d), big(no, d),
            big(nb + no, d), big(4, nb + no, w),
            big(own, d), big(own, d), big(own, d), big(own, d),
            pltpu.VMEM((6, 16, d), F32), pltpu.VMEM((5, 16, d), F32),
            pltpu.SemaphoreType.DMA((17,)), pltpu.SemaphoreType.DMA((40,)), pltpu.SemaphoreType.DMA((40,)),
        ],
        compiler_params=pltpu.CompilerParams(vmem_limit_bytes=VMEM_LIMIT, collective_id=cid, has_side_effects=True),
        cost_estimate=pl.CostEstimate(
            flops=14 * tok * d * w, bytes_accessed=10 * tok * d, transcendentals=0
        ),
        name="tail_stage",
    )(gt, na, gm, ctx, dya, w_qkv, w_out, upk, upo, dnk, dno, x, dy, pown, py, ga, sa, bo, bd, small, smallf)


def layout(seq_lens, index):
    ends = jnp.cumsum(seq_lens, dtype=jnp.int32)
    starts = ends - seq_lens
    first = jnp.zeros_like(index)
    for s in range(1, seq_lens.shape[0]):
        first = jnp.where(index >= starts[s], starts[s], first)
    return first, index - first


def head_perm(v, bit):
    return lax.ppermute(v, "head", [(k, k ^ bit) for k in range(4)])


def dp_perm(v, bit):
    return lax.ppermute(v, "dp", [(k, k ^ bit) for k in range(8)])


def fast_body(inputs, lengths, attn_gain, attn_shift, mlp_gain, mlp_shift, w_qkv, b_qkv, w_out, b_out,
              w_up, b_up, w_down, b_down, cotangent):
    own, _ = inputs.shape
    n = 4
    tok = own * n
    j = lax.axis_index("head")
    pos = j.astype(jnp.int32).reshape(1)
    rows = lambda v: v.reshape(1, -1)
    ga, sa, gm, sm = rows(attn_gain), rows(attn_shift), rows(mlp_gain), rows(mlp_shift)
    bq, bu = rows(b_qkv), rows(b_up)
    lens = lengths[0]

    freqs = jnp.asarray(np.broadcast_to(FREQS[:, None], (HALF, 128)))
    (g_mlp, na, dy_all, qt, kt, vt, dot, kn, vn, cos, sin, p_own, p_far, up_keep, up_send, dn_keep, dn_send, small,
     smallf) = head_stage(inputs, cotangent, w_up, w_down, w_qkv, w_out, bu, bq, gm, sm, ga, sa, freqs, lens, n, 0)
    up_other = dp_perm(up_send, 1)
    dn_other = dp_perm(dn_send, 2)
    p_y = head_perm(p_far, 2)
    gt, ctx = attention(lens, pos, cos, sin, qt, kt, vt, dot, kn, vn, own, tok // 2, halved=True)
    quad = lambda v: v.reshape(2, 2, v.shape[1], v.shape[2])
    output, grad_inputs, grad_w_up, grad_w_down, grad_w_qkv, grad_w_out, sums = tail_stage(
        gt, na, g_mlp, ctx, dy_all, w_qkv, w_out, quad(up_keep), quad(up_other), quad(dn_keep), quad(dn_other),
        inputs, cotangent, p_own, p_y, ga, sa, rows(b_out), rows(b_down), small, smallf, 1
    )
    return (output, grad_inputs, sums[0], sums[1], sums[5], sums[6], grad_w_qkv, sums[2:5].reshape(-1),
            grad_w_out, sums[7], grad_w_up, sums[8:12].reshape(-1), grad_w_down, sums[7])


def general_body(inputs, lengths, attn_gain, attn_shift, mlp_gain, mlp_shift, w_qkv, b_qkv, w_out, b_out,
                 w_up, b_up, w_down, b_down, cotangent):
    own, d = inputs.shape
    n = lax.axis_size("head")
    n_dp = lax.axis_size("dp")
    tok = own * n
    w = d // n
    j = lax.axis_index("head")
    pos = j.astype(jnp.int32).reshape(1)
    rows = lambda v: v.reshape(1, -1)
    ga, sa, gm, sm = rows(attn_gain), rows(attn_shift), rows(mlp_gain), rows(mlp_shift)
    bq, bu = rows(b_qkv), rows(b_up)
    lens = lengths[0]
    gather = lambda v: lax.all_gather(v, "head", axis=0, tiled=True)
    over_dp = lambda v, axis: lax.psum_scatter(v, "dp", scatter_dimension=axis, tiled=True)
    over_head = lambda v: lax.psum_scatter(v, "head", scatter_dimension=0, tiled=True)
    x_all = gather(inputs)
    dy_all = gather(cotangent)
    _, position = layout(lens, jnp.arange(tok, dtype=jnp.int32))
    freqs = 10000.0 ** (-(2.0 * jnp.arange(HALF, dtype=F32)) / ROT)
    angle = freqs[:, None] * position.astype(F32)[None, :]
    cos, sin = jnp.cos(angle), jnp.sin(angle)
    part, g_mlp, dwu, dwd, small, smallf = mlp(pos, x_all, dy_all, w_up, w_down, bu, gm, sm, n)
    qt, kt, vt, dot, kn, vn, na = proj(pos, x_all, dy_all, w_qkv, bq, w_out, ga, sa, cos, sin, n, tok, 0)
    gt, ctx = attention(
        lens, jnp.zeros((1,), jnp.int32), cos, sin, qt, kt, vt, dot, kn, vn, own, tok // 2
    )
    total, dwq, bias_q, small_q = post(pos, gt, na, g_mlp, w_qkv, ga, sa, n)
    attn_part = mm(ctx, lax.dynamic_slice_in_dim(w_out, j * w, w, 0), TN)
    bias = b_out.astype(F32) + b_down.astype(F32)
    output = inputs.astype(F32) + over_head((attn_part + part.astype(F32)).astype(BF)).astype(F32) + bias
    g_sum = over_head(total).astype(F32)
    normed, inv = norm_parts(inputs)
    grad_inputs = cotangent.astype(F32) + inv * (
        g_sum - jnp.mean(g_sum, axis=-1, keepdims=True) - normed * jnp.mean(g_sum * normed, axis=-1, keepdims=True)
    )
    dw_out = mm(ctx, dy_all).astype(BF)
    spread = lambda v: lax.all_to_all(v, "head", split_axis=1, concat_axis=0, tiled=True)
    grad_w_up = over_dp(dwu, 0).astype(F32)
    grad_w_down = over_dp(spread(dwd), 0).astype(F32)
    grad_w_out = over_dp(spread(dw_out), 0).astype(F32)
    qkv = over_dp(jnp.transpose(dwq, (0, 2, 1)).reshape(d, 3 * w), 0)
    qkv = lax.all_gather(qkv.reshape(d // n_dp, 3, w), "head", axis=2, tiled=True).reshape(d // n_dp, 3 * d)
    grad_w_qkv = lax.dynamic_slice_in_dim(qkv, j * 3 * w, 3 * w, 1).astype(F32)
    slots = jnp.where(jnp.arange(n)[:, None] == j, smallf[0:1], 0.0).reshape(-1)
    slots_q = jnp.where(jnp.arange(n)[None, :, None] == j, bias_q[0].reshape(3, 1, w), 0.0).reshape(-1)
    sums = lax.psum((small_q[0], small_q[1], small[0], small[1], slots_q, small[2] / n, slots), ("dp", "head"))
    return (output.astype(BF), grad_inputs, sums[0], sums[1], sums[2], sums[3], grad_w_qkv, sums[4],
            grad_w_out, sums[5], grad_w_up, sums[6], grad_w_down, sums[5])


def solution(mesh):
    fast = mesh.shape["dp"] == 8 and mesh.shape["head"] == 4
    whole = P(("dp", "head"), None)
    weight = P("dp", "head")
    return jax.shard_map(
        fast_body if fast else general_body,
        mesh=mesh,
        in_specs=(whole, P("dp", None)) + (P(),) * 12 + (whole,),
        out_specs=(whole, whole, P(), P(), P(), P(), weight, P(), weight, P(), weight, P(), weight, P()),
        check_vma=False,
    )
```

```python
import functools

import jax
import jax.numpy as jnp
import numpy as np
from jax import lax
from jax.experimental import pallas as pl
from jax.experimental.pallas import tpu as pltpu
from jax.sharding import PartitionSpec as P

HD = 64
ROT = 16
HALF = ROT // 2
NN = (((1,), (0,)), ((), ()))
NT = (((1,), (1,)), ((), ()))
TN = (((0,), (0,)), ((), ()))
FREQS = (10000.0 ** (-(2.0 * np.arange(HALF)) / ROT)).astype(np.float32)
BF = jnp.bfloat16
F32 = jnp.float32
VMEM_LIMIT = 62 * 1024 * 1024


def mm(a, b, dims=NN):
    return lax.dot_general(a, b, dims, preferred_element_type=F32)


def norm_parts(x):
    v = x.astype(F32)
    center = v - jnp.mean(v, axis=-1, keepdims=True)
    inv = lax.rsqrt(jnp.mean(center * center, axis=-1, keepdims=True) + 1e-5)
    return center * inv, inv


def mlp_kernel(prev, final, pos, *refs):
    x_ref, dy_ref, wu, wd, bu, gain, shift = refs[:7]
    refs = refs[7:]
    if prev:
        pwu, pwd, psmall, psmallf = refs[:4]
        refs = refs[4:]
    part_ref, g_ref, out_wu, out_wd, small, smallf = refs[:6]
    if final:
        dwu, dwd = refs[6:8]
    else:
        dwu, dwd = out_wu, out_wd
    step = pl.program_id(0)

    @pl.when(step == 0)
    def _():
        if prev:
            dwu[...] = pwu[...]
            dwd[...] = pwd[...]
            small[...] = psmall[...]
            smallf[...] = psmallf[...]
        else:
            dwu[...] = jnp.zeros_like(dwu)
            dwd[...] = jnp.zeros_like(dwd)
            small[...] = jnp.zeros_like(small)
            smallf[...] = jnp.zeros_like(smallf)

    normed, _unused = norm_parts(x_ref[...])
    scale = gain[...].astype(F32)
    nm = (normed * scale + shift[...].astype(F32)).astype(BF)
    dy = dy_ref[...]
    pre = mm(nm, wu[...]) + bu[...].astype(F32)
    cdf = 0.5 + 0.5 * lax.erf(pre * (0.5**0.5))
    hid = (pre * cdf).astype(BF)
    slope = cdf + pre * (jnp.exp(-0.5 * pre * pre) * 0.3989422804014327)
    gp = (mm(dy, wd[...], NT) * slope).astype(BF)
    part_ref[...] = mm(hid, wd[...]).astype(BF)
    r = mm(gp, wu[...], NT)
    g_ref[...] = (r * scale).astype(BF)
    smallf[0:1, :] += jnp.sum(gp.astype(F32), axis=0, keepdims=True)
    small[0:1, :] += jnp.sum(r * normed, axis=0, keepdims=True)
    small[1:2, :] += jnp.sum(r, axis=0, keepdims=True)
    small[2:3, :] += jnp.sum(dy.astype(F32), axis=0, keepdims=True)
    dwd[...] += mm(hid, dy, TN)
    dwu[...] += mm(nm, gp, TN)

    if final:

        @pl.when(step == pl.num_programs(0) - 1)
        def _():
            out_wu[...] = dwu[...].astype(BF)
            out_wd[...] = dwd[...].astype(BF)


def mlp(pos, x, dy, wu, wd, bu, gain, shift, n, prev=None, final=True, tt=512):
    tok, d = x.shape
    f = wu.shape[1] // n
    row = lambda i, p: (i, 0)
    zero = lambda i, p: (0, 0)
    one = pl.Buffered(1)
    const = lambda shape: pl.BlockSpec(shape, zero, pipeline_mode=one)
    accs = [const((d, f)), const((f, d)), const((8, d)), const((8, f))]
    kind = BF if final else F32
    grid_spec = pltpu.PrefetchScalarGridSpec(
        num_scalar_prefetch=1,
        grid=(tok // tt,),
        in_specs=[
            pl.BlockSpec((tt, d), row),
            pl.BlockSpec((tt, d), row),
            pl.BlockSpec((d, f), lambda i, p: (0, p[0]), pipeline_mode=one),
            pl.BlockSpec((f, d), lambda i, p: (p[0], 0), pipeline_mode=one),
            pl.BlockSpec((1, f), lambda i, p: (0, p[0])),
            const((1, d)),
            const((1, d)),
        ]
        + (accs if prev is not None else []),
        out_specs=[pl.BlockSpec((tt, d), row), pl.BlockSpec((tt, d), row)] + accs,
        scratch_shapes=[pltpu.VMEM((d, f), F32), pltpu.VMEM((f, d), F32)] if final else [],
    )
    return pl.pallas_call(
        functools.partial(mlp_kernel, prev is not None, final),
        grid_spec=grid_spec,
        out_shape=(
            jax.ShapeDtypeStruct((tok, d), BF),
            jax.ShapeDtypeStruct((tok, d), BF),
            jax.ShapeDtypeStruct((d, f), kind),
            jax.ShapeDtypeStruct((f, d), kind),
            jax.ShapeDtypeStruct((8, d), F32),
            jax.ShapeDtypeStruct((8, f), F32),
        ),
        compiler_params=pltpu.CompilerParams(vmem_limit_bytes=VMEM_LIMIT),
        cost_estimate=pl.CostEstimate(
            flops=12 * tok * d * f, bytes_accessed=8 * tok * d + 12 * d * f, transcendentals=2 * tok * f
        ),
        name="mlp",
    )(pos, x, dy, wu, wd, bu, gain, shift, *(prev or ()))


def proj_kernel(nh, prev, pos, *refs):
    x_ref, dy_ref, wq, wk, wv, bq, bk, bv, wo, gain, shift, cos, sin = refs[:13]
    qt, kt, vt, dot, kn, vn, na_ref = refs[13 + (7 if prev else 0) :]
    normed, _unused = norm_parts(x_ref[...])
    na = (normed * gain[...].astype(F32) + shift[...].astype(F32)).astype(BF)
    na_ref[...] = na
    co = cos[...]
    si = sin[...]

    def rotated(t, scale):
        rows = []
        for h in range(nh):
            u = t[h * HD : (h + 1) * HD]
            u1 = u[:HALF]
            u2 = u[HALF:ROT]
            rows += [u1 * co - u2 * si, u2 * co + u1 * si, u[ROT:]]
        out = jnp.concatenate(rows, axis=0).astype(BF)
        return out if scale is None else out * jnp.asarray(scale, BF)

    def triple(w, b):
        return (mm(na, w[...]) + b[...].astype(F32)).astype(BF)

    qt[...] = rotated(triple(wq, bq).astype(F32).T, HD**-0.5)
    keys = rotated(triple(wk, bk).astype(F32).T, None)
    kt[...] = keys
    kn[...] = keys.T
    values = triple(wv, bv)
    vn[...] = values
    vt[...] = values.T
    dot[...] = mm(wo[...], dy_ref[...], NT).astype(BF)


def proj(pos, x, dy, w_qkv, b_qkv, w_out, gain, shift, cos, sin, n, total, first, prev=None, tt=512):
    tok, d = x.shape
    w = d // n
    nh = w // HD
    off = first // tt
    row = lambda i, p: (i, 0)
    zero = lambda i, p: (0, 0)
    one = pl.Buffered(1)
    wspec = lambda k: pl.BlockSpec((d, w), lambda i, p: (0, k * n + p[0]), pipeline_mode=one)
    bspec = lambda k: pl.BlockSpec((1, w), lambda i, p: (0, k * n + p[0]))
    lane = lambda rows: pl.BlockSpec((rows, tt), lambda i, p: (0, off + i))
    nat = lambda cols: pl.BlockSpec((tt, cols), lambda i, p: (off + i, 0))
    shapes = [(w, total)] * 4 + [(total, w)] * 2 + [(total, d)]
    grid_spec = pltpu.PrefetchScalarGridSpec(
        num_scalar_prefetch=1,
        grid=(tok // tt,),
        in_specs=[pl.BlockSpec((tt, d), row), pl.BlockSpec((tt, d), row)]
        + [wspec(0), wspec(1), wspec(2), bspec(0), bspec(1), bspec(2)]
        + [pl.BlockSpec((w, d), lambda i, p: (p[0], 0), pipeline_mode=one)]
        + [pl.BlockSpec((1, d), zero), pl.BlockSpec((1, d), zero), lane(HALF), lane(HALF)]
        + ([pl.BlockSpec(memory_space=pl.ANY)] * 7 if prev is not None else []),
        out_specs=[lane(w)] * 4 + [nat(w)] * 2 + [nat(d)],
    )
    return pl.pallas_call(
        functools.partial(proj_kernel, nh, prev is not None),
        grid_spec=grid_spec,
        out_shape=tuple(jax.ShapeDtypeStruct(s, BF) for s in shapes),
        input_output_aliases={14 + k: k for k in range(7)} if prev is not None else {},
        compiler_params=pltpu.CompilerParams(vmem_limit_bytes=VMEM_LIMIT),
        cost_estimate=pl.CostEstimate(
            flops=8 * tok * d * w, bytes_accessed=6 * tok * d + 12 * tok * w + 8 * d * w, transcendentals=0
        ),
        name="proj",
    )(pos, x, dy, w_qkv, w_qkv, w_qkv, b_qkv, b_qkv, b_qkv, w_out, gain, shift, cos, sin, *(prev or ()))


def head_kernel(nh, x_hbm, dy_hbm, wu_hbm, wd_hbm, wqkv_hbm, wo_hbm, vec, lens,
                g_out, na_out, dy_out, qt, kt, vt, dot, kn, vn, cos, sin, p_own, p_far, up_keep, up_send, dn0, dn1, dn2, dn3,
                small, smallf,
                xs, dys, wu, wd, wqkv, wt, wo, bias_t, parts, far_in, near_in, dwu, dwd, load, send, recv):
    step = pl.program_id(0)
    i = lax.axis_index("dp")
    j = lax.axis_index("head")
    own, d = x_hbm.shape
    f = wu.shape[1]
    w = wo.shape[0]
    half = own // 2
    core = {"head": j ^ 1}
    across = {"head": j ^ 2}

    def remote(src, dst, k, to):
        return pltpu.make_async_remote_copy(
            src_ref=src, dst_ref=dst, send_sem=send.at[k], recv_sem=recv.at[k], device_id=to,
            device_id_type=pl.DeviceIdType.MESH)

    lo, hi = pl.ds(0, half), pl.ds(half, half)
    copies = [
        remote(x_hbm, xs.at[1], 0, core),
        remote(dy_hbm, dys.at[1], 1, core),
        remote(x_hbm.at[lo], xs.at[2, lo], 2, across),
        remote(dy_hbm.at[lo], dys.at[2, lo], 3, across),
        remote(x_hbm.at[hi], xs.at[3, lo], 4, across),
        remote(dy_hbm.at[hi], dys.at[3, lo], 5, across),
        remote(xs.at[2, lo], xs.at[2, hi], 6, core),
        remote(dys.at[2, lo], dys.at[2, hi], 7, core),
        remote(xs.at[3, lo], xs.at[3, hi], 8, core),
        remote(dys.at[3, lo], dys.at[3, hi], 9, core),
        remote(parts.at[1], near_in, 10, core),
        remote(parts.at[2, hi], far_in.at[lo], 11, core),
        remote(parts.at[3, hi], far_in.at[hi], 12, core),
    ]
    locals_ = [
        pltpu.make_async_copy(x_hbm, xs.at[0], load.at[0]),
        pltpu.make_async_copy(dy_hbm, dys.at[0], load.at[1]),
        pltpu.make_async_copy(wu_hbm.at[:, pl.ds(j * f, f)], wu, load.at[2]),
        pltpu.make_async_copy(wd_hbm.at[pl.ds(j * f, f)], wd, load.at[3]),
        pltpu.make_async_copy(wo_hbm.at[pl.ds(j * w, w)], wo, load.at[4]),
    ] + [
        pltpu.make_async_copy(wqkv_hbm.at[:, pl.ds(k * d + j * w, w)], wqkv.at[:, pl.ds(k * w, w)], load.at[5 + k])
        for k in range(3)
    ]

    @pl.when(step == 0)
    def _():
        barrier = pltpu.get_barrier_semaphore()
        for to in (core, across):
            pl.semaphore_signal(barrier, inc=1, device_id=to, device_id_type=pl.DeviceIdType.MESH)
        for c in locals_:
            c.start()
        pl.semaphore_wait(barrier, 2)
        for c in copies[:6]:
            c.start()
        dwu[...] = jnp.zeros_like(dwu)
        dwd[...] = jnp.zeros_like(dwd)
        small[...] = jnp.zeros_like(small)
        smallf[...] = jnp.zeros_like(smallf)
        for c in locals_:
            c.wait()
        for k in range(3):
            wt[k * w : (k + 1) * w, :] = wqkv[:, k * w : (k + 1) * w].T
            row = vec[8 + k : 9 + k, pl.ds(pl.multiple_of(j * w, 128), w)]
            bias_t[k * w : (k + 1) * w, :] = jnp.broadcast_to(row, (128, w)).T

    @pl.when(step == 1)
    def _():
        copies[0].wait_recv()
        copies[1].wait_recv()

    @pl.when(step == 2)
    def _():
        copies[6].wait_recv()
        copies[7].wait_recv()

    @pl.when(step == 3)
    def _():
        copies[8].wait_recv()
        copies[9].wait_recv()

    normed, _unused = norm_parts(xs[step])
    scale = vec[2:3, :]
    nm = (normed * scale + vec[3:4, :]).astype(BF)
    na = (normed * vec[0:1, :] + vec[1:2, :]).astype(BF)
    dy = dys[step]
    na_out[...] = na
    dy_out[...] = dy
    pre = mm(nm, wu[...]) + vec[pl.ds(4 + j, 1), :]
    cdf = 0.5 + 0.5 * lax.erf(pre * (0.5**0.5))
    hid = (pre * cdf).astype(BF)
    slope = cdf + pre * (jnp.exp(-0.5 * pre * pre) * 0.3989422804014327)
    gp = (mm(dy, wd[...], NT) * slope).astype(BF)
    parts[step] = mm(hid, wd[...]).astype(BF)
    r = mm(gp, wu[...], NT)
    g_out[...] = (r * scale).astype(BF)
    smallf[0:1, :] += jnp.sum(gp.astype(F32), axis=0, keepdims=True)
    small[0:1, :] += jnp.sum(r * normed, axis=0, keepdims=True)
    small[1:2, :] += jnp.sum(r, axis=0, keepdims=True)
    small[2:3, :] += jnp.sum(dy.astype(F32), axis=0, keepdims=True)
    dwd[...] += mm(hid, dy, TN)
    dwu[...] += mm(nm, gp, TN)

    @pl.when(step == 1)
    def _():
        for k in (2, 3):
            copies[k].wait_recv()
            copies[k + 4].start()
        copies[10].start()

    @pl.when(step == 2)
    def _():
        for k in (4, 5):
            copies[k].wait_recv()
            copies[k + 4].start()
        copies[11].start()

    @pl.when(step == 3)
    def _():
        copies[12].start()
        rows = up_keep.shape[1]
        for b in range(4):
            for ref, at in ((up_keep, 2 * b + i % 2), (up_send, 2 * b + 1 - i % 2)):
                ref[b] = dwu[pl.ds(pl.multiple_of(at * rows, rows), rows), :].astype(BF)
            ref = (dn0, dn1, dn2, dn3)[b]
            for x in range(2):
                at = 2 * ((i // 2) ^ b) + x
                ref[x] = dwd[pl.ds(pl.multiple_of(at * rows, rows), rows), :].astype(BF)

    lane = lax.broadcasted_iota(jnp.int32, (1, own), 1)
    far = jnp.where(lane < half, j ^ 2, j ^ 3) * own + (step - 2) * half + lane % half
    index = jnp.where(step == 0, j * own + lane, jnp.where(step == 1, (j ^ 1) * own + lane, far))
    begin = jnp.zeros_like(index)
    total = jnp.int32(0)
    for s in range(lens.shape[0] - 1):
        total = total + lens[s]
        begin = jnp.where(index >= total, total, begin)
    sub = lax.broadcasted_iota(jnp.int32, (HALF, own), 0)
    freqs = jnp.zeros((HALF, own), F32)
    for k in range(HALF):
        freqs = jnp.where(sub == k, float(FREQS[k]), freqs)
    angle = freqs * (index - begin).astype(F32)
    co = jnp.cos(angle)
    si = jnp.sin(angle)
    cos[...] = co
    sin[...] = si

    def projected(k):
        b = bias_t[k * w : (k + 1) * w, :]
        t = mm(wt[k * w : (k + 1) * w, :], na, NT)
        return (t + jnp.concatenate([b] * (own // 128), axis=1)).astype(BF)

    def rotated(t, factor):
        rows = []
        for h in range(nh):
            u = t[h * HD : (h + 1) * HD].astype(F32)
            u1 = u[:HALF]
            u2 = u[HALF:ROT]
            rows += [u1 * co - u2 * si, u2 * co + u1 * si, u[ROT:]]
        out = jnp.concatenate(rows, axis=0)
        return (out if factor is None else out * factor).astype(BF)

    qt[...] = rotated(projected(0), HD**-0.5)
    keys = rotated(projected(1), None)
    kt[...] = keys
    kn[...] = keys.T
    values = projected(2)
    vt[...] = values
    vn[...] = values.T
    dot[...] = mm(wo[...], dy, NT).astype(BF)

    @pl.when(step == 3)
    def _():
        copies[10].wait_recv()
        p_own[...] = (parts[0].astype(F32) + near_in[...].astype(F32)).astype(BF)
        copies[11].wait_recv()
        p_far[lo] = (parts[2, lo].astype(F32) + far_in[lo].astype(F32)).astype(BF)
        copies[12].wait_recv()
        p_far[hi] = (parts[3, lo].astype(F32) + far_in[hi].astype(F32)).astype(BF)
        for c in copies:
            c.wait_send()


def head_stage(x, dy, w_up, w_down, w_qkv, w_out, vec, lens, n, cid):
    own, d = x.shape
    tok = own * n
    w = d // n
    f = w_up.shape[1] // n
    row = lambda i: (i, 0)
    lane = lambda rows: pl.BlockSpec((rows, own), lambda i: (0, i))
    nat = lambda cols: pl.BlockSpec((own, cols), row)
    one = pl.Buffered(1)
    const = lambda shape: pl.BlockSpec(shape, lambda i: (0,) * len(shape), pipeline_mode=one)
    hbm = pl.BlockSpec(memory_space=pl.ANY)
    sds = jax.ShapeDtypeStruct
    return pl.pallas_call(
        functools.partial(head_kernel, w // HD),
        grid=(n,),
        in_specs=[hbm] * 6
        + [const((16, d)), pl.BlockSpec(memory_space=pltpu.SMEM)],
        out_specs=[nat(d)] * 3
        + [lane(w)] * 4
        + [nat(w)] * 2
        + [lane(HALF)] * 2
        + [const((own, d))] * 2
        + [const((4, d // 8, f))] * 2
        + [const((2, f // 8, d))] * 4
        + [const((8, d)), const((8, f))],
        out_shape=tuple(
            [sds((tok, d), BF)] * 3
            + [sds((w, tok), BF)] * 4
            + [sds((tok, w), BF)] * 2
            + [sds((HALF, tok), F32)] * 2
            + [sds((own, d), BF)] * 2
            + [sds((4, d // 8, f), BF)] * 2
            + [sds((2, f // 8, d), BF)] * 4
            + [sds((8, d), F32), sds((8, f), F32)]
        ),
        scratch_shapes=[
            pltpu.VMEM((4, own, d), BF),
            pltpu.VMEM((4, own, d), BF),
            pltpu.VMEM((d, f), BF),
            pltpu.VMEM((f, d), BF),
            pltpu.VMEM((d, 3 * w), BF),
            pltpu.VMEM((3 * w, d), BF),
            pltpu.VMEM((w, d), BF),
            pltpu.VMEM((3 * w, 128), F32),
            pltpu.VMEM((4, own, d), BF),
            pltpu.VMEM((own, d), BF),
            pltpu.VMEM((own, d), BF),
            pltpu.VMEM((d, f), F32),
            pltpu.VMEM((f, d), F32),
            pltpu.SemaphoreType.DMA((8,)),
            pltpu.SemaphoreType.DMA((13,)),
            pltpu.SemaphoreType.DMA((13,)),
        ],
        compiler_params=pltpu.CompilerParams(
            vmem_limit_bytes=VMEM_LIMIT, collective_id=cid, has_side_effects=True
        ),
        cost_estimate=pl.CostEstimate(
            flops=12 * tok * d * f + 10 * tok * d * w, bytes_accessed=12 * tok * d + 8 * d * f, transcendentals=2 * tok * f
        ),
        name="head_stage",
    )(x, dy, w_up, w_down, w_qkv, w_out, vec, lens)


def attn_kernel(nh, tok, blk, per, halved, lens, rel, cos, sin, qt, kt, vt, dot, kn, vn,
                gt_ref, ctx_ref, exps, peaks, dk, dv, oacc, dqacc, mrow, lrow, drow, qpad, dopad):
    nseq = lens.shape[0]
    nblk = tok // blk
    shift = rel[0]

    def place(b):
        chunk = (b // per) ^ shift
        half = b % per
        at = chunk * per + half
        if halved:
            at = jnp.where(chunk < 2, at, 4 + (chunk - 2) + 2 * half)
        return pl.multiple_of(at * blk, blk)

    dk[...] = jnp.zeros_like(dk)
    dv[...] = jnp.zeros_like(dv)
    qpad[...] = jnp.zeros_like(qpad)
    dopad[...] = jnp.zeros_like(dopad)
    rows_iota = lax.broadcasted_iota(jnp.int32, (blk, blk), 0)
    cols_iota = lax.broadcasted_iota(jnp.int32, (1, blk), 1)

    def one_block(i, carry):
        first_tok = i * blk
        begin = jnp.int32(0)
        total = jnp.int32(0)
        for s in range(nseq - 1):
            total = total + lens[s]
            begin = jnp.where(total <= first_tok, total, begin)
        low = begin // blk
        cols = pl.ds(place(i), blk)
        query_idx = cols_iota + first_tok
        start_row = jnp.zeros_like(query_idx)
        total = jnp.int32(0)
        for s in range(nseq - 1):
            total = total + lens[s]
            start_row = jnp.where(query_idx >= total, total, start_row)
        for h in range(nh):
            half = (h % 2) * HD
            qpad[h, half : half + HD, :] = qt[h * HD : (h + 1) * HD, cols]
            dopad[h, half : half + HD, :] = dot[h * HD : (h + 1) * HD, cols]
        mrow[...] = jnp.full_like(mrow, -1e30)
        lrow[...] = jnp.zeros_like(lrow)
        oacc[...] = jnp.zeros_like(oacc)
        dqacc[...] = jnp.zeros_like(dqacc)

        def forward(step, c):
            b = i - step
            krow = place(b)
            kidx = rows_iota + b * blk
            allowed = (kidx >= start_row) & (kidx <= query_idx)
            for h in range(nh):
                pair = (h // 2) * 128
                s = mm(kn[pl.ds(krow, blk), pair : pair + 128], qpad[h])
                s = jnp.where(allowed, s, -1e30)
                old = mrow[h : h + 1, :]
                new = jnp.maximum(old, jnp.max(s, axis=0, keepdims=True))
                e = jnp.exp(s - new)
                alpha = jnp.exp(old - new)
                lrow[h : h + 1, :] = lrow[h : h + 1, :] * alpha + jnp.sum(e, axis=0, keepdims=True)
                mrow[h : h + 1, :] = new
                peaks[step, h : h + 1, :] = new
                exps[h, step] = e
                oacc[h] = oacc[h] * alpha + mm(vt[h * HD : (h + 1) * HD, pl.ds(krow, blk)], e.astype(BF))
            return c

        lax.fori_loop(0, i - low + 1, forward, 0)
        for h in range(nh):
            hs = slice(h * HD, (h + 1) * HD)
            inv = 1.0 / lrow[h : h + 1, :]
            o = oacc[h] * inv
            drow[h : h + 1, :] = jnp.sum(o * dot[hs, cols].astype(F32), axis=0, keepdims=True)
            lrow[h : h + 1, :] = inv
            ctx_ref[hs, cols] = o.astype(BF)

        def backward(step, c):
            kcols = pl.ds(place(i - step), blk)
            for h in range(nh):
                pair = (h // 2) * 128
                hs = slice(h * HD, (h + 1) * HD)
                factor = jnp.exp(peaks[step, h : h + 1, :] - mrow[h : h + 1, :]) * lrow[h : h + 1, :]
                p = exps[h, step] * factor
                dp = mm(vn[kcols, pair : pair + 128], dopad[h])
                ds = (p * (dp - drow[h : h + 1, :])).astype(BF)
                dv[hs, kcols] += mm(dot[hs, cols], p.astype(BF), NT)
                dk[hs, kcols] += mm(qt[hs, cols], ds, NT)
                dqacc[hs, :] += mm(kt[hs, kcols], ds)
            return c

        lax.fori_loop(0, i - low + 1, backward, 0)
        co = cos[:, cols]
        si = sin[:, cols]
        for h in range(nh):
            base = h * HD
            g = dqacc[base : base + HD, :] * (HD**-0.5)
            g1 = g[:HALF]
            g2 = g[HALF:ROT]
            gt_ref[base : base + HD, cols] = jnp.concatenate(
                [g1 * co + g2 * si, g2 * co - g1 * si, g[ROT:]], axis=0
            ).astype(BF)
        return carry

    lax.fori_loop(0, nblk, one_block, 0)

    def finish(i, carry):
        cols = pl.ds(pl.multiple_of(i * blk, blk), blk)
        co = cos[:, cols]
        si = sin[:, cols]
        for h in range(nh):
            base = h * HD
            g = dk[base : base + HD, cols]
            g1 = g[:HALF]
            g2 = g[HALF:ROT]
            gt_ref[nh * HD + base : nh * HD + base + HD, cols] = jnp.concatenate(
                [g1 * co + g2 * si, g2 * co - g1 * si, g[ROT:]], axis=0
            ).astype(BF)
        gt_ref[2 * nh * HD :, cols] = dv[:, cols].astype(BF)
        return carry

    lax.fori_loop(0, nblk, finish, 0)


def attention(lens, rel, cos, sin, qt, kt, vt, dot, kn, vn, chunk, maxlen, halved=False, blk=256):
    width, tok = qt.shape
    nh = width // HD
    wb = maxlen // blk + 1
    vm = pl.BlockSpec(memory_space=pltpu.VMEM)
    sm = pl.BlockSpec(memory_space=pltpu.SMEM)
    return pl.pallas_call(
        functools.partial(attn_kernel, nh, tok, blk, chunk // blk, halved),
        out_shape=(jax.ShapeDtypeStruct((3 * width, tok), BF), jax.ShapeDtypeStruct((width, tok), BF)),
        in_specs=[sm, sm] + [vm] * 8,
        out_specs=(vm, vm),
        scratch_shapes=[
            pltpu.VMEM((nh, wb, blk, blk), F32),
            pltpu.VMEM((wb, 8, blk), F32),
            pltpu.VMEM((width, tok), F32),
            pltpu.VMEM((width, tok), F32),
            pltpu.VMEM((nh, HD, blk), F32),
            pltpu.VMEM((width, blk), F32),
            pltpu.VMEM((8, blk), F32),
            pltpu.VMEM((8, blk), F32),
            pltpu.VMEM((8, blk), F32),
            pltpu.VMEM((nh, 128, blk), BF),
            pltpu.VMEM((nh, 128, blk), BF),
        ],
        compiler_params=pltpu.CompilerParams(vmem_limit_bytes=VMEM_LIMIT),
        cost_estimate=pl.CostEstimate(
            flops=20 * width * tok * maxlen, bytes_accessed=20 * width * tok, transcendentals=nh * tok * maxlen
        ),
        name="attention",
    )(lens, rel, cos, sin, qt, kt, vt, dot, kn, vn)


def post_kernel(pos, gt_ref, na_ref, gm_ref, wq, wk, wv, gain, shift, g_ref, out_w, bias, small, dw):
    step = pl.program_id(0)

    @pl.when(step == 0)
    def _():
        dw[...] = jnp.zeros_like(dw)
        bias[...] = jnp.zeros_like(bias)
        small[...] = jnp.zeros_like(small)

    gt = gt_ref[...]
    na = na_ref[...]
    w = wq.shape[1]
    scale = gain[...].astype(F32)
    gn = gt.T
    r = mm(gn[:, :w], wq[...], NT) + mm(gn[:, w : 2 * w], wk[...], NT) + mm(gn[:, 2 * w :], wv[...], NT)
    g_ref[...] = (r * scale + gm_ref[...].astype(F32)).astype(BF)
    small[0:1, :] += jnp.sum(r * na.astype(F32), axis=0, keepdims=True)
    small[1:2, :] += jnp.sum(r, axis=0, keepdims=True)
    bias[0:1, :] += jnp.sum(gn.astype(F32), axis=0, keepdims=True)
    dw[...] += mm(gt, na)

    @pl.when(step == pl.num_programs(0) - 1)
    def _():
        for b in range(dw.shape[1] // 128):
            out_w[b] = dw[:, b * 128 : (b + 1) * 128].astype(BF)
        small[0:1, :] = (small[0:1, :] - shift[...].astype(F32) * small[1:2, :]) / scale


def post(pos, gt, na, gm, w_qkv, gain, shift, n, tt=512):
    tok, d = na.shape
    w = d // n
    row = lambda i, p: (i, 0)
    zero = lambda i, p: (0, 0)
    one = pl.Buffered(1)
    const = lambda shape: pl.BlockSpec(shape, zero, pipeline_mode=one)
    wspec = lambda k: pl.BlockSpec((d, w), lambda i, p: (0, k * n + p[0]), pipeline_mode=one)
    grid_spec = pltpu.PrefetchScalarGridSpec(
        num_scalar_prefetch=1,
        grid=(tok // tt,),
        in_specs=[
            pl.BlockSpec((3 * w, tt), lambda i, p: (0, i)),
            pl.BlockSpec((tt, d), row),
            pl.BlockSpec((tt, d), row),
            wspec(0),
            wspec(1),
            wspec(2),
            const((1, d)),
            const((1, d)),
        ],
        out_specs=[
            pl.BlockSpec((tt, d), row),
            pl.BlockSpec((d // 128, 3 * w, 128), lambda i, p: (0, 0, 0), pipeline_mode=one),
            const((8, 3 * w)),
            const((8, d)),
        ],
        scratch_shapes=[pltpu.VMEM((3 * w, d), F32)],
    )
    return pl.pallas_call(
        post_kernel,
        grid_spec=grid_spec,
        out_shape=(
            jax.ShapeDtypeStruct((tok, d), BF),
            jax.ShapeDtypeStruct((d // 128, 3 * w, 128), BF),
            jax.ShapeDtypeStruct((8, 3 * w), F32),
            jax.ShapeDtypeStruct((8, d), F32),
        ),
        compiler_params=pltpu.CompilerParams(vmem_limit_bytes=VMEM_LIMIT),
        cost_estimate=pl.CostEstimate(
            flops=12 * tok * d * w, bytes_accessed=8 * tok * d + 6 * tok * w + 18 * d * w, transcendentals=0
        ),
        name="post",
    )(pos, gt, na, gm, w_qkv, w_qkv, w_qkv, gain, shift)


def tail_kernel(gt_h, na_h, gm_h, ctx_h, dya_h, wqkv_h, wo_h, upk_h, upo_h, dn0_h, dn1_h, dn2_h, dn3_h, x_h, pown_h, py_h,
                vec, small, smallf,
                out_ref, g_ref, wup_ref, wdn_ref, wq_ref, wout_ref, sums_ref,
                gt, na, gm, ctx, dya, wqkv, wo, upk, upo, dn, xo, pown, py,
                ctx_in, up4, up_in, dn_in, up2, dn2, up_in2,
                dwq, qa_in, qb_in, qa4, qb4, qa_in2, qb_in2, qa2, qb2, qa_in3, qb_in3, qfin, q_own,
                dwo, wo_in, wo4, wo_in2, wo2, wo_in3, piece, owner_in,
                far_in, near_in, far_sum, y_in, sm, sm_in, load, send, recv):
    i = lax.axis_index("dp")
    j = lax.axis_index("head")
    own, d = x_h.shape
    w = wqkv.shape[1] // 3
    half = own // 2
    bx = i % 2
    b0 = (i // 2) % 2
    b1 = i // 4
    mesh_id = pl.DeviceIdType.MESH
    core, across, diag = {"head": j ^ 1}, {"head": j ^ 2}, {"head": j ^ 3}
    px, p0, p1 = {"dp": i ^ 1}, {"dp": i ^ 2}, {"dp": i ^ 4}
    lo, hi = pl.ds(0, half), pl.ds(half, half)
    count = [0]

    def remote(src, dst, to):
        k = count[0]
        count[0] += 1
        return pltpu.make_async_remote_copy(
            src_ref=src, dst_ref=dst, send_sem=send.at[k], recv_sem=recv.at[k], device_id=to, device_id_type=mesh_id)

    def local(src, dst, k):
        return pltpu.make_async_copy(src, dst, load.at[k])

    loads = [
        local(upk_h, upk, 0), local(upo_h, upo, 1), local(dn0_h, dn.at[0], 2), local(dn1_h, dn.at[1], 3),
        local(gt_h, gt, 4), local(na_h, na, 5), local(ctx_h, ctx, 6), local(dya_h, dya, 7), local(gm_h, gm, 8),
        local(wqkv_h.at[:, pl.ds(j * w, w)], wqkv.at[:, pl.ds(0, w)], 9),
        local(wqkv_h.at[:, pl.ds(d + j * w, w)], wqkv.at[:, pl.ds(w, w)], 10),
        local(wqkv_h.at[:, pl.ds(2 * d + j * w, w)], wqkv.at[:, pl.ds(2 * w, w)], 11),
        local(wo_h, wo, 12), local(x_h, xo, 13), local(pown_h, pown, 14), local(py_h, py, 15),
        local(dn2_h, dn.at[2], 16), local(dn3_h, dn.at[3], 17),
    ]
    c_ctx = [
        remote(ctx_h.at[:, pl.ds(2 * own, half)], ctx_in.at[1, :, lo], across),
        remote(ctx_h.at[:, pl.ds(3 * own, half)], ctx_in.at[1, :, hi], across),
        remote(ctx_h.at[:, pl.ds(2 * own + half, half)], ctx_in.at[2, :, lo], diag),
        remote(ctx_h.at[:, pl.ds(3 * own + half, half)], ctx_in.at[2, :, hi], diag),
        remote(ctx_h.at[:, pl.ds(own, own)], ctx_in.at[0], core),
    ]
    c_up0 = remote(up4.at[:, 1 - b0], up_in, p0)
    c_dnx = remote(dn2.at[1 - bx], dn_in, px)
    c_up1 = remote(up2.at[1 - b1], up_in2, p1)
    rows = dwq.shape[3] // 2
    ra, rb = pl.ds(0, rows), pl.ds(rows, rows)
    c_qa = remote(dwq.at[:, :, 1 - bx, ra], qa_in, px)
    c_qb = remote(dwq.at[:, 1 - b0, :, rb], qb_in, p0)
    c_qa0 = remote(qa4.at[:, 1 - b0], qa_in2, p0)
    c_qbx = remote(qb4.at[:, 1 - bx], qb_in2, px)
    c_qa1 = remote(qa2.at[1 - b1], qa_in3, p1)
    c_qb1 = remote(qb2.at[1 - b1], qb_in3, p1)
    c_wox = remote(dwo.at[:, :, 1 - bx], wo_in, px)
    c_wo0 = remote(wo4.at[:, 1 - b0], wo_in2, p0)
    c_wo1 = remote(wo2.at[1 - b1], wo_in3, p1)
    c_g = [
        remote(gm.at[pl.ds(2 * own + half, half)], far_in.at[lo], core),
        remote(gm.at[pl.ds(3 * own + half, half)], far_in.at[hi], core),
        remote(gm.at[pl.ds(own, own)], near_in, core),
    ]
    c_y = [remote(far_sum.at[lo], y_in.at[lo], across), remote(far_sum.at[hi], y_in.at[hi], across)]
    c_sm = [remote(sm.at[s], sm_in.at[s], to) for s, to in enumerate((core, across, px, p0, p1))]
    dests = []
    c_own = []
    for r in range(4):
        di, dj = 2 * j + i // 4, (i % 4) ^ r
        dests.append((di, dj))
        c_own.append(remote(piece.at[:, pl.ds(pl.multiple_of(dj * w, 128), w)], owner_in.at[i % 4], {"dp": di, "head": dj}))
    c_q = []
    q_dst = []
    for t in range(3):
        dst = (t - j + 4) % 4
        q_dst.append(dst)
        c_q.append(remote(qfin.at[(3 * dst + t) // 4], q_own.at[t], {"head": dst}))

    barrier = pltpu.get_barrier_semaphore()
    for to in (core, across, diag, px, p0, p1):
        pl.semaphore_signal(barrier, inc=1, device_id=to, device_id_type=mesh_id)
    for c in loads:
        c.start()
    for r in range(4):
        si, sj = 4 * (i % 2) + (j ^ r), i // 2

        @pl.when((si != i) | (sj != j))
        def _():
            pl.semaphore_signal(barrier, inc=1, device_id={"dp": si, "head": sj}, device_id_type=mesh_id)

    to_self = jnp.where(2 * j + i // 4 == i, 1, 0)
    pl.semaphore_wait(barrier, 10 - to_self)

    for c in c_ctx:
        c.start()

    def added(a, b):
        return a.astype(F32) + b.astype(F32)

    for k in range(4):
        loads[k].wait()
    up4[:, 1 - b0] = added(upk[:, 1 - b0], upo[:, 1 - b0]).astype(BF)
    c_up0.start()
    loads[16].wait()
    loads[17].wait()
    dn2[...] = (added(dn[0], dn[1]) + added(dn[2], dn[3])).astype(BF)
    c_dnx.start()

    loads[4].wait()
    loads[5].wait()
    for k in range(4):
        t = mm(gt[...], na[:, 256 * k : 256 * (k + 1)]).astype(BF)
        dwq[k // 2, k % 2, 0] = t[:, :128]
        dwq[k // 2, k % 2, 1] = t[:, 128:]
    c_qa.start()
    c_qb.start()
    loads[6].wait()
    loads[7].wait()
    t = mm(ctx[...], dya[...]).astype(BF)
    for b in range(8):
        dwo[b // 4, (b // 2) % 2, b % 2] = t[32 * b : 32 * (b + 1)]
    c_wox.start()

    for k in range(8, 12):
        loads[k].wait()
    scale = vec[0:1, :]
    ones = jnp.zeros((1, d), F32)
    s_gain, s_shift, s_bias = ones, ones, jnp.zeros((1, 3 * w), F32)

    def tile(at, size, sums):
        ts = slice(at, at + size)
        gn = gt[:, ts].T
        r = mm(gn, wqkv[...], NT)
        gm[ts, :] = (r * scale + gm[ts, :].astype(F32)).astype(BF)
        return (
            sums[0] + jnp.sum(r * na[ts, :].astype(F32), axis=0, keepdims=True),
            sums[1] + jnp.sum(r, axis=0, keepdims=True),
            sums[2] + jnp.sum(gn.astype(F32), axis=0, keepdims=True),
        )

    sums = (s_gain, s_shift, s_bias)
    sums = tile(2 * own, own, sums)
    c_g[0].start()
    sums = tile(3 * own, own, sums)
    c_g[1].start()
    c_up0.wait_recv()
    mine = added(upk[:, b0], upo[:, b0]) + up_in[...].astype(F32)
    up2[...] = mine.astype(BF)
    c_up1.start()
    c_g[0].wait_recv()
    far_sum[lo] = added(gm[2 * own : 2 * own + half], far_in[lo]).astype(BF)
    c_y[0].start()
    c_g[1].wait_recv()
    far_sum[hi] = added(gm[3 * own : 3 * own + half], far_in[hi]).astype(BF)
    c_y[1].start()
    sums = tile(own, own, sums)
    c_g[2].start()
    sums = tile(0, own, sums)

    sm[0] = jnp.zeros((16, d), F32)
    shift = vec[1:2, :]
    sm[0, 0:1, :] = (sums[0] - shift * sums[1]) / scale
    sm[0, 1:2, :] = sums[1]
    for k in range(3):
        sm[0, 2 + k : 3 + k, pl.ds(pl.multiple_of(j * w, 128), w)] = sums[2][:, k * w : (k + 1) * w]
    sm[0, 5:7, :] = small[0:2, :]
    sm[0, 7:8, :] = small[2:3, :] * 0.25
    sm[0, pl.ds(8 + j, 1), :] = smallf[0:1, :]
    c_sm[0].start()

    c_qa.wait_recv()
    qa4[...] = added(dwq[:, :, bx, ra], qa_in[...]).astype(BF)
    c_qa0.start()
    c_qb.wait_recv()
    qb4[...] = added(dwq[:, b0, :, rb], qb_in[...]).astype(BF)
    c_qbx.start()
    c_wox.wait_recv()
    wo4[...] = added(dwo[:, :, bx], wo_in[...]).astype(BF)
    c_wo0.start()

    def small_step(s):
        c_sm[s].wait_recv()
        sm[s + 1] = sm[s] + sm_in[s]
        if s < 4:
            c_sm[s + 1].start()

    small_step(0)
    for k in range(12, 16):
        loads[k].wait()
    attn = mm(ctx[:, :own], wo[pl.ds(pl.multiple_of(j * w, 128), w), :], TN)
    c_ctx[4].wait_recv()
    attn += mm(ctx_in[0], wo[pl.ds(pl.multiple_of((j ^ 1) * w, 128), w), :], TN)
    for k in range(4):
        c_ctx[k].wait_recv()
    attn += mm(ctx_in[1], wo[pl.ds(pl.multiple_of((j ^ 2) * w, 128), w), :], TN)
    attn += mm(ctx_in[2], wo[pl.ds(pl.multiple_of((j ^ 3) * w, 128), w), :], TN)
    out_ref[...] = (
        xo[...].astype(F32) + attn + added(pown[...], py[...]) + (vec[11:12, :] + vec[12:13, :])
    ).astype(BF)
    small_step(1)

    c_qa0.wait_recv()
    qa2[...] = added(qa4[:, b0], qa_in2[...]).astype(BF)
    c_qa1.start()
    c_qbx.wait_recv()
    qb2[...] = added(qb4[:, bx], qb_in2[...]).astype(BF)
    c_qb1.start()
    c_wo0.wait_recv()
    wo2[...] = added(wo4[:, b0], wo_in2[...]).astype(BF)
    c_wo1.start()
    small_step(2)
    c_up1.wait_recv()
    wup_ref[...] = added(up2[b1], up_in2[...]).astype(BF)
    c_dnx.wait_recv()
    piece[: dn2.shape[1], :] = added(dn2[bx], dn_in[...]).astype(BF)
    small_step(3)
    c_qa1.wait_recv()
    c_qb1.wait_recv()
    done = jnp.concatenate([added(qa2[b1], qa_in3[...]), added(qb2[b1], qb_in3[...])], axis=0).astype(BF)
    for k in range(3):
        qfin[k] = done[k * w : (k + 1) * w]
    for t in range(3):

        @pl.when(q_dst[t] != j)
        def _():
            c_q[t].start()

        @pl.when(q_dst[t] == j)
        def _():
            q_own[t] = qfin[(3 * j + t) // 4]

    c_wo1.wait_recv()
    piece[dn2.shape[1] :, :] = added(wo2[b1], wo_in3[...]).astype(BF)
    for r in range(4):
        di, dj = dests[r]

        @pl.when((di != i) | (dj != j))
        def _():
            c_own[r].start()

        @pl.when((di == i) & (dj == j))
        def _():
            owner_in[i % 4] = piece[:, pl.ds(pl.multiple_of(dj * w, 128), w)]

    small_step(4)
    sums_ref[...] = sm[5]

    c_g[2].wait_recv()
    near = added(gm[0:own], near_in[...])
    c_y[0].wait_recv()
    c_y[1].wait_recv()
    g_ref[...] = near + y_in[...].astype(F32)

    for t in range(3):

        @pl.when(q_dst[t] != j)
        def _():
            c_q[t].wait_recv()

        wq_ref[:, t * w : (t + 1) * w] = q_own[t].astype(F32).T.astype(BF)
    for r in range(4):
        di, dj = dests[r]

        @pl.when((di != i) | (dj != j))
        def _():
            c_own[r].wait_recv()

    nd = dn2.shape[1]
    no = wo2.shape[1]
    for a in range(4):
        wdn_ref[a * nd : (a + 1) * nd, :] = owner_in[a, :nd]
        wout_ref[a * no : (a + 1) * no, :] = owner_in[a, nd:]

    for c in c_ctx + [c_up0, c_dnx, c_up1, c_qa, c_qb, c_qa0, c_qbx, c_qa1, c_qb1, c_wox, c_wo0, c_wo1] + c_g + c_y + c_sm:
        c.wait_send()
    for t in range(3):

        @pl.when(q_dst[t] != j)
        def _():
            c_q[t].wait_send()

    for r in range(4):
        di, dj = dests[r]

        @pl.when((di != i) | (dj != j))
        def _():
            c_own[r].wait_send()


def tail_stage(gt, na, gm, ctx, dya, w_qkv, w_out, upk, upo, dn, x, pown, py, vec, small, smallf, cid):
    own, d = x.shape
    tok = na.shape[0]
    w = d // 4
    vm = pl.BlockSpec(memory_space=pltpu.VMEM)
    hbm = pl.BlockSpec(memory_space=pl.ANY)
    sds = jax.ShapeDtypeStruct
    big = lambda *s: pltpu.VMEM(s, BF)
    nb = d // 8
    no = w // 8
    r2 = 3 * w // 2
    return pl.pallas_call(
        tail_kernel,
        in_specs=[hbm] * 16 + [vm] * 3,
        out_specs=[vm] * 7,
        out_shape=(
            sds((own, d), BF), sds((own, d), F32), sds((nb, d), BF), sds((4 * nb, w), BF),
            sds((nb, 3 * w), BF), sds((4 * no, w), BF), sds((16, d), F32),
        ),
        scratch_shapes=[
            big(3 * w, tok), big(tok, d), big(tok, d), big(w, tok), big(tok, d), big(d, 3 * w), big(d, d),
            big(2, 2, nb, d), big(2, 2, nb, d), big(4, 2, nb, d),
            big(own, d), big(own, d), big(own, d),
            big(3, w, own), big(2, 2, nb, d), big(2, nb, d), big(nb, d),
            big(2, nb, d), big(2, nb, d), big(nb, d),
            big(2, 2, 2, 3 * w, 128), big(2, 2, r2, 128), big(2, 2, r2, 128), big(2, 2, r2, 128), big(2, 2, r2, 128),
            big(2, r2, 128), big(2, r2, 128), big(2, r2, 128), big(2, r2, 128), big(r2, 128), big(r2, 128),
            big(3, w, 128), big(3, w, 128),
            big(2, 2, 2, no, d), big(2, 2, no, d), big(2, 2, no, d), big(2, no, d), big(2, no, d), big(no, d),
            big(nb + no, d), big(4, nb + no, w),
            big(own, d), big(own, d), big(own, d), big(own, d),
            pltpu.VMEM((6, 16, d), F32), pltpu.VMEM((5, 16, d), F32),
            pltpu.SemaphoreType.DMA((18,)), pltpu.SemaphoreType.DMA((40,)), pltpu.SemaphoreType.DMA((40,)),
        ],
        compiler_params=pltpu.CompilerParams(vmem_limit_bytes=VMEM_LIMIT, collective_id=cid, has_side_effects=True),
        cost_estimate=pl.CostEstimate(
            flops=14 * tok * d * w, bytes_accessed=10 * tok * d, transcendentals=0
        ),
        name="tail_stage",
    )(gt, na, gm, ctx, dya, w_qkv, w_out, upk, upo, *dn, x, pown, py, vec, small, smallf)


def final_kernel(out_t, g_ref, x_ref, dy_ref, wup, wdn, wq, wout, sums,
                 out, gin, ga, sa, gm, sm, dwq, bq, dwout, bo, dwup, bu, dwdn, bd):
    out[...] = out_t[...]
    normed, inv = norm_parts(x_ref[...])
    g = g_ref[...]
    gin[...] = dy_ref[...].astype(F32) + inv * (
        g - jnp.mean(g, axis=-1, keepdims=True) - normed * jnp.mean(g * normed, axis=-1, keepdims=True)
    )

    @pl.when(pl.program_id(0) == 0)
    def _():
        d = sums.shape[1]
        for ref, first, count in ((ga, 0, 1), (sa, 1, 1), (bq, 2, 3), (gm, 5, 1), (sm, 6, 1), (bo, 7, 1), (bd, 7, 1), (bu, 8, 4)):
            for k in range(count):
                ref[k * d : (k + 1) * d] = sums[first + k, :]
        dwup[...] = wup[...].astype(F32)
        dwdn[...] = wdn[...].astype(F32)
        dwq[...] = wq[...].astype(F32)
        dwout[...] = wout[...].astype(F32)


def final_stage(out_t, g, x, dy, wup, wdn, wq, wout, sums, steps=4):
    own, d = x.shape
    row = pl.BlockSpec((own // steps, d), lambda i: (i, 0))
    const = lambda v: pl.BlockSpec(v.shape, lambda i: (0,) * len(v.shape))
    sds = lambda *s: jax.ShapeDtypeStruct(s, F32)
    like = lambda v: sds(*v.shape)
    outs = (
        jax.ShapeDtypeStruct((own, d), BF), sds(own, d), sds(d), sds(d), sds(d), sds(d), like(wq), sds(3 * d),
        like(wout), sds(d), like(wup), sds(4 * d), like(wdn), sds(d),
    )
    return pl.pallas_call(
        final_kernel,
        grid=(steps,),
        in_specs=[row, row, row, row] + [const(v) for v in (wup, wdn, wq, wout, sums)],
        out_specs=[row, row] + [const(v) for v in outs[2:]],
        out_shape=outs,
        compiler_params=pltpu.CompilerParams(vmem_limit_bytes=VMEM_LIMIT),
        name="final_stage",
    )(out_t, g, x, dy, wup, wdn, wq, wout, sums)


def layout(seq_lens, index):
    ends = jnp.cumsum(seq_lens, dtype=jnp.int32)
    starts = ends - seq_lens
    first = jnp.zeros_like(index)
    for s in range(1, seq_lens.shape[0]):
        first = jnp.where(index >= starts[s], starts[s], first)
    return first, index - first


def head_perm(v, bit):
    return lax.ppermute(v, "head", [(k, k ^ bit) for k in range(4)])


def dp_perm(v, bit):
    return lax.ppermute(v, "dp", [(k, k ^ bit) for k in range(8)])


def fast_body(inputs, lengths, attn_gain, attn_shift, mlp_gain, mlp_shift, w_qkv, b_qkv, w_out, b_out,
              w_up, b_up, w_down, b_down, cotangent):
    own, d = inputs.shape
    n = 4
    tok = own * n
    w = d // n
    pos = lax.axis_index("head").astype(jnp.int32).reshape(1)
    lens = lengths[0]
    vec = jnp.concatenate(
        [attn_gain, attn_shift, mlp_gain, mlp_shift, b_up, b_qkv, b_out, b_down, jnp.zeros((3 * d,), BF)]
    ).astype(F32).reshape(16, d)
    (g_mlp, na, dy_all, qt, kt, vt, dot, kn, vn, cos, sin, p_own, p_far, up_keep, up_send, *dn, small,
     smallf) = head_stage(inputs, cotangent, w_up, w_down, w_qkv, w_out, vec, lens, n, 0)
    up_other = dp_perm(up_send, 1)
    dn = [dn[0]] + [dp_perm(dn[k], 2 * k) for k in (1, 2, 3)]
    p_y = head_perm(p_far, 2)
    gt, ctx = attention(lens, pos, cos, sin, qt, kt, vt, dot, kn, vn, own, tok // 2, halved=True)
    quad = lambda v: v.reshape(2, 2, v.shape[1], v.shape[2])
    out_t, g, wup, wdn, wq, wout, sums = tail_stage(
        gt, na, g_mlp, ctx, dy_all, w_qkv, w_out, quad(up_keep), quad(up_other), dn, inputs, p_own, p_y, vec, small, smallf, 1
    )
    return tuple(final_stage(out_t, g, inputs, cotangent, wup, wdn, wq, wout, sums))


def general_body(inputs, lengths, attn_gain, attn_shift, mlp_gain, mlp_shift, w_qkv, b_qkv, w_out, b_out,
                 w_up, b_up, w_down, b_down, cotangent):
    own, d = inputs.shape
    n = lax.axis_size("head")
    n_dp = lax.axis_size("dp")
    tok = own * n
    w = d // n
    f = w_up.shape[1] // n
    j = lax.axis_index("head")
    pos = j.astype(jnp.int32).reshape(1)
    rows = lambda v: v.reshape(1, -1)
    ga, sa, gm, sm = rows(attn_gain), rows(attn_shift), rows(mlp_gain), rows(mlp_shift)
    bq, bu = rows(b_qkv), rows(b_up)
    lens = lengths[0]
    gather = lambda v: lax.all_gather(v, "head", axis=0, tiled=True)
    over_dp = lambda v, axis: lax.psum_scatter(v, "dp", scatter_dimension=axis, tiled=True)
    over_head = lambda v: lax.psum_scatter(v, "head", scatter_dimension=0, tiled=True)
    x_all = gather(inputs)
    dy_all = gather(cotangent)
    first, position = layout(lens, jnp.arange(tok, dtype=jnp.int32))
    freqs = 10000.0 ** (-(2.0 * jnp.arange(HALF, dtype=F32)) / ROT)
    angle = freqs[:, None] * position.astype(F32)[None, :]
    cos, sin = jnp.cos(angle), jnp.sin(angle)
    part, g_mlp, dwu, dwd, small, smallf = mlp(pos, x_all, dy_all, w_up, w_down, bu, gm, sm, n)
    qt, kt, vt, dot, kn, vn, na = proj(pos, x_all, dy_all, w_qkv, bq, w_out, ga, sa, cos, sin, n, tok, 0)
    gt, ctx = attention(
        lens, jnp.zeros((1,), jnp.int32), cos, sin, qt, kt, vt, dot, kn, vn, own, tok // 2
    )
    total, dwq, bias_q, small_q = post(pos, gt, na, g_mlp, w_qkv, ga, sa, n)
    attn_part = mm(ctx, lax.dynamic_slice_in_dim(w_out, j * w, w, 0), TN)
    bias = b_out.astype(F32) + b_down.astype(F32)
    output = inputs.astype(F32) + over_head((attn_part + part.astype(F32)).astype(BF)).astype(F32) + bias
    g_sum = over_head(total).astype(F32)
    normed, inv = norm_parts(inputs)
    grad_inputs = cotangent.astype(F32) + inv * (
        g_sum - jnp.mean(g_sum, axis=-1, keepdims=True) - normed * jnp.mean(g_sum * normed, axis=-1, keepdims=True)
    )
    dw_out = mm(ctx, dy_all).astype(BF)
    spread = lambda v: lax.all_to_all(v, "head", split_axis=1, concat_axis=0, tiled=True)
    grad_w_up = over_dp(dwu, 0).astype(F32)
    grad_w_down = over_dp(spread(dwd), 0).astype(F32)
    grad_w_out = over_dp(spread(dw_out), 0).astype(F32)
    qkv = over_dp(jnp.transpose(dwq, (0, 2, 1)).reshape(d, 3 * w), 0)
    qkv = lax.all_gather(qkv.reshape(d // n_dp, 3, w), "head", axis=2, tiled=True).reshape(d // n_dp, 3 * d)
    grad_w_qkv = lax.dynamic_slice_in_dim(qkv, j * 3 * w, 3 * w, 1).astype(F32)
    slots = jnp.where(jnp.arange(n)[:, None] == j, smallf[0:1], 0.0).reshape(-1)
    slots_q = jnp.where(jnp.arange(n)[None, :, None] == j, bias_q[0].reshape(3, 1, w), 0.0).reshape(-1)
    sums = lax.psum((small_q[0], small_q[1], small[0], small[1], slots_q, small[2] / n, slots), ("dp", "head"))
    return (output.astype(BF), grad_inputs, sums[0], sums[1], sums[2], sums[3], grad_w_qkv, sums[4],
            grad_w_out, sums[5], grad_w_up, sums[6], grad_w_down, sums[5])


def solution(mesh):
    fast = mesh.shape["dp"] == 8 and mesh.shape["head"] == 4
    whole = P(("dp", "head"), None)
    weight = P("dp", "head")
    return jax.shard_map(
        fast_body if fast else general_body,
        mesh=mesh,
        in_specs=(whole, P("dp", None)) + (P(),) * 12 + (whole,),
        out_specs=(whole, whole, P(), P(), P(), P(), weight, P(), weight, P(), weight, P(), weight, P()),
        check_vma=False,
    )
```

```python
import functools

import jax
import jax.numpy as jnp
import numpy as np
from jax import lax
from jax.experimental import pallas as pl
from jax.experimental.pallas import tpu as pltpu
from jax.sharding import PartitionSpec as P

HD = 64
ROT = 16
HALF = ROT // 2
NN = (((1,), (0,)), ((), ()))
NT = (((1,), (1,)), ((), ()))
TN = (((0,), (0,)), ((), ()))
FREQS = (10000.0 ** (-(2.0 * np.arange(HALF)) / ROT)).astype(np.float32)
BF = jnp.bfloat16
F32 = jnp.float32
VMEM_LIMIT = 62 * 1024 * 1024


def mm(a, b, dims=NN):
    return lax.dot_general(a, b, dims, preferred_element_type=F32)


def flat(v):
    return v.astype(F32).reshape(1, v.shape[0])


def norm_parts(x):
    v = x.astype(F32)
    center = v - jnp.mean(v, axis=-1, keepdims=True)
    inv = lax.rsqrt(jnp.mean(center * center, axis=-1, keepdims=True) + 1e-5)
    return center * inv, inv


def mlp_kernel(prev, final, pos, *refs):
    x_ref, dy_ref, wu, wd, bu, gain, shift = refs[:7]
    refs = refs[7:]
    if prev:
        pwu, pwd, psmall, psmallf = refs[:4]
        refs = refs[4:]
    part_ref, g_ref, out_wu, out_wd, small, smallf = refs[:6]
    if final:
        dwu, dwd = refs[6:8]
    else:
        dwu, dwd = out_wu, out_wd
    step = pl.program_id(0)

    @pl.when(step == 0)
    def _():
        if prev:
            dwu[...] = pwu[...]
            dwd[...] = pwd[...]
            small[...] = psmall[...]
            smallf[...] = psmallf[...]
        else:
            dwu[...] = jnp.zeros_like(dwu)
            dwd[...] = jnp.zeros_like(dwd)
            small[...] = jnp.zeros_like(small)
            smallf[...] = jnp.zeros_like(smallf)

    normed, _unused = norm_parts(x_ref[...])
    scale = gain[...].astype(F32)
    nm = (normed * scale + shift[...].astype(F32)).astype(BF)
    dy = dy_ref[...]
    pre = mm(nm, wu[...]) + bu[...].astype(F32)
    cdf = 0.5 + 0.5 * lax.erf(pre * (0.5**0.5))
    hid = (pre * cdf).astype(BF)
    slope = cdf + pre * (jnp.exp(-0.5 * pre * pre) * 0.3989422804014327)
    gp = (mm(dy, wd[...], NT) * slope).astype(BF)
    part_ref[...] = mm(hid, wd[...]).astype(BF)
    r = mm(gp, wu[...], NT)
    g_ref[...] = (r * scale).astype(BF)
    smallf[0:1, :] += jnp.sum(gp.astype(F32), axis=0, keepdims=True)
    small[0:1, :] += jnp.sum(r * normed, axis=0, keepdims=True)
    small[1:2, :] += jnp.sum(r, axis=0, keepdims=True)
    small[2:3, :] += jnp.sum(dy.astype(F32), axis=0, keepdims=True)
    dwd[...] += mm(hid, dy, TN)
    dwu[...] += mm(nm, gp, TN)

    if final:

        @pl.when(step == pl.num_programs(0) - 1)
        def _():
            out_wu[...] = dwu[...].astype(BF)
            out_wd[...] = dwd[...].astype(BF)


def mlp(pos, x, dy, wu, wd, bu, gain, shift, n, prev=None, final=True, tt=512):
    tok, d = x.shape
    f = wu.shape[1] // n
    row = lambda i, p: (i, 0)
    zero = lambda i, p: (0, 0)
    one = pl.Buffered(1)
    const = lambda shape: pl.BlockSpec(shape, zero, pipeline_mode=one)
    accs = [const((d, f)), const((f, d)), const((8, d)), const((8, f))]
    kind = BF if final else F32
    grid_spec = pltpu.PrefetchScalarGridSpec(
        num_scalar_prefetch=1,
        grid=(tok // tt,),
        in_specs=[
            pl.BlockSpec((tt, d), row),
            pl.BlockSpec((tt, d), row),
            pl.BlockSpec((d, f), lambda i, p: (0, p[0]), pipeline_mode=one),
            pl.BlockSpec((f, d), lambda i, p: (p[0], 0), pipeline_mode=one),
            pl.BlockSpec((1, f), lambda i, p: (0, p[0])),
            const((1, d)),
            const((1, d)),
        ]
        + (accs if prev is not None else []),
        out_specs=[pl.BlockSpec((tt, d), row), pl.BlockSpec((tt, d), row)] + accs,
        scratch_shapes=[pltpu.VMEM((d, f), F32), pltpu.VMEM((f, d), F32)] if final else [],
    )
    return pl.pallas_call(
        functools.partial(mlp_kernel, prev is not None, final),
        grid_spec=grid_spec,
        out_shape=(
            jax.ShapeDtypeStruct((tok, d), BF),
            jax.ShapeDtypeStruct((tok, d), BF),
            jax.ShapeDtypeStruct((d, f), kind),
            jax.ShapeDtypeStruct((f, d), kind),
            jax.ShapeDtypeStruct((8, d), F32),
            jax.ShapeDtypeStruct((8, f), F32),
        ),
        compiler_params=pltpu.CompilerParams(vmem_limit_bytes=VMEM_LIMIT),
        cost_estimate=pl.CostEstimate(
            flops=12 * tok * d * f, bytes_accessed=8 * tok * d + 12 * d * f, transcendentals=2 * tok * f
        ),
        name="mlp",
    )(pos, x, dy, wu, wd, bu, gain, shift, *(prev or ()))


def proj_kernel(nh, prev, pos, *refs):
    x_ref, dy_ref, wq, wk, wv, bq, bk, bv, wo, gain, shift, cos, sin = refs[:13]
    qt, kt, vt, dot, kn, vn, na_ref = refs[13 + (7 if prev else 0) :]
    normed, _unused = norm_parts(x_ref[...])
    na = (normed * gain[...].astype(F32) + shift[...].astype(F32)).astype(BF)
    na_ref[...] = na
    co = cos[...]
    si = sin[...]

    def rotated(t, scale):
        rows = []
        for h in range(nh):
            u = t[h * HD : (h + 1) * HD]
            u1 = u[:HALF]
            u2 = u[HALF:ROT]
            rows += [u1 * co - u2 * si, u2 * co + u1 * si, u[ROT:]]
        out = jnp.concatenate(rows, axis=0).astype(BF)
        return out if scale is None else out * jnp.asarray(scale, BF)

    def triple(w, b):
        return (mm(na, w[...]) + b[...].astype(F32)).astype(BF)

    qt[...] = rotated(triple(wq, bq).astype(F32).T, HD**-0.5)
    keys = rotated(triple(wk, bk).astype(F32).T, None)
    kt[...] = keys
    kn[...] = keys.T
    values = triple(wv, bv)
    vn[...] = values
    vt[...] = values.T
    dot[...] = mm(wo[...], dy_ref[...], NT).astype(BF)


def proj(pos, x, dy, w_qkv, b_qkv, w_out, gain, shift, cos, sin, n, total, first, prev=None, tt=512):
    tok, d = x.shape
    w = d // n
    nh = w // HD
    off = first // tt
    row = lambda i, p: (i, 0)
    zero = lambda i, p: (0, 0)
    one = pl.Buffered(1)
    wspec = lambda k: pl.BlockSpec((d, w), lambda i, p: (0, k * n + p[0]), pipeline_mode=one)
    bspec = lambda k: pl.BlockSpec((1, w), lambda i, p: (0, k * n + p[0]))
    lane = lambda rows: pl.BlockSpec((rows, tt), lambda i, p: (0, off + i))
    nat = lambda cols: pl.BlockSpec((tt, cols), lambda i, p: (off + i, 0))
    shapes = [(w, total)] * 4 + [(total, w)] * 2 + [(total, d)]
    grid_spec = pltpu.PrefetchScalarGridSpec(
        num_scalar_prefetch=1,
        grid=(tok // tt,),
        in_specs=[pl.BlockSpec((tt, d), row), pl.BlockSpec((tt, d), row)]
        + [wspec(0), wspec(1), wspec(2), bspec(0), bspec(1), bspec(2)]
        + [pl.BlockSpec((w, d), lambda i, p: (p[0], 0), pipeline_mode=one)]
        + [pl.BlockSpec((1, d), zero), pl.BlockSpec((1, d), zero), lane(HALF), lane(HALF)]
        + ([pl.BlockSpec(memory_space=pl.ANY)] * 7 if prev is not None else []),
        out_specs=[lane(w)] * 4 + [nat(w)] * 2 + [nat(d)],
    )
    return pl.pallas_call(
        functools.partial(proj_kernel, nh, prev is not None),
        grid_spec=grid_spec,
        out_shape=tuple(jax.ShapeDtypeStruct(s, BF) for s in shapes),
        input_output_aliases={14 + k: k for k in range(7)} if prev is not None else {},
        compiler_params=pltpu.CompilerParams(vmem_limit_bytes=VMEM_LIMIT),
        cost_estimate=pl.CostEstimate(
            flops=8 * tok * d * w, bytes_accessed=6 * tok * d + 12 * tok * w + 8 * d * w, transcendentals=0
        ),
        name="proj",
    )(pos, x, dy, w_qkv, w_qkv, w_qkv, b_qkv, b_qkv, b_qkv, w_out, gain, shift, cos, sin, *(prev or ()))


def head_kernel(nh, x_hbm, dy_hbm, wu_hbm, wd_hbm, wqkv_hbm, wo_hbm, gain_a, shift_a, gain_m, shift_m, bu, bq, lens,
                g_out, na_out, dy_out, qt, kt, vt, dot, kn, vn, cos, sin, p_own, p_far, up_keep, up_send, dn0, dn1, dn2, dn3,
                small, smallf,
                xs, dys, wu, wd, wqkv, wt, wo, bias_t, parts, far_in, near_in, dwu, dwd, load, send, recv):
    step = pl.program_id(0)
    i = lax.axis_index("dp")
    j = lax.axis_index("head")
    own, d = x_hbm.shape
    f = wu.shape[1]
    w = wo.shape[0]
    half = own // 2
    core = {"head": j ^ 1}
    across = {"head": j ^ 2}

    def remote(src, dst, k, to):
        return pltpu.make_async_remote_copy(
            src_ref=src, dst_ref=dst, send_sem=send.at[k], recv_sem=recv.at[k], device_id=to,
            device_id_type=pl.DeviceIdType.MESH)

    lo, hi = pl.ds(0, half), pl.ds(half, half)
    copies = [
        remote(x_hbm, xs.at[1], 0, core),
        remote(dy_hbm, dys.at[1], 1, core),
        remote(x_hbm.at[lo], xs.at[2, lo], 2, across),
        remote(dy_hbm.at[lo], dys.at[2, lo], 3, across),
        remote(x_hbm.at[hi], xs.at[3, lo], 4, across),
        remote(dy_hbm.at[hi], dys.at[3, lo], 5, across),
        remote(xs.at[2, lo], xs.at[2, hi], 6, core),
        remote(dys.at[2, lo], dys.at[2, hi], 7, core),
        remote(xs.at[3, lo], xs.at[3, hi], 8, core),
        remote(dys.at[3, lo], dys.at[3, hi], 9, core),
        remote(parts.at[1], near_in, 10, core),
        remote(parts.at[2, hi], far_in.at[lo], 11, core),
        remote(parts.at[3, hi], far_in.at[hi], 12, core),
    ]
    locals_ = [
        pltpu.make_async_copy(x_hbm, xs.at[0], load.at[0]),
        pltpu.make_async_copy(dy_hbm, dys.at[0], load.at[1]),
        pltpu.make_async_copy(wu_hbm.at[:, pl.ds(j * f, f)], wu, load.at[2]),
        pltpu.make_async_copy(wd_hbm.at[pl.ds(j * f, f)], wd, load.at[3]),
        pltpu.make_async_copy(wo_hbm.at[pl.ds(j * w, w)], wo, load.at[4]),
    ] + [
        pltpu.make_async_copy(wqkv_hbm.at[:, pl.ds(k * d + j * w, w)], wqkv.at[:, pl.ds(k * w, w)], load.at[5 + k])
        for k in range(3)
    ]

    @pl.when(step == 0)
    def _():
        barrier = pltpu.get_barrier_semaphore()
        for to in (core, across):
            pl.semaphore_signal(barrier, inc=1, device_id=to, device_id_type=pl.DeviceIdType.MESH)
        for c in locals_:
            c.start()
        pl.semaphore_wait(barrier, 2)
        for c in copies[:6]:
            c.start()
        dwu[...] = jnp.zeros_like(dwu)
        dwd[...] = jnp.zeros_like(dwd)
        small[...] = jnp.zeros_like(small)
        smallf[...] = jnp.zeros_like(smallf)
        for c in locals_:
            c.wait()
        for k in range(3):
            wt[k * w : (k + 1) * w, :] = wqkv[:, k * w : (k + 1) * w].T
            row = flat(bq[pl.ds(pl.multiple_of(k * d + j * w, 256), w)])
            bias_t[k * w : (k + 1) * w, :] = jnp.broadcast_to(row, (128, w)).T

    @pl.when(step == 1)
    def _():
        copies[0].wait_recv()
        copies[1].wait_recv()

    @pl.when(step == 2)
    def _():
        copies[6].wait_recv()
        copies[7].wait_recv()

    @pl.when(step == 3)
    def _():
        copies[8].wait_recv()
        copies[9].wait_recv()

    normed, _unused = norm_parts(xs[step])
    scale = flat(gain_m[...])
    nm = (normed * scale + flat(shift_m[...])).astype(BF)
    na = (normed * flat(gain_a[...]) + flat(shift_a[...])).astype(BF)
    dy = dys[step]
    na_out[...] = na
    dy_out[...] = dy
    pre = mm(nm, wu[...]) + flat(bu[pl.ds(pl.multiple_of(j * f, 1024), f)])
    cdf = 0.5 + 0.5 * lax.erf(pre * (0.5**0.5))
    hid = (pre * cdf).astype(BF)
    slope = cdf + pre * (jnp.exp(-0.5 * pre * pre) * 0.3989422804014327)
    gp = (mm(dy, wd[...], NT) * slope).astype(BF)
    parts[step] = mm(hid, wd[...]).astype(BF)
    r = mm(gp, wu[...], NT)
    g_out[...] = (r * scale).astype(BF)
    smallf[0:1, :] += jnp.sum(gp.astype(F32), axis=0, keepdims=True)
    small[0:1, :] += jnp.sum(r * normed, axis=0, keepdims=True)
    small[1:2, :] += jnp.sum(r, axis=0, keepdims=True)
    small[2:3, :] += jnp.sum(dy.astype(F32), axis=0, keepdims=True)
    dwd[...] += mm(hid, dy, TN)
    dwu[...] += mm(nm, gp, TN)

    @pl.when(step == 1)
    def _():
        for k in (2, 3):
            copies[k].wait_recv()
            copies[k + 4].start()
        copies[10].start()

    @pl.when(step == 2)
    def _():
        for k in (4, 5):
            copies[k].wait_recv()
            copies[k + 4].start()
        copies[11].start()

    @pl.when(step == 3)
    def _():
        copies[12].start()
        rows = up_keep.shape[1]
        for b in range(4):
            for ref, at in ((up_keep, 2 * b + i % 2), (up_send, 2 * b + 1 - i % 2)):
                ref[b] = dwu[pl.ds(pl.multiple_of(at * rows, rows), rows), :].astype(BF)
            ref = (dn0, dn1, dn2, dn3)[b]
            for x in range(2):
                at = 2 * ((i // 2) ^ b) + x
                ref[x] = dwd[pl.ds(pl.multiple_of(at * rows, rows), rows), :].astype(BF)

    lane = lax.broadcasted_iota(jnp.int32, (1, own), 1)
    far = jnp.where(lane < half, j ^ 2, j ^ 3) * own + (step - 2) * half + lane % half
    index = jnp.where(step == 0, j * own + lane, jnp.where(step == 1, (j ^ 1) * own + lane, far))
    begin = jnp.zeros_like(index)
    total = jnp.int32(0)
    for s in range(lens.shape[0] - 1):
        total = total + lens[s]
        begin = jnp.where(index >= total, total, begin)
    sub = lax.broadcasted_iota(jnp.int32, (HALF, own), 0)
    freqs = jnp.zeros((HALF, own), F32)
    for k in range(HALF):
        freqs = jnp.where(sub == k, float(FREQS[k]), freqs)
    angle = freqs * (index - begin).astype(F32)
    co = jnp.cos(angle)
    si = jnp.sin(angle)
    cos[...] = co
    sin[...] = si

    def projected(k):
        b = bias_t[k * w : (k + 1) * w, :]
        t = mm(wt[k * w : (k + 1) * w, :], na, NT)
        return (t + jnp.concatenate([b] * (own // 128), axis=1)).astype(BF)

    def rotated(t, factor):
        rows = []
        for h in range(nh):
            u = t[h * HD : (h + 1) * HD].astype(F32)
            u1 = u[:HALF]
            u2 = u[HALF:ROT]
            rows += [u1 * co - u2 * si, u2 * co + u1 * si, u[ROT:]]
        out = jnp.concatenate(rows, axis=0)
        return (out if factor is None else out * factor).astype(BF)

    qt[...] = rotated(projected(0), HD**-0.5)
    keys = rotated(projected(1), None)
    kt[...] = keys
    kn[...] = keys.T
    values = projected(2)
    vt[...] = values
    vn[...] = values.T
    dot[...] = mm(wo[...], dy, NT).astype(BF)

    @pl.when(step == 3)
    def _():
        copies[10].wait_recv()
        p_own[...] = (parts[0].astype(F32) + near_in[...].astype(F32)).astype(BF)
        copies[11].wait_recv()
        p_far[lo] = (parts[2, lo].astype(F32) + far_in[lo].astype(F32)).astype(BF)
        copies[12].wait_recv()
        p_far[hi] = (parts[3, lo].astype(F32) + far_in[hi].astype(F32)).astype(BF)
        for c in copies:
            c.wait_send()


def head_stage(x, dy, w_up, w_down, w_qkv, w_out, ga, sa, gm, sm, bu, bq, lens, n, cid):
    own, d = x.shape
    tok = own * n
    w = d // n
    f = w_up.shape[1] // n
    row = lambda i: (i, 0)
    lane = lambda rows: pl.BlockSpec((rows, own), lambda i: (0, i))
    nat = lambda cols: pl.BlockSpec((own, cols), row)
    one = pl.Buffered(1)
    const = lambda shape: pl.BlockSpec(shape, lambda i: (0,) * len(shape), pipeline_mode=one)
    hbm = pl.BlockSpec(memory_space=pl.ANY)
    sds = jax.ShapeDtypeStruct
    return pl.pallas_call(
        functools.partial(head_kernel, w // HD),
        grid=(n,),
        in_specs=[hbm] * 6
        + [const(v.shape) for v in (ga, sa, gm, sm, bu, bq)]
        + [pl.BlockSpec(memory_space=pltpu.SMEM)],
        out_specs=[nat(d)] * 3
        + [lane(w)] * 4
        + [nat(w)] * 2
        + [lane(HALF)] * 2
        + [const((own, d))] * 2
        + [const((4, d // 8, f))] * 2
        + [const((2, f // 8, d))] * 4
        + [const((8, d)), const((8, f))],
        out_shape=tuple(
            [sds((tok, d), BF)] * 3
            + [sds((w, tok), BF)] * 4
            + [sds((tok, w), BF)] * 2
            + [sds((HALF, tok), F32)] * 2
            + [sds((own, d), BF)] * 2
            + [sds((4, d // 8, f), BF)] * 2
            + [sds((2, f // 8, d), BF)] * 4
            + [sds((8, d), F32), sds((8, f), F32)]
        ),
        scratch_shapes=[
            pltpu.VMEM((4, own, d), BF),
            pltpu.VMEM((4, own, d), BF),
            pltpu.VMEM((d, f), BF),
            pltpu.VMEM((f, d), BF),
            pltpu.VMEM((d, 3 * w), BF),
            pltpu.VMEM((3 * w, d), BF),
            pltpu.VMEM((w, d), BF),
            pltpu.VMEM((3 * w, 128), F32),
            pltpu.VMEM((4, own, d), BF),
            pltpu.VMEM((own, d), BF),
            pltpu.VMEM((own, d), BF),
            pltpu.VMEM((d, f), F32),
            pltpu.VMEM((f, d), F32),
            pltpu.SemaphoreType.DMA((8,)),
            pltpu.SemaphoreType.DMA((13,)),
            pltpu.SemaphoreType.DMA((13,)),
        ],
        compiler_params=pltpu.CompilerParams(
            vmem_limit_bytes=VMEM_LIMIT, collective_id=cid, has_side_effects=True
        ),
        cost_estimate=pl.CostEstimate(
            flops=12 * tok * d * f + 10 * tok * d * w, bytes_accessed=12 * tok * d + 8 * d * f, transcendentals=2 * tok * f
        ),
        name="head_stage",
    )(x, dy, w_up, w_down, w_qkv, w_out, ga, sa, gm, sm, bu, bq, lens)


def attn_kernel(nh, tok, blk, per, halved, lens, rel, cos, sin, qt, kt, vt, dot, kn, vn,
                gt_ref, ctx_ref, exps, low_exps, dk, dv, oacc, dqacc, mpart, lpart, rowsc, qpad, dopad):
    nseq = lens.shape[0]
    nblk = tok // blk
    shift = rel[0]
    heads = range(nh)

    def place(b):
        chunk = (b // per) ^ shift
        half = b % per
        at = chunk * per + half
        if halved:
            at = jnp.where(chunk < 2, at, 4 + (chunk - 2) + 2 * half)
        return pl.multiple_of(at * blk, blk)

    def rows_of(h):
        return slice(h * HD, (h + 1) * HD)

    def pair_of(h):
        return slice((h // 2) * 128, (h // 2) * 128 + 128)

    def fold(v, op):
        return op(v.reshape(blk // 8, 8, blk), axis=0)

    def begin_of(at):
        begin = jnp.int32(0)
        total = jnp.int32(0)
        for s in range(nseq - 1):
            total = total + lens[s]
            begin = jnp.where(at >= total, total, begin)
        return begin

    dk[...] = jnp.zeros_like(dk)
    dv[...] = jnp.zeros_like(dv)
    qpad[...] = jnp.zeros_like(qpad)
    dopad[...] = jnp.zeros_like(dopad)
    rows_iota = lax.broadcasted_iota(jnp.int32, (blk, blk), 0)
    cols_iota = lax.broadcasted_iota(jnp.int32, (1, blk), 1)

    def one_block(i, carry):
        first_tok = i * blk
        count = i - begin_of(first_tok) // blk + 1
        last_begin = begin_of(first_tok + blk - 1)
        cols = pl.ds(place(i), blk)
        query_idx = cols_iota + first_tok
        start_row = begin_of(query_idx)
        for h in heads:
            half = (h % 2) * HD
            qpad[h, half : half + HD, :] = qt[rows_of(h), cols]

        krow = pl.ds(place(i), blk)
        kidx = rows_iota + first_tok
        allowed = (kidx >= start_row) & (kidx <= query_idx)
        for h in heads:
            s = jnp.where(allowed, mm(kn[krow, pair_of(h)], qpad[h]), -1e30)
            exps[h, 0] = s
            mpart[h] = fold(s, jnp.max)

        def scores(step, c):
            b = i - step
            krow = pl.ds(place(b), blk)
            edge = last_begin > b * blk

            @pl.when(edge)
            def _():
                allowed = (rows_iota + b * blk) >= start_row
                for h in heads:
                    s = jnp.where(allowed, mm(kn[krow, pair_of(h)], qpad[h]), -1e30)
                    exps[h, step] = s
                    mpart[h] = jnp.maximum(mpart[h], fold(s, jnp.max))

            @pl.when(jnp.logical_not(edge))
            def _():
                for h in heads:
                    s = mm(kn[krow, pair_of(h)], qpad[h])
                    exps[h, step] = s
                    mpart[h] = jnp.maximum(mpart[h], fold(s, jnp.max))

            return c

        lax.fori_loop(1, count, scores, 0)
        for h in heads:
            rowsc[h : h + 1, :] = jnp.max(mpart[h], axis=0, keepdims=True)
        lpart[...] = jnp.zeros_like(lpart)
        oacc[...] = jnp.zeros_like(oacc)

        def weights(step, c):
            kcols = pl.ds(place(i - step), blk)
            for h in heads:
                e = jnp.exp(exps[h, step] - rowsc[h : h + 1, :])
                exps[h, step] = e
                lpart[h] += fold(e, jnp.sum)
                low = e.astype(BF)
                low_exps[h, step] = low
                oacc[h] += mm(vt[rows_of(h), kcols], low)
            return c

        lax.fori_loop(0, count, weights, 0)
        for h in heads:
            half = (h % 2) * HD
            inv = 1.0 / jnp.sum(lpart[h], axis=0, keepdims=True)
            o = oacc[h] * inv
            ctx_ref[rows_of(h), cols] = o.astype(BF)
            scaled = (dot[rows_of(h), cols].astype(F32) * inv).astype(BF)
            dopad[h, half : half + HD, :] = scaled
            rowsc[h : h + 1, :] = jnp.sum(o * scaled.astype(F32), axis=0, keepdims=True)
        dqacc[...] = jnp.zeros_like(dqacc)

        def backward(step, c):
            kcols = pl.ds(place(i - step), blk)
            for h in heads:
                half = (h % 2) * HD
                hs = rows_of(h)
                dp = mm(vn[kcols, pair_of(h)], dopad[h])
                ds = (exps[h, step] * (dp - rowsc[h : h + 1, :])).astype(BF)
                dv[hs, kcols] += mm(dopad[h, half : half + HD, :], low_exps[h, step], NT)
                dk[hs, kcols] += mm(qt[hs, cols], ds, NT)
                dqacc[hs, :] += mm(kt[hs, kcols], ds)
            return c

        lax.fori_loop(0, count, backward, 0)
        co = cos[:, cols]
        si = sin[:, cols]
        for h in heads:
            base = h * HD
            g = dqacc[base : base + HD, :] * (HD**-0.5)
            g1 = g[:HALF]
            g2 = g[HALF:ROT]
            gt_ref[base : base + HD, cols] = jnp.concatenate(
                [g1 * co + g2 * si, g2 * co - g1 * si, g[ROT:]], axis=0
            ).astype(BF)
        return carry

    lax.fori_loop(0, nblk, one_block, 0)

    def finish(i, carry):
        cols = pl.ds(pl.multiple_of(i * blk, blk), blk)
        co = cos[:, cols]
        si = sin[:, cols]
        for h in heads:
            base = h * HD
            g = dk[base : base + HD, cols]
            g1 = g[:HALF]
            g2 = g[HALF:ROT]
            gt_ref[nh * HD + base : nh * HD + base + HD, cols] = jnp.concatenate(
                [g1 * co + g2 * si, g2 * co - g1 * si, g[ROT:]], axis=0
            ).astype(BF)
        gt_ref[2 * nh * HD :, cols] = dv[:, cols].astype(BF)
        return carry

    lax.fori_loop(0, nblk, finish, 0)


def attention(lens, rel, cos, sin, qt, kt, vt, dot, kn, vn, chunk, maxlen, halved=False, blk=256):
    width, tok = qt.shape
    nh = width // HD
    wb = maxlen // blk + 1
    vm = pl.BlockSpec(memory_space=pltpu.VMEM)
    sm = pl.BlockSpec(memory_space=pltpu.SMEM)
    return pl.pallas_call(
        functools.partial(attn_kernel, nh, tok, blk, chunk // blk, halved),
        out_shape=(jax.ShapeDtypeStruct((3 * width, tok), BF), jax.ShapeDtypeStruct((width, tok), BF)),
        in_specs=[sm, sm] + [vm] * 8,
        out_specs=(vm, vm),
        scratch_shapes=[
            pltpu.VMEM((nh, wb, blk, blk), F32),
            pltpu.VMEM((nh, wb, blk, blk), BF),
            pltpu.VMEM((width, tok), F32),
            pltpu.VMEM((width, tok), F32),
            pltpu.VMEM((nh, HD, blk), F32),
            pltpu.VMEM((width, blk), F32),
            pltpu.VMEM((nh, 8, blk), F32),
            pltpu.VMEM((nh, 8, blk), F32),
            pltpu.VMEM((8, blk), F32),
            pltpu.VMEM((nh, 128, blk), BF),
            pltpu.VMEM((nh, 128, blk), BF),
        ],
        compiler_params=pltpu.CompilerParams(vmem_limit_bytes=VMEM_LIMIT),
        cost_estimate=pl.CostEstimate(
            flops=20 * width * tok * maxlen, bytes_accessed=20 * width * tok, transcendentals=nh * tok * maxlen
        ),
        name="attention",
    )(lens, rel, cos, sin, qt, kt, vt, dot, kn, vn)


def post_kernel(pos, gt_ref, na_ref, gm_ref, wq, wk, wv, gain, shift, g_ref, out_w, bias, small, dw):
    step = pl.program_id(0)

    @pl.when(step == 0)
    def _():
        dw[...] = jnp.zeros_like(dw)
        bias[...] = jnp.zeros_like(bias)
        small[...] = jnp.zeros_like(small)

    gt = gt_ref[...]
    na = na_ref[...]
    w = wq.shape[1]
    scale = gain[...].astype(F32)
    gn = gt.T
    r = mm(gn[:, :w], wq[...], NT) + mm(gn[:, w : 2 * w], wk[...], NT) + mm(gn[:, 2 * w :], wv[...], NT)
    g_ref[...] = (r * scale + gm_ref[...].astype(F32)).astype(BF)
    small[0:1, :] += jnp.sum(r * na.astype(F32), axis=0, keepdims=True)
    small[1:2, :] += jnp.sum(r, axis=0, keepdims=True)
    bias[0:1, :] += jnp.sum(gn.astype(F32), axis=0, keepdims=True)
    dw[...] += mm(gt, na)

    @pl.when(step == pl.num_programs(0) - 1)
    def _():
        for b in range(dw.shape[1] // 128):
            out_w[b] = dw[:, b * 128 : (b + 1) * 128].astype(BF)
        small[0:1, :] = (small[0:1, :] - shift[...].astype(F32) * small[1:2, :]) / scale


def post(pos, gt, na, gm, w_qkv, gain, shift, n, tt=512):
    tok, d = na.shape
    w = d // n
    row = lambda i, p: (i, 0)
    zero = lambda i, p: (0, 0)
    one = pl.Buffered(1)
    const = lambda shape: pl.BlockSpec(shape, zero, pipeline_mode=one)
    wspec = lambda k: pl.BlockSpec((d, w), lambda i, p: (0, k * n + p[0]), pipeline_mode=one)
    grid_spec = pltpu.PrefetchScalarGridSpec(
        num_scalar_prefetch=1,
        grid=(tok // tt,),
        in_specs=[
            pl.BlockSpec((3 * w, tt), lambda i, p: (0, i)),
            pl.BlockSpec((tt, d), row),
            pl.BlockSpec((tt, d), row),
            wspec(0),
            wspec(1),
            wspec(2),
            const((1, d)),
            const((1, d)),
        ],
        out_specs=[
            pl.BlockSpec((tt, d), row),
            pl.BlockSpec((d // 128, 3 * w, 128), lambda i, p: (0, 0, 0), pipeline_mode=one),
            const((8, 3 * w)),
            const((8, d)),
        ],
        scratch_shapes=[pltpu.VMEM((3 * w, d), F32)],
    )
    return pl.pallas_call(
        post_kernel,
        grid_spec=grid_spec,
        out_shape=(
            jax.ShapeDtypeStruct((tok, d), BF),
            jax.ShapeDtypeStruct((d // 128, 3 * w, 128), BF),
            jax.ShapeDtypeStruct((8, 3 * w), F32),
            jax.ShapeDtypeStruct((8, d), F32),
        ),
        compiler_params=pltpu.CompilerParams(vmem_limit_bytes=VMEM_LIMIT),
        cost_estimate=pl.CostEstimate(
            flops=12 * tok * d * w, bytes_accessed=8 * tok * d + 6 * tok * w + 18 * d * w, transcendentals=0
        ),
        name="post",
    )(pos, gt, na, gm, w_qkv, w_qkv, w_qkv, gain, shift)


def tail_kernel(gt_h, na_h, gm_h, ctx_h, dya_h, wqkv_h, wo_h, upk_h, upo_h, dn0_h, dn1_h, dn2_h, dn3_h, x_h, pown_h, py_h,
                gain, shift_ref, bo, bd, small, smallf,
                out_ref, g_ref, wup_ref, wdn_ref, wq_ref, wout_ref, sums_ref,
                gt, na, gm, ctx, dya, wqkv, wo, upk, upo, dn, xo, pown, py,
                ctx_in, up4, up_in, dn_in, dn2,
                dwq, qa_in, qb_in, qa4, qb4, qa_in2, qb_in2, qa2, qb2, qa_in3, qb_in3, qfin, q_own,
                dwo, wo_in, wo4, wo_in2, wo2, wo_in3, piece, owner_in,
                far_in, near_in, far_sum, y_in, sm, sm_in, load, send, recv):
    i = lax.axis_index("dp")
    j = lax.axis_index("head")
    own, d = x_h.shape
    w = wqkv.shape[1] // 3
    half = own // 2
    bx = i % 2
    b0 = (i // 2) % 2
    b1 = i // 4
    mesh_id = pl.DeviceIdType.MESH
    core, across, diag = {"head": j ^ 1}, {"head": j ^ 2}, {"head": j ^ 3}
    px, p0, p1 = {"dp": i ^ 1}, {"dp": i ^ 2}, {"dp": i ^ 4}
    lo, hi = pl.ds(0, half), pl.ds(half, half)
    count = [0]

    def remote(src, dst, to):
        k = count[0]
        count[0] += 1
        return pltpu.make_async_remote_copy(
            src_ref=src, dst_ref=dst, send_sem=send.at[k], recv_sem=recv.at[k], device_id=to, device_id_type=mesh_id)

    def local(src, dst, k):
        return pltpu.make_async_copy(src, dst, load.at[k])

    loads = [
        local(upk_h, upk, 0), local(upo_h, upo, 1), local(dn0_h, dn.at[0], 2), local(dn1_h, dn.at[1], 3),
        local(gt_h, gt, 4), local(na_h, na, 5), local(ctx_h, ctx, 6), local(dya_h, dya, 7), local(gm_h, gm, 8),
        local(wqkv_h.at[:, pl.ds(j * w, w)], wqkv.at[:, pl.ds(0, w)], 9),
        local(wqkv_h.at[:, pl.ds(d + j * w, w)], wqkv.at[:, pl.ds(w, w)], 10),
        local(wqkv_h.at[:, pl.ds(2 * d + j * w, w)], wqkv.at[:, pl.ds(2 * w, w)], 11),
        local(wo_h, wo, 12), local(x_h, xo, 13), local(pown_h, pown, 14), local(py_h, py, 15),
        local(dn2_h, dn.at[2], 16), local(dn3_h, dn.at[3], 17),
    ]
    c_ctx = [
        remote(ctx_h.at[:, pl.ds(2 * own, half)], ctx_in.at[1, :, lo], across),
        remote(ctx_h.at[:, pl.ds(3 * own, half)], ctx_in.at[1, :, hi], across),
        remote(ctx_h.at[:, pl.ds(2 * own + half, half)], ctx_in.at[2, :, lo], diag),
        remote(ctx_h.at[:, pl.ds(3 * own + half, half)], ctx_in.at[2, :, hi], diag),
        remote(ctx_h.at[:, pl.ds(own, own)], ctx_in.at[0], core),
    ]
    z = i // 2
    c_up = [remote(up4.at[z ^ k], up_in.at[k - 1], {"dp": i ^ (2 * k)}) for k in (1, 2, 3)]
    c_dnx = remote(dn2.at[1 - bx], dn_in, px)
    rows = dwq.shape[3] // 2
    ra, rb = pl.ds(0, rows), pl.ds(rows, rows)
    c_qa = remote(dwq.at[:, :, 1 - bx, ra], qa_in, px)
    c_qb = remote(dwq.at[:, :, 1 - bx, rb], qb_in, px)
    c_qa0 = remote(qa4.at[:, 1 - b0], qa_in2, p0)
    c_qb0 = remote(qb4.at[:, 1 - b0], qb_in2, p0)
    c_qa1 = remote(qa2.at[1 - b1], qa_in3, p1)
    c_qb1 = remote(qb2.at[1 - b1], qb_in3, p1)
    c_wox = remote(dwo.at[:, :, 1 - bx], wo_in, px)
    c_wo0 = remote(wo4.at[:, 1 - b0], wo_in2, p0)
    c_wo1 = remote(wo2.at[1 - b1], wo_in3, p1)
    c_g = [
        remote(gm.at[pl.ds(2 * own + half, half)], far_in.at[lo], core),
        remote(gm.at[pl.ds(3 * own + half, half)], far_in.at[hi], core),
        remote(gm.at[pl.ds(own, own)], near_in, core),
    ]
    c_y = [remote(far_sum.at[lo], y_in.at[lo], across), remote(far_sum.at[hi], y_in.at[hi], across)]
    c_sm = [remote(sm.at[s], sm_in.at[s], to) for s, to in enumerate((core, across, px, p0, p1))]
    dests = []
    c_own = []
    for r in range(4):
        di, dj = 2 * j + i // 4, (i % 4) ^ r
        dests.append((di, dj))
        c_own.append(remote(piece.at[:, pl.ds(pl.multiple_of(dj * w, 128), w)], owner_in.at[i % 4], {"dp": di, "head": dj}))
    c_q = []
    q_dst = []
    for t in range(3):
        dst = (t - j + 4) % 4
        q_dst.append(dst)
        c_q.append(remote(qfin.at[(3 * dst + t) // 4], q_own.at[t], {"head": dst}))

    barrier = pltpu.get_barrier_semaphore()
    for to in (core, across, diag, px, p0, p1, {"dp": i ^ 6}):
        pl.semaphore_signal(barrier, inc=1, device_id=to, device_id_type=mesh_id)
    for c in loads:
        c.start()
    for r in range(4):
        si, sj = 4 * (i % 2) + (j ^ r), i // 2

        @pl.when((si != i) | (sj != j))
        def _():
            pl.semaphore_signal(barrier, inc=1, device_id={"dp": si, "head": sj}, device_id_type=mesh_id)

    to_self = jnp.where(2 * j + i // 4 == i, 1, 0)
    pl.semaphore_wait(barrier, 11 - to_self)

    for c in c_ctx:
        c.start()

    def added(a, b):
        return a.astype(F32) + b.astype(F32)

    for k in range(4):
        loads[k].wait()
    up4[...] = added(upk[...], upo[...]).astype(BF)
    for c in c_up:
        c.start()
    loads[16].wait()
    loads[17].wait()
    dn2[...] = (added(dn[0], dn[1]) + added(dn[2], dn[3])).astype(BF)
    c_dnx.start()

    loads[4].wait()
    loads[5].wait()
    for part, c in ((ra, c_qa), (rb, c_qb)):
        left = gt[part, :]
        for k in range(4):
            t = mm(left, na[:, 256 * k : 256 * (k + 1)]).astype(BF)
            dwq[k // 2, k % 2, 0, part] = t[:, :128]
            dwq[k // 2, k % 2, 1, part] = t[:, 128:]
        c.start()
    loads[6].wait()
    loads[7].wait()
    t = mm(ctx[...], dya[...]).astype(BF)
    for b in range(8):
        dwo[b // 4, (b // 2) % 2, b % 2] = t[32 * b : 32 * (b + 1)]
    c_wox.start()

    for k in range(8, 12):
        loads[k].wait()
    scale = flat(gain[...])
    ones = jnp.zeros((1, d), F32)
    s_gain, s_shift, s_bias = ones, ones, jnp.zeros((1, 3 * w), F32)

    def tile(at, size, sums):
        ts = slice(at, at + size)
        gn = gt[:, ts].T
        r = mm(gn, wqkv[...], NT)
        gm[ts, :] = (r * scale + gm[ts, :].astype(F32)).astype(BF)
        return (
            sums[0] + jnp.sum(r * na[ts, :].astype(F32), axis=0, keepdims=True),
            sums[1] + jnp.sum(r, axis=0, keepdims=True),
            sums[2] + jnp.sum(gn.astype(F32), axis=0, keepdims=True),
        )

    sums = (s_gain, s_shift, s_bias)
    sums = tile(2 * own, own, sums)
    c_g[0].start()
    sums = tile(3 * own, own, sums)
    c_g[1].start()
    c_g[0].wait_recv()
    far_sum[lo] = added(gm[2 * own : 2 * own + half], far_in[lo]).astype(BF)
    c_y[0].start()
    sums = tile(own, own, sums)
    c_g[2].start()
    c_g[1].wait_recv()
    far_sum[hi] = added(gm[3 * own : 3 * own + half], far_in[hi]).astype(BF)
    c_y[1].start()
    sums = tile(0, own, sums)

    sm[0] = jnp.zeros((16, d), F32)
    shift = flat(shift_ref[...])
    sm[0, 0:1, :] = (sums[0] - shift * sums[1]) / scale
    sm[0, 1:2, :] = sums[1]
    for k in range(3):
        sm[0, 2 + k : 3 + k, pl.ds(pl.multiple_of(j * w, 128), w)] = sums[2][:, k * w : (k + 1) * w]
    sm[0, 5:7, :] = small[0:2, :]
    sm[0, 7:8, :] = small[2:3, :] * 0.25
    sm[0, pl.ds(8 + j, 1), :] = smallf[0:1, :]
    c_sm[0].start()

    def small_step(s):
        c_sm[s].wait_recv()
        sm[s + 1] = sm[s] + sm_in[s]
        if s < 4:
            c_sm[s + 1].start()

    for k in range(12, 16):
        loads[k].wait()
    attn = mm(ctx[:, :own], wo[pl.ds(pl.multiple_of(j * w, 128), w), :], TN)
    c_ctx[4].wait_recv()
    attn += mm(ctx_in[0], wo[pl.ds(pl.multiple_of((j ^ 1) * w, 128), w), :], TN)
    for k in range(4):
        c_ctx[k].wait_recv()
    attn += mm(ctx_in[1], wo[pl.ds(pl.multiple_of((j ^ 2) * w, 128), w), :], TN)
    attn += mm(ctx_in[2], wo[pl.ds(pl.multiple_of((j ^ 3) * w, 128), w), :], TN)
    out_ref[...] = (
        xo[...].astype(F32) + attn + added(pown[...], py[...]) + (flat(bo[...]) + flat(bd[...]))
    ).astype(BF)
    small_step(0)

    c_qa.wait_recv()
    qa4[...] = added(dwq[:, :, bx, ra], qa_in[...]).astype(BF)
    c_qa0.start()
    small_step(1)
    c_qa0.wait_recv()
    qa2[...] = added(qa4[:, b0], qa_in2[...]).astype(BF)
    c_qa1.start()
    c_qb.wait_recv()
    qb4[...] = added(dwq[:, :, bx, rb], qb_in[...]).astype(BF)
    c_qb0.start()
    small_step(2)
    for c in c_up:
        c.wait_recv()
    wup_ref[...] = (up4[z].astype(F32) + up_in[0].astype(F32) + added(up_in[1], up_in[2])).astype(BF)
    c_dnx.wait_recv()
    nd = dn2.shape[1]
    piece[:nd, :] = added(dn2[bx], dn_in[...]).astype(BF)
    c_wox.wait_recv()
    wo4[...] = added(dwo[:, :, bx], wo_in[...]).astype(BF)
    c_wo0.start()
    c_qb0.wait_recv()
    qb2[...] = added(qb4[:, b0], qb_in2[...]).astype(BF)
    c_qb1.start()
    small_step(3)
    c_wo0.wait_recv()
    wo2[...] = added(wo4[:, b0], wo_in2[...]).astype(BF)
    c_wo1.start()
    c_qa1.wait_recv()
    c_qb1.wait_recv()
    done = jnp.concatenate([added(qa2[b1], qa_in3[...]), added(qb2[b1], qb_in3[...])], axis=0).astype(BF)
    for k in range(3):
        qfin[k] = done[k * w : (k + 1) * w]
    for t in range(3):

        @pl.when(q_dst[t] != j)
        def _():
            c_q[t].start()

        @pl.when(q_dst[t] == j)
        def _():
            q_own[t] = qfin[(3 * j + t) // 4]

    c_wo1.wait_recv()
    piece[nd:, :] = added(wo2[b1], wo_in3[...]).astype(BF)
    for r in range(4):
        di, dj = dests[r]

        @pl.when((di != i) | (dj != j))
        def _():
            c_own[r].start()

        @pl.when((di == i) & (dj == j))
        def _():
            owner_in[i % 4] = piece[:, pl.ds(pl.multiple_of(dj * w, 128), w)]

    small_step(4)
    sums_ref[...] = sm[5]

    c_g[2].wait_recv()
    near = added(gm[0:own], near_in[...])
    c_y[0].wait_recv()
    c_y[1].wait_recv()
    g_ref[...] = near + y_in[...].astype(F32)

    for t in range(3):

        @pl.when(q_dst[t] != j)
        def _():
            c_q[t].wait_recv()

        wq_ref[:, t * w : (t + 1) * w] = q_own[t].astype(F32).T.astype(BF)
    for r in range(4):
        di, dj = dests[r]

        @pl.when((di != i) | (dj != j))
        def _():
            c_own[r].wait_recv()

    no = wo2.shape[1]
    for a in range(4):
        wdn_ref[a * nd : (a + 1) * nd, :] = owner_in[a, :nd]
        wout_ref[a * no : (a + 1) * no, :] = owner_in[a, nd:]

    for c in c_ctx + c_up + [c_dnx, c_qa, c_qb, c_qa0, c_qb0, c_qa1, c_qb1, c_wox, c_wo0, c_wo1] + c_g + c_y + c_sm:
        c.wait_send()
    for t in range(3):

        @pl.when(q_dst[t] != j)
        def _():
            c_q[t].wait_send()

    for r in range(4):
        di, dj = dests[r]

        @pl.when((di != i) | (dj != j))
        def _():
            c_own[r].wait_send()


def tail_stage(gt, na, gm, ctx, dya, w_qkv, w_out, upk, upo, dn, x, pown, py, ga, sa, bo, bd, small, smallf, cid):
    own, d = x.shape
    tok = na.shape[0]
    w = d // 4
    vm = pl.BlockSpec(memory_space=pltpu.VMEM)
    hbm = pl.BlockSpec(memory_space=pl.ANY)
    sds = jax.ShapeDtypeStruct
    big = lambda *s: pltpu.VMEM(s, BF)
    nb = d // 8
    no = w // 8
    r2 = 3 * w // 2
    return pl.pallas_call(
        tail_kernel,
        in_specs=[hbm] * 16 + [vm] * 6,
        out_specs=[vm] * 7,
        out_shape=(
            sds((own, d), BF), sds((own, d), F32), sds((nb, d), BF), sds((4 * nb, w), BF),
            sds((nb, 3 * w), BF), sds((4 * no, w), BF), sds((16, d), F32),
        ),
        scratch_shapes=[
            big(3 * w, tok), big(tok, d), big(tok, d), big(w, tok), big(tok, d), big(d, 3 * w), big(d, d),
            big(4, nb, d), big(4, nb, d), big(4, 2, nb, d),
            big(own, d), big(own, d), big(own, d),
            big(3, w, own), big(4, nb, d), big(3, nb, d), big(nb, d), big(2, nb, d),
            big(2, 2, 2, 3 * w, 128), big(2, 2, r2, 128), big(2, 2, r2, 128), big(2, 2, r2, 128), big(2, 2, r2, 128),
            big(2, r2, 128), big(2, r2, 128), big(2, r2, 128), big(2, r2, 128), big(r2, 128), big(r2, 128),
            big(3, w, 128), big(3, w, 128),
            big(2, 2, 2, no, d), big(2, 2, no, d), big(2, 2, no, d), big(2, no, d), big(2, no, d), big(no, d),
            big(nb + no, d), big(4, nb + no, w),
            big(own, d), big(own, d), big(own, d), big(own, d),
            pltpu.VMEM((6, 16, d), F32), pltpu.VMEM((5, 16, d), F32),
            pltpu.SemaphoreType.DMA((18,)), pltpu.SemaphoreType.DMA((40,)), pltpu.SemaphoreType.DMA((40,)),
        ],
        compiler_params=pltpu.CompilerParams(vmem_limit_bytes=VMEM_LIMIT, collective_id=cid, has_side_effects=True),
        cost_estimate=pl.CostEstimate(
            flops=14 * tok * d * w, bytes_accessed=10 * tok * d, transcendentals=0
        ),
        name="tail_stage",
    )(gt, na, gm, ctx, dya, w_qkv, w_out, upk, upo, *dn, x, pown, py, ga, sa, bo, bd, small, smallf)


def final_kernel(out_t, g_ref, x_ref, dy_ref, wup, wdn, wq, wout, sums,
                 out, gin, ga, sa, gm, sm, dwq, bq, dwout, bo, dwup, bu, dwdn, bd):
    out[...] = out_t[...]
    normed, inv = norm_parts(x_ref[...])
    g = g_ref[...]
    gin[...] = dy_ref[...].astype(F32) + inv * (
        g - jnp.mean(g, axis=-1, keepdims=True) - normed * jnp.mean(g * normed, axis=-1, keepdims=True)
    )

    @pl.when(pl.program_id(0) == 0)
    def _():
        d = sums.shape[1]
        for ref, first, count in ((ga, 0, 1), (sa, 1, 1), (bq, 2, 3), (gm, 5, 1), (sm, 6, 1), (bo, 7, 1), (bd, 7, 1), (bu, 8, 4)):
            for k in range(count):
                ref[k * d : (k + 1) * d] = sums[first + k, :]
        dwup[...] = wup[...].astype(F32)
        dwdn[...] = wdn[...].astype(F32)
        dwq[...] = wq[...].astype(F32)
        dwout[...] = wout[...].astype(F32)


def final_stage(out_t, g, x, dy, wup, wdn, wq, wout, sums, steps=4):
    own, d = x.shape
    row = pl.BlockSpec((own // steps, d), lambda i: (i, 0))
    const = lambda v: pl.BlockSpec(v.shape, lambda i: (0,) * len(v.shape))
    sds = lambda *s: jax.ShapeDtypeStruct(s, F32)
    like = lambda v: sds(*v.shape)
    outs = (
        jax.ShapeDtypeStruct((own, d), BF), sds(own, d), sds(d), sds(d), sds(d), sds(d), like(wq), sds(3 * d),
        like(wout), sds(d), like(wup), sds(4 * d), like(wdn), sds(d),
    )
    return pl.pallas_call(
        final_kernel,
        grid=(steps,),
        in_specs=[row, row, row, row] + [const(v) for v in (wup, wdn, wq, wout, sums)],
        out_specs=[row, row] + [const(v) for v in outs[2:]],
        out_shape=outs,
        compiler_params=pltpu.CompilerParams(vmem_limit_bytes=VMEM_LIMIT),
        name="final_stage",
    )(out_t, g, x, dy, wup, wdn, wq, wout, sums)


def layout(seq_lens, index):
    ends = jnp.cumsum(seq_lens, dtype=jnp.int32)
    starts = ends - seq_lens
    first = jnp.zeros_like(index)
    for s in range(1, seq_lens.shape[0]):
        first = jnp.where(index >= starts[s], starts[s], first)
    return first, index - first


def head_perm(v, bit):
    return lax.ppermute(v, "head", [(k, k ^ bit) for k in range(4)])


def dp_perm(v, bit):
    return lax.ppermute(v, "dp", [(k, k ^ bit) for k in range(8)])


def fast_body(inputs, lengths, attn_gain, attn_shift, mlp_gain, mlp_shift, w_qkv, b_qkv, w_out, b_out,
              w_up, b_up, w_down, b_down, cotangent):
    own, d = inputs.shape
    n = 4
    tok = own * n
    w = d // n
    pos = lax.axis_index("head").astype(jnp.int32).reshape(1)
    lens = lengths[0]
    (g_mlp, na, dy_all, qt, kt, vt, dot, kn, vn, cos, sin, p_own, p_far, up_keep, up_send, *dn, small,
     smallf) = head_stage(
        inputs, cotangent, w_up, w_down, w_qkv, w_out, attn_gain, attn_shift, mlp_gain, mlp_shift, b_up, b_qkv, lens, n, 0
    )
    up_other = dp_perm(up_send, 1)
    dn = [dn[0]] + [dp_perm(dn[k], 2 * k) for k in (1, 2, 3)]
    p_y = head_perm(p_far, 2)
    gt, ctx = attention(lens, pos, cos, sin, qt, kt, vt, dot, kn, vn, own, tok // 2, halved=True)
    out_t, g, wup, wdn, wq, wout, sums = tail_stage(
        gt, na, g_mlp, ctx, dy_all, w_qkv, w_out, up_keep, up_other, dn, inputs, p_own, p_y,
        attn_gain, attn_shift, b_out, b_down, small, smallf, 1
    )
    return tuple(final_stage(out_t, g, inputs, cotangent, wup, wdn, wq, wout, sums))


def general_body(inputs, lengths, attn_gain, attn_shift, mlp_gain, mlp_shift, w_qkv, b_qkv, w_out, b_out,
                 w_up, b_up, w_down, b_down, cotangent):
    own, d = inputs.shape
    n = lax.axis_size("head")
    n_dp = lax.axis_size("dp")
    tok = own * n
    w = d // n
    f = w_up.shape[1] // n
    j = lax.axis_index("head")
    pos = j.astype(jnp.int32).reshape(1)
    rows = lambda v: v.reshape(1, -1)
    ga, sa, gm, sm = rows(attn_gain), rows(attn_shift), rows(mlp_gain), rows(mlp_shift)
    bq, bu = rows(b_qkv), rows(b_up)
    lens = lengths[0]
    gather = lambda v: lax.all_gather(v, "head", axis=0, tiled=True)
    over_dp = lambda v, axis: lax.psum_scatter(v, "dp", scatter_dimension=axis, tiled=True)
    over_head = lambda v: lax.psum_scatter(v, "head", scatter_dimension=0, tiled=True)
    x_all = gather(inputs)
    dy_all = gather(cotangent)
    first, position = layout(lens, jnp.arange(tok, dtype=jnp.int32))
    freqs = 10000.0 ** (-(2.0 * jnp.arange(HALF, dtype=F32)) / ROT)
    angle = freqs[:, None] * position.astype(F32)[None, :]
    cos, sin = jnp.cos(angle), jnp.sin(angle)
    part, g_mlp, dwu, dwd, small, smallf = mlp(pos, x_all, dy_all, w_up, w_down, bu, gm, sm, n)
    qt, kt, vt, dot, kn, vn, na = proj(pos, x_all, dy_all, w_qkv, bq, w_out, ga, sa, cos, sin, n, tok, 0)
    gt, ctx = attention(
        lens, jnp.zeros((1,), jnp.int32), cos, sin, qt, kt, vt, dot, kn, vn, own, tok // 2
    )
    total, dwq, bias_q, small_q = post(pos, gt, na, g_mlp, w_qkv, ga, sa, n)
    attn_part = mm(ctx, lax.dynamic_slice_in_dim(w_out, j * w, w, 0), TN)
    bias = b_out.astype(F32) + b_down.astype(F32)
    output = inputs.astype(F32) + over_head((attn_part + part.astype(F32)).astype(BF)).astype(F32) + bias
    g_sum = over_head(total).astype(F32)
    normed, inv = norm_parts(inputs)
    grad_inputs = cotangent.astype(F32) + inv * (
        g_sum - jnp.mean(g_sum, axis=-1, keepdims=True) - normed * jnp.mean(g_sum * normed, axis=-1, keepdims=True)
    )
    dw_out = mm(ctx, dy_all).astype(BF)
    spread = lambda v: lax.all_to_all(v, "head", split_axis=1, concat_axis=0, tiled=True)
    grad_w_up = over_dp(dwu, 0).astype(F32)
    grad_w_down = over_dp(spread(dwd), 0).astype(F32)
    grad_w_out = over_dp(spread(dw_out), 0).astype(F32)
    qkv = over_dp(jnp.transpose(dwq, (0, 2, 1)).reshape(d, 3 * w), 0)
    qkv = lax.all_gather(qkv.reshape(d // n_dp, 3, w), "head", axis=2, tiled=True).reshape(d // n_dp, 3 * d)
    grad_w_qkv = lax.dynamic_slice_in_dim(qkv, j * 3 * w, 3 * w, 1).astype(F32)
    slots = jnp.where(jnp.arange(n)[:, None] == j, smallf[0:1], 0.0).reshape(-1)
    slots_q = jnp.where(jnp.arange(n)[None, :, None] == j, bias_q[0].reshape(3, 1, w), 0.0).reshape(-1)
    sums = lax.psum((small_q[0], small_q[1], small[0], small[1], slots_q, small[2] / n, slots), ("dp", "head"))
    return (output.astype(BF), grad_inputs, sums[0], sums[1], sums[2], sums[3], grad_w_qkv, sums[4],
            grad_w_out, sums[5], grad_w_up, sums[6], grad_w_down, sums[5])


def solution(mesh):
    fast = mesh.shape["dp"] == 8 and mesh.shape["head"] == 4
    whole = P(("dp", "head"), None)
    weight = P("dp", "head")
    return jax.shard_map(
        fast_body if fast else general_body,
        mesh=mesh,
        in_specs=(whole, P("dp", None)) + (P(),) * 12 + (whole,),
        out_specs=(whole, whole, P(), P(), P(), P(), weight, P(), weight, P(), weight, P(), weight, P()),
        check_vma=False,
    )
```

```python
import functools

import jax
import jax.numpy as jnp
import numpy as np
from jax import lax
from jax.experimental import pallas as pl
from jax.experimental.pallas import tpu as pltpu
from jax.sharding import PartitionSpec as P

HD = 64
ROT = 16
HALF = ROT // 2
NN = (((1,), (0,)), ((), ()))
NT = (((1,), (1,)), ((), ()))
TN = (((0,), (0,)), ((), ()))
FREQS = (10000.0 ** (-(2.0 * np.arange(HALF)) / ROT)).astype(np.float32)
BF = jnp.bfloat16
F32 = jnp.float32
VMEM_LIMIT = 62 * 1024 * 1024


def mm(a, b, dims=NN):
    return lax.dot_general(a, b, dims, preferred_element_type=F32)


def flat(v):
    return v.astype(F32).reshape(1, v.shape[0])


def norm_parts(x):
    v = x.astype(F32)
    center = v - jnp.mean(v, axis=-1, keepdims=True)
    inv = lax.rsqrt(jnp.mean(center * center, axis=-1, keepdims=True) + 1e-5)
    return center * inv, inv


def mlp_kernel(prev, final, pos, *refs):
    x_ref, dy_ref, wu, wd, bu, gain, shift = refs[:7]
    refs = refs[7:]
    if prev:
        pwu, pwd, psmall, psmallf = refs[:4]
        refs = refs[4:]
    part_ref, g_ref, out_wu, out_wd, small, smallf = refs[:6]
    if final:
        dwu, dwd = refs[6:8]
    else:
        dwu, dwd = out_wu, out_wd
    step = pl.program_id(0)

    @pl.when(step == 0)
    def _():
        if prev:
            dwu[...] = pwu[...]
            dwd[...] = pwd[...]
            small[...] = psmall[...]
            smallf[...] = psmallf[...]
        else:
            dwu[...] = jnp.zeros_like(dwu)
            dwd[...] = jnp.zeros_like(dwd)
            small[...] = jnp.zeros_like(small)
            smallf[...] = jnp.zeros_like(smallf)

    normed, _unused = norm_parts(x_ref[...])
    scale = gain[...].astype(F32)
    nm = (normed * scale + shift[...].astype(F32)).astype(BF)
    dy = dy_ref[...]
    pre = mm(nm, wu[...]) + bu[...].astype(F32)
    cdf = 0.5 + 0.5 * lax.erf(pre * (0.5**0.5))
    hid = (pre * cdf).astype(BF)
    slope = cdf + pre * (jnp.exp(-0.5 * pre * pre) * 0.3989422804014327)
    gp = (mm(dy, wd[...], NT) * slope).astype(BF)
    part_ref[...] = mm(hid, wd[...]).astype(BF)
    r = mm(gp, wu[...], NT)
    g_ref[...] = (r * scale).astype(BF)
    smallf[0:1, :] += jnp.sum(gp.astype(F32), axis=0, keepdims=True)
    small[0:1, :] += jnp.sum(r * normed, axis=0, keepdims=True)
    small[1:2, :] += jnp.sum(r, axis=0, keepdims=True)
    small[2:3, :] += jnp.sum(dy.astype(F32), axis=0, keepdims=True)
    dwd[...] += mm(hid, dy, TN)
    dwu[...] += mm(nm, gp, TN)

    if final:

        @pl.when(step == pl.num_programs(0) - 1)
        def _():
            out_wu[...] = dwu[...].astype(BF)
            out_wd[...] = dwd[...].astype(BF)


def mlp(pos, x, dy, wu, wd, bu, gain, shift, n, prev=None, final=True, tt=512):
    tok, d = x.shape
    f = wu.shape[1] // n
    row = lambda i, p: (i, 0)
    zero = lambda i, p: (0, 0)
    one = pl.Buffered(1)
    const = lambda shape: pl.BlockSpec(shape, zero, pipeline_mode=one)
    accs = [const((d, f)), const((f, d)), const((8, d)), const((8, f))]
    kind = BF if final else F32
    grid_spec = pltpu.PrefetchScalarGridSpec(
        num_scalar_prefetch=1,
        grid=(tok // tt,),
        in_specs=[
            pl.BlockSpec((tt, d), row),
            pl.BlockSpec((tt, d), row),
            pl.BlockSpec((d, f), lambda i, p: (0, p[0]), pipeline_mode=one),
            pl.BlockSpec((f, d), lambda i, p: (p[0], 0), pipeline_mode=one),
            pl.BlockSpec((1, f), lambda i, p: (0, p[0])),
            const((1, d)),
            const((1, d)),
        ]
        + (accs if prev is not None else []),
        out_specs=[pl.BlockSpec((tt, d), row), pl.BlockSpec((tt, d), row)] + accs,
        scratch_shapes=[pltpu.VMEM((d, f), F32), pltpu.VMEM((f, d), F32)] if final else [],
    )
    return pl.pallas_call(
        functools.partial(mlp_kernel, prev is not None, final),
        grid_spec=grid_spec,
        out_shape=(
            jax.ShapeDtypeStruct((tok, d), BF),
            jax.ShapeDtypeStruct((tok, d), BF),
            jax.ShapeDtypeStruct((d, f), kind),
            jax.ShapeDtypeStruct((f, d), kind),
            jax.ShapeDtypeStruct((8, d), F32),
            jax.ShapeDtypeStruct((8, f), F32),
        ),
        compiler_params=pltpu.CompilerParams(vmem_limit_bytes=VMEM_LIMIT),
        cost_estimate=pl.CostEstimate(
            flops=12 * tok * d * f, bytes_accessed=8 * tok * d + 12 * d * f, transcendentals=2 * tok * f
        ),
        name="mlp",
    )(pos, x, dy, wu, wd, bu, gain, shift, *(prev or ()))


def proj_kernel(nh, prev, pos, *refs):
    x_ref, dy_ref, wq, wk, wv, bq, bk, bv, wo, gain, shift, cos, sin = refs[:13]
    qt, kt, vt, dot, kn, vn, na_ref = refs[13 + (7 if prev else 0) :]
    normed, _unused = norm_parts(x_ref[...])
    na = (normed * gain[...].astype(F32) + shift[...].astype(F32)).astype(BF)
    na_ref[...] = na
    co = cos[...]
    si = sin[...]

    def rotated(t, scale):
        rows = []
        for h in range(nh):
            u = t[h * HD : (h + 1) * HD]
            u1 = u[:HALF]
            u2 = u[HALF:ROT]
            rows += [u1 * co - u2 * si, u2 * co + u1 * si, u[ROT:]]
        out = jnp.concatenate(rows, axis=0).astype(BF)
        return out if scale is None else out * jnp.asarray(scale, BF)

    def triple(w, b):
        return (mm(na, w[...]) + b[...].astype(F32)).astype(BF)

    qt[...] = rotated(triple(wq, bq).astype(F32).T, HD**-0.5)
    keys = rotated(triple(wk, bk).astype(F32).T, None)
    kt[...] = keys
    kn[...] = keys.T
    values = triple(wv, bv)
    vn[...] = values
    vt[...] = values.T
    dot[...] = mm(wo[...], dy_ref[...], NT).astype(BF)


def proj(pos, x, dy, w_qkv, b_qkv, w_out, gain, shift, cos, sin, n, total, first, prev=None, tt=512):
    tok, d = x.shape
    w = d // n
    nh = w // HD
    off = first // tt
    row = lambda i, p: (i, 0)
    zero = lambda i, p: (0, 0)
    one = pl.Buffered(1)
    wspec = lambda k: pl.BlockSpec((d, w), lambda i, p: (0, k * n + p[0]), pipeline_mode=one)
    bspec = lambda k: pl.BlockSpec((1, w), lambda i, p: (0, k * n + p[0]))
    lane = lambda rows: pl.BlockSpec((rows, tt), lambda i, p: (0, off + i))
    nat = lambda cols: pl.BlockSpec((tt, cols), lambda i, p: (off + i, 0))
    shapes = [(w, total)] * 4 + [(total, w)] * 2 + [(total, d)]
    grid_spec = pltpu.PrefetchScalarGridSpec(
        num_scalar_prefetch=1,
        grid=(tok // tt,),
        in_specs=[pl.BlockSpec((tt, d), row), pl.BlockSpec((tt, d), row)]
        + [wspec(0), wspec(1), wspec(2), bspec(0), bspec(1), bspec(2)]
        + [pl.BlockSpec((w, d), lambda i, p: (p[0], 0), pipeline_mode=one)]
        + [pl.BlockSpec((1, d), zero), pl.BlockSpec((1, d), zero), lane(HALF), lane(HALF)]
        + ([pl.BlockSpec(memory_space=pl.ANY)] * 7 if prev is not None else []),
        out_specs=[lane(w)] * 4 + [nat(w)] * 2 + [nat(d)],
    )
    return pl.pallas_call(
        functools.partial(proj_kernel, nh, prev is not None),
        grid_spec=grid_spec,
        out_shape=tuple(jax.ShapeDtypeStruct(s, BF) for s in shapes),
        input_output_aliases={14 + k: k for k in range(7)} if prev is not None else {},
        compiler_params=pltpu.CompilerParams(vmem_limit_bytes=VMEM_LIMIT),
        cost_estimate=pl.CostEstimate(
            flops=8 * tok * d * w, bytes_accessed=6 * tok * d + 12 * tok * w + 8 * d * w, transcendentals=0
        ),
        name="proj",
    )(pos, x, dy, w_qkv, w_qkv, w_qkv, b_qkv, b_qkv, b_qkv, w_out, gain, shift, cos, sin, *(prev or ()))


def head_kernel(nh, x_hbm, dy_hbm, wu_hbm, wd_hbm, wqkv_hbm, wo_hbm, gain_a, shift_a, gain_m, shift_m, bu, bq, lens,
                g_out, na_out, dy_out, qt, kt, vt, dot, kn, vn, cos, sin, p_own, p_far, up_keep, up_send, dn0, dn1, dn2, dn3,
                w_t, small, smallf,
                xs, dys, wu, wd, wqkv, wt, wo, bias_t, parts, far_in, near_in, dwu, dwd, load, send, recv):
    step = pl.program_id(0)
    i = lax.axis_index("dp")
    j = lax.axis_index("head")
    own, d = x_hbm.shape
    f = wu.shape[1]
    w = wo.shape[0]
    half = own // 2
    core = {"head": j ^ 1}
    across = {"head": j ^ 2}

    def remote(src, dst, k, to):
        return pltpu.make_async_remote_copy(
            src_ref=src, dst_ref=dst, send_sem=send.at[k], recv_sem=recv.at[k], device_id=to,
            device_id_type=pl.DeviceIdType.MESH)

    lo, hi = pl.ds(0, half), pl.ds(half, half)
    copies = [
        remote(x_hbm, xs.at[1], 0, core),
        remote(dy_hbm, dys.at[1], 1, core),
        remote(x_hbm.at[lo], xs.at[2, lo], 2, across),
        remote(dy_hbm.at[lo], dys.at[2, lo], 3, across),
        remote(x_hbm.at[hi], xs.at[3, lo], 4, across),
        remote(dy_hbm.at[hi], dys.at[3, lo], 5, across),
        remote(xs.at[2, lo], xs.at[2, hi], 6, core),
        remote(dys.at[2, lo], dys.at[2, hi], 7, core),
        remote(xs.at[3, lo], xs.at[3, hi], 8, core),
        remote(dys.at[3, lo], dys.at[3, hi], 9, core),
        remote(parts.at[1], near_in, 10, core),
        remote(parts.at[2, hi], far_in.at[lo], 11, core),
        remote(parts.at[3, hi], far_in.at[hi], 12, core),
    ]
    locals_ = [
        pltpu.make_async_copy(x_hbm, xs.at[0], load.at[0]),
        pltpu.make_async_copy(dy_hbm, dys.at[0], load.at[1]),
        pltpu.make_async_copy(wu_hbm.at[:, pl.ds(j * f, f)], wu, load.at[2]),
        pltpu.make_async_copy(wd_hbm.at[pl.ds(j * f, f)], wd, load.at[3]),
        pltpu.make_async_copy(wo_hbm.at[pl.ds(j * w, w)], wo, load.at[4]),
    ] + [
        pltpu.make_async_copy(wqkv_hbm.at[:, pl.ds(k * d + j * w, w)], wqkv.at[:, pl.ds(k * w, w)], load.at[5 + k])
        for k in range(3)
    ]

    @pl.when(step == 0)
    def _():
        barrier = pltpu.get_barrier_semaphore()
        for to in (core, across):
            pl.semaphore_signal(barrier, inc=1, device_id=to, device_id_type=pl.DeviceIdType.MESH)
        for c in locals_:
            c.start()
        pl.semaphore_wait(barrier, 2)
        for c in copies[:6]:
            c.start()
        dwu[...] = jnp.zeros_like(dwu)
        dwd[...] = jnp.zeros_like(dwd)
        small[...] = jnp.zeros_like(small)
        smallf[...] = jnp.zeros_like(smallf)
        for c in locals_:
            c.wait()
        for k in range(3):
            wt[k * w : (k + 1) * w, :] = wqkv[:, k * w : (k + 1) * w].T
            row = flat(bq[pl.ds(pl.multiple_of(k * d + j * w, 256), w)])
            bias_t[k * w : (k + 1) * w, :] = jnp.broadcast_to(row, (128, w)).T

    @pl.when(step == 1)
    def _():
        copies[0].wait_recv()

    @pl.when(step == 2)
    def _():
        copies[6].wait_recv()

    @pl.when(step == 3)
    def _():
        copies[8].wait_recv()

    normed, _unused = norm_parts(xs[step])
    scale = flat(gain_m[...])
    nm = (normed * scale + flat(shift_m[...])).astype(BF)
    na = (normed * flat(gain_a[...]) + flat(shift_a[...])).astype(BF)
    na_out[...] = na
    pre = mm(nm, wu[...]) + flat(bu[pl.ds(pl.multiple_of(j * f, 1024), f)])
    cdf = 0.5 + 0.5 * lax.erf(pre * (0.5**0.5))
    hid = (pre * cdf).astype(BF)
    slope = cdf + pre * (jnp.exp(-0.5 * pre * pre) * 0.3989422804014327)
    parts[step] = mm(hid, wd[...]).astype(BF)

    lane = lax.broadcasted_iota(jnp.int32, (1, own), 1)
    far = jnp.where(lane < half, j ^ 2, j ^ 3) * own + (step - 2) * half + lane % half
    index = jnp.where(step == 0, j * own + lane, jnp.where(step == 1, (j ^ 1) * own + lane, far))
    begin = jnp.zeros_like(index)
    total = jnp.int32(0)
    for s in range(lens.shape[0] - 1):
        total = total + lens[s]
        begin = jnp.where(index >= total, total, begin)
    sub = lax.broadcasted_iota(jnp.int32, (HALF, own), 0)
    freqs = jnp.zeros((HALF, own), F32)
    for k in range(HALF):
        freqs = jnp.where(sub == k, float(FREQS[k]), freqs)
    angle = freqs * (index - begin).astype(F32)
    co = jnp.cos(angle)
    si = jnp.sin(angle)
    cos[...] = co
    sin[...] = si

    def projected(k):
        b = bias_t[k * w : (k + 1) * w, :]
        t = mm(wt[k * w : (k + 1) * w, :], na, NT)
        return (t + jnp.concatenate([b] * (own // 128), axis=1)).astype(BF)

    def rotated(t, factor):
        rows = []
        for h in range(nh):
            u = t[h * HD : (h + 1) * HD].astype(F32)
            u1 = u[:HALF]
            u2 = u[HALF:ROT]
            rows += [u1 * co - u2 * si, u2 * co + u1 * si, u[ROT:]]
        out = jnp.concatenate(rows, axis=0)
        return (out if factor is None else out * factor).astype(BF)

    qt[...] = rotated(projected(0), HD**-0.5)
    keys = rotated(projected(1), None)
    kt[...] = keys
    kn[...] = keys.T
    values = projected(2)
    vt[...] = values
    vn[...] = values.T

    @pl.when(step == 1)
    def _():
        copies[1].wait_recv()
        copies[10].start()
        copies[2].wait_recv()
        copies[6].start()

    @pl.when(step == 2)
    def _():
        copies[7].wait_recv()
        copies[11].start()

    @pl.when(step == 3)
    def _():
        copies[12].start()
        copies[5].wait_recv()
        copies[9].start()
        copies[9].wait_recv()

    dy = dys[step]
    dy_out[...] = dy
    gp = (mm(dy, wd[...], NT) * slope).astype(BF)
    r = mm(gp, wu[...], NT)
    g_out[...] = (r * scale).astype(BF)
    smallf[0:1, :] += jnp.sum(gp.astype(F32), axis=0, keepdims=True)
    small[0:1, :] += jnp.sum(r * normed, axis=0, keepdims=True)
    small[1:2, :] += jnp.sum(r, axis=0, keepdims=True)
    small[2:3, :] += jnp.sum(dy.astype(F32), axis=0, keepdims=True)
    dwd[...] += mm(hid, dy, TN)
    dwu[...] += mm(nm, gp, TN)
    dot[...] = mm(wo[...], dy, NT).astype(BF)

    @pl.when(step == 1)
    def _():
        copies[3].wait_recv()
        copies[7].start()

    @pl.when(step == 2)
    def _():
        copies[4].wait_recv()
        copies[8].start()

    @pl.when(step == 3)
    def _():
        rows = dwu.shape[0] // 8
        keep = dn0.shape[1]
        for b in range(4):
            for ref, at in ((up_keep, 2 * b + i % 2), (up_send, 2 * b + 1 - i % 2)):
                at = pl.multiple_of(at * rows, rows)
                ref[b, :rows] = dwu[pl.ds(at, rows), :].astype(BF)
                ref[b, rows:] = dwd[pl.ds(at + keep, rows - keep), :].astype(BF)
            ref = (dn0, dn1, dn2, dn3)[b]
            for x in range(2):
                at = 2 * ((i // 2) ^ b) + x
                ref[x] = dwd[pl.ds(pl.multiple_of(at * rows, rows), keep), :].astype(BF)
        w_t[...] = wt[...]
        copies[10].wait_recv()
        p_own[...] = (parts[0].astype(F32) + near_in[...].astype(F32)).astype(BF)
        copies[11].wait_recv()
        p_far[lo] = (parts[2, lo].astype(F32) + far_in[lo].astype(F32)).astype(BF)
        copies[12].wait_recv()
        p_far[hi] = (parts[3, lo].astype(F32) + far_in[hi].astype(F32)).astype(BF)
        for c in copies:
            c.wait_send()


def head_stage(x, dy, w_up, w_down, w_qkv, w_out, ga, sa, gm, sm, bu, bq, lens, n, cid):
    own, d = x.shape
    tok = own * n
    w = d // n
    f = w_up.shape[1] // n
    row = lambda i: (i, 0)
    lane = lambda rows: pl.BlockSpec((rows, own), lambda i: (0, i))
    nat = lambda cols: pl.BlockSpec((own, cols), row)
    one = pl.Buffered(1)
    const = lambda shape: pl.BlockSpec(shape, lambda i: (0,) * len(shape), pipeline_mode=one)
    hbm = pl.BlockSpec(memory_space=pl.ANY)
    sds = jax.ShapeDtypeStruct
    return pl.pallas_call(
        functools.partial(head_kernel, w // HD),
        grid=(n,),
        in_specs=[hbm] * 6
        + [const(v.shape) for v in (ga, sa, gm, sm, bu, bq)]
        + [pl.BlockSpec(memory_space=pltpu.SMEM)],
        out_specs=[nat(d)] * 3
        + [lane(w)] * 4
        + [nat(w)] * 2
        + [lane(HALF)] * 2
        + [const((own, d))] * 2
        + [const((4, d // 8 + d // 32, d))] * 2
        + [const((2, 3 * d // 32, d))] * 4
        + [const((3 * w, d)), const((8, d)), const((8, f))],
        out_shape=tuple(
            [sds((tok, d), BF)] * 3
            + [sds((w, tok), BF)] * 4
            + [sds((tok, w), BF)] * 2
            + [sds((HALF, tok), F32)] * 2
            + [sds((own, d), BF)] * 2
            + [sds((4, d // 8 + d // 32, d), BF)] * 2
            + [sds((2, 3 * d // 32, d), BF)] * 4
            + [sds((3 * w, d), BF), sds((8, d), F32), sds((8, f), F32)]
        ),
        scratch_shapes=[
            pltpu.VMEM((4, own, d), BF),
            pltpu.VMEM((4, own, d), BF),
            pltpu.VMEM((d, f), BF),
            pltpu.VMEM((f, d), BF),
            pltpu.VMEM((d, 3 * w), BF),
            pltpu.VMEM((3 * w, d), BF),
            pltpu.VMEM((w, d), BF),
            pltpu.VMEM((3 * w, 128), F32),
            pltpu.VMEM((4, own, d), BF),
            pltpu.VMEM((own, d), BF),
            pltpu.VMEM((own, d), BF),
            pltpu.VMEM((d, f), F32),
            pltpu.VMEM((f, d), F32),
            pltpu.SemaphoreType.DMA((8,)),
            pltpu.SemaphoreType.DMA((13,)),
            pltpu.SemaphoreType.DMA((13,)),
        ],
        compiler_params=pltpu.CompilerParams(
            vmem_limit_bytes=VMEM_LIMIT, collective_id=cid, has_side_effects=True
        ),
        cost_estimate=pl.CostEstimate(
            flops=12 * tok * d * f + 10 * tok * d * w, bytes_accessed=12 * tok * d + 8 * d * f, transcendentals=2 * tok * f
        ),
        name="head_stage",
    )(x, dy, w_up, w_down, w_qkv, w_out, ga, sa, gm, sm, bu, bq, lens)


def attn_kernel(nh, tok, blk, per, halved, lens, rel, cos, sin, qt, kt, vt, dot, kn, vn,
                gt_ref, ctx_ref, exps, low_exps, dk, dv, oacc, dqacc, mpart, lpart, rowsc, qpad, dopad):
    nseq = lens.shape[0]
    nblk = tok // blk
    shift = rel[0]
    heads = range(nh)

    def place(b):
        chunk = (b // per) ^ shift
        half = b % per
        at = chunk * per + half
        if halved:
            at = jnp.where(chunk < 2, at, 4 + (chunk - 2) + 2 * half)
        return pl.multiple_of(at * blk, blk)

    def rows_of(h):
        return slice(h * HD, (h + 1) * HD)

    def pair_of(h):
        return slice((h // 2) * 128, (h // 2) * 128 + 128)

    def fold(v, op):
        return op(v.reshape(blk // 8, 8, blk), axis=0)

    def begin_of(at):
        begin = jnp.int32(0)
        total = jnp.int32(0)
        for s in range(nseq - 1):
            total = total + lens[s]
            begin = jnp.where(at >= total, total, begin)
        return begin

    dk[...] = jnp.zeros_like(dk)
    dv[...] = jnp.zeros_like(dv)
    qpad[...] = jnp.zeros_like(qpad)
    dopad[...] = jnp.zeros_like(dopad)
    rows_iota = lax.broadcasted_iota(jnp.int32, (blk, blk), 0)
    cols_iota = lax.broadcasted_iota(jnp.int32, (1, blk), 1)

    def one_block(i, carry):
        first_tok = i * blk
        count = i - begin_of(first_tok) // blk + 1
        last_begin = begin_of(first_tok + blk - 1)
        cols = pl.ds(place(i), blk)
        query_idx = cols_iota + first_tok
        start_row = begin_of(query_idx)
        for h in heads:
            half = (h % 2) * HD
            qpad[h, half : half + HD, :] = qt[rows_of(h), cols]

        krow = pl.ds(place(i), blk)
        kidx = rows_iota + first_tok
        allowed = (kidx >= start_row) & (kidx <= query_idx)
        for h in heads:
            s = jnp.where(allowed, mm(kn[krow, pair_of(h)], qpad[h]), -1e30)
            exps[h, 0] = s
            mpart[h] = fold(s, jnp.max)

        def scores(step, c):
            b = i - step
            krow = pl.ds(place(b), blk)
            edge = last_begin > b * blk

            @pl.when(edge)
            def _():
                allowed = (rows_iota + b * blk) >= start_row
                for h in heads:
                    s = jnp.where(allowed, mm(kn[krow, pair_of(h)], qpad[h]), -1e30)
                    exps[h, step] = s
                    mpart[h] = jnp.maximum(mpart[h], fold(s, jnp.max))

            @pl.when(jnp.logical_not(edge))
            def _():
                for h in heads:
                    s = mm(kn[krow, pair_of(h)], qpad[h])
                    exps[h, step] = s
                    mpart[h] = jnp.maximum(mpart[h], fold(s, jnp.max))

            return c

        lax.fori_loop(1, count, scores, 0)
        for h in heads:
            rowsc[h : h + 1, :] = jnp.max(mpart[h], axis=0, keepdims=True)
        lpart[...] = jnp.zeros_like(lpart)
        oacc[...] = jnp.zeros_like(oacc)

        def weights(step, c):
            kcols = pl.ds(place(i - step), blk)
            for h in heads:
                e = jnp.exp(exps[h, step] - rowsc[h : h + 1, :])
                exps[h, step] = e
                lpart[h] += fold(e, jnp.sum)
                low = e.astype(BF)
                low_exps[h, step] = low
                oacc[h] += mm(vt[rows_of(h), kcols], low)
            return c

        lax.fori_loop(0, count, weights, 0)
        for h in heads:
            half = (h % 2) * HD
            inv = 1.0 / jnp.sum(lpart[h], axis=0, keepdims=True)
            o = oacc[h] * inv
            ctx_ref[rows_of(h), cols] = o.astype(BF)
            scaled = (dot[rows_of(h), cols].astype(F32) * inv).astype(BF)
            dopad[h, half : half + HD, :] = scaled
            rowsc[h : h + 1, :] = jnp.sum(o * scaled.astype(F32), axis=0, keepdims=True)
        dqacc[...] = jnp.zeros_like(dqacc)

        def backward(step, c):
            kcols = pl.ds(place(i - step), blk)
            for h in heads:
                half = (h % 2) * HD
                hs = rows_of(h)
                dp = mm(vn[kcols, pair_of(h)], dopad[h])
                ds = (exps[h, step] * (dp - rowsc[h : h + 1, :])).astype(BF)
                dv[hs, kcols] += mm(dopad[h, half : half + HD, :], low_exps[h, step], NT)
                dk[hs, kcols] += mm(qt[hs, cols], ds, NT)
                dqacc[hs, :] += mm(kt[hs, kcols], ds)
            return c

        lax.fori_loop(0, count, backward, 0)
        co = cos[:, cols]
        si = sin[:, cols]
        for h in heads:
            base = h * HD
            g = dqacc[base : base + HD, :] * (HD**-0.5)
            g1 = g[:HALF]
            g2 = g[HALF:ROT]
            gt_ref[base : base + HD, cols] = jnp.concatenate(
                [g1 * co + g2 * si, g2 * co - g1 * si, g[ROT:]], axis=0
            ).astype(BF)
        return carry

    lax.fori_loop(0, nblk, one_block, 0)

    def finish(i, carry):
        cols = pl.ds(pl.multiple_of(i * blk, blk), blk)
        co = cos[:, cols]
        si = sin[:, cols]
        for h in heads:
            base = h * HD
            g = dk[base : base + HD, cols]
            g1 = g[:HALF]
            g2 = g[HALF:ROT]
            gt_ref[nh * HD + base : nh * HD + base + HD, cols] = jnp.concatenate(
                [g1 * co + g2 * si, g2 * co - g1 * si, g[ROT:]], axis=0
            ).astype(BF)
        gt_ref[2 * nh * HD :, cols] = dv[:, cols].astype(BF)
        return carry

    lax.fori_loop(0, nblk, finish, 0)


def attention(lens, rel, cos, sin, qt, kt, vt, dot, kn, vn, chunk, maxlen, halved=False, blk=256):
    width, tok = qt.shape
    nh = width // HD
    wb = maxlen // blk + 1
    vm = pl.BlockSpec(memory_space=pltpu.VMEM)
    sm = pl.BlockSpec(memory_space=pltpu.SMEM)
    return pl.pallas_call(
        functools.partial(attn_kernel, nh, tok, blk, chunk // blk, halved),
        out_shape=(jax.ShapeDtypeStruct((3 * width, tok), BF), jax.ShapeDtypeStruct((width, tok), BF)),
        in_specs=[sm, sm] + [vm] * 8,
        out_specs=(vm, vm),
        scratch_shapes=[
            pltpu.VMEM((nh, wb, blk, blk), F32),
            pltpu.VMEM((nh, wb, blk, blk), BF),
            pltpu.VMEM((width, tok), F32),
            pltpu.VMEM((width, tok), F32),
            pltpu.VMEM((nh, HD, blk), F32),
            pltpu.VMEM((width, blk), F32),
            pltpu.VMEM((nh, 8, blk), F32),
            pltpu.VMEM((nh, 8, blk), F32),
            pltpu.VMEM((8, blk), F32),
            pltpu.VMEM((nh, 128, blk), BF),
            pltpu.VMEM((nh, 128, blk), BF),
        ],
        compiler_params=pltpu.CompilerParams(vmem_limit_bytes=VMEM_LIMIT),
        cost_estimate=pl.CostEstimate(
            flops=20 * width * tok * maxlen, bytes_accessed=20 * width * tok, transcendentals=nh * tok * maxlen
        ),
        name="attention",
    )(lens, rel, cos, sin, qt, kt, vt, dot, kn, vn)


def post_kernel(pos, gt_ref, na_ref, gm_ref, wq, wk, wv, gain, shift, g_ref, out_w, bias, small, dw):
    step = pl.program_id(0)

    @pl.when(step == 0)
    def _():
        dw[...] = jnp.zeros_like(dw)
        bias[...] = jnp.zeros_like(bias)
        small[...] = jnp.zeros_like(small)

    gt = gt_ref[...]
    na = na_ref[...]
    w = wq.shape[1]
    scale = gain[...].astype(F32)
    gn = gt.T
    r = mm(gn[:, :w], wq[...], NT) + mm(gn[:, w : 2 * w], wk[...], NT) + mm(gn[:, 2 * w :], wv[...], NT)
    g_ref[...] = (r * scale + gm_ref[...].astype(F32)).astype(BF)
    small[0:1, :] += jnp.sum(r * na.astype(F32), axis=0, keepdims=True)
    small[1:2, :] += jnp.sum(r, axis=0, keepdims=True)
    bias[0:1, :] += jnp.sum(gn.astype(F32), axis=0, keepdims=True)
    dw[...] += mm(gt, na)

    @pl.when(step == pl.num_programs(0) - 1)
    def _():
        for b in range(dw.shape[1] // 128):
            out_w[b] = dw[:, b * 128 : (b + 1) * 128].astype(BF)
        small[0:1, :] = (small[0:1, :] - shift[...].astype(F32) * small[1:2, :]) / scale


def post(pos, gt, na, gm, w_qkv, gain, shift, n, tt=512):
    tok, d = na.shape
    w = d // n
    row = lambda i, p: (i, 0)
    zero = lambda i, p: (0, 0)
    one = pl.Buffered(1)
    const = lambda shape: pl.BlockSpec(shape, zero, pipeline_mode=one)
    wspec = lambda k: pl.BlockSpec((d, w), lambda i, p: (0, k * n + p[0]), pipeline_mode=one)
    grid_spec = pltpu.PrefetchScalarGridSpec(
        num_scalar_prefetch=1,
        grid=(tok // tt,),
        in_specs=[
            pl.BlockSpec((3 * w, tt), lambda i, p: (0, i)),
            pl.BlockSpec((tt, d), row),
            pl.BlockSpec((tt, d), row),
            wspec(0),
            wspec(1),
            wspec(2),
            const((1, d)),
            const((1, d)),
        ],
        out_specs=[
            pl.BlockSpec((tt, d), row),
            pl.BlockSpec((d // 128, 3 * w, 128), lambda i, p: (0, 0, 0), pipeline_mode=one),
            const((8, 3 * w)),
            const((8, d)),
        ],
        scratch_shapes=[pltpu.VMEM((3 * w, d), F32)],
    )
    return pl.pallas_call(
        post_kernel,
        grid_spec=grid_spec,
        out_shape=(
            jax.ShapeDtypeStruct((tok, d), BF),
            jax.ShapeDtypeStruct((d // 128, 3 * w, 128), BF),
            jax.ShapeDtypeStruct((8, 3 * w), F32),
            jax.ShapeDtypeStruct((8, d), F32),
        ),
        compiler_params=pltpu.CompilerParams(vmem_limit_bytes=VMEM_LIMIT),
        cost_estimate=pl.CostEstimate(
            flops=12 * tok * d * w, bytes_accessed=8 * tok * d + 6 * tok * w + 18 * d * w, transcendentals=0
        ),
        name="post",
    )(pos, gt, na, gm, w_qkv, w_qkv, w_qkv, gain, shift)


def tail_kernel(gt_h, na_h, gm_h, ctx_h, dya_h, wt_h, wo_h, upk_h, upo_h, dn0_h, dn1_h, dn2_h, dn3_h, x_h, pown_h, py_h,
                gain, shift_ref, bo, bd, small, smallf,
                out_ref, g_ref, wup_ref, wdn_ref, wq_ref, wout_ref, sums_ref,
                gt, na, gm, ctx, dya, wt, wo, upk, upo, dn, xo, pown, py,
                ctx_in, up4, up_in, dn_in, dn2,
                dwq, qa_in, qb_in, qa4, qb4, qa_in2, qb_in2, qa2, qb2, qa_in3, qb_in3, qfin, q_own,
                dwo, wo_in, wo4, wo_in2, wo2, wo_in3, piece, piece2, owner_in, owner_in2,
                far_in, near_in, far_sum, y_in, sm, sm_in, load, send, recv):
    i = lax.axis_index("dp")
    j = lax.axis_index("head")
    own, d = x_h.shape
    w = wt.shape[0] // 3
    half = own // 2
    bx = i % 2
    b0 = (i // 2) % 2
    b1 = i // 4
    z = i // 2
    mesh_id = pl.DeviceIdType.MESH
    core, across, diag = {"head": j ^ 1}, {"head": j ^ 2}, {"head": j ^ 3}
    px, p0, p1 = {"dp": i ^ 1}, {"dp": i ^ 2}, {"dp": i ^ 4}
    lo, hi = pl.ds(0, half), pl.ds(half, half)
    count = [0]
    started = []

    def remote(src, dst, to):
        k = count[0]
        count[0] += 1
        return pltpu.make_async_remote_copy(
            src_ref=src, dst_ref=dst, send_sem=send.at[k], recv_sem=recv.at[k], device_id=to, device_id_type=mesh_id)

    def go(*copies):
        for c in copies:
            c.start()
            started.append(c)

    def local(src, dst, k):
        return pltpu.make_async_copy(src, dst, load.at[k])

    loads = [
        local(upk_h, upk, 0), local(upo_h, upo, 1),
        local(dn0_h, dn.at[0], 2), local(dn1_h, dn.at[1], 3), local(dn2_h, dn.at[2], 4), local(dn3_h, dn.at[3], 5),
        local(gt_h, gt, 6), local(na_h, na, 7), local(wt_h, wt, 8), local(ctx_h, ctx, 9), local(dya_h, dya, 10),
        local(gm_h, gm, 11), local(wo_h, wo, 12), local(x_h, xo, 13), local(pown_h, pown, 14), local(py_h, py, 15),
    ]
    c_ctx = [
        remote(ctx_h.at[:, pl.ds(2 * own, half)], ctx_in.at[1, :, lo], across),
        remote(ctx_h.at[:, pl.ds(3 * own, half)], ctx_in.at[1, :, hi], across),
        remote(ctx_h.at[:, pl.ds(2 * own + half, half)], ctx_in.at[2, :, lo], diag),
        remote(ctx_h.at[:, pl.ds(3 * own + half, half)], ctx_in.at[2, :, hi], diag),
        remote(ctx_h.at[:, pl.ds(own, own)], ctx_in.at[0], core),
    ]
    c_up = [remote(up4.at[z ^ k], up_in.at[k - 1], {"dp": i ^ (2 * k)}) for k in (1, 2, 3)]
    c_dnx = remote(dn2.at[1 - bx], dn_in, px)
    rows = dwq.shape[3] // 2
    ra, rb = pl.ds(0, rows), pl.ds(rows, rows)
    c_qa = remote(dwq.at[:, :, 1 - bx, ra], qa_in, px)
    c_qb = remote(dwq.at[:, :, 1 - bx, rb], qb_in, px)
    c_qa0 = remote(qa4.at[:, 1 - b0], qa_in2, p0)
    c_qb0 = remote(qb4.at[:, 1 - b0], qb_in2, p0)
    c_qa1 = remote(qa2.at[1 - b1], qa_in3, p1)
    c_qb1 = remote(qb2.at[1 - b1], qb_in3, p1)
    c_wox = remote(dwo.at[:, :, 1 - bx], wo_in, px)
    c_wo0 = remote(wo4.at[:, 1 - b0], wo_in2, p0)
    c_wo1 = remote(wo2.at[1 - b1], wo_in3, p1)
    c_g = [
        remote(gm.at[pl.ds(2 * own + half, half)], far_in.at[lo], core),
        remote(gm.at[pl.ds(3 * own + half, half)], far_in.at[hi], core),
        remote(gm.at[pl.ds(own, own)], near_in, core),
    ]
    c_y = [remote(far_sum.at[lo], y_in.at[lo], across), remote(far_sum.at[hi], y_in.at[hi], across)]
    c_sm = [remote(sm.at[s], sm_in.at[s], to) for s, to in enumerate((core, across, px, p0, p1))]
    dests = []
    c_own, c_own2 = [], []
    for r in range(4):
        di, dj = 2 * j + i // 4, (i % 4) ^ r
        dests.append((di, dj))
        cut = pl.ds(pl.multiple_of(dj * w, 128), w)
        c_own.append(remote(piece.at[:, cut], owner_in.at[i % 4], {"dp": di, "head": dj}))
        c_own2.append(remote(piece2.at[:, cut], owner_in2.at[i % 4], {"dp": di, "head": dj}))
    c_q = []
    q_dst = []
    for t in range(3):
        dst = (t - j + 4) % 4
        q_dst.append(dst)
        c_q.append(remote(qfin.at[(3 * dst + t) // 4], q_own.at[t], {"head": dst}))

    barrier = pltpu.get_barrier_semaphore()
    for to in (core, across, diag, px, p0, p1, {"dp": i ^ 6}):
        pl.semaphore_signal(barrier, inc=1, device_id=to, device_id_type=mesh_id)
    for c in loads:
        c.start()
    for r in range(4):
        si, sj = 4 * (i % 2) + (j ^ r), i // 2

        @pl.when((si != i) | (sj != j))
        def _():
            pl.semaphore_signal(barrier, inc=1, device_id={"dp": si, "head": sj}, device_id_type=mesh_id)

    to_self = jnp.where(2 * j + i // 4 == i, 1, 0)
    pl.semaphore_wait(barrier, 11 - to_self)

    go(*c_ctx)

    def added(a, b):
        return a.astype(F32) + b.astype(F32)

    def ready(first, last):
        for k in range(first, last):
            loads[k].wait()

    ready(0, 2)
    up4[...] = added(upk[...], upo[...]).astype(BF)
    go(*c_up)
    ready(2, 6)
    dn2[...] = (added(dn[0], dn[1]) + added(dn[2], dn[3])).astype(BF)
    go(c_dnx)

    ready(6, 9)
    gains = [jnp.zeros((1, 256), F32)] * 4
    for part, c in ((ra, c_qa), (rb, c_qb)):
        left = gt[part, :]
        for k in range(4):
            t = mm(left, na[:, 256 * k : 256 * (k + 1)])
            gains[k] += jnp.sum(t * wt[part, 256 * k : 256 * (k + 1)].astype(F32), axis=0, keepdims=True)
            t = t.astype(BF)
            dwq[k // 2, k % 2, 0, part] = t[:, :128]
            dwq[k // 2, k % 2, 1, part] = t[:, 128:]
        if c is c_qa:
            go(c)
    s_bias = mm(jnp.ones((8, gt.shape[1]), BF), gt[...], NT)[0:1]
    high = s_bias.astype(BF)
    low = (s_bias - high.astype(F32)).astype(BF)
    s_shift = mm(jnp.broadcast_to(high, (8, 3 * w)), wt[...])[0:1] + mm(jnp.broadcast_to(low, (8, 3 * w)), wt[...])[0:1]
    s_gain = jnp.concatenate(gains, axis=1)
    scale = flat(gain[...])

    sm[0] = jnp.zeros((16, d), F32)
    sm[0, 0:1, :] = (s_gain - flat(shift_ref[...]) * s_shift) / scale
    sm[0, 1:2, :] = s_shift
    for k in range(3):
        sm[0, 2 + k : 3 + k, pl.ds(pl.multiple_of(j * w, 128), w)] = s_bias[:, k * w : (k + 1) * w]
    sm[0, 5:7, :] = small[0:2, :]
    sm[0, 7:8, :] = small[2:3, :] * 0.25
    sm[0, pl.ds(8 + j, 1), :] = smallf[0:1, :]
    go(c_sm[0])

    def small_step(s):
        c_sm[s].wait_recv()
        sm[s + 1] = sm[s] + sm_in[s]
        if s < 4:
            go(c_sm[s + 1])

    ready(9, 11)
    t = mm(ctx[...], dya[...]).astype(BF)
    for b in range(8):
        dwo[b // 4, (b // 2) % 2, b % 2] = t[32 * b : 32 * (b + 1)]
    small_step(0)

    ready(11, 12)

    def tile(at):
        ts = slice(at, at + own)
        r = mm(gt[:, ts].T, wt[...])
        gm[ts, :] = (r * scale + gm[ts, :].astype(F32)).astype(BF)

    tile(2 * own)
    go(c_g[0])
    tile(3 * own)
    go(c_g[1])
    c_g[0].wait_recv()
    far_sum[lo] = added(gm[2 * own : 2 * own + half], far_in[lo]).astype(BF)
    go(c_y[0])
    small_step(1)
    go(c_qb, c_wox)
    c_g[1].wait_recv()
    far_sum[hi] = added(gm[3 * own : 3 * own + half], far_in[hi]).astype(BF)
    go(c_y[1])
    tile(own)
    go(c_g[2])
    small_step(2)
    c_qa.wait_recv()
    qa4[...] = added(dwq[:, :, bx, ra], qa_in[...]).astype(BF)
    go(c_qa0)
    tile(0)
    small_step(3)

    ready(12, 16)
    attn = mm(ctx[:, :own], wo[pl.ds(pl.multiple_of(j * w, 128), w), :], TN)
    c_ctx[4].wait_recv()
    attn += mm(ctx_in[0], wo[pl.ds(pl.multiple_of((j ^ 1) * w, 128), w), :], TN)
    for k in range(4):
        c_ctx[k].wait_recv()
    attn += mm(ctx_in[1], wo[pl.ds(pl.multiple_of((j ^ 2) * w, 128), w), :], TN)
    attn += mm(ctx_in[2], wo[pl.ds(pl.multiple_of((j ^ 3) * w, 128), w), :], TN)
    out_ref[...] = (
        xo[...].astype(F32) + attn + added(pown[...], py[...]) + (flat(bo[...]) + flat(bd[...]))
    ).astype(BF)

    c_qa0.wait_recv()
    qa2[...] = added(qa4[:, b0], qa_in2[...]).astype(BF)
    go(c_qa1)
    c_qb.wait_recv()
    qb4[...] = added(dwq[:, :, bx, rb], qb_in[...]).astype(BF)
    go(c_qb0)
    for c in c_up:
        c.wait_recv()
    c_dnx.wait_recv()
    mine = up4[z].astype(F32) + up_in[0].astype(F32) + added(up_in[1], up_in[2])
    nu = wup_ref.shape[0]
    nd = dn2.shape[1]
    wup_ref[...] = mine[:nu].astype(BF)
    piece[:nd, :] = added(dn2[bx], dn_in[...]).astype(BF)
    piece[nd:, :] = mine[nu:].astype(BF)

    def hand_over(source, copies, target):
        for r in range(4):
            di, dj = dests[r]

            @pl.when((di != i) | (dj != j))
            def _():
                copies[r].start()

            @pl.when((di == i) & (dj == j))
            def _():
                target[i % 4] = source[:, pl.ds(pl.multiple_of(dj * w, 128), w)]

    hand_over(piece, c_own, owner_in)
    small_step(4)
    sums_ref[...] = sm[5]
    c_wox.wait_recv()
    wo4[...] = added(dwo[:, :, bx], wo_in[...]).astype(BF)
    go(c_wo0)
    c_qb0.wait_recv()
    qb2[...] = added(qb4[:, b0], qb_in2[...]).astype(BF)
    go(c_qb1)
    c_wo0.wait_recv()
    wo2[...] = added(wo4[:, b0], wo_in2[...]).astype(BF)
    go(c_wo1)
    c_qa1.wait_recv()
    c_qb1.wait_recv()
    done = jnp.concatenate([added(qa2[b1], qa_in3[...]), added(qb2[b1], qb_in3[...])], axis=0).astype(BF)
    for k in range(3):
        qfin[k] = done[k * w : (k + 1) * w]
    for t in range(3):

        @pl.when(q_dst[t] != j)
        def _():
            c_q[t].start()

        @pl.when(q_dst[t] == j)
        def _():
            q_own[t] = qfin[(3 * j + t) // 4]

    c_wo1.wait_recv()
    piece2[...] = added(wo2[b1], wo_in3[...]).astype(BF)
    hand_over(piece2, c_own2, owner_in2)

    c_g[2].wait_recv()
    c_y[0].wait_recv()
    g_ref[lo] = added(gm[lo], near_in[lo]) + y_in[lo].astype(F32)
    c_y[1].wait_recv()
    g_ref[hi] = added(gm[hi], near_in[hi]) + y_in[hi].astype(F32)

    for t in range(3):

        @pl.when(q_dst[t] != j)
        def _():
            c_q[t].wait_recv()

        wq_ref[:, t * w : (t + 1) * w] = q_own[t].astype(F32).T.astype(BF)
    for r in range(4):
        di, dj = dests[r]

        @pl.when((di != i) | (dj != j))
        def _():
            c_own[r].wait_recv()
            c_own2[r].wait_recv()

    nd = piece.shape[0]
    no = piece2.shape[0]
    for a in range(4):
        wdn_ref[a * nd : (a + 1) * nd, :] = owner_in[a]
        wout_ref[a * no : (a + 1) * no, :] = owner_in2[a]

    for c in started:
        c.wait_send()
    for t in range(3):

        @pl.when(q_dst[t] != j)
        def _():
            c_q[t].wait_send()

    for r in range(4):
        di, dj = dests[r]

        @pl.when((di != i) | (dj != j))
        def _():
            c_own[r].wait_send()
            c_own2[r].wait_send()


def tail_stage(gt, na, gm, ctx, dya, wt, w_out, upk, upo, dn, x, pown, py, ga, sa, bo, bd, small, smallf, cid):
    own, d = x.shape
    tok = na.shape[0]
    w = d // 4
    vm = pl.BlockSpec(memory_space=pltpu.VMEM)
    hbm = pl.BlockSpec(memory_space=pl.ANY)
    sds = jax.ShapeDtypeStruct
    big = lambda *s: pltpu.VMEM(s, BF)
    nb = d // 8
    nu = upk.shape[1]
    nd = dn[0].shape[1]
    no = w // 8
    r2 = 3 * w // 2
    return pl.pallas_call(
        tail_kernel,
        in_specs=[hbm] * 16 + [vm] * 6,
        out_specs=[vm] * 7,
        out_shape=(
            sds((own, d), BF), sds((own, d), F32), sds((nb, d), BF), sds((4 * nb, w), BF),
            sds((nb, 3 * w), BF), sds((4 * no, w), BF), sds((16, d), F32),
        ),
        scratch_shapes=[
            big(3 * w, tok), big(tok, d), big(tok, d), big(w, tok), big(tok, d), big(3 * w, d), big(d, d),
            big(4, nu, d), big(4, nu, d), big(4, 2, nd, d),
            big(own, d), big(own, d), big(own, d),
            big(3, w, own), big(4, nu, d), big(3, nu, d), big(nd, d), big(2, nd, d),
            big(2, 2, 2, 3 * w, 128), big(2, 2, r2, 128), big(2, 2, r2, 128), big(2, 2, r2, 128), big(2, 2, r2, 128),
            big(2, r2, 128), big(2, r2, 128), big(2, r2, 128), big(2, r2, 128), big(r2, 128), big(r2, 128),
            big(3, w, 128), big(3, w, 128),
            big(2, 2, 2, no, d), big(2, 2, no, d), big(2, 2, no, d), big(2, no, d), big(2, no, d), big(no, d),
            big(nb, d), big(no, d), big(4, nb, w), big(4, no, w),
            big(own, d), big(own, d), big(own, d), big(own, d),
            pltpu.VMEM((6, 16, d), F32), pltpu.VMEM((5, 16, d), F32),
            pltpu.SemaphoreType.DMA((16,)), pltpu.SemaphoreType.DMA((40,)), pltpu.SemaphoreType.DMA((40,)),
        ],
        compiler_params=pltpu.CompilerParams(vmem_limit_bytes=VMEM_LIMIT, collective_id=cid, has_side_effects=True),
        cost_estimate=pl.CostEstimate(
            flops=14 * tok * d * w, bytes_accessed=10 * tok * d, transcendentals=0
        ),
        name="tail_stage",
    )(gt, na, gm, ctx, dya, wt, w_out, upk, upo, *dn, x, pown, py, ga, sa, bo, bd, small, smallf)


def final_kernel(out_t, g_ref, x_ref, dy_ref, wup, wdn, wq, wout, sums,
                 out, gin, ga, sa, gm, sm, dwq, bq, dwout, bo, dwup, bu, dwdn, bd):
    out[...] = out_t[...]
    normed, inv = norm_parts(x_ref[...])
    g = g_ref[...]
    gin[...] = dy_ref[...].astype(F32) + inv * (
        g - jnp.mean(g, axis=-1, keepdims=True) - normed * jnp.mean(g * normed, axis=-1, keepdims=True)
    )

    @pl.when(pl.program_id(0) == 0)
    def _():
        d = sums.shape[1]
        for ref, first, count in ((ga, 0, 1), (sa, 1, 1), (bq, 2, 3), (gm, 5, 1), (sm, 6, 1), (bo, 7, 1), (bd, 7, 1), (bu, 8, 4)):
            for k in range(count):
                ref[k * d : (k + 1) * d] = sums[first + k, :]
        dwup[...] = wup[...].astype(F32)
        dwdn[...] = wdn[...].astype(F32)
        dwq[...] = wq[...].astype(F32)
        dwout[...] = wout[...].astype(F32)


def final_stage(out_t, g, x, dy, wup, wdn, wq, wout, sums, steps=4):
    own, d = x.shape
    row = pl.BlockSpec((own // steps, d), lambda i: (i, 0))
    const = lambda v: pl.BlockSpec(v.shape, lambda i: (0,) * len(v.shape))
    sds = lambda *s: jax.ShapeDtypeStruct(s, F32)
    like = lambda v: sds(*v.shape)
    outs = (
        jax.ShapeDtypeStruct((own, d), BF), sds(own, d), sds(d), sds(d), sds(d), sds(d), like(wq), sds(3 * d),
        like(wout), sds(d), like(wup), sds(4 * d), like(wdn), sds(d),
    )
    return pl.pallas_call(
        final_kernel,
        grid=(steps,),
        in_specs=[row, row, row, row] + [const(v) for v in (wup, wdn, wq, wout, sums)],
        out_specs=[row, row] + [const(v) for v in outs[2:]],
        out_shape=outs,
        compiler_params=pltpu.CompilerParams(vmem_limit_bytes=VMEM_LIMIT),
        name="final_stage",
    )(out_t, g, x, dy, wup, wdn, wq, wout, sums)


def layout(seq_lens, index):
    ends = jnp.cumsum(seq_lens, dtype=jnp.int32)
    starts = ends - seq_lens
    first = jnp.zeros_like(index)
    for s in range(1, seq_lens.shape[0]):
        first = jnp.where(index >= starts[s], starts[s], first)
    return first, index - first


def head_perm(v, bit):
    return lax.ppermute(v, "head", [(k, k ^ bit) for k in range(4)])


def dp_perm(v, bit):
    return lax.ppermute(v, "dp", [(k, k ^ bit) for k in range(8)])


def fast_body(inputs, lengths, attn_gain, attn_shift, mlp_gain, mlp_shift, w_qkv, b_qkv, w_out, b_out,
              w_up, b_up, w_down, b_down, cotangent):
    own, d = inputs.shape
    n = 4
    tok = own * n
    w = d // n
    pos = lax.axis_index("head").astype(jnp.int32).reshape(1)
    lens = lengths[0]
    (g_mlp, na, dy_all, qt, kt, vt, dot, kn, vn, cos, sin, p_own, p_far, up_keep, up_send, *dn, wt, small,
     smallf) = head_stage(
        inputs, cotangent, w_up, w_down, w_qkv, w_out, attn_gain, attn_shift, mlp_gain, mlp_shift, b_up, b_qkv, lens, n, 0
    )
    up_other = dp_perm(up_send, 1)
    dn = [dn[0]] + [dp_perm(dn[k], 2 * k) for k in (1, 2, 3)]
    p_y = head_perm(p_far, 2)
    gt, ctx = attention(lens, pos, cos, sin, qt, kt, vt, dot, kn, vn, own, tok // 2, halved=True)
    out_t, g, wup, wdn, wq, wout, sums = tail_stage(
        gt, na, g_mlp, ctx, dy_all, wt, w_out, up_keep, up_other, dn, inputs, p_own, p_y,
        attn_gain, attn_shift, b_out, b_down, small, smallf, 1
    )
    return tuple(final_stage(out_t, g, inputs, cotangent, wup, wdn, wq, wout, sums))


def general_body(inputs, lengths, attn_gain, attn_shift, mlp_gain, mlp_shift, w_qkv, b_qkv, w_out, b_out,
                 w_up, b_up, w_down, b_down, cotangent):
    own, d = inputs.shape
    n = lax.axis_size("head")
    n_dp = lax.axis_size("dp")
    tok = own * n
    w = d // n
    f = w_up.shape[1] // n
    j = lax.axis_index("head")
    pos = j.astype(jnp.int32).reshape(1)
    rows = lambda v: v.reshape(1, -1)
    ga, sa, gm, sm = rows(attn_gain), rows(attn_shift), rows(mlp_gain), rows(mlp_shift)
    bq, bu = rows(b_qkv), rows(b_up)
    lens = lengths[0]
    gather = lambda v: lax.all_gather(v, "head", axis=0, tiled=True)
    over_dp = lambda v, axis: lax.psum_scatter(v, "dp", scatter_dimension=axis, tiled=True)
    over_head = lambda v: lax.psum_scatter(v, "head", scatter_dimension=0, tiled=True)
    x_all = gather(inputs)
    dy_all = gather(cotangent)
    first, position = layout(lens, jnp.arange(tok, dtype=jnp.int32))
    freqs = 10000.0 ** (-(2.0 * jnp.arange(HALF, dtype=F32)) / ROT)
    angle = freqs[:, None] * position.astype(F32)[None, :]
    cos, sin = jnp.cos(angle), jnp.sin(angle)
    part, g_mlp, dwu, dwd, small, smallf = mlp(pos, x_all, dy_all, w_up, w_down, bu, gm, sm, n)
    qt, kt, vt, dot, kn, vn, na = proj(pos, x_all, dy_all, w_qkv, bq, w_out, ga, sa, cos, sin, n, tok, 0)
    gt, ctx = attention(
        lens, jnp.zeros((1,), jnp.int32), cos, sin, qt, kt, vt, dot, kn, vn, own, tok // 2
    )
    total, dwq, bias_q, small_q = post(pos, gt, na, g_mlp, w_qkv, ga, sa, n)
    attn_part = mm(ctx, lax.dynamic_slice_in_dim(w_out, j * w, w, 0), TN)
    bias = b_out.astype(F32) + b_down.astype(F32)
    output = inputs.astype(F32) + over_head((attn_part + part.astype(F32)).astype(BF)).astype(F32) + bias
    g_sum = over_head(total).astype(F32)
    normed, inv = norm_parts(inputs)
    grad_inputs = cotangent.astype(F32) + inv * (
        g_sum - jnp.mean(g_sum, axis=-1, keepdims=True) - normed * jnp.mean(g_sum * normed, axis=-1, keepdims=True)
    )
    dw_out = mm(ctx, dy_all).astype(BF)
    spread = lambda v: lax.all_to_all(v, "head", split_axis=1, concat_axis=0, tiled=True)
    grad_w_up = over_dp(dwu, 0).astype(F32)
    grad_w_down = over_dp(spread(dwd), 0).astype(F32)
    grad_w_out = over_dp(spread(dw_out), 0).astype(F32)
    qkv = over_dp(jnp.transpose(dwq, (0, 2, 1)).reshape(d, 3 * w), 0)
    qkv = lax.all_gather(qkv.reshape(d // n_dp, 3, w), "head", axis=2, tiled=True).reshape(d // n_dp, 3 * d)
    grad_w_qkv = lax.dynamic_slice_in_dim(qkv, j * 3 * w, 3 * w, 1).astype(F32)
    slots = jnp.where(jnp.arange(n)[:, None] == j, smallf[0:1], 0.0).reshape(-1)
    slots_q = jnp.where(jnp.arange(n)[None, :, None] == j, bias_q[0].reshape(3, 1, w), 0.0).reshape(-1)
    sums = lax.psum((small_q[0], small_q[1], small[0], small[1], slots_q, small[2] / n, slots), ("dp", "head"))
    return (output.astype(BF), grad_inputs, sums[0], sums[1], sums[2], sums[3], grad_w_qkv, sums[4],
            grad_w_out, sums[5], grad_w_up, sums[6], grad_w_down, sums[5])


def solution(mesh):
    fast = mesh.shape["dp"] == 8 and mesh.shape["head"] == 4
    whole = P(("dp", "head"), None)
    weight = P("dp", "head")
    return jax.shard_map(
        fast_body if fast else general_body,
        mesh=mesh,
        in_specs=(whole, P("dp", None)) + (P(),) * 12 + (whole,),
        out_specs=(whole, whole, P(), P(), P(), P(), weight, P(), weight, P(), weight, P(), weight, P()),
        check_vma=False,
    )
```

```python
import functools

import jax
import jax.numpy as jnp
import numpy as np
from jax import lax
from jax.experimental import pallas as pl
from jax.experimental.pallas import tpu as pltpu
from jax.sharding import PartitionSpec as P

HD = 64
ROT = 16
HALF = ROT // 2
NN = (((1,), (0,)), ((), ()))
NT = (((1,), (1,)), ((), ()))
TN = (((0,), (0,)), ((), ()))
FREQS = (10000.0 ** (-(2.0 * np.arange(HALF)) / ROT)).astype(np.float32)
BF = jnp.bfloat16
F32 = jnp.float32
VMEM_LIMIT = 62 * 1024 * 1024


def mm(a, b, dims=NN):
    return lax.dot_general(a, b, dims, preferred_element_type=F32)


def flat(v):
    return v.astype(F32).reshape(1, v.shape[0])


def norm_parts(x):
    v = x.astype(F32)
    center = v - jnp.mean(v, axis=-1, keepdims=True)
    inv = lax.rsqrt(jnp.mean(center * center, axis=-1, keepdims=True) + 1e-5)
    return center * inv, inv


def mlp_kernel(prev, final, pos, *refs):
    x_ref, dy_ref, wu, wd, bu, gain, shift = refs[:7]
    refs = refs[7:]
    if prev:
        pwu, pwd, psmall, psmallf = refs[:4]
        refs = refs[4:]
    part_ref, g_ref, out_wu, out_wd, small, smallf = refs[:6]
    if final:
        dwu, dwd = refs[6:8]
    else:
        dwu, dwd = out_wu, out_wd
    step = pl.program_id(0)

    @pl.when(step == 0)
    def _():
        if prev:
            dwu[...] = pwu[...]
            dwd[...] = pwd[...]
            small[...] = psmall[...]
            smallf[...] = psmallf[...]
        else:
            dwu[...] = jnp.zeros_like(dwu)
            dwd[...] = jnp.zeros_like(dwd)
            small[...] = jnp.zeros_like(small)
            smallf[...] = jnp.zeros_like(smallf)

    normed, _unused = norm_parts(x_ref[...])
    scale = gain[...].astype(F32)
    nm = (normed * scale + shift[...].astype(F32)).astype(BF)
    dy = dy_ref[...]
    pre = mm(nm, wu[...]) + bu[...].astype(F32)
    cdf = 0.5 + 0.5 * lax.erf(pre * (0.5**0.5))
    hid = (pre * cdf).astype(BF)
    slope = cdf + pre * (jnp.exp(-0.5 * pre * pre) * 0.3989422804014327)
    gp = (mm(dy, wd[...], NT) * slope).astype(BF)
    part_ref[...] = mm(hid, wd[...]).astype(BF)
    r = mm(gp, wu[...], NT)
    g_ref[...] = (r * scale).astype(BF)
    smallf[0:1, :] += jnp.sum(gp.astype(F32), axis=0, keepdims=True)
    small[0:1, :] += jnp.sum(r * normed, axis=0, keepdims=True)
    small[1:2, :] += jnp.sum(r, axis=0, keepdims=True)
    small[2:3, :] += jnp.sum(dy.astype(F32), axis=0, keepdims=True)
    dwd[...] += mm(hid, dy, TN)
    dwu[...] += mm(nm, gp, TN)

    if final:

        @pl.when(step == pl.num_programs(0) - 1)
        def _():
            out_wu[...] = dwu[...].astype(BF)
            out_wd[...] = dwd[...].astype(BF)


def mlp(pos, x, dy, wu, wd, bu, gain, shift, n, prev=None, final=True, tt=512):
    tok, d = x.shape
    f = wu.shape[1] // n
    row = lambda i, p: (i, 0)
    zero = lambda i, p: (0, 0)
    one = pl.Buffered(1)
    const = lambda shape: pl.BlockSpec(shape, zero, pipeline_mode=one)
    accs = [const((d, f)), const((f, d)), const((8, d)), const((8, f))]
    kind = BF if final else F32
    grid_spec = pltpu.PrefetchScalarGridSpec(
        num_scalar_prefetch=1,
        grid=(tok // tt,),
        in_specs=[
            pl.BlockSpec((tt, d), row),
            pl.BlockSpec((tt, d), row),
            pl.BlockSpec((d, f), lambda i, p: (0, p[0]), pipeline_mode=one),
            pl.BlockSpec((f, d), lambda i, p: (p[0], 0), pipeline_mode=one),
            pl.BlockSpec((1, f), lambda i, p: (0, p[0])),
            const((1, d)),
            const((1, d)),
        ]
        + (accs if prev is not None else []),
        out_specs=[pl.BlockSpec((tt, d), row), pl.BlockSpec((tt, d), row)] + accs,
        scratch_shapes=[pltpu.VMEM((d, f), F32), pltpu.VMEM((f, d), F32)] if final else [],
    )
    return pl.pallas_call(
        functools.partial(mlp_kernel, prev is not None, final),
        grid_spec=grid_spec,
        out_shape=(
            jax.ShapeDtypeStruct((tok, d), BF),
            jax.ShapeDtypeStruct((tok, d), BF),
            jax.ShapeDtypeStruct((d, f), kind),
            jax.ShapeDtypeStruct((f, d), kind),
            jax.ShapeDtypeStruct((8, d), F32),
            jax.ShapeDtypeStruct((8, f), F32),
        ),
        compiler_params=pltpu.CompilerParams(vmem_limit_bytes=VMEM_LIMIT),
        cost_estimate=pl.CostEstimate(
            flops=12 * tok * d * f, bytes_accessed=8 * tok * d + 12 * d * f, transcendentals=2 * tok * f
        ),
        name="mlp",
    )(pos, x, dy, wu, wd, bu, gain, shift, *(prev or ()))


def proj_kernel(nh, prev, pos, *refs):
    x_ref, dy_ref, wq, wk, wv, bq, bk, bv, wo, gain, shift, cos, sin = refs[:13]
    qt, kt, vt, dot, kn, vn, na_ref = refs[13 + (7 if prev else 0) :]
    normed, _unused = norm_parts(x_ref[...])
    na = (normed * gain[...].astype(F32) + shift[...].astype(F32)).astype(BF)
    na_ref[...] = na
    co = cos[...]
    si = sin[...]

    def rotated(t, scale):
        rows = []
        for h in range(nh):
            u = t[h * HD : (h + 1) * HD]
            u1 = u[:HALF]
            u2 = u[HALF:ROT]
            rows += [u1 * co - u2 * si, u2 * co + u1 * si, u[ROT:]]
        out = jnp.concatenate(rows, axis=0).astype(BF)
        return out if scale is None else out * jnp.asarray(scale, BF)

    def triple(w, b):
        return (mm(na, w[...]) + b[...].astype(F32)).astype(BF)

    qt[...] = rotated(triple(wq, bq).astype(F32).T, HD**-0.5)
    keys = rotated(triple(wk, bk).astype(F32).T, None)
    kt[...] = keys
    kn[...] = keys.T
    values = triple(wv, bv)
    vn[...] = values
    vt[...] = values.T
    dot[...] = mm(wo[...], dy_ref[...], NT).astype(BF)


def proj(pos, x, dy, w_qkv, b_qkv, w_out, gain, shift, cos, sin, n, total, first, prev=None, tt=512):
    tok, d = x.shape
    w = d // n
    nh = w // HD
    off = first // tt
    row = lambda i, p: (i, 0)
    zero = lambda i, p: (0, 0)
    one = pl.Buffered(1)
    wspec = lambda k: pl.BlockSpec((d, w), lambda i, p: (0, k * n + p[0]), pipeline_mode=one)
    bspec = lambda k: pl.BlockSpec((1, w), lambda i, p: (0, k * n + p[0]))
    lane = lambda rows: pl.BlockSpec((rows, tt), lambda i, p: (0, off + i))
    nat = lambda cols: pl.BlockSpec((tt, cols), lambda i, p: (off + i, 0))
    shapes = [(w, total)] * 4 + [(total, w)] * 2 + [(total, d)]
    grid_spec = pltpu.PrefetchScalarGridSpec(
        num_scalar_prefetch=1,
        grid=(tok // tt,),
        in_specs=[pl.BlockSpec((tt, d), row), pl.BlockSpec((tt, d), row)]
        + [wspec(0), wspec(1), wspec(2), bspec(0), bspec(1), bspec(2)]
        + [pl.BlockSpec((w, d), lambda i, p: (p[0], 0), pipeline_mode=one)]
        + [pl.BlockSpec((1, d), zero), pl.BlockSpec((1, d), zero), lane(HALF), lane(HALF)]
        + ([pl.BlockSpec(memory_space=pl.ANY)] * 7 if prev is not None else []),
        out_specs=[lane(w)] * 4 + [nat(w)] * 2 + [nat(d)],
    )
    return pl.pallas_call(
        functools.partial(proj_kernel, nh, prev is not None),
        grid_spec=grid_spec,
        out_shape=tuple(jax.ShapeDtypeStruct(s, BF) for s in shapes),
        input_output_aliases={14 + k: k for k in range(7)} if prev is not None else {},
        compiler_params=pltpu.CompilerParams(vmem_limit_bytes=VMEM_LIMIT),
        cost_estimate=pl.CostEstimate(
            flops=8 * tok * d * w, bytes_accessed=6 * tok * d + 12 * tok * w + 8 * d * w, transcendentals=0
        ),
        name="proj",
    )(pos, x, dy, w_qkv, w_qkv, w_qkv, b_qkv, b_qkv, b_qkv, w_out, gain, shift, cos, sin, *(prev or ()))


def head_kernel(nh, x_hbm, dy_hbm, wu_hbm, wd_hbm, wqkv_hbm, wo_hbm, gain_a, shift_a, gain_m, shift_m, bu, bq, lens,
                g_out, na_out, dy_out, qt, kt, vt, dot, kn, vn, cos, sin, p_own, p_far, up_keep, up_send, dn0, dn1, dn2, dn3,
                w_t, small, smallf,
                xs, dys, wu, wd, wqkv, wt, wo, bias_t, bias_all, bias_u, parts, far_in, near_in, dwu, dwd, load, send, recv):
    step = pl.program_id(0)
    i = lax.axis_index("dp")
    j = lax.axis_index("head")
    own, d = x_hbm.shape
    f = wu.shape[1]
    w = wo.shape[0]
    half = own // 2
    core = {"head": j ^ 1}
    across = {"head": j ^ 2}

    def remote(src, dst, k, to):
        return pltpu.make_async_remote_copy(
            src_ref=src, dst_ref=dst, send_sem=send.at[k], recv_sem=recv.at[k], device_id=to,
            device_id_type=pl.DeviceIdType.MESH)

    lo, hi = pl.ds(0, half), pl.ds(half, half)
    copies = [
        remote(x_hbm, xs.at[1], 0, core),
        remote(dy_hbm, dys.at[1], 1, core),
        remote(x_hbm.at[lo], xs.at[2, lo], 2, across),
        remote(dy_hbm.at[lo], dys.at[2, lo], 3, across),
        remote(x_hbm.at[hi], xs.at[3, lo], 4, across),
        remote(dy_hbm.at[hi], dys.at[3, lo], 5, across),
        remote(xs.at[2, lo], xs.at[2, hi], 6, core),
        remote(dys.at[2, lo], dys.at[2, hi], 7, core),
        remote(xs.at[3, lo], xs.at[3, hi], 8, core),
        remote(dys.at[3, lo], dys.at[3, hi], 9, core),
        remote(parts.at[1], near_in, 10, core),
        remote(parts.at[2, hi], far_in.at[lo], 11, core),
        remote(parts.at[3, hi], far_in.at[hi], 12, core),
    ]
    locals_ = [
        pltpu.make_async_copy(x_hbm, xs.at[0], load.at[0]),
        pltpu.make_async_copy(dy_hbm, dys.at[0], load.at[1]),
        pltpu.make_async_copy(wo_hbm.at[pl.ds(j * w, w)], wo, load.at[2]),
    ] + [
        pltpu.make_async_copy(wqkv_hbm.at[:, pl.ds(k * d + j * w, w)], wqkv.at[:, pl.ds(k * w, w)], load.at[3 + k])
        for k in range(3)
    ]
    part = f // 8
    for k in range(8):
        there, here = pl.ds(4 * k * part + j * part, part), pl.ds(k * part, part)
        locals_.append(pltpu.make_async_copy(wu_hbm.at[:, there], wu.at[:, here], load.at[6 + k]))
        locals_.append(pltpu.make_async_copy(wd_hbm.at[there], wd.at[here], load.at[14 + k]))

    @pl.when(step == 0)
    def _():
        barrier = pltpu.get_barrier_semaphore()
        for to in (core, across):
            pl.semaphore_signal(barrier, inc=1, device_id=to, device_id_type=pl.DeviceIdType.MESH)
        for c in locals_:
            c.start()
        pl.semaphore_wait(barrier, 2)
        for c in copies[:6]:
            c.start()
        dwu[...] = jnp.zeros_like(dwu)
        dwd[...] = jnp.zeros_like(dwd)
        small[...] = jnp.zeros_like(small)
        smallf[...] = jnp.zeros_like(smallf)
        for c in locals_:
            c.wait()
        for k in range(3):
            wt[k * w : (k + 1) * w, :] = wqkv[:, k * w : (k + 1) * w].T
            row = flat(bq[pl.ds(pl.multiple_of(k * d + j * w, 256), w)])
            bias_t[k * w : (k + 1) * w, :] = jnp.broadcast_to(row, (128, w)).T
        bias_all[0:1, :] = flat(bu[...])
        for k in range(8):
            bias_u[0:1, k * part : (k + 1) * part] = bias_all[0:1, pl.ds(pl.multiple_of(4 * k * part + j * part, 128), part)]

    @pl.when(step == 1)
    def _():
        copies[0].wait_recv()

    @pl.when(step == 2)
    def _():
        copies[6].wait_recv()

    @pl.when(step == 3)
    def _():
        copies[8].wait_recv()

    normed, _unused = norm_parts(xs[step])
    scale = flat(gain_m[...])
    nm = (normed * scale + flat(shift_m[...])).astype(BF)
    na = (normed * flat(gain_a[...]) + flat(shift_a[...])).astype(BF)
    na_out[...] = na
    pre = mm(nm, wu[...]) + bias_u[0:1, :]
    cdf = 0.5 + 0.5 * lax.erf(pre * (0.5**0.5))
    hid = (pre * cdf).astype(BF)
    slope = cdf + pre * (jnp.exp(-0.5 * pre * pre) * 0.3989422804014327)
    parts[step] = mm(hid, wd[...]).astype(BF)

    lane = lax.broadcasted_iota(jnp.int32, (1, own), 1)
    far = jnp.where(lane < half, j ^ 2, j ^ 3) * own + (step - 2) * half + lane % half
    index = jnp.where(step == 0, j * own + lane, jnp.where(step == 1, (j ^ 1) * own + lane, far))
    begin = jnp.zeros_like(index)
    total = jnp.int32(0)
    for s in range(lens.shape[0] - 1):
        total = total + lens[s]
        begin = jnp.where(index >= total, total, begin)
    sub = lax.broadcasted_iota(jnp.int32, (HALF, own), 0)
    freqs = jnp.zeros((HALF, own), F32)
    for k in range(HALF):
        freqs = jnp.where(sub == k, float(FREQS[k]), freqs)
    angle = freqs * (index - begin).astype(F32)
    co = jnp.cos(angle)
    si = jnp.sin(angle)
    cos[...] = co
    sin[...] = si

    def projected(k):
        b = bias_t[k * w : (k + 1) * w, :]
        t = mm(wt[k * w : (k + 1) * w, :], na, NT)
        return (t + jnp.concatenate([b] * (own // 128), axis=1)).astype(BF)

    def rotated(t, factor):
        rows = []
        for h in range(nh):
            u = t[h * HD : (h + 1) * HD].astype(F32)
            u1 = u[:HALF]
            u2 = u[HALF:ROT]
            rows += [u1 * co - u2 * si, u2 * co + u1 * si, u[ROT:]]
        out = jnp.concatenate(rows, axis=0)
        return (out if factor is None else out * factor).astype(BF)

    qt[...] = rotated(projected(0), HD**-0.5)
    keys = rotated(projected(1), None)
    kt[...] = keys
    kn[...] = keys.T
    values = projected(2)
    vt[...] = values
    vn[...] = values.T

    @pl.when(step == 1)
    def _():
        copies[1].wait_recv()
        copies[10].start()
        copies[2].wait_recv()
        copies[6].start()

    @pl.when(step == 2)
    def _():
        copies[7].wait_recv()
        copies[11].start()

    @pl.when(step == 3)
    def _():
        copies[12].start()
        copies[5].wait_recv()
        copies[9].start()
        copies[9].wait_recv()

    dy = dys[step]
    dy_out[...] = dy
    gp = (mm(dy, wd[...], NT) * slope).astype(BF)
    r = mm(gp, wu[...], NT)
    g_out[...] = (r * scale).astype(BF)
    smallf[0:1, :] += jnp.sum(gp.astype(F32), axis=0, keepdims=True)
    small[0:1, :] += jnp.sum(r * normed, axis=0, keepdims=True)
    small[1:2, :] += jnp.sum(r, axis=0, keepdims=True)
    small[2:3, :] += jnp.sum(dy.astype(F32), axis=0, keepdims=True)
    dwd[...] += mm(hid, dy, TN)
    dwu[...] += mm(nm, gp, TN)
    dot[...] = mm(wo[...], dy, NT).astype(BF)

    @pl.when(step == 1)
    def _():
        copies[3].wait_recv()
        copies[7].start()

    @pl.when(step == 2)
    def _():
        copies[4].wait_recv()
        copies[8].start()

    @pl.when(step == 3)
    def _():
        rows = dwu.shape[0] // 8
        keep = dn0.shape[1]
        for b in range(4):
            for ref, at in ((up_keep, 2 * b + i % 2), (up_send, 2 * b + 1 - i % 2)):
                at = pl.multiple_of(at * rows, rows)
                ref[b, :rows] = dwu[pl.ds(at, rows), :].astype(BF)
                ref[b, rows:] = dwd[pl.ds(at + keep, rows - keep), :].astype(BF)
            ref = (dn0, dn1, dn2, dn3)[b]
            for x in range(2):
                at = 2 * ((i // 2) ^ b) + x
                ref[x] = dwd[pl.ds(pl.multiple_of(at * rows, rows), keep), :].astype(BF)
        w_t[...] = wt[...]
        copies[10].wait_recv()
        p_own[...] = (parts[0].astype(F32) + near_in[...].astype(F32)).astype(BF)
        copies[11].wait_recv()
        p_far[lo] = (parts[2, lo].astype(F32) + far_in[lo].astype(F32)).astype(BF)
        copies[12].wait_recv()
        p_far[hi] = (parts[3, lo].astype(F32) + far_in[hi].astype(F32)).astype(BF)
        for c in copies:
            c.wait_send()


def head_stage(x, dy, w_up, w_down, w_qkv, w_out, ga, sa, gm, sm, bu, bq, lens, n, cid):
    own, d = x.shape
    tok = own * n
    w = d // n
    f = w_up.shape[1] // n
    row = lambda i: (i, 0)
    lane = lambda rows: pl.BlockSpec((rows, own), lambda i: (0, i))
    nat = lambda cols: pl.BlockSpec((own, cols), row)
    one = pl.Buffered(1)
    const = lambda shape: pl.BlockSpec(shape, lambda i: (0,) * len(shape), pipeline_mode=one)
    hbm = pl.BlockSpec(memory_space=pl.ANY)
    sds = jax.ShapeDtypeStruct
    return pl.pallas_call(
        functools.partial(head_kernel, w // HD),
        grid=(n,),
        in_specs=[hbm] * 6
        + [const(v.shape) for v in (ga, sa, gm, sm, bu, bq)]
        + [pl.BlockSpec(memory_space=pltpu.SMEM)],
        out_specs=[nat(d)] * 3
        + [lane(w)] * 4
        + [nat(w)] * 2
        + [lane(HALF)] * 2
        + [const((own, d))] * 2
        + [const((4, d // 8 + d // 32, d))] * 2
        + [const((2, 3 * d // 32, d))] * 4
        + [const((3 * w, d)), const((8, d)), const((8, f))],
        out_shape=tuple(
            [sds((tok, d), BF)] * 3
            + [sds((w, tok), BF)] * 4
            + [sds((tok, w), BF)] * 2
            + [sds((HALF, tok), F32)] * 2
            + [sds((own, d), BF)] * 2
            + [sds((4, d // 8 + d // 32, d), BF)] * 2
            + [sds((2, 3 * d // 32, d), BF)] * 4
            + [sds((3 * w, d), BF), sds((8, d), F32), sds((8, f), F32)]
        ),
        scratch_shapes=[
            pltpu.VMEM((4, own, d), BF),
            pltpu.VMEM((4, own, d), BF),
            pltpu.VMEM((d, f), BF),
            pltpu.VMEM((f, d), BF),
            pltpu.VMEM((d, 3 * w), BF),
            pltpu.VMEM((3 * w, d), BF),
            pltpu.VMEM((w, d), BF),
            pltpu.VMEM((3 * w, 128), F32),
            pltpu.VMEM((8, 4 * f), F32),
            pltpu.VMEM((8, f), F32),
            pltpu.VMEM((4, own, d), BF),
            pltpu.VMEM((own, d), BF),
            pltpu.VMEM((own, d), BF),
            pltpu.VMEM((d, f), F32),
            pltpu.VMEM((f, d), F32),
            pltpu.SemaphoreType.DMA((22,)),
            pltpu.SemaphoreType.DMA((13,)),
            pltpu.SemaphoreType.DMA((13,)),
        ],
        compiler_params=pltpu.CompilerParams(
            vmem_limit_bytes=VMEM_LIMIT, collective_id=cid, has_side_effects=True
        ),
        cost_estimate=pl.CostEstimate(
            flops=12 * tok * d * f + 10 * tok * d * w, bytes_accessed=12 * tok * d + 8 * d * f, transcendentals=2 * tok * f
        ),
        name="head_stage",
    )(x, dy, w_up, w_down, w_qkv, w_out, ga, sa, gm, sm, bu, bq, lens)


def attn_kernel(nh, tok, blk, per, halved, lens, rel, cos, sin, qt, kt, vt, dot, kn, vn,
                gt_ref, ctx_ref, exps, low_exps, dk, dv, oacc, dqacc, mpart, lpart, rowsc, qpad, dopad):
    nseq = lens.shape[0]
    nblk = tok // blk
    shift = rel[0]
    heads = range(nh)

    def place(b):
        chunk = (b // per) ^ shift
        half = b % per
        at = chunk * per + half
        if halved:
            at = jnp.where(chunk < 2, at, 4 + (chunk - 2) + 2 * half)
        return pl.multiple_of(at * blk, blk)

    def rows_of(h):
        return slice(h * HD, (h + 1) * HD)

    def pair_of(h):
        return slice((h // 2) * 128, (h // 2) * 128 + 128)

    def fold(v, op):
        return op(v.reshape(blk // 8, 8, blk), axis=0)

    def begin_of(at):
        begin = jnp.int32(0)
        total = jnp.int32(0)
        for s in range(nseq - 1):
            total = total + lens[s]
            begin = jnp.where(at >= total, total, begin)
        return begin

    dk[...] = jnp.zeros_like(dk)
    dv[...] = jnp.zeros_like(dv)
    qpad[...] = jnp.zeros_like(qpad)
    dopad[...] = jnp.zeros_like(dopad)
    rows_iota = lax.broadcasted_iota(jnp.int32, (blk, blk), 0)
    cols_iota = lax.broadcasted_iota(jnp.int32, (1, blk), 1)

    def one_block(i, carry):
        first_tok = i * blk
        count = i - begin_of(first_tok) // blk + 1
        last_begin = begin_of(first_tok + blk - 1)
        cols = pl.ds(place(i), blk)
        query_idx = cols_iota + first_tok
        start_row = begin_of(query_idx)
        for h in heads:
            half = (h % 2) * HD
            qpad[h, half : half + HD, :] = qt[rows_of(h), cols]

        krow = pl.ds(place(i), blk)
        kidx = rows_iota + first_tok
        allowed = (kidx >= start_row) & (kidx <= query_idx)
        for h in heads:
            s = jnp.where(allowed, mm(kn[krow, pair_of(h)], qpad[h]), -1e30)
            exps[h, 0] = s
            mpart[h] = fold(s, jnp.max)

        def scores(step, c):
            b = i - step
            krow = pl.ds(place(b), blk)
            edge = last_begin > b * blk

            @pl.when(edge)
            def _():
                allowed = (rows_iota + b * blk) >= start_row
                for h in heads:
                    s = jnp.where(allowed, mm(kn[krow, pair_of(h)], qpad[h]), -1e30)
                    exps[h, step] = s
                    mpart[h] = jnp.maximum(mpart[h], fold(s, jnp.max))

            @pl.when(jnp.logical_not(edge))
            def _():
                for h in heads:
                    s = mm(kn[krow, pair_of(h)], qpad[h])
                    exps[h, step] = s
                    mpart[h] = jnp.maximum(mpart[h], fold(s, jnp.max))

            return c

        lax.fori_loop(1, count, scores, 0)
        for h in heads:
            rowsc[h : h + 1, :] = jnp.max(mpart[h], axis=0, keepdims=True)
        lpart[...] = jnp.zeros_like(lpart)
        oacc[...] = jnp.zeros_like(oacc)

        def weights(step, c):
            kcols = pl.ds(place(i - step), blk)
            for h in heads:
                e = jnp.exp(exps[h, step] - rowsc[h : h + 1, :])
                exps[h, step] = e
                lpart[h] += fold(e, jnp.sum)
                low = e.astype(BF)
                low_exps[h, step] = low
                oacc[h] += mm(vt[rows_of(h), kcols], low)
            return c

        lax.fori_loop(0, count, weights, 0)
        for h in heads:
            half = (h % 2) * HD
            inv = 1.0 / jnp.sum(lpart[h], axis=0, keepdims=True)
            o = oacc[h] * inv
            ctx_ref[rows_of(h), cols] = o.astype(BF)
            scaled = (dot[rows_of(h), cols].astype(F32) * inv).astype(BF)
            dopad[h, half : half + HD, :] = scaled
            rowsc[h : h + 1, :] = jnp.sum(o * scaled.astype(F32), axis=0, keepdims=True)
        dqacc[...] = jnp.zeros_like(dqacc)

        def backward(step, c):
            kcols = pl.ds(place(i - step), blk)
            for h in heads:
                half = (h % 2) * HD
                hs = rows_of(h)
                dp = mm(vn[kcols, pair_of(h)], dopad[h])
                ds = (exps[h, step] * (dp - rowsc[h : h + 1, :])).astype(BF)
                dv[hs, kcols] += mm(dopad[h, half : half + HD, :], low_exps[h, step], NT)
                dk[hs, kcols] += mm(qt[hs, cols], ds, NT)
                dqacc[hs, :] += mm(kt[hs, kcols], ds)
            return c

        lax.fori_loop(0, count, backward, 0)
        co = cos[:, cols]
        si = sin[:, cols]
        for h in heads:
            base = h * HD
            g = dqacc[base : base + HD, :] * (HD**-0.5)
            g1 = g[:HALF]
            g2 = g[HALF:ROT]
            gt_ref[base : base + HD, cols] = jnp.concatenate(
                [g1 * co + g2 * si, g2 * co - g1 * si, g[ROT:]], axis=0
            ).astype(BF)
        return carry

    lax.fori_loop(0, nblk, one_block, 0)

    def finish(i, carry):
        cols = pl.ds(pl.multiple_of(i * blk, blk), blk)
        co = cos[:, cols]
        si = sin[:, cols]
        for h in heads:
            base = h * HD
            g = dk[base : base + HD, cols]
            g1 = g[:HALF]
            g2 = g[HALF:ROT]
            gt_ref[nh * HD + base : nh * HD + base + HD, cols] = jnp.concatenate(
                [g1 * co + g2 * si, g2 * co - g1 * si, g[ROT:]], axis=0
            ).astype(BF)
        gt_ref[2 * nh * HD :, cols] = dv[:, cols].astype(BF)
        return carry

    lax.fori_loop(0, nblk, finish, 0)


def attention(lens, rel, cos, sin, qt, kt, vt, dot, kn, vn, chunk, maxlen, halved=False, blk=256):
    width, tok = qt.shape
    nh = width // HD
    wb = maxlen // blk + 1
    vm = pl.BlockSpec(memory_space=pltpu.VMEM)
    sm = pl.BlockSpec(memory_space=pltpu.SMEM)
    return pl.pallas_call(
        functools.partial(attn_kernel, nh, tok, blk, chunk // blk, halved),
        out_shape=(jax.ShapeDtypeStruct((3 * width, tok), BF), jax.ShapeDtypeStruct((width, tok), BF)),
        in_specs=[sm, sm] + [vm] * 8,
        out_specs=(vm, vm),
        scratch_shapes=[
            pltpu.VMEM((nh, wb, blk, blk), F32),
            pltpu.VMEM((nh, wb, blk, blk), BF),
            pltpu.VMEM((width, tok), F32),
            pltpu.VMEM((width, tok), F32),
            pltpu.VMEM((nh, HD, blk), F32),
            pltpu.VMEM((width, blk), F32),
            pltpu.VMEM((nh, 8, blk), F32),
            pltpu.VMEM((nh, 8, blk), F32),
            pltpu.VMEM((8, blk), F32),
            pltpu.VMEM((nh, 128, blk), BF),
            pltpu.VMEM((nh, 128, blk), BF),
        ],
        compiler_params=pltpu.CompilerParams(vmem_limit_bytes=VMEM_LIMIT),
        cost_estimate=pl.CostEstimate(
            flops=20 * width * tok * maxlen, bytes_accessed=20 * width * tok, transcendentals=nh * tok * maxlen
        ),
        name="attention",
    )(lens, rel, cos, sin, qt, kt, vt, dot, kn, vn)


def post_kernel(pos, gt_ref, na_ref, gm_ref, wq, wk, wv, gain, shift, g_ref, out_w, bias, small, dw):
    step = pl.program_id(0)

    @pl.when(step == 0)
    def _():
        dw[...] = jnp.zeros_like(dw)
        bias[...] = jnp.zeros_like(bias)
        small[...] = jnp.zeros_like(small)

    gt = gt_ref[...]
    na = na_ref[...]
    w = wq.shape[1]
    scale = gain[...].astype(F32)
    gn = gt.T
    r = mm(gn[:, :w], wq[...], NT) + mm(gn[:, w : 2 * w], wk[...], NT) + mm(gn[:, 2 * w :], wv[...], NT)
    g_ref[...] = (r * scale + gm_ref[...].astype(F32)).astype(BF)
    small[0:1, :] += jnp.sum(r * na.astype(F32), axis=0, keepdims=True)
    small[1:2, :] += jnp.sum(r, axis=0, keepdims=True)
    bias[0:1, :] += jnp.sum(gn.astype(F32), axis=0, keepdims=True)
    dw[...] += mm(gt, na)

    @pl.when(step == pl.num_programs(0) - 1)
    def _():
        for b in range(dw.shape[1] // 128):
            out_w[b] = dw[:, b * 128 : (b + 1) * 128].astype(BF)
        small[0:1, :] = (small[0:1, :] - shift[...].astype(F32) * small[1:2, :]) / scale


def post(pos, gt, na, gm, w_qkv, gain, shift, n, tt=512):
    tok, d = na.shape
    w = d // n
    row = lambda i, p: (i, 0)
    zero = lambda i, p: (0, 0)
    one = pl.Buffered(1)
    const = lambda shape: pl.BlockSpec(shape, zero, pipeline_mode=one)
    wspec = lambda k: pl.BlockSpec((d, w), lambda i, p: (0, k * n + p[0]), pipeline_mode=one)
    grid_spec = pltpu.PrefetchScalarGridSpec(
        num_scalar_prefetch=1,
        grid=(tok // tt,),
        in_specs=[
            pl.BlockSpec((3 * w, tt), lambda i, p: (0, i)),
            pl.BlockSpec((tt, d), row),
            pl.BlockSpec((tt, d), row),
            wspec(0),
            wspec(1),
            wspec(2),
            const((1, d)),
            const((1, d)),
        ],
        out_specs=[
            pl.BlockSpec((tt, d), row),
            pl.BlockSpec((d // 128, 3 * w, 128), lambda i, p: (0, 0, 0), pipeline_mode=one),
            const((8, 3 * w)),
            const((8, d)),
        ],
        scratch_shapes=[pltpu.VMEM((3 * w, d), F32)],
    )
    return pl.pallas_call(
        post_kernel,
        grid_spec=grid_spec,
        out_shape=(
            jax.ShapeDtypeStruct((tok, d), BF),
            jax.ShapeDtypeStruct((d // 128, 3 * w, 128), BF),
            jax.ShapeDtypeStruct((8, 3 * w), F32),
            jax.ShapeDtypeStruct((8, d), F32),
        ),
        compiler_params=pltpu.CompilerParams(vmem_limit_bytes=VMEM_LIMIT),
        cost_estimate=pl.CostEstimate(
            flops=12 * tok * d * w, bytes_accessed=8 * tok * d + 6 * tok * w + 18 * d * w, transcendentals=0
        ),
        name="post",
    )(pos, gt, na, gm, w_qkv, w_qkv, w_qkv, gain, shift)


def tail_kernel(gt_h, na_h, gm_h, ctx_h, dya_h, wt_h, wo_h, upk_h, upo_h, dn0_h, dn1_h, dn2_h, dn3_h, x_h, pown_h, py_h,
                gain, shift_ref, bo, bd, small, smallf,
                out_ref, g_ref, wup_ref, wdn_ref, wq_ref, wout_ref, sums_ref,
                gt, na, gm, ctx, dya, wt, wo, upk, upo, dn, xo, pown, py,
                ctx_in, up4, up_in, dn_in, dn2,
                dwq, qa_in, qb_in, qa4, qb4, qa_in2, qb_in2, qa2, qb2, qa_in3, qb_in3, qfin, q_own,
                dwo, wo_in, wo4, wo_in2, wo2, wo_in3, fin, piece2, own_in, owner_in2,
                far_in, near_in, far_sum, y_in, sm, sm_in, load, send, recv):
    i = lax.axis_index("dp")
    j = lax.axis_index("head")
    own, d = x_h.shape
    w = wt.shape[0] // 3
    half = own // 2
    bx = i % 2
    b0 = (i // 2) % 2
    b1 = i // 4
    z = i // 2
    mesh_id = pl.DeviceIdType.MESH
    core, across, diag = {"head": j ^ 1}, {"head": j ^ 2}, {"head": j ^ 3}
    px, p0, p1 = {"dp": i ^ 1}, {"dp": i ^ 2}, {"dp": i ^ 4}
    lo, hi = pl.ds(0, half), pl.ds(half, half)
    count = [0]
    started = []

    def remote(src, dst, to):
        k = count[0]
        count[0] += 1
        return pltpu.make_async_remote_copy(
            src_ref=src, dst_ref=dst, send_sem=send.at[k], recv_sem=recv.at[k], device_id=to, device_id_type=mesh_id)

    def go(*copies):
        for c in copies:
            c.start()
            started.append(c)

    def local(src, dst, k):
        return pltpu.make_async_copy(src, dst, load.at[k])

    loads = [
        local(upk_h, upk, 0), local(upo_h, upo, 1),
        local(dn0_h, dn.at[0], 2), local(dn1_h, dn.at[1], 3), local(dn2_h, dn.at[2], 4), local(dn3_h, dn.at[3], 5),
        local(gt_h, gt, 6), local(na_h, na, 7), local(wt_h, wt, 8), local(ctx_h, ctx, 9), local(dya_h, dya, 10),
        local(gm_h, gm, 11), local(wo_h, wo, 12), local(x_h, xo, 13), local(pown_h, pown, 14), local(py_h, py, 15),
    ]
    c_ctx = [
        remote(ctx_h.at[:, pl.ds(2 * own, half)], ctx_in.at[1, :, lo], across),
        remote(ctx_h.at[:, pl.ds(3 * own, half)], ctx_in.at[1, :, hi], across),
        remote(ctx_h.at[:, pl.ds(2 * own + half, half)], ctx_in.at[2, :, lo], diag),
        remote(ctx_h.at[:, pl.ds(3 * own + half, half)], ctx_in.at[2, :, hi], diag),
        remote(ctx_h.at[:, pl.ds(own, own)], ctx_in.at[0], core),
    ]
    c_up = [remote(up4.at[z ^ k], up_in.at[k - 1], {"dp": i ^ (2 * k)}) for k in (1, 2, 3)]
    c_dnx = remote(dn2.at[1 - bx], dn_in, px)
    rows = dwq.shape[3] // 2
    ra, rb = pl.ds(0, rows), pl.ds(rows, rows)
    c_qa = remote(dwq.at[:, :, 1 - bx, ra], qa_in, px)
    c_qb = remote(dwq.at[:, :, 1 - bx, rb], qb_in, px)
    c_qa0 = remote(qa4.at[:, 1 - b0], qa_in2, p0)
    c_qb0 = remote(qb4.at[:, 1 - b0], qb_in2, p0)
    c_qa1 = remote(qa2.at[1 - b1], qa_in3, p1)
    c_qb1 = remote(qb2.at[1 - b1], qb_in3, p1)
    c_wox = remote(dwo.at[:, :, 1 - bx], wo_in, px)
    c_wo0 = remote(wo4.at[:, 1 - b0], wo_in2, p0)
    c_wo1 = remote(wo2.at[1 - b1], wo_in3, p1)
    c_g = [
        remote(gm.at[pl.ds(2 * own + half, half)], far_in.at[lo], core),
        remote(gm.at[pl.ds(3 * own + half, half)], far_in.at[hi], core),
        remote(gm.at[pl.ds(own, own)], near_in, core),
    ]
    c_y = [remote(far_sum.at[lo], y_in.at[lo], across), remote(far_sum.at[hi], y_in.at[hi], across)]
    c_sm = [remote(sm.at[s], sm_in.at[s], to) for s, to in enumerate((core, across, px, p0, p1))]
    c_own = [remote(fin.at[j ^ r], own_in.at[j], {"head": j ^ r}) for r in (1, 2, 3)]
    dests = []
    c_own2 = []
    for r in range(4):
        di, dj = 2 * j + i // 4, (i % 4) ^ r
        dests.append((di, dj))
        cut = pl.ds(pl.multiple_of(dj * w, 128), w)
        c_own2.append(remote(piece2.at[:, cut], owner_in2.at[i % 4], {"dp": di, "head": dj}))
    c_q = []
    q_dst = []
    for t in range(3):
        dst = (t - j + 4) % 4
        q_dst.append(dst)
        c_q.append(remote(qfin.at[(3 * dst + t) // 4], q_own.at[t], {"head": dst}))

    barrier = pltpu.get_barrier_semaphore()
    for to in (core, across, diag, px, p0, p1, {"dp": i ^ 6}):
        pl.semaphore_signal(barrier, inc=1, device_id=to, device_id_type=mesh_id)
    for c in loads:
        c.start()
    for r in range(4):
        si, sj = 4 * (i % 2) + (j ^ r), i // 2

        @pl.when((si != i) | (sj != j))
        def _():
            pl.semaphore_signal(barrier, inc=1, device_id={"dp": si, "head": sj}, device_id_type=mesh_id)

    to_self = jnp.where(2 * j + i // 4 == i, 1, 0)
    pl.semaphore_wait(barrier, 11 - to_self)

    go(*c_ctx)

    def added(a, b):
        return a.astype(F32) + b.astype(F32)

    def ready(first, last):
        for k in range(first, last):
            loads[k].wait()

    ready(0, 2)
    up4[...] = added(upk[...], upo[...]).astype(BF)
    go(*c_up)
    ready(2, 6)
    dn2[...] = (added(dn[0], dn[1]) + added(dn[2], dn[3])).astype(BF)
    go(c_dnx)

    ready(6, 9)
    gains = [jnp.zeros((1, 256), F32)] * 4
    for part, c in ((ra, c_qa), (rb, c_qb)):
        left = gt[part, :]
        for k in range(4):
            t = mm(left, na[:, 256 * k : 256 * (k + 1)])
            gains[k] += jnp.sum(t * wt[part, 256 * k : 256 * (k + 1)].astype(F32), axis=0, keepdims=True)
            t = t.astype(BF)
            dwq[k // 2, k % 2, 0, part] = t[:, :128]
            dwq[k // 2, k % 2, 1, part] = t[:, 128:]
        if c is c_qa:
            go(c)
    s_bias = mm(jnp.ones((8, gt.shape[1]), BF), gt[...], NT)[0:1]
    high = s_bias.astype(BF)
    low = (s_bias - high.astype(F32)).astype(BF)
    s_shift = mm(jnp.broadcast_to(high, (8, 3 * w)), wt[...])[0:1] + mm(jnp.broadcast_to(low, (8, 3 * w)), wt[...])[0:1]
    s_gain = jnp.concatenate(gains, axis=1)
    scale = flat(gain[...])

    sm[0] = jnp.zeros((16, d), F32)
    sm[0, 0:1, :] = (s_gain - flat(shift_ref[...]) * s_shift) / scale
    sm[0, 1:2, :] = s_shift
    for k in range(3):
        sm[0, 2 + k : 3 + k, pl.ds(pl.multiple_of(j * w, 128), w)] = s_bias[:, k * w : (k + 1) * w]
    sm[0, 5:7, :] = small[0:2, :]
    sm[0, 7:8, :] = small[2:3, :] * 0.25
    part_u = d // 8
    for b in range(8):
        at = pl.multiple_of((b % 2) * 4 * part_u + j * part_u, 128)
        sm[0, 8 + b // 2 : 9 + b // 2, pl.ds(at, part_u)] = smallf[0:1, b * part_u : (b + 1) * part_u]
    go(c_sm[0])

    def small_step(s):
        c_sm[s].wait_recv()
        sm[s + 1] = sm[s] + sm_in[s]
        if s < 4:
            go(c_sm[s + 1])

    ready(9, 11)
    t = mm(ctx[...], dya[...]).astype(BF)
    for b in range(8):
        dwo[b // 4, (b // 2) % 2, b % 2] = t[32 * b : 32 * (b + 1)]
    small_step(0)

    ready(11, 12)

    def tile(at):
        ts = slice(at, at + own)
        r = mm(gt[:, ts].T, wt[...])
        gm[ts, :] = (r * scale + gm[ts, :].astype(F32)).astype(BF)

    tile(2 * own)
    go(c_g[0])
    tile(3 * own)
    go(c_g[1])
    c_g[0].wait_recv()
    far_sum[lo] = added(gm[2 * own : 2 * own + half], far_in[lo]).astype(BF)
    go(c_y[0])
    small_step(1)
    go(c_qb, c_wox)
    c_g[1].wait_recv()
    far_sum[hi] = added(gm[3 * own : 3 * own + half], far_in[hi]).astype(BF)
    go(c_y[1])
    tile(own)
    go(c_g[2])
    small_step(2)
    c_qa.wait_recv()
    qa4[...] = added(dwq[:, :, bx, ra], qa_in[...]).astype(BF)
    go(c_qa0)
    tile(0)
    small_step(3)

    ready(12, 16)
    attn = mm(ctx[:, :own], wo[pl.ds(pl.multiple_of(j * w, 128), w), :], TN)
    c_ctx[4].wait_recv()
    attn += mm(ctx_in[0], wo[pl.ds(pl.multiple_of((j ^ 1) * w, 128), w), :], TN)
    for k in range(4):
        c_ctx[k].wait_recv()
    attn += mm(ctx_in[1], wo[pl.ds(pl.multiple_of((j ^ 2) * w, 128), w), :], TN)
    attn += mm(ctx_in[2], wo[pl.ds(pl.multiple_of((j ^ 3) * w, 128), w), :], TN)
    out_ref[...] = (
        xo[...].astype(F32) + attn + added(pown[...], py[...]) + (flat(bo[...]) + flat(bd[...]))
    ).astype(BF)

    c_qa0.wait_recv()
    qa2[...] = added(qa4[:, b0], qa_in2[...]).astype(BF)
    go(c_qa1)
    c_qb.wait_recv()
    qb4[...] = added(dwq[:, :, bx, rb], qb_in[...]).astype(BF)
    go(c_qb0)
    for c in c_up:
        c.wait_recv()
    c_dnx.wait_recv()
    mine = up4[z].astype(F32) + up_in[0].astype(F32) + added(up_in[1], up_in[2])
    nu = wup_ref.shape[0]
    nd = dn2.shape[1]
    down = added(dn2[bx], dn_in[...])
    for a in range(4):
        cut = slice(a * w, (a + 1) * w)
        fin[a, :nu] = mine[:nu, cut].astype(BF)
        fin[a, nu : nu + nd] = down[:, cut].astype(BF)
        fin[a, nu + nd :] = mine[nu:, cut].astype(BF)
    go(*c_own)
    own_in[j] = fin[j]
    small_step(4)
    sums_ref[...] = sm[5]
    c_wox.wait_recv()
    wo4[...] = added(dwo[:, :, bx], wo_in[...]).astype(BF)
    go(c_wo0)
    c_qb0.wait_recv()
    qb2[...] = added(qb4[:, b0], qb_in2[...]).astype(BF)
    go(c_qb1)
    c_wo0.wait_recv()
    wo2[...] = added(wo4[:, b0], wo_in2[...]).astype(BF)
    go(c_wo1)
    c_qa1.wait_recv()
    c_qb1.wait_recv()
    done = jnp.concatenate([added(qa2[b1], qa_in3[...]), added(qb2[b1], qb_in3[...])], axis=0).astype(BF)
    for k in range(3):
        qfin[k] = done[k * w : (k + 1) * w]
    for t in range(3):

        @pl.when(q_dst[t] != j)
        def _():
            c_q[t].start()

        @pl.when(q_dst[t] == j)
        def _():
            q_own[t] = qfin[(3 * j + t) // 4]

    c_wo1.wait_recv()
    piece2[...] = added(wo2[b1], wo_in3[...]).astype(BF)
    for r in range(4):
        di, dj = dests[r]

        @pl.when((di != i) | (dj != j))
        def _():
            c_own2[r].start()

        @pl.when((di == i) & (dj == j))
        def _():
            owner_in2[i % 4] = piece2[:, pl.ds(pl.multiple_of(dj * w, 128), w)]


    c_g[2].wait_recv()
    c_y[0].wait_recv()
    g_ref[lo] = added(gm[lo], near_in[lo]) + y_in[lo].astype(F32)
    c_y[1].wait_recv()
    g_ref[hi] = added(gm[hi], near_in[hi]) + y_in[hi].astype(F32)

    for t in range(3):

        @pl.when(q_dst[t] != j)
        def _():
            c_q[t].wait_recv()

        wq_ref[:, t * w : (t + 1) * w] = q_own[t].astype(F32).T.astype(BF)
    for r in range(4):
        di, dj = dests[r]

        @pl.when((di != i) | (dj != j))
        def _():
            c_own2[r].wait_recv()

    for c in c_own:
        c.wait_recv()
    no = piece2.shape[0]
    for a in range(4):
        wup_ref[:, a * part_u : (a + 1) * part_u] = own_in[a, :nu, :part_u]
        wup_ref[:, (4 + a) * part_u : (5 + a) * part_u] = own_in[a, :nu, part_u:]
        wdn_ref[a * nu : (a + 1) * nu, :] = own_in[a, nu:]
        wout_ref[a * no : (a + 1) * no, :] = owner_in2[a]

    for c in started:
        c.wait_send()
    for t in range(3):

        @pl.when(q_dst[t] != j)
        def _():
            c_q[t].wait_send()

    for r in range(4):
        di, dj = dests[r]

        @pl.when((di != i) | (dj != j))
        def _():
            c_own2[r].wait_send()


def tail_stage(gt, na, gm, ctx, dya, wt, w_out, upk, upo, dn, x, pown, py, ga, sa, bo, bd, small, smallf, cid):
    own, d = x.shape
    tok = na.shape[0]
    w = d // 4
    vm = pl.BlockSpec(memory_space=pltpu.VMEM)
    hbm = pl.BlockSpec(memory_space=pl.ANY)
    sds = jax.ShapeDtypeStruct
    big = lambda *s: pltpu.VMEM(s, BF)
    nb = d // 8
    nu = upk.shape[1]
    nd = dn[0].shape[1]
    no = w // 8
    r2 = 3 * w // 2
    return pl.pallas_call(
        tail_kernel,
        in_specs=[hbm] * 16 + [vm] * 6,
        out_specs=[vm] * 7,
        out_shape=(
            sds((own, d), BF), sds((own, d), F32), sds((nb, d), BF), sds((4 * nb, w), BF),
            sds((nb, 3 * w), BF), sds((4 * no, w), BF), sds((16, d), F32),
        ),
        scratch_shapes=[
            big(3 * w, tok), big(tok, d), big(tok, d), big(w, tok), big(tok, d), big(3 * w, d), big(d, d),
            big(4, nu, d), big(4, nu, d), big(4, 2, nd, d),
            big(own, d), big(own, d), big(own, d),
            big(3, w, own), big(4, nu, d), big(3, nu, d), big(nd, d), big(2, nd, d),
            big(2, 2, 2, 3 * w, 128), big(2, 2, r2, 128), big(2, 2, r2, 128), big(2, 2, r2, 128), big(2, 2, r2, 128),
            big(2, r2, 128), big(2, r2, 128), big(2, r2, 128), big(2, r2, 128), big(r2, 128), big(r2, 128),
            big(3, w, 128), big(3, w, 128),
            big(2, 2, 2, no, d), big(2, 2, no, d), big(2, 2, no, d), big(2, no, d), big(2, no, d), big(no, d),
            big(4, 2 * nb, w), big(no, d), big(4, 2 * nb, w), big(4, no, w),
            big(own, d), big(own, d), big(own, d), big(own, d),
            pltpu.VMEM((6, 16, d), F32), pltpu.VMEM((5, 16, d), F32),
            pltpu.SemaphoreType.DMA((16,)), pltpu.SemaphoreType.DMA((40,)), pltpu.SemaphoreType.DMA((40,)),
        ],
        compiler_params=pltpu.CompilerParams(vmem_limit_bytes=VMEM_LIMIT, collective_id=cid, has_side_effects=True),
        cost_estimate=pl.CostEstimate(
            flops=14 * tok * d * w, bytes_accessed=10 * tok * d, transcendentals=0
        ),
        name="tail_stage",
    )(gt, na, gm, ctx, dya, wt, w_out, upk, upo, *dn, x, pown, py, ga, sa, bo, bd, small, smallf)


def final_kernel(out_t, g_ref, x_ref, dy_ref, wup, wdn, wq, wout, sums,
                 out, gin, ga, sa, gm, sm, dwq, bq, dwout, bo, dwup, bu, dwdn, bd):
    out[...] = out_t[...]
    normed, inv = norm_parts(x_ref[...])
    g = g_ref[...]
    gin[...] = dy_ref[...].astype(F32) + inv * (
        g - jnp.mean(g, axis=-1, keepdims=True) - normed * jnp.mean(g * normed, axis=-1, keepdims=True)
    )

    @pl.when(pl.program_id(0) == 0)
    def _():
        d = sums.shape[1]
        for ref, first, count in ((ga, 0, 1), (sa, 1, 1), (bq, 2, 3), (gm, 5, 1), (sm, 6, 1), (bo, 7, 1), (bd, 7, 1), (bu, 8, 4)):
            for k in range(count):
                ref[k * d : (k + 1) * d] = sums[first + k, :]
        dwup[...] = wup[...].astype(F32)
        dwdn[...] = wdn[...].astype(F32)
        dwq[...] = wq[...].astype(F32)
        dwout[...] = wout[...].astype(F32)


def final_stage(out_t, g, x, dy, wup, wdn, wq, wout, sums, steps=4):
    own, d = x.shape
    row = pl.BlockSpec((own // steps, d), lambda i: (i, 0))
    const = lambda v: pl.BlockSpec(v.shape, lambda i: (0,) * len(v.shape))
    sds = lambda *s: jax.ShapeDtypeStruct(s, F32)
    like = lambda v: sds(*v.shape)
    outs = (
        jax.ShapeDtypeStruct((own, d), BF), sds(own, d), sds(d), sds(d), sds(d), sds(d), like(wq), sds(3 * d),
        like(wout), sds(d), like(wup), sds(4 * d), like(wdn), sds(d),
    )
    return pl.pallas_call(
        final_kernel,
        grid=(steps,),
        in_specs=[row, row, row, row] + [const(v) for v in (wup, wdn, wq, wout, sums)],
        out_specs=[row, row] + [const(v) for v in outs[2:]],
        out_shape=outs,
        compiler_params=pltpu.CompilerParams(vmem_limit_bytes=VMEM_LIMIT),
        name="final_stage",
    )(out_t, g, x, dy, wup, wdn, wq, wout, sums)


def layout(seq_lens, index):
    ends = jnp.cumsum(seq_lens, dtype=jnp.int32)
    starts = ends - seq_lens
    first = jnp.zeros_like(index)
    for s in range(1, seq_lens.shape[0]):
        first = jnp.where(index >= starts[s], starts[s], first)
    return first, index - first


def head_perm(v, bit):
    return lax.ppermute(v, "head", [(k, k ^ bit) for k in range(4)])


def dp_perm(v, bit):
    return lax.ppermute(v, "dp", [(k, k ^ bit) for k in range(8)])


def fast_body(inputs, lengths, attn_gain, attn_shift, mlp_gain, mlp_shift, w_qkv, b_qkv, w_out, b_out,
              w_up, b_up, w_down, b_down, cotangent):
    own, d = inputs.shape
    n = 4
    tok = own * n
    w = d // n
    pos = lax.axis_index("head").astype(jnp.int32).reshape(1)
    lens = lengths[0]
    (g_mlp, na, dy_all, qt, kt, vt, dot, kn, vn, cos, sin, p_own, p_far, up_keep, up_send, *dn, wt, small,
     smallf) = head_stage(
        inputs, cotangent, w_up, w_down, w_qkv, w_out, attn_gain, attn_shift, mlp_gain, mlp_shift, b_up, b_qkv, lens, n, 0
    )
    up_other = dp_perm(up_send, 1)
    dn = [dn[0]] + [dp_perm(dn[k], 2 * k) for k in (1, 2, 3)]
    p_y = head_perm(p_far, 2)
    gt, ctx = attention(lens, pos, cos, sin, qt, kt, vt, dot, kn, vn, own, tok // 2, halved=True)
    out_t, g, wup, wdn, wq, wout, sums = tail_stage(
        gt, na, g_mlp, ctx, dy_all, wt, w_out, up_keep, up_other, dn, inputs, p_own, p_y,
        attn_gain, attn_shift, b_out, b_down, small, smallf, 1
    )
    return tuple(final_stage(out_t, g, inputs, cotangent, wup, wdn, wq, wout, sums))


def general_body(inputs, lengths, attn_gain, attn_shift, mlp_gain, mlp_shift, w_qkv, b_qkv, w_out, b_out,
                 w_up, b_up, w_down, b_down, cotangent):
    own, d = inputs.shape
    n = lax.axis_size("head")
    n_dp = lax.axis_size("dp")
    tok = own * n
    w = d // n
    f = w_up.shape[1] // n
    j = lax.axis_index("head")
    pos = j.astype(jnp.int32).reshape(1)
    rows = lambda v: v.reshape(1, -1)
    ga, sa, gm, sm = rows(attn_gain), rows(attn_shift), rows(mlp_gain), rows(mlp_shift)
    bq, bu = rows(b_qkv), rows(b_up)
    lens = lengths[0]
    gather = lambda v: lax.all_gather(v, "head", axis=0, tiled=True)
    over_dp = lambda v, axis: lax.psum_scatter(v, "dp", scatter_dimension=axis, tiled=True)
    over_head = lambda v: lax.psum_scatter(v, "head", scatter_dimension=0, tiled=True)
    x_all = gather(inputs)
    dy_all = gather(cotangent)
    first, position = layout(lens, jnp.arange(tok, dtype=jnp.int32))
    freqs = 10000.0 ** (-(2.0 * jnp.arange(HALF, dtype=F32)) / ROT)
    angle = freqs[:, None] * position.astype(F32)[None, :]
    cos, sin = jnp.cos(angle), jnp.sin(angle)
    part, g_mlp, dwu, dwd, small, smallf = mlp(pos, x_all, dy_all, w_up, w_down, bu, gm, sm, n)
    qt, kt, vt, dot, kn, vn, na = proj(pos, x_all, dy_all, w_qkv, bq, w_out, ga, sa, cos, sin, n, tok, 0)
    gt, ctx = attention(
        lens, jnp.zeros((1,), jnp.int32), cos, sin, qt, kt, vt, dot, kn, vn, own, tok // 2
    )
    total, dwq, bias_q, small_q = post(pos, gt, na, g_mlp, w_qkv, ga, sa, n)
    attn_part = mm(ctx, lax.dynamic_slice_in_dim(w_out, j * w, w, 0), TN)
    bias = b_out.astype(F32) + b_down.astype(F32)
    output = inputs.astype(F32) + over_head((attn_part + part.astype(F32)).astype(BF)).astype(F32) + bias
    g_sum = over_head(total).astype(F32)
    normed, inv = norm_parts(inputs)
    grad_inputs = cotangent.astype(F32) + inv * (
        g_sum - jnp.mean(g_sum, axis=-1, keepdims=True) - normed * jnp.mean(g_sum * normed, axis=-1, keepdims=True)
    )
    dw_out = mm(ctx, dy_all).astype(BF)
    spread = lambda v: lax.all_to_all(v, "head", split_axis=1, concat_axis=0, tiled=True)
    grad_w_up = over_dp(dwu, 0).astype(F32)
    grad_w_down = over_dp(spread(dwd), 0).astype(F32)
    grad_w_out = over_dp(spread(dw_out), 0).astype(F32)
    qkv = over_dp(jnp.transpose(dwq, (0, 2, 1)).reshape(d, 3 * w), 0)
    qkv = lax.all_gather(qkv.reshape(d // n_dp, 3, w), "head", axis=2, tiled=True).reshape(d // n_dp, 3 * d)
    grad_w_qkv = lax.dynamic_slice_in_dim(qkv, j * 3 * w, 3 * w, 1).astype(F32)
    slots = jnp.where(jnp.arange(n)[:, None] == j, smallf[0:1], 0.0).reshape(-1)
    slots_q = jnp.where(jnp.arange(n)[None, :, None] == j, bias_q[0].reshape(3, 1, w), 0.0).reshape(-1)
    sums = lax.psum((small_q[0], small_q[1], small[0], small[1], slots_q, small[2] / n, slots), ("dp", "head"))
    return (output.astype(BF), grad_inputs, sums[0], sums[1], sums[2], sums[3], grad_w_qkv, sums[4],
            grad_w_out, sums[5], grad_w_up, sums[6], grad_w_down, sums[5])


def solution(mesh):
    fast = mesh.shape["dp"] == 8 and mesh.shape["head"] == 4
    whole = P(("dp", "head"), None)
    weight = P("dp", "head")
    return jax.shard_map(
        fast_body if fast else general_body,
        mesh=mesh,
        in_specs=(whole, P("dp", None)) + (P(),) * 12 + (whole,),
        out_specs=(whole, whole, P(), P(), P(), P(), weight, P(), weight, P(), weight, P(), weight, P()),
        check_vma=False,
    )
```

```python
import functools

import jax
import jax.numpy as jnp
import numpy as np
from jax import lax
from jax.experimental import pallas as pl
from jax.experimental.pallas import tpu as pltpu
from jax.sharding import PartitionSpec as P

HD = 64
ROT = 16
HALF = ROT // 2
NN = (((1,), (0,)), ((), ()))
NT = (((1,), (1,)), ((), ()))
TN = (((0,), (0,)), ((), ()))
FREQS = (10000.0 ** (-(2.0 * np.arange(HALF)) / ROT)).astype(np.float32)
BF = jnp.bfloat16
F32 = jnp.float32
VMEM_LIMIT = 62 * 1024 * 1024


def mm(a, b, dims=NN):
    return lax.dot_general(a, b, dims, preferred_element_type=F32)


def flat(v):
    return v.astype(F32).reshape(1, v.shape[0])


def norm_parts(x):
    v = x.astype(F32)
    center = v - jnp.mean(v, axis=-1, keepdims=True)
    inv = lax.rsqrt(jnp.mean(center * center, axis=-1, keepdims=True) + 1e-5)
    return center * inv, inv


def mlp_kernel(prev, final, pos, *refs):
    x_ref, dy_ref, wu, wd, bu, gain, shift = refs[:7]
    refs = refs[7:]
    if prev:
        pwu, pwd, psmall, psmallf = refs[:4]
        refs = refs[4:]
    part_ref, g_ref, out_wu, out_wd, small, smallf = refs[:6]
    if final:
        dwu, dwd = refs[6:8]
    else:
        dwu, dwd = out_wu, out_wd
    step = pl.program_id(0)

    @pl.when(step == 0)
    def _():
        if prev:
            dwu[...] = pwu[...]
            dwd[...] = pwd[...]
            small[...] = psmall[...]
            smallf[...] = psmallf[...]
        else:
            dwu[...] = jnp.zeros_like(dwu)
            dwd[...] = jnp.zeros_like(dwd)
            small[...] = jnp.zeros_like(small)
            smallf[...] = jnp.zeros_like(smallf)

    normed, _unused = norm_parts(x_ref[...])
    scale = gain[...].astype(F32)
    nm = (normed * scale + shift[...].astype(F32)).astype(BF)
    dy = dy_ref[...]
    pre = mm(nm, wu[...]) + bu[...].astype(F32)
    cdf = 0.5 + 0.5 * lax.erf(pre * (0.5**0.5))
    hid = (pre * cdf).astype(BF)
    slope = cdf + pre * (jnp.exp(-0.5 * pre * pre) * 0.3989422804014327)
    gp = (mm(dy, wd[...], NT) * slope).astype(BF)
    part_ref[...] = mm(hid, wd[...]).astype(BF)
    r = mm(gp, wu[...], NT)
    g_ref[...] = (r * scale).astype(BF)
    smallf[0:1, :] += jnp.sum(gp.astype(F32), axis=0, keepdims=True)
    small[0:1, :] += jnp.sum(r * normed, axis=0, keepdims=True)
    small[1:2, :] += jnp.sum(r, axis=0, keepdims=True)
    small[2:3, :] += jnp.sum(dy.astype(F32), axis=0, keepdims=True)
    dwd[...] += mm(hid, dy, TN)
    dwu[...] += mm(nm, gp, TN)

    if final:

        @pl.when(step == pl.num_programs(0) - 1)
        def _():
            out_wu[...] = dwu[...].astype(BF)
            out_wd[...] = dwd[...].astype(BF)


def mlp(pos, x, dy, wu, wd, bu, gain, shift, n, prev=None, final=True, tt=512):
    tok, d = x.shape
    f = wu.shape[1] // n
    row = lambda i, p: (i, 0)
    zero = lambda i, p: (0, 0)
    one = pl.Buffered(1)
    const = lambda shape: pl.BlockSpec(shape, zero, pipeline_mode=one)
    accs = [const((d, f)), const((f, d)), const((8, d)), const((8, f))]
    kind = BF if final else F32
    grid_spec = pltpu.PrefetchScalarGridSpec(
        num_scalar_prefetch=1,
        grid=(tok // tt,),
        in_specs=[
            pl.BlockSpec((tt, d), row),
            pl.BlockSpec((tt, d), row),
            pl.BlockSpec((d, f), lambda i, p: (0, p[0]), pipeline_mode=one),
            pl.BlockSpec((f, d), lambda i, p: (p[0], 0), pipeline_mode=one),
            pl.BlockSpec((1, f), lambda i, p: (0, p[0])),
            const((1, d)),
            const((1, d)),
        ]
        + (accs if prev is not None else []),
        out_specs=[pl.BlockSpec((tt, d), row), pl.BlockSpec((tt, d), row)] + accs,
        scratch_shapes=[pltpu.VMEM((d, f), F32), pltpu.VMEM((f, d), F32)] if final else [],
    )
    return pl.pallas_call(
        functools.partial(mlp_kernel, prev is not None, final),
        grid_spec=grid_spec,
        out_shape=(
            jax.ShapeDtypeStruct((tok, d), BF),
            jax.ShapeDtypeStruct((tok, d), BF),
            jax.ShapeDtypeStruct((d, f), kind),
            jax.ShapeDtypeStruct((f, d), kind),
            jax.ShapeDtypeStruct((8, d), F32),
            jax.ShapeDtypeStruct((8, f), F32),
        ),
        compiler_params=pltpu.CompilerParams(vmem_limit_bytes=VMEM_LIMIT),
        cost_estimate=pl.CostEstimate(
            flops=12 * tok * d * f, bytes_accessed=8 * tok * d + 12 * d * f, transcendentals=2 * tok * f
        ),
        name="mlp",
    )(pos, x, dy, wu, wd, bu, gain, shift, *(prev or ()))


def proj_kernel(nh, prev, pos, *refs):
    x_ref, dy_ref, wq, wk, wv, bq, bk, bv, wo, gain, shift, cos, sin = refs[:13]
    qt, kt, vt, dot, kn, vn, na_ref = refs[13 + (7 if prev else 0) :]
    normed, _unused = norm_parts(x_ref[...])
    na = (normed * gain[...].astype(F32) + shift[...].astype(F32)).astype(BF)
    na_ref[...] = na
    co = cos[...]
    si = sin[...]

    def rotated(t, scale):
        rows = []
        for h in range(nh):
            u = t[h * HD : (h + 1) * HD]
            u1 = u[:HALF]
            u2 = u[HALF:ROT]
            rows += [u1 * co - u2 * si, u2 * co + u1 * si, u[ROT:]]
        out = jnp.concatenate(rows, axis=0).astype(BF)
        return out if scale is None else out * jnp.asarray(scale, BF)

    def triple(w, b):
        return (mm(na, w[...]) + b[...].astype(F32)).astype(BF)

    qt[...] = rotated(triple(wq, bq).astype(F32).T, HD**-0.5)
    keys = rotated(triple(wk, bk).astype(F32).T, None)
    kt[...] = keys
    kn[...] = keys.T
    values = triple(wv, bv)
    vn[...] = values
    vt[...] = values.T
    dot[...] = mm(wo[...], dy_ref[...], NT).astype(BF)


def proj(pos, x, dy, w_qkv, b_qkv, w_out, gain, shift, cos, sin, n, total, first, prev=None, tt=512):
    tok, d = x.shape
    w = d // n
    nh = w // HD
    off = first // tt
    row = lambda i, p: (i, 0)
    zero = lambda i, p: (0, 0)
    one = pl.Buffered(1)
    wspec = lambda k: pl.BlockSpec((d, w), lambda i, p: (0, k * n + p[0]), pipeline_mode=one)
    bspec = lambda k: pl.BlockSpec((1, w), lambda i, p: (0, k * n + p[0]))
    lane = lambda rows: pl.BlockSpec((rows, tt), lambda i, p: (0, off + i))
    nat = lambda cols: pl.BlockSpec((tt, cols), lambda i, p: (off + i, 0))
    shapes = [(w, total)] * 4 + [(total, w)] * 2 + [(total, d)]
    grid_spec = pltpu.PrefetchScalarGridSpec(
        num_scalar_prefetch=1,
        grid=(tok // tt,),
        in_specs=[pl.BlockSpec((tt, d), row), pl.BlockSpec((tt, d), row)]
        + [wspec(0), wspec(1), wspec(2), bspec(0), bspec(1), bspec(2)]
        + [pl.BlockSpec((w, d), lambda i, p: (p[0], 0), pipeline_mode=one)]
        + [pl.BlockSpec((1, d), zero), pl.BlockSpec((1, d), zero), lane(HALF), lane(HALF)]
        + ([pl.BlockSpec(memory_space=pl.ANY)] * 7 if prev is not None else []),
        out_specs=[lane(w)] * 4 + [nat(w)] * 2 + [nat(d)],
    )
    return pl.pallas_call(
        functools.partial(proj_kernel, nh, prev is not None),
        grid_spec=grid_spec,
        out_shape=tuple(jax.ShapeDtypeStruct(s, BF) for s in shapes),
        input_output_aliases={14 + k: k for k in range(7)} if prev is not None else {},
        compiler_params=pltpu.CompilerParams(vmem_limit_bytes=VMEM_LIMIT),
        cost_estimate=pl.CostEstimate(
            flops=8 * tok * d * w, bytes_accessed=6 * tok * d + 12 * tok * w + 8 * d * w, transcendentals=0
        ),
        name="proj",
    )(pos, x, dy, w_qkv, w_qkv, w_qkv, b_qkv, b_qkv, b_qkv, w_out, gain, shift, cos, sin, *(prev or ()))


def head_kernel(nh, x_hbm, dy_hbm, wu_hbm, wd_hbm, wqkv_hbm, wo_hbm, gain_a, shift_a, gain_m, shift_m, bu, bq, lens,
                g_out, na_out, dy_out, qt, kt, vt, dot, kn, vn, cos, sin, p_own, p_far, up_keep, up_send, dn0, dn1, dn2, dn3,
                w_t, small, smallf,
                xs, dys, wu, wd, wqkv, wt, wo, bias_t, bias_all, bias_u, parts, far_in, near_in, dwu, dwd, load, send, recv):
    step = pl.program_id(0)
    i = lax.axis_index("dp")
    j = lax.axis_index("head")
    own, d = x_hbm.shape
    f = wu.shape[1]
    w = wo.shape[0]
    half = own // 2
    core = {"head": j ^ 1}
    across = {"head": j ^ 2}

    def remote(src, dst, k, to):
        return pltpu.make_async_remote_copy(
            src_ref=src, dst_ref=dst, send_sem=send.at[k], recv_sem=recv.at[k], device_id=to,
            device_id_type=pl.DeviceIdType.MESH)

    lo, hi = pl.ds(0, half), pl.ds(half, half)
    copies = [
        remote(x_hbm, xs.at[1], 0, core),
        remote(dy_hbm, dys.at[1], 1, core),
        remote(x_hbm.at[lo], xs.at[2, lo], 2, across),
        remote(dy_hbm.at[lo], dys.at[2, lo], 3, across),
        remote(x_hbm.at[hi], xs.at[3, lo], 4, across),
        remote(dy_hbm.at[hi], dys.at[3, lo], 5, across),
        remote(xs.at[2, lo], xs.at[2, hi], 6, core),
        remote(dys.at[2, lo], dys.at[2, hi], 7, core),
        remote(xs.at[3, lo], xs.at[3, hi], 8, core),
        remote(dys.at[3, lo], dys.at[3, hi], 9, core),
        remote(parts.at[1], near_in, 10, core),
        remote(parts.at[2, hi], far_in.at[lo], 11, core),
        remote(parts.at[3, hi], far_in.at[hi], 12, core),
    ]
    locals_ = [
        pltpu.make_async_copy(x_hbm, xs.at[0], load.at[0]),
        pltpu.make_async_copy(dy_hbm, dys.at[0], load.at[1]),
        pltpu.make_async_copy(wo_hbm.at[pl.ds(j * w, w)], wo, load.at[2]),
    ] + [
        pltpu.make_async_copy(wqkv_hbm.at[:, pl.ds(k * d + j * w, w)], wqkv.at[:, pl.ds(k * w, w)], load.at[3 + k])
        for k in range(3)
    ]
    part = f // 8
    for k in range(8):
        there, here = pl.ds(4 * k * part + j * part, part), pl.ds(k * part, part)
        locals_.append(pltpu.make_async_copy(wu_hbm.at[:, there], wu.at[:, here], load.at[6 + k]))
        locals_.append(pltpu.make_async_copy(wd_hbm.at[there], wd.at[here], load.at[14 + k]))

    @pl.when(step == 0)
    def _():
        barrier = pltpu.get_barrier_semaphore()
        for to in (core, across):
            pl.semaphore_signal(barrier, inc=1, device_id=to, device_id_type=pl.DeviceIdType.MESH)
        for c in locals_:
            c.start()
        pl.semaphore_wait(barrier, 2)
        for c in copies[:6]:
            c.start()
        dwu[...] = jnp.zeros_like(dwu)
        dwd[...] = jnp.zeros_like(dwd)
        small[...] = jnp.zeros_like(small)
        smallf[...] = jnp.zeros_like(smallf)
        for c in locals_:
            c.wait()
        for k in range(3):
            wt[k * w : (k + 1) * w, :] = wqkv[:, k * w : (k + 1) * w].T
            row = flat(bq[pl.ds(pl.multiple_of(k * d + j * w, 256), w)])
            bias_t[k * w : (k + 1) * w, :] = jnp.broadcast_to(row, (128, w)).T
        bias_all[0:1, :] = flat(bu[...])
        for k in range(8):
            bias_u[0:1, k * part : (k + 1) * part] = bias_all[0:1, pl.ds(pl.multiple_of(4 * k * part + j * part, 128), part)]

    @pl.when(step == 1)
    def _():
        copies[0].wait_recv()

    @pl.when(step == 2)
    def _():
        copies[6].wait_recv()

    @pl.when(step == 3)
    def _():
        copies[8].wait_recv()

    normed, _unused = norm_parts(xs[step])
    scale = flat(gain_m[...])
    nm = (normed * scale + flat(shift_m[...])).astype(BF)
    na = (normed * flat(gain_a[...]) + flat(shift_a[...])).astype(BF)
    na_out[...] = na
    pre = mm(nm, wu[...]) + bias_u[0:1, :]
    cdf = 0.5 + 0.5 * lax.erf(pre * (0.5**0.5))
    hid = (pre * cdf).astype(BF)
    slope = cdf + pre * (jnp.exp(-0.5 * pre * pre) * 0.3989422804014327)
    parts[step] = mm(hid, wd[...]).astype(BF)

    lane = lax.broadcasted_iota(jnp.int32, (1, own), 1)
    far = jnp.where(lane < half, j ^ 2, j ^ 3) * own + (step - 2) * half + lane % half
    index = jnp.where(step == 0, j * own + lane, jnp.where(step == 1, (j ^ 1) * own + lane, far))
    begin = jnp.zeros_like(index)
    total = jnp.int32(0)
    for s in range(lens.shape[0] - 1):
        total = total + lens[s]
        begin = jnp.where(index >= total, total, begin)
    sub = lax.broadcasted_iota(jnp.int32, (HALF, own), 0)
    freqs = jnp.zeros((HALF, own), F32)
    for k in range(HALF):
        freqs = jnp.where(sub == k, float(FREQS[k]), freqs)
    angle = freqs * (index - begin).astype(F32)
    co = jnp.cos(angle)
    si = jnp.sin(angle)
    cos[...] = co
    sin[...] = si

    def projected(k):
        b = bias_t[k * w : (k + 1) * w, :]
        t = mm(wt[k * w : (k + 1) * w, :], na, NT)
        return (t + jnp.concatenate([b] * (own // 128), axis=1)).astype(BF)

    def rotated(t, factor):
        rows = []
        for h in range(nh):
            u = t[h * HD : (h + 1) * HD].astype(F32)
            u1 = u[:HALF]
            u2 = u[HALF:ROT]
            rows += [u1 * co - u2 * si, u2 * co + u1 * si, u[ROT:]]
        out = jnp.concatenate(rows, axis=0)
        return (out if factor is None else out * factor).astype(BF)

    qt[...] = rotated(projected(0), HD**-0.5)
    keys = rotated(projected(1), None)
    kt[...] = keys
    kn[...] = keys.T
    values = projected(2)
    vt[...] = values
    vn[...] = values.T

    @pl.when(step == 1)
    def _():
        copies[1].wait_recv()
        copies[10].start()
        copies[2].wait_recv()
        copies[6].start()

    @pl.when(step == 2)
    def _():
        copies[7].wait_recv()
        copies[11].start()

    @pl.when(step == 3)
    def _():
        copies[12].start()
        copies[5].wait_recv()
        copies[9].start()
        copies[9].wait_recv()

    dy = dys[step]
    dy_out[...] = dy
    gp = (mm(dy, wd[...], NT) * slope).astype(BF)
    r = mm(gp, wu[...], NT)
    g_out[...] = (r * scale).astype(BF)
    smallf[0:1, :] += jnp.sum(gp.astype(F32), axis=0, keepdims=True)
    small[0:1, :] += jnp.sum(r * normed, axis=0, keepdims=True)
    small[1:2, :] += jnp.sum(r, axis=0, keepdims=True)
    small[2:3, :] += jnp.sum(dy.astype(F32), axis=0, keepdims=True)
    dwd[...] += mm(hid, dy, TN)
    dwu[...] += mm(nm, gp, TN)
    dot[...] = mm(wo[...], dy, NT).astype(BF)

    @pl.when(step == 1)
    def _():
        copies[3].wait_recv()
        copies[7].start()

    @pl.when(step == 2)
    def _():
        copies[4].wait_recv()
        copies[8].start()

    @pl.when(step == 3)
    def _():
        rows = dwu.shape[0] // 8
        keep = dn0.shape[1]
        for b in range(4):
            for ref, at in ((up_keep, 2 * b + i % 2), (up_send, 2 * b + 1 - i % 2)):
                at = pl.multiple_of(at * rows, rows)
                ref[b, :rows] = dwu[pl.ds(at, rows), :].astype(BF)
                ref[b, rows:] = dwd[pl.ds(at + keep, rows - keep), :].astype(BF)
            ref = (dn0, dn1, dn2, dn3)[b]
            for x in range(2):
                at = 2 * ((i // 2) ^ b) + x
                ref[x] = dwd[pl.ds(pl.multiple_of(at * rows, rows), keep), :].astype(BF)
        w_t[...] = wt[...]
        copies[10].wait_recv()
        p_own[...] = (parts[0].astype(F32) + near_in[...].astype(F32)).astype(BF)
        copies[11].wait_recv()
        p_far[lo] = (parts[2, lo].astype(F32) + far_in[lo].astype(F32)).astype(BF)
        copies[12].wait_recv()
        p_far[hi] = (parts[3, lo].astype(F32) + far_in[hi].astype(F32)).astype(BF)
        for c in copies:
            c.wait_send()


def head_stage(x, dy, w_up, w_down, w_qkv, w_out, ga, sa, gm, sm, bu, bq, lens, n, cid):
    own, d = x.shape
    tok = own * n
    w = d // n
    f = w_up.shape[1] // n
    row = lambda i: (i, 0)
    lane = lambda rows: pl.BlockSpec((rows, own), lambda i: (0, i))
    nat = lambda cols: pl.BlockSpec((own, cols), row)
    one = pl.Buffered(1)
    const = lambda shape: pl.BlockSpec(shape, lambda i: (0,) * len(shape), pipeline_mode=one)
    hbm = pl.BlockSpec(memory_space=pl.ANY)
    sds = jax.ShapeDtypeStruct
    return pl.pallas_call(
        functools.partial(head_kernel, w // HD),
        grid=(n,),
        in_specs=[hbm] * 6
        + [const(v.shape) for v in (ga, sa, gm, sm, bu, bq)]
        + [pl.BlockSpec(memory_space=pltpu.SMEM)],
        out_specs=[nat(d)] * 3
        + [lane(w)] * 4
        + [nat(w)] * 2
        + [lane(HALF)] * 2
        + [const((own, d))] * 2
        + [const((4, d // 8 + d // 32, d))] * 2
        + [const((2, 3 * d // 32, d))] * 4
        + [const((3 * w, d)), const((8, d)), const((8, f))],
        out_shape=tuple(
            [sds((tok, d), BF)] * 3
            + [sds((w, tok), BF)] * 4
            + [sds((tok, w), BF)] * 2
            + [sds((HALF, tok), F32)] * 2
            + [sds((own, d), BF)] * 2
            + [sds((4, d // 8 + d // 32, d), BF)] * 2
            + [sds((2, 3 * d // 32, d), BF)] * 4
            + [sds((3 * w, d), BF), sds((8, d), F32), sds((8, f), F32)]
        ),
        scratch_shapes=[
            pltpu.VMEM((4, own, d), BF),
            pltpu.VMEM((4, own, d), BF),
            pltpu.VMEM((d, f), BF),
            pltpu.VMEM((f, d), BF),
            pltpu.VMEM((d, 3 * w), BF),
            pltpu.VMEM((3 * w, d), BF),
            pltpu.VMEM((w, d), BF),
            pltpu.VMEM((3 * w, 128), F32),
            pltpu.VMEM((8, 4 * f), F32),
            pltpu.VMEM((8, f), F32),
            pltpu.VMEM((4, own, d), BF),
            pltpu.VMEM((own, d), BF),
            pltpu.VMEM((own, d), BF),
            pltpu.VMEM((d, f), F32),
            pltpu.VMEM((f, d), F32),
            pltpu.SemaphoreType.DMA((22,)),
            pltpu.SemaphoreType.DMA((13,)),
            pltpu.SemaphoreType.DMA((13,)),
        ],
        compiler_params=pltpu.CompilerParams(
            vmem_limit_bytes=VMEM_LIMIT, collective_id=cid, has_side_effects=True
        ),
        cost_estimate=pl.CostEstimate(
            flops=12 * tok * d * f + 10 * tok * d * w, bytes_accessed=12 * tok * d + 8 * d * f, transcendentals=2 * tok * f
        ),
        name="head_stage",
    )(x, dy, w_up, w_down, w_qkv, w_out, ga, sa, gm, sm, bu, bq, lens)


def attn_kernel(nh, tok, blk, per, halved, lens, rel, cos, sin, qt, kt, vt, dot, kn, vn,
                gt_ref, ctx_ref, exps, low_exps, dk, dv, oacc, dqacc, mpart, lpart, rowsc, qpad, dopad):
    nseq = lens.shape[0]
    nblk = tok // blk
    shift = rel[0]
    heads = range(nh)

    def place(b):
        chunk = (b // per) ^ shift
        half = b % per
        at = chunk * per + half
        if halved:
            at = jnp.where(chunk < 2, at, 4 + (chunk - 2) + 2 * half)
        return pl.multiple_of(at * blk, blk)

    def rows_of(h):
        return slice(h * HD, (h + 1) * HD)

    def pair_of(h):
        return slice((h // 2) * 128, (h // 2) * 128 + 128)

    def fold(v, op):
        return op(v.reshape(blk // 8, 8, blk), axis=0)

    def begin_of(at):
        begin = jnp.int32(0)
        total = jnp.int32(0)
        for s in range(nseq - 1):
            total = total + lens[s]
            begin = jnp.where(at >= total, total, begin)
        return begin

    dk[...] = jnp.zeros_like(dk)
    dv[...] = jnp.zeros_like(dv)
    qpad[...] = jnp.zeros_like(qpad)
    dopad[...] = jnp.zeros_like(dopad)
    rows_iota = lax.broadcasted_iota(jnp.int32, (blk, blk), 0)
    cols_iota = lax.broadcasted_iota(jnp.int32, (1, blk), 1)

    def one_block(i, carry):
        first_tok = i * blk
        count = i - begin_of(first_tok) // blk + 1
        last_begin = begin_of(first_tok + blk - 1)
        cols = pl.ds(place(i), blk)
        query_idx = cols_iota + first_tok
        start_row = begin_of(query_idx)
        for h in heads:
            half = (h % 2) * HD
            qpad[h, half : half + HD, :] = qt[rows_of(h), cols]

        krow = pl.ds(place(i), blk)
        kidx = rows_iota + first_tok
        allowed = (kidx >= start_row) & (kidx <= query_idx)
        for h in heads:
            s = jnp.where(allowed, mm(kn[krow, pair_of(h)], qpad[h]), -1e30)
            exps[h, 0] = s
            mpart[h] = fold(s, jnp.max)

        def scores(step, c):
            b = i - step
            krow = pl.ds(place(b), blk)
            edge = last_begin > b * blk

            @pl.when(edge)
            def _():
                allowed = (rows_iota + b * blk) >= start_row
                for h in heads:
                    s = jnp.where(allowed, mm(kn[krow, pair_of(h)], qpad[h]), -1e30)
                    exps[h, step] = s
                    mpart[h] = jnp.maximum(mpart[h], fold(s, jnp.max))

            @pl.when(jnp.logical_not(edge))
            def _():
                for h in heads:
                    s = mm(kn[krow, pair_of(h)], qpad[h])
                    exps[h, step] = s
                    mpart[h] = jnp.maximum(mpart[h], fold(s, jnp.max))

            return c

        lax.fori_loop(1, count, scores, 0)
        for h in heads:
            rowsc[h : h + 1, :] = jnp.max(mpart[h], axis=0, keepdims=True)
        lpart[...] = jnp.zeros_like(lpart)
        oacc[...] = jnp.zeros_like(oacc)

        def weights(step, c):
            kcols = pl.ds(place(i - step), blk)
            for h in heads:
                e = jnp.exp(exps[h, step] - rowsc[h : h + 1, :])
                exps[h, step] = e
                lpart[h] += fold(e, jnp.sum)
                low = e.astype(BF)
                low_exps[h, step] = low
                oacc[h] += mm(vt[rows_of(h), kcols], low)
            return c

        lax.fori_loop(0, count, weights, 0)
        for h in heads:
            half = (h % 2) * HD
            inv = 1.0 / jnp.sum(lpart[h], axis=0, keepdims=True)
            o = oacc[h] * inv
            ctx_ref[rows_of(h), cols] = o.astype(BF)
            scaled = (dot[rows_of(h), cols].astype(F32) * inv).astype(BF)
            dopad[h, half : half + HD, :] = scaled
            rowsc[h : h + 1, :] = jnp.sum(o * scaled.astype(F32), axis=0, keepdims=True)
        dqacc[...] = jnp.zeros_like(dqacc)

        def backward(step, c):
            kcols = pl.ds(place(i - step), blk)
            dps = [mm(vn[kcols, pair_of(h)], dopad[h]) for h in heads]
            dss = [(exps[h, step] * (dps[h] - rowsc[h : h + 1, :])).astype(BF) for h in heads]
            dvs = [mm(dopad[h, (h % 2) * HD : (h % 2) * HD + HD, :], low_exps[h, step], NT) for h in heads]
            dks = [mm(qt[rows_of(h), cols], dss[h], NT) for h in heads]
            dqs = [mm(kt[rows_of(h), kcols], dss[h]) for h in heads]
            for h in heads:
                dv[rows_of(h), kcols] += dvs[h]
                dk[rows_of(h), kcols] += dks[h]
                dqacc[rows_of(h), :] += dqs[h]
            return c

        lax.fori_loop(0, count, backward, 0)
        co = cos[:, cols]
        si = sin[:, cols]
        for h in heads:
            base = h * HD
            g = dqacc[base : base + HD, :] * (HD**-0.5)
            g1 = g[:HALF]
            g2 = g[HALF:ROT]
            gt_ref[base : base + HD, cols] = jnp.concatenate(
                [g1 * co + g2 * si, g2 * co - g1 * si, g[ROT:]], axis=0
            ).astype(BF)
        return carry

    lax.fori_loop(0, nblk, one_block, 0)

    def finish(i, carry):
        cols = pl.ds(pl.multiple_of(i * blk, blk), blk)
        co = cos[:, cols]
        si = sin[:, cols]
        for h in heads:
            base = h * HD
            g = dk[base : base + HD, cols]
            g1 = g[:HALF]
            g2 = g[HALF:ROT]
            gt_ref[nh * HD + base : nh * HD + base + HD, cols] = jnp.concatenate(
                [g1 * co + g2 * si, g2 * co - g1 * si, g[ROT:]], axis=0
            ).astype(BF)
        gt_ref[2 * nh * HD :, cols] = dv[:, cols].astype(BF)
        return carry

    lax.fori_loop(0, nblk, finish, 0)


def attention(lens, rel, cos, sin, qt, kt, vt, dot, kn, vn, chunk, maxlen, halved=False, blk=256):
    width, tok = qt.shape
    nh = width // HD
    wb = maxlen // blk + 1
    vm = pl.BlockSpec(memory_space=pltpu.VMEM)
    sm = pl.BlockSpec(memory_space=pltpu.SMEM)
    return pl.pallas_call(
        functools.partial(attn_kernel, nh, tok, blk, chunk // blk, halved),
        out_shape=(jax.ShapeDtypeStruct((3 * width, tok), BF), jax.ShapeDtypeStruct((width, tok), BF)),
        in_specs=[sm, sm] + [vm] * 8,
        out_specs=(vm, vm),
        scratch_shapes=[
            pltpu.VMEM((nh, wb, blk, blk), F32),
            pltpu.VMEM((nh, wb, blk, blk), BF),
            pltpu.VMEM((width, tok), F32),
            pltpu.VMEM((width, tok), F32),
            pltpu.VMEM((nh, HD, blk), F32),
            pltpu.VMEM((width, blk), F32),
            pltpu.VMEM((nh, 8, blk), F32),
            pltpu.VMEM((nh, 8, blk), F32),
            pltpu.VMEM((8, blk), F32),
            pltpu.VMEM((nh, 128, blk), BF),
            pltpu.VMEM((nh, 128, blk), BF),
        ],
        compiler_params=pltpu.CompilerParams(vmem_limit_bytes=VMEM_LIMIT),
        cost_estimate=pl.CostEstimate(
            flops=20 * width * tok * maxlen, bytes_accessed=20 * width * tok, transcendentals=nh * tok * maxlen
        ),
        name="attention",
    )(lens, rel, cos, sin, qt, kt, vt, dot, kn, vn)


def post_kernel(pos, gt_ref, na_ref, gm_ref, wq, wk, wv, gain, shift, g_ref, out_w, bias, small, dw):
    step = pl.program_id(0)

    @pl.when(step == 0)
    def _():
        dw[...] = jnp.zeros_like(dw)
        bias[...] = jnp.zeros_like(bias)
        small[...] = jnp.zeros_like(small)

    gt = gt_ref[...]
    na = na_ref[...]
    w = wq.shape[1]
    scale = gain[...].astype(F32)
    gn = gt.T
    r = mm(gn[:, :w], wq[...], NT) + mm(gn[:, w : 2 * w], wk[...], NT) + mm(gn[:, 2 * w :], wv[...], NT)
    g_ref[...] = (r * scale + gm_ref[...].astype(F32)).astype(BF)
    small[0:1, :] += jnp.sum(r * na.astype(F32), axis=0, keepdims=True)
    small[1:2, :] += jnp.sum(r, axis=0, keepdims=True)
    bias[0:1, :] += jnp.sum(gn.astype(F32), axis=0, keepdims=True)
    dw[...] += mm(gt, na)

    @pl.when(step == pl.num_programs(0) - 1)
    def _():
        for b in range(dw.shape[1] // 128):
            out_w[b] = dw[:, b * 128 : (b + 1) * 128].astype(BF)
        small[0:1, :] = (small[0:1, :] - shift[...].astype(F32) * small[1:2, :]) / scale


def post(pos, gt, na, gm, w_qkv, gain, shift, n, tt=512):
    tok, d = na.shape
    w = d // n
    row = lambda i, p: (i, 0)
    zero = lambda i, p: (0, 0)
    one = pl.Buffered(1)
    const = lambda shape: pl.BlockSpec(shape, zero, pipeline_mode=one)
    wspec = lambda k: pl.BlockSpec((d, w), lambda i, p: (0, k * n + p[0]), pipeline_mode=one)
    grid_spec = pltpu.PrefetchScalarGridSpec(
        num_scalar_prefetch=1,
        grid=(tok // tt,),
        in_specs=[
            pl.BlockSpec((3 * w, tt), lambda i, p: (0, i)),
            pl.BlockSpec((tt, d), row),
            pl.BlockSpec((tt, d), row),
            wspec(0),
            wspec(1),
            wspec(2),
            const((1, d)),
            const((1, d)),
        ],
        out_specs=[
            pl.BlockSpec((tt, d), row),
            pl.BlockSpec((d // 128, 3 * w, 128), lambda i, p: (0, 0, 0), pipeline_mode=one),
            const((8, 3 * w)),
            const((8, d)),
        ],
        scratch_shapes=[pltpu.VMEM((3 * w, d), F32)],
    )
    return pl.pallas_call(
        post_kernel,
        grid_spec=grid_spec,
        out_shape=(
            jax.ShapeDtypeStruct((tok, d), BF),
            jax.ShapeDtypeStruct((d // 128, 3 * w, 128), BF),
            jax.ShapeDtypeStruct((8, 3 * w), F32),
            jax.ShapeDtypeStruct((8, d), F32),
        ),
        compiler_params=pltpu.CompilerParams(vmem_limit_bytes=VMEM_LIMIT),
        cost_estimate=pl.CostEstimate(
            flops=12 * tok * d * w, bytes_accessed=8 * tok * d + 6 * tok * w + 18 * d * w, transcendentals=0
        ),
        name="post",
    )(pos, gt, na, gm, w_qkv, w_qkv, w_qkv, gain, shift)


def tail_kernel(gt_h, na_h, gm_h, ctx_h, dya_h, wt_h, wo_h, upk_h, upo_h, dn0_h, dn1_h, dn2_h, dn3_h, x_h, pown_h, py_h,
                gain, shift_ref, bo, bd, small, smallf,
                out_ref, g_ref, wup_ref, wdn_ref, wq_ref, wout_ref, sums_ref,
                gt, na, gm, ctx, dya, wt, wo, upk, upo, dn, xo, pown, py,
                ctx_in, up4, up_in, dn_in, dn2,
                dwq, qa_in, qb_in, qa4, qb4, qa_in2, qb_in2, qa2, qb2, qa_in3, qb_in3, qfin, q_own,
                dwo, wo_in, wo4, wo_in2, wo2, wo_in3, fin, piece2, own_in, owner_in2,
                far_in, near_in, far_sum, y_in, sm, sm_in, load, send, recv):
    i = lax.axis_index("dp")
    j = lax.axis_index("head")
    own, d = x_h.shape
    w = wt.shape[0] // 3
    half = own // 2
    bx = i % 2
    b0 = (i // 2) % 2
    b1 = i // 4
    z = i // 2
    mesh_id = pl.DeviceIdType.MESH
    core, across, diag = {"head": j ^ 1}, {"head": j ^ 2}, {"head": j ^ 3}
    px, p0, p1 = {"dp": i ^ 1}, {"dp": i ^ 2}, {"dp": i ^ 4}
    lo, hi = pl.ds(0, half), pl.ds(half, half)
    count = [0]
    started = []

    def remote(src, dst, to):
        k = count[0]
        count[0] += 1
        return pltpu.make_async_remote_copy(
            src_ref=src, dst_ref=dst, send_sem=send.at[k], recv_sem=recv.at[k], device_id=to, device_id_type=mesh_id)

    def go(*copies):
        for c in copies:
            c.start()
            started.append(c)

    def local(src, dst, k):
        return pltpu.make_async_copy(src, dst, load.at[k])

    loads = [
        local(upk_h, upk, 0), local(upo_h, upo, 1),
        local(dn0_h, dn.at[0], 2), local(dn1_h, dn.at[1], 3), local(dn2_h, dn.at[2], 4), local(dn3_h, dn.at[3], 5),
        local(gt_h, gt, 6), local(na_h, na, 7), local(wt_h, wt, 8), local(ctx_h, ctx, 9), local(dya_h, dya, 10),
        local(gm_h, gm, 11), local(wo_h, wo, 12), local(x_h, xo, 13), local(pown_h, pown, 14), local(py_h, py, 15),
    ]
    c_ctx = [
        remote(ctx_h.at[:, pl.ds(2 * own, half)], ctx_in.at[1, :, lo], across),
        remote(ctx_h.at[:, pl.ds(3 * own, half)], ctx_in.at[1, :, hi], across),
        remote(ctx_h.at[:, pl.ds(2 * own + half, half)], ctx_in.at[2, :, lo], diag),
        remote(ctx_h.at[:, pl.ds(3 * own + half, half)], ctx_in.at[2, :, hi], diag),
        remote(ctx_h.at[:, pl.ds(own, own)], ctx_in.at[0], core),
    ]
    c_up = [remote(up4.at[z ^ k], up_in.at[k - 1], {"dp": i ^ (2 * k)}) for k in (1, 2, 3)]
    c_dnx = remote(dn2.at[1 - bx], dn_in, px)
    rows = dwq.shape[3] // 2
    ra, rb = pl.ds(0, rows), pl.ds(rows, rows)
    c_qa = remote(dwq.at[:, :, 1 - bx, ra], qa_in, px)
    c_qb = remote(dwq.at[:, :, 1 - bx, rb], qb_in, px)
    c_qa0 = remote(qa4.at[:, 1 - b0], qa_in2, p0)
    c_qb0 = remote(qb4.at[:, 1 - b0], qb_in2, p0)
    c_qa1 = remote(qa2.at[1 - b1], qa_in3, p1)
    c_qb1 = remote(qb2.at[1 - b1], qb_in3, p1)
    c_wox = remote(dwo.at[:, :, 1 - bx], wo_in, px)
    c_wo0 = remote(wo4.at[:, 1 - b0], wo_in2, p0)
    c_wo1 = remote(wo2.at[1 - b1], wo_in3, p1)
    c_g = [
        remote(gm.at[pl.ds(2 * own + half, half)], far_in.at[lo], core),
        remote(gm.at[pl.ds(3 * own + half, half)], far_in.at[hi], core),
        remote(gm.at[pl.ds(own, own)], near_in, core),
    ]
    c_y = [remote(far_sum.at[lo], y_in.at[lo], across), remote(far_sum.at[hi], y_in.at[hi], across)]
    c_sm = [remote(sm.at[s], sm_in.at[s], to) for s, to in enumerate((core, across, px, p0, p1))]
    c_own = [remote(fin.at[j ^ r], own_in.at[j], {"head": j ^ r}) for r in (1, 2, 3)]
    dests = []
    c_own2 = []
    for r in range(4):
        di, dj = 2 * j + i // 4, (i % 4) ^ r
        dests.append((di, dj))
        cut = pl.ds(pl.multiple_of(dj * w, 128), w)
        c_own2.append(remote(piece2.at[:, cut], owner_in2.at[i % 4], {"dp": di, "head": dj}))
    c_q = []
    q_dst = []
    for t in range(3):
        dst = (t - j + 4) % 4
        q_dst.append(dst)
        c_q.append(remote(qfin.at[(3 * dst + t) // 4], q_own.at[t], {"head": dst}))

    barrier = pltpu.get_barrier_semaphore()
    for to in (core, across, diag, px, p0, p1, {"dp": i ^ 6}):
        pl.semaphore_signal(barrier, inc=1, device_id=to, device_id_type=mesh_id)
    for c in loads:
        c.start()
    for r in range(4):
        si, sj = 4 * (i % 2) + (j ^ r), i // 2

        @pl.when((si != i) | (sj != j))
        def _():
            pl.semaphore_signal(barrier, inc=1, device_id={"dp": si, "head": sj}, device_id_type=mesh_id)

    to_self = jnp.where(2 * j + i // 4 == i, 1, 0)
    pl.semaphore_wait(barrier, 11 - to_self)

    go(*c_ctx)

    def added(a, b):
        return a.astype(F32) + b.astype(F32)

    def ready(first, last):
        for k in range(first, last):
            loads[k].wait()

    ready(0, 2)
    up4[...] = added(upk[...], upo[...]).astype(BF)
    go(*c_up)
    ready(2, 6)
    dn2[...] = (added(dn[0], dn[1]) + added(dn[2], dn[3])).astype(BF)
    go(c_dnx)

    ready(6, 9)
    gains = [jnp.zeros((1, 256), F32)] * 4
    for part, c in ((ra, c_qa), (rb, c_qb)):
        left = gt[part, :]
        for k in range(4):
            t = mm(left, na[:, 256 * k : 256 * (k + 1)])
            gains[k] += jnp.sum(t * wt[part, 256 * k : 256 * (k + 1)].astype(F32), axis=0, keepdims=True)
            t = t.astype(BF)
            dwq[k // 2, k % 2, 0, part] = t[:, :128]
            dwq[k // 2, k % 2, 1, part] = t[:, 128:]
        if c is c_qa:
            go(c)
    s_bias = mm(jnp.ones((8, gt.shape[1]), BF), gt[...], NT)[0:1]
    high = s_bias.astype(BF)
    low = (s_bias - high.astype(F32)).astype(BF)
    s_shift = mm(jnp.broadcast_to(high, (8, 3 * w)), wt[...])[0:1] + mm(jnp.broadcast_to(low, (8, 3 * w)), wt[...])[0:1]
    s_gain = jnp.concatenate(gains, axis=1)
    scale = flat(gain[...])

    sm[0] = jnp.zeros((16, d), F32)
    sm[0, 0:1, :] = (s_gain - flat(shift_ref[...]) * s_shift) / scale
    sm[0, 1:2, :] = s_shift
    for k in range(3):
        sm[0, 2 + k : 3 + k, pl.ds(pl.multiple_of(j * w, 128), w)] = s_bias[:, k * w : (k + 1) * w]
    sm[0, 5:7, :] = small[0:2, :]
    sm[0, 7:8, :] = small[2:3, :] * 0.25
    part_u = d // 8
    for b in range(8):
        at = pl.multiple_of((b % 2) * 4 * part_u + j * part_u, 128)
        sm[0, 8 + b // 2 : 9 + b // 2, pl.ds(at, part_u)] = smallf[0:1, b * part_u : (b + 1) * part_u]
    go(c_sm[0])

    def small_step(s):
        c_sm[s].wait_recv()
        sm[s + 1] = sm[s] + sm_in[s]
        if s < 4:
            go(c_sm[s + 1])

    ready(9, 11)
    t = mm(ctx[...], dya[...]).astype(BF)
    for b in range(8):
        dwo[b // 4, (b // 2) % 2, b % 2] = t[32 * b : 32 * (b + 1)]
    small_step(0)

    ready(11, 12)

    def tile(at):
        ts = slice(at, at + own)
        r = mm(gt[:, ts].T, wt[...])
        gm[ts, :] = (r * scale + gm[ts, :].astype(F32)).astype(BF)

    tile(2 * own)
    go(c_g[0])
    tile(3 * own)
    go(c_g[1])
    c_g[0].wait_recv()
    far_sum[lo] = added(gm[2 * own : 2 * own + half], far_in[lo]).astype(BF)
    go(c_y[0])
    small_step(1)
    go(c_qb, c_wox)
    c_g[1].wait_recv()
    far_sum[hi] = added(gm[3 * own : 3 * own + half], far_in[hi]).astype(BF)
    go(c_y[1])
    tile(own)
    go(c_g[2])
    small_step(2)
    c_qa.wait_recv()
    qa4[...] = added(dwq[:, :, bx, ra], qa_in[...]).astype(BF)
    go(c_qa0)
    tile(0)
    small_step(3)

    ready(12, 16)
    attn = mm(ctx[:, :own], wo[pl.ds(pl.multiple_of(j * w, 128), w), :], TN)
    c_ctx[4].wait_recv()
    attn += mm(ctx_in[0], wo[pl.ds(pl.multiple_of((j ^ 1) * w, 128), w), :], TN)
    for k in range(4):
        c_ctx[k].wait_recv()
    attn += mm(ctx_in[1], wo[pl.ds(pl.multiple_of((j ^ 2) * w, 128), w), :], TN)
    attn += mm(ctx_in[2], wo[pl.ds(pl.multiple_of((j ^ 3) * w, 128), w), :], TN)
    out_ref[...] = (
        xo[...].astype(F32) + attn + added(pown[...], py[...]) + (flat(bo[...]) + flat(bd[...]))
    ).astype(BF)

    c_qa0.wait_recv()
    qa2[...] = added(qa4[:, b0], qa_in2[...]).astype(BF)
    go(c_qa1)
    c_qb.wait_recv()
    qb4[...] = added(dwq[:, :, bx, rb], qb_in[...]).astype(BF)
    go(c_qb0)
    for c in c_up:
        c.wait_recv()
    c_dnx.wait_recv()
    mine = up4[z].astype(F32) + up_in[0].astype(F32) + added(up_in[1], up_in[2])
    nu = wup_ref.shape[0]
    nd = dn2.shape[1]
    down = added(dn2[bx], dn_in[...])
    for a in range(4):
        cut = slice(a * w, (a + 1) * w)
        fin[a, :nu] = mine[:nu, cut].astype(BF)
        fin[a, nu : nu + nd] = down[:, cut].astype(BF)
        fin[a, nu + nd :] = mine[nu:, cut].astype(BF)
    go(*c_own)
    own_in[j] = fin[j]
    small_step(4)
    sums_ref[...] = sm[5]
    c_wox.wait_recv()
    wo4[...] = added(dwo[:, :, bx], wo_in[...]).astype(BF)
    go(c_wo0)
    c_qb0.wait_recv()
    qb2[...] = added(qb4[:, b0], qb_in2[...]).astype(BF)
    go(c_qb1)
    c_wo0.wait_recv()
    wo2[...] = added(wo4[:, b0], wo_in2[...]).astype(BF)
    go(c_wo1)
    c_qa1.wait_recv()
    c_qb1.wait_recv()
    done = jnp.concatenate([added(qa2[b1], qa_in3[...]), added(qb2[b1], qb_in3[...])], axis=0).astype(BF)
    for k in range(3):
        qfin[k] = done[k * w : (k + 1) * w]
    for t in range(3):

        @pl.when(q_dst[t] != j)
        def _():
            c_q[t].start()

        @pl.when(q_dst[t] == j)
        def _():
            q_own[t] = qfin[(3 * j + t) // 4]

    c_wo1.wait_recv()
    piece2[...] = added(wo2[b1], wo_in3[...]).astype(BF)
    for r in range(4):
        di, dj = dests[r]

        @pl.when((di != i) | (dj != j))
        def _():
            c_own2[r].start()

        @pl.when((di == i) & (dj == j))
        def _():
            owner_in2[i % 4] = piece2[:, pl.ds(pl.multiple_of(dj * w, 128), w)]


    c_g[2].wait_recv()
    c_y[0].wait_recv()
    g_ref[lo] = added(gm[lo], near_in[lo]) + y_in[lo].astype(F32)
    c_y[1].wait_recv()
    g_ref[hi] = added(gm[hi], near_in[hi]) + y_in[hi].astype(F32)

    for t in range(3):

        @pl.when(q_dst[t] != j)
        def _():
            c_q[t].wait_recv()

        wq_ref[:, t * w : (t + 1) * w] = q_own[t].astype(F32).T.astype(BF)
    for r in range(4):
        di, dj = dests[r]

        @pl.when((di != i) | (dj != j))
        def _():
            c_own2[r].wait_recv()

    for c in c_own:
        c.wait_recv()
    no = piece2.shape[0]
    for a in range(4):
        wup_ref[:, a * part_u : (a + 1) * part_u] = own_in[a, :nu, :part_u]
        wup_ref[:, (4 + a) * part_u : (5 + a) * part_u] = own_in[a, :nu, part_u:]
        wdn_ref[a * nu : (a + 1) * nu, :] = own_in[a, nu:]
        wout_ref[a * no : (a + 1) * no, :] = owner_in2[a]

    for c in started:
        c.wait_send()
    for t in range(3):

        @pl.when(q_dst[t] != j)
        def _():
            c_q[t].wait_send()

    for r in range(4):
        di, dj = dests[r]

        @pl.when((di != i) | (dj != j))
        def _():
            c_own2[r].wait_send()


def tail_stage(gt, na, gm, ctx, dya, wt, w_out, upk, upo, dn, x, pown, py, ga, sa, bo, bd, small, smallf, cid):
    own, d = x.shape
    tok = na.shape[0]
    w = d // 4
    vm = pl.BlockSpec(memory_space=pltpu.VMEM)
    hbm = pl.BlockSpec(memory_space=pl.ANY)
    sds = jax.ShapeDtypeStruct
    big = lambda *s: pltpu.VMEM(s, BF)
    nb = d // 8
    nu = upk.shape[1]
    nd = dn[0].shape[1]
    no = w // 8
    r2 = 3 * w // 2
    return pl.pallas_call(
        tail_kernel,
        in_specs=[hbm] * 16 + [vm] * 6,
        out_specs=[vm] * 7,
        out_shape=(
            sds((own, d), BF), sds((own, d), F32), sds((nb, d), BF), sds((4 * nb, w), BF),
            sds((nb, 3 * w), BF), sds((4 * no, w), BF), sds((16, d), F32),
        ),
        scratch_shapes=[
            big(3 * w, tok), big(tok, d), big(tok, d), big(w, tok), big(tok, d), big(3 * w, d), big(d, d),
            big(4, nu, d), big(4, nu, d), big(4, 2, nd, d),
            big(own, d), big(own, d), big(own, d),
            big(3, w, own), big(4, nu, d), big(3, nu, d), big(nd, d), big(2, nd, d),
            big(2, 2, 2, 3 * w, 128), big(2, 2, r2, 128), big(2, 2, r2, 128), big(2, 2, r2, 128), big(2, 2, r2, 128),
            big(2, r2, 128), big(2, r2, 128), big(2, r2, 128), big(2, r2, 128), big(r2, 128), big(r2, 128),
            big(3, w, 128), big(3, w, 128),
            big(2, 2, 2, no, d), big(2, 2, no, d), big(2, 2, no, d), big(2, no, d), big(2, no, d), big(no, d),
            big(4, 2 * nb, w), big(no, d), big(4, 2 * nb, w), big(4, no, w),
            big(own, d), big(own, d), big(own, d), big(own, d),
            pltpu.VMEM((6, 16, d), F32), pltpu.VMEM((5, 16, d), F32),
            pltpu.SemaphoreType.DMA((16,)), pltpu.SemaphoreType.DMA((40,)), pltpu.SemaphoreType.DMA((40,)),
        ],
        compiler_params=pltpu.CompilerParams(vmem_limit_bytes=VMEM_LIMIT, collective_id=cid, has_side_effects=True),
        cost_estimate=pl.CostEstimate(
            flops=14 * tok * d * w, bytes_accessed=10 * tok * d, transcendentals=0
        ),
        name="tail_stage",
    )(gt, na, gm, ctx, dya, wt, w_out, upk, upo, *dn, x, pown, py, ga, sa, bo, bd, small, smallf)


def final_kernel(out_t, g_ref, x_ref, dy_ref, wup, wdn, wq, wout, sums,
                 out, gin, ga, sa, gm, sm, dwq, bq, dwout, bo, dwup, bu, dwdn, bd):
    out[...] = out_t[...]
    normed, inv = norm_parts(x_ref[...])
    g = g_ref[...]
    gin[...] = dy_ref[...].astype(F32) + inv * (
        g - jnp.mean(g, axis=-1, keepdims=True) - normed * jnp.mean(g * normed, axis=-1, keepdims=True)
    )

    @pl.when(pl.program_id(0) == 0)
    def _():
        d = sums.shape[1]
        for ref, first, count in ((ga, 0, 1), (sa, 1, 1), (bq, 2, 3), (gm, 5, 1), (sm, 6, 1), (bo, 7, 1), (bd, 7, 1), (bu, 8, 4)):
            for k in range(count):
                ref[k * d : (k + 1) * d] = sums[first + k, :]
        dwup[...] = wup[...].astype(F32)
        dwdn[...] = wdn[...].astype(F32)
        dwq[...] = wq[...].astype(F32)
        dwout[...] = wout[...].astype(F32)


def final_stage(out_t, g, x, dy, wup, wdn, wq, wout, sums, steps=4):
    own, d = x.shape
    row = pl.BlockSpec((own // steps, d), lambda i: (i, 0))
    const = lambda v: pl.BlockSpec(v.shape, lambda i: (0,) * len(v.shape))
    sds = lambda *s: jax.ShapeDtypeStruct(s, F32)
    like = lambda v: sds(*v.shape)
    outs = (
        jax.ShapeDtypeStruct((own, d), BF), sds(own, d), sds(d), sds(d), sds(d), sds(d), like(wq), sds(3 * d),
        like(wout), sds(d), like(wup), sds(4 * d), like(wdn), sds(d),
    )
    return pl.pallas_call(
        final_kernel,
        grid=(steps,),
        in_specs=[row, row, row, row] + [const(v) for v in (wup, wdn, wq, wout, sums)],
        out_specs=[row, row] + [const(v) for v in outs[2:]],
        out_shape=outs,
        compiler_params=pltpu.CompilerParams(vmem_limit_bytes=VMEM_LIMIT),
        name="final_stage",
    )(out_t, g, x, dy, wup, wdn, wq, wout, sums)


def layout(seq_lens, index):
    ends = jnp.cumsum(seq_lens, dtype=jnp.int32)
    starts = ends - seq_lens
    first = jnp.zeros_like(index)
    for s in range(1, seq_lens.shape[0]):
        first = jnp.where(index >= starts[s], starts[s], first)
    return first, index - first


def head_perm(v, bit):
    return lax.ppermute(v, "head", [(k, k ^ bit) for k in range(4)])


def dp_perm(v, bit):
    return lax.ppermute(v, "dp", [(k, k ^ bit) for k in range(8)])


def fast_body(inputs, lengths, attn_gain, attn_shift, mlp_gain, mlp_shift, w_qkv, b_qkv, w_out, b_out,
              w_up, b_up, w_down, b_down, cotangent):
    own, d = inputs.shape
    n = 4
    tok = own * n
    w = d // n
    pos = lax.axis_index("head").astype(jnp.int32).reshape(1)
    lens = lengths[0]
    (g_mlp, na, dy_all, qt, kt, vt, dot, kn, vn, cos, sin, p_own, p_far, up_keep, up_send, *dn, wt, small,
     smallf) = head_stage(
        inputs, cotangent, w_up, w_down, w_qkv, w_out, attn_gain, attn_shift, mlp_gain, mlp_shift, b_up, b_qkv, lens, n, 0
    )
    up_other = dp_perm(up_send, 1)
    dn = [dn[0]] + [dp_perm(dn[k], 2 * k) for k in (1, 2, 3)]
    p_y = head_perm(p_far, 2)
    gt, ctx = attention(lens, pos, cos, sin, qt, kt, vt, dot, kn, vn, own, tok // 2, halved=True)
    out_t, g, wup, wdn, wq, wout, sums = tail_stage(
        gt, na, g_mlp, ctx, dy_all, wt, w_out, up_keep, up_other, dn, inputs, p_own, p_y,
        attn_gain, attn_shift, b_out, b_down, small, smallf, 1
    )
    return tuple(final_stage(out_t, g, inputs, cotangent, wup, wdn, wq, wout, sums))


def general_body(inputs, lengths, attn_gain, attn_shift, mlp_gain, mlp_shift, w_qkv, b_qkv, w_out, b_out,
                 w_up, b_up, w_down, b_down, cotangent):
    own, d = inputs.shape
    n = lax.axis_size("head")
    n_dp = lax.axis_size("dp")
    tok = own * n
    w = d // n
    f = w_up.shape[1] // n
    j = lax.axis_index("head")
    pos = j.astype(jnp.int32).reshape(1)
    rows = lambda v: v.reshape(1, -1)
    ga, sa, gm, sm = rows(attn_gain), rows(attn_shift), rows(mlp_gain), rows(mlp_shift)
    bq, bu = rows(b_qkv), rows(b_up)
    lens = lengths[0]
    gather = lambda v: lax.all_gather(v, "head", axis=0, tiled=True)
    over_dp = lambda v, axis: lax.psum_scatter(v, "dp", scatter_dimension=axis, tiled=True)
    over_head = lambda v: lax.psum_scatter(v, "head", scatter_dimension=0, tiled=True)
    x_all = gather(inputs)
    dy_all = gather(cotangent)
    first, position = layout(lens, jnp.arange(tok, dtype=jnp.int32))
    freqs = 10000.0 ** (-(2.0 * jnp.arange(HALF, dtype=F32)) / ROT)
    angle = freqs[:, None] * position.astype(F32)[None, :]
    cos, sin = jnp.cos(angle), jnp.sin(angle)
    part, g_mlp, dwu, dwd, small, smallf = mlp(pos, x_all, dy_all, w_up, w_down, bu, gm, sm, n)
    qt, kt, vt, dot, kn, vn, na = proj(pos, x_all, dy_all, w_qkv, bq, w_out, ga, sa, cos, sin, n, tok, 0)
    gt, ctx = attention(
        lens, jnp.zeros((1,), jnp.int32), cos, sin, qt, kt, vt, dot, kn, vn, own, tok // 2
    )
    total, dwq, bias_q, small_q = post(pos, gt, na, g_mlp, w_qkv, ga, sa, n)
    attn_part = mm(ctx, lax.dynamic_slice_in_dim(w_out, j * w, w, 0), TN)
    bias = b_out.astype(F32) + b_down.astype(F32)
    output = inputs.astype(F32) + over_head((attn_part + part.astype(F32)).astype(BF)).astype(F32) + bias
    g_sum = over_head(total).astype(F32)
    normed, inv = norm_parts(inputs)
    grad_inputs = cotangent.astype(F32) + inv * (
        g_sum - jnp.mean(g_sum, axis=-1, keepdims=True) - normed * jnp.mean(g_sum * normed, axis=-1, keepdims=True)
    )
    dw_out = mm(ctx, dy_all).astype(BF)
    spread = lambda v: lax.all_to_all(v, "head", split_axis=1, concat_axis=0, tiled=True)
    grad_w_up = over_dp(dwu, 0).astype(F32)
    grad_w_down = over_dp(spread(dwd), 0).astype(F32)
    grad_w_out = over_dp(spread(dw_out), 0).astype(F32)
    qkv = over_dp(jnp.transpose(dwq, (0, 2, 1)).reshape(d, 3 * w), 0)
    qkv = lax.all_gather(qkv.reshape(d // n_dp, 3, w), "head", axis=2, tiled=True).reshape(d // n_dp, 3 * d)
    grad_w_qkv = lax.dynamic_slice_in_dim(qkv, j * 3 * w, 3 * w, 1).astype(F32)
    slots = jnp.where(jnp.arange(n)[:, None] == j, smallf[0:1], 0.0).reshape(-1)
    slots_q = jnp.where(jnp.arange(n)[None, :, None] == j, bias_q[0].reshape(3, 1, w), 0.0).reshape(-1)
    sums = lax.psum((small_q[0], small_q[1], small[0], small[1], slots_q, small[2] / n, slots), ("dp", "head"))
    return (output.astype(BF), grad_inputs, sums[0], sums[1], sums[2], sums[3], grad_w_qkv, sums[4],
            grad_w_out, sums[5], grad_w_up, sums[6], grad_w_down, sums[5])


def solution(mesh):
    fast = mesh.shape["dp"] == 8 and mesh.shape["head"] == 4
    whole = P(("dp", "head"), None)
    weight = P("dp", "head")
    return jax.shard_map(
        fast_body if fast else general_body,
        mesh=mesh,
        in_specs=(whole, P("dp", None)) + (P(),) * 12 + (whole,),
        out_specs=(whole, whole, P(), P(), P(), P(), weight, P(), weight, P(), weight, P(), weight, P()),
        check_vma=False,
    )
```

```python
import functools

import jax
import jax.numpy as jnp
import numpy as np
from jax import lax
from jax.experimental import pallas as pl
from jax.experimental.pallas import tpu as pltpu
from jax.sharding import PartitionSpec as P

HD = 64
ROT = 16
HALF = ROT // 2
NN = (((1,), (0,)), ((), ()))
NT = (((1,), (1,)), ((), ()))
TN = (((0,), (0,)), ((), ()))
FREQS = (10000.0 ** (-(2.0 * np.arange(HALF)) / ROT)).astype(np.float32)
BF = jnp.bfloat16
F32 = jnp.float32
VMEM_LIMIT = 62 * 1024 * 1024


def mm(a, b, dims=NN):
    return lax.dot_general(a, b, dims, preferred_element_type=F32)


def flat(v):
    return v.astype(F32).reshape(1, v.shape[0])


def norm_parts(x):
    v = x.astype(F32)
    center = v - jnp.mean(v, axis=-1, keepdims=True)
    inv = lax.rsqrt(jnp.mean(center * center, axis=-1, keepdims=True) + 1e-5)
    return center * inv, inv


def mlp_kernel(prev, final, pos, *refs):
    x_ref, dy_ref, wu, wd, bu, gain, shift = refs[:7]
    refs = refs[7:]
    if prev:
        pwu, pwd, psmall, psmallf = refs[:4]
        refs = refs[4:]
    part_ref, g_ref, out_wu, out_wd, small, smallf = refs[:6]
    if final:
        dwu, dwd = refs[6:8]
    else:
        dwu, dwd = out_wu, out_wd
    step = pl.program_id(0)

    @pl.when(step == 0)
    def _():
        if prev:
            dwu[...] = pwu[...]
            dwd[...] = pwd[...]
            small[...] = psmall[...]
            smallf[...] = psmallf[...]
        else:
            dwu[...] = jnp.zeros_like(dwu)
            dwd[...] = jnp.zeros_like(dwd)
            small[...] = jnp.zeros_like(small)
            smallf[...] = jnp.zeros_like(smallf)

    normed, _unused = norm_parts(x_ref[...])
    scale = gain[...].astype(F32)
    nm = (normed * scale + shift[...].astype(F32)).astype(BF)
    dy = dy_ref[...]
    pre = mm(nm, wu[...]) + bu[...].astype(F32)
    cdf = 0.5 + 0.5 * lax.erf(pre * (0.5**0.5))
    hid = (pre * cdf).astype(BF)
    slope = cdf + pre * (jnp.exp(-0.5 * pre * pre) * 0.3989422804014327)
    gp = (mm(dy, wd[...], NT) * slope).astype(BF)
    part_ref[...] = mm(hid, wd[...]).astype(BF)
    r = mm(gp, wu[...], NT)
    g_ref[...] = (r * scale).astype(BF)
    smallf[0:1, :] += jnp.sum(gp.astype(F32), axis=0, keepdims=True)
    small[0:1, :] += jnp.sum(r * normed, axis=0, keepdims=True)
    small[1:2, :] += jnp.sum(r, axis=0, keepdims=True)
    small[2:3, :] += jnp.sum(dy.astype(F32), axis=0, keepdims=True)
    dwd[...] += mm(hid, dy, TN)
    dwu[...] += mm(nm, gp, TN)

    if final:

        @pl.when(step == pl.num_programs(0) - 1)
        def _():
            out_wu[...] = dwu[...].astype(BF)
            out_wd[...] = dwd[...].astype(BF)


def mlp(pos, x, dy, wu, wd, bu, gain, shift, n, prev=None, final=True, tt=512):
    tok, d = x.shape
    f = wu.shape[1] // n
    row = lambda i, p: (i, 0)
    zero = lambda i, p: (0, 0)
    one = pl.Buffered(1)
    const = lambda shape: pl.BlockSpec(shape, zero, pipeline_mode=one)
    accs = [const((d, f)), const((f, d)), const((8, d)), const((8, f))]
    kind = BF if final else F32
    grid_spec = pltpu.PrefetchScalarGridSpec(
        num_scalar_prefetch=1,
        grid=(tok // tt,),
        in_specs=[
            pl.BlockSpec((tt, d), row),
            pl.BlockSpec((tt, d), row),
            pl.BlockSpec((d, f), lambda i, p: (0, p[0]), pipeline_mode=one),
            pl.BlockSpec((f, d), lambda i, p: (p[0], 0), pipeline_mode=one),
            pl.BlockSpec((1, f), lambda i, p: (0, p[0])),
            const((1, d)),
            const((1, d)),
        ]
        + (accs if prev is not None else []),
        out_specs=[pl.BlockSpec((tt, d), row), pl.BlockSpec((tt, d), row)] + accs,
        scratch_shapes=[pltpu.VMEM((d, f), F32), pltpu.VMEM((f, d), F32)] if final else [],
    )
    return pl.pallas_call(
        functools.partial(mlp_kernel, prev is not None, final),
        grid_spec=grid_spec,
        out_shape=(
            jax.ShapeDtypeStruct((tok, d), BF),
            jax.ShapeDtypeStruct((tok, d), BF),
            jax.ShapeDtypeStruct((d, f), kind),
            jax.ShapeDtypeStruct((f, d), kind),
            jax.ShapeDtypeStruct((8, d), F32),
            jax.ShapeDtypeStruct((8, f), F32),
        ),
        compiler_params=pltpu.CompilerParams(vmem_limit_bytes=VMEM_LIMIT),
        cost_estimate=pl.CostEstimate(
            flops=12 * tok * d * f, bytes_accessed=8 * tok * d + 12 * d * f, transcendentals=2 * tok * f
        ),
        name="mlp",
    )(pos, x, dy, wu, wd, bu, gain, shift, *(prev or ()))


def proj_kernel(nh, prev, pos, *refs):
    x_ref, dy_ref, wq, wk, wv, bq, bk, bv, wo, gain, shift, cos, sin = refs[:13]
    qt, kt, vt, dot, kn, vn, na_ref = refs[13 + (7 if prev else 0) :]
    normed, _unused = norm_parts(x_ref[...])
    na = (normed * gain[...].astype(F32) + shift[...].astype(F32)).astype(BF)
    na_ref[...] = na
    co = cos[...]
    si = sin[...]

    def rotated(t, scale):
        rows = []
        for h in range(nh):
            u = t[h * HD : (h + 1) * HD]
            u1 = u[:HALF]
            u2 = u[HALF:ROT]
            rows += [u1 * co - u2 * si, u2 * co + u1 * si, u[ROT:]]
        out = jnp.concatenate(rows, axis=0).astype(BF)
        return out if scale is None else out * jnp.asarray(scale, BF)

    def triple(w, b):
        return (mm(na, w[...]) + b[...].astype(F32)).astype(BF)

    qt[...] = rotated(triple(wq, bq).astype(F32).T, HD**-0.5)
    keys = rotated(triple(wk, bk).astype(F32).T, None)
    kt[...] = keys
    kn[...] = keys.T
    values = triple(wv, bv)
    vn[...] = values
    vt[...] = values.T
    dot[...] = mm(wo[...], dy_ref[...], NT).astype(BF)


def proj(pos, x, dy, w_qkv, b_qkv, w_out, gain, shift, cos, sin, n, total, first, prev=None, tt=512):
    tok, d = x.shape
    w = d // n
    nh = w // HD
    off = first // tt
    row = lambda i, p: (i, 0)
    zero = lambda i, p: (0, 0)
    one = pl.Buffered(1)
    wspec = lambda k: pl.BlockSpec((d, w), lambda i, p: (0, k * n + p[0]), pipeline_mode=one)
    bspec = lambda k: pl.BlockSpec((1, w), lambda i, p: (0, k * n + p[0]))
    lane = lambda rows: pl.BlockSpec((rows, tt), lambda i, p: (0, off + i))
    nat = lambda cols: pl.BlockSpec((tt, cols), lambda i, p: (off + i, 0))
    shapes = [(w, total)] * 4 + [(total, w)] * 2 + [(total, d)]
    grid_spec = pltpu.PrefetchScalarGridSpec(
        num_scalar_prefetch=1,
        grid=(tok // tt,),
        in_specs=[pl.BlockSpec((tt, d), row), pl.BlockSpec((tt, d), row)]
        + [wspec(0), wspec(1), wspec(2), bspec(0), bspec(1), bspec(2)]
        + [pl.BlockSpec((w, d), lambda i, p: (p[0], 0), pipeline_mode=one)]
        + [pl.BlockSpec((1, d), zero), pl.BlockSpec((1, d), zero), lane(HALF), lane(HALF)]
        + ([pl.BlockSpec(memory_space=pl.ANY)] * 7 if prev is not None else []),
        out_specs=[lane(w)] * 4 + [nat(w)] * 2 + [nat(d)],
    )
    return pl.pallas_call(
        functools.partial(proj_kernel, nh, prev is not None),
        grid_spec=grid_spec,
        out_shape=tuple(jax.ShapeDtypeStruct(s, BF) for s in shapes),
        input_output_aliases={14 + k: k for k in range(7)} if prev is not None else {},
        compiler_params=pltpu.CompilerParams(vmem_limit_bytes=VMEM_LIMIT),
        cost_estimate=pl.CostEstimate(
            flops=8 * tok * d * w, bytes_accessed=6 * tok * d + 12 * tok * w + 8 * d * w, transcendentals=0
        ),
        name="proj",
    )(pos, x, dy, w_qkv, w_qkv, w_qkv, b_qkv, b_qkv, b_qkv, w_out, gain, shift, cos, sin, *(prev or ()))


def head_kernel(nh, x_hbm, dy_hbm, wu_hbm, wd_hbm, wqkv_hbm, wo_hbm, gain_a, shift_a, gain_m, shift_m, bu, bq, lens,
                g_out, na_out, dy_out, qt, kt, vt, dot, kn, vn, cos, sin, p_own, p_far, up_keep, up_send, dn0, dn1, dn2, dn3,
                w_t, small, smallf,
                xs, dys, wu, wd, wqkv, wt, wo, bias_t, bias_all, bias_u, parts, far_in, near_in, dwu, dwd, load, send, recv):
    step = pl.program_id(0)
    i = lax.axis_index("dp")
    j = lax.axis_index("head")
    own, d = x_hbm.shape
    f = wu.shape[1]
    w = wo.shape[0]
    half = own // 2
    core = {"head": j ^ 1}
    across = {"head": j ^ 2}

    def remote(src, dst, k, to):
        return pltpu.make_async_remote_copy(
            src_ref=src, dst_ref=dst, send_sem=send.at[k], recv_sem=recv.at[k], device_id=to,
            device_id_type=pl.DeviceIdType.MESH)

    lo, hi = pl.ds(0, half), pl.ds(half, half)
    copies = [
        remote(x_hbm, xs.at[1], 0, core),
        remote(dy_hbm, dys.at[1], 1, core),
        remote(x_hbm.at[lo], xs.at[2, lo], 2, across),
        remote(dy_hbm.at[lo], dys.at[2, lo], 3, across),
        remote(x_hbm.at[hi], xs.at[3, lo], 4, across),
        remote(dy_hbm.at[hi], dys.at[3, lo], 5, across),
        remote(xs.at[2, lo], xs.at[2, hi], 6, core),
        remote(dys.at[2, lo], dys.at[2, hi], 7, core),
        remote(xs.at[3, lo], xs.at[3, hi], 8, core),
        remote(dys.at[3, lo], dys.at[3, hi], 9, core),
        remote(parts.at[1], near_in, 10, core),
        remote(parts.at[2, hi], far_in.at[lo], 11, core),
        remote(parts.at[3, hi], far_in.at[hi], 12, core),
    ]
    locals_ = [
        pltpu.make_async_copy(x_hbm, xs.at[0], load.at[0]),
        pltpu.make_async_copy(dy_hbm, dys.at[0], load.at[1]),
        pltpu.make_async_copy(wo_hbm.at[pl.ds(j * w, w)], wo, load.at[2]),
    ] + [
        pltpu.make_async_copy(wqkv_hbm.at[:, pl.ds(k * d + j * w, w)], wqkv.at[:, pl.ds(k * w, w)], load.at[3 + k])
        for k in range(3)
    ]
    part = f // 8
    for k in range(8):
        there, here = pl.ds(4 * k * part + j * part, part), pl.ds(k * part, part)
        locals_.append(pltpu.make_async_copy(wu_hbm.at[:, there], wu.at[:, here], load.at[6 + k]))
        locals_.append(pltpu.make_async_copy(wd_hbm.at[there], wd.at[here], load.at[14 + k]))

    @pl.when(step == 0)
    def _():
        barrier = pltpu.get_barrier_semaphore()
        for to in (core, across):
            pl.semaphore_signal(barrier, inc=1, device_id=to, device_id_type=pl.DeviceIdType.MESH)
        for c in locals_:
            c.start()
        pl.semaphore_wait(barrier, 2)
        for c in copies[:6]:
            c.start()
        dwu[...] = jnp.zeros_like(dwu)
        dwd[...] = jnp.zeros_like(dwd)
        small[...] = jnp.zeros_like(small)
        smallf[...] = jnp.zeros_like(smallf)
        for c in locals_:
            c.wait()
        for k in range(3):
            wt[k * w : (k + 1) * w, :] = wqkv[:, k * w : (k + 1) * w].T
            row = flat(bq[pl.ds(pl.multiple_of(k * d + j * w, 256), w)])
            bias_t[k * w : (k + 1) * w, :] = jnp.broadcast_to(row, (128, w)).T
        bias_all[0:1, :] = flat(bu[...])
        for k in range(8):
            bias_u[0:1, k * part : (k + 1) * part] = bias_all[0:1, pl.ds(pl.multiple_of(4 * k * part + j * part, 128), part)]

    @pl.when(step == 1)
    def _():
        copies[0].wait_recv()

    @pl.when(step == 2)
    def _():
        copies[6].wait_recv()

    @pl.when(step == 3)
    def _():
        copies[8].wait_recv()

    normed, _unused = norm_parts(xs[step])
    scale = flat(gain_m[...])
    nm = (normed * scale + flat(shift_m[...])).astype(BF)
    na = (normed * flat(gain_a[...]) + flat(shift_a[...])).astype(BF)
    na_out[...] = na
    pre = mm(nm, wu[...]) + bias_u[0:1, :]
    cdf = 0.5 + 0.5 * lax.erf(pre * (0.5**0.5))
    hid = (pre * cdf).astype(BF)
    slope = cdf + pre * (jnp.exp(-0.5 * pre * pre) * 0.3989422804014327)
    parts[step] = mm(hid, wd[...]).astype(BF)

    lane = lax.broadcasted_iota(jnp.int32, (1, own), 1)
    far = jnp.where(lane < half, j ^ 2, j ^ 3) * own + (step - 2) * half + lane % half
    index = jnp.where(step == 0, j * own + lane, jnp.where(step == 1, (j ^ 1) * own + lane, far))
    begin = jnp.zeros_like(index)
    total = jnp.int32(0)
    for s in range(lens.shape[0] - 1):
        total = total + lens[s]
        begin = jnp.where(index >= total, total, begin)
    sub = lax.broadcasted_iota(jnp.int32, (HALF, own), 0)
    freqs = jnp.zeros((HALF, own), F32)
    for k in range(HALF):
        freqs = jnp.where(sub == k, float(FREQS[k]), freqs)
    angle = freqs * (index - begin).astype(F32)
    co = jnp.cos(angle)
    si = jnp.sin(angle)
    cos[...] = co
    sin[...] = si

    def projected(k):
        b = bias_t[k * w : (k + 1) * w, :]
        t = mm(wt[k * w : (k + 1) * w, :], na, NT)
        return (t + jnp.concatenate([b] * (own // 128), axis=1)).astype(BF)

    def rotated(t, factor):
        rows = []
        for h in range(nh):
            u = t[h * HD : (h + 1) * HD].astype(F32)
            u1 = u[:HALF]
            u2 = u[HALF:ROT]
            rows += [u1 * co - u2 * si, u2 * co + u1 * si, u[ROT:]]
        out = jnp.concatenate(rows, axis=0)
        return (out if factor is None else out * factor).astype(BF)

    qt[...] = rotated(projected(0), HD**-0.5)
    keys = rotated(projected(1), None)
    kt[...] = keys
    kn[...] = keys.T
    values = projected(2)
    vt[...] = values
    vn[...] = values.T

    @pl.when(step == 1)
    def _():
        copies[1].wait_recv()
        copies[10].start()
        copies[2].wait_recv()
        copies[6].start()

    @pl.when(step == 2)
    def _():
        copies[7].wait_recv()
        copies[11].start()

    @pl.when(step == 3)
    def _():
        copies[12].start()
        copies[5].wait_recv()
        copies[9].start()
        copies[9].wait_recv()

    dy = dys[step]
    dy_out[...] = dy
    gp = (mm(dy, wd[...], NT) * slope).astype(BF)
    r = mm(gp, wu[...], NT)
    g_out[...] = (r * scale).astype(BF)
    smallf[0:1, :] += jnp.sum(gp.astype(F32), axis=0, keepdims=True)
    small[0:1, :] += jnp.sum(r * normed, axis=0, keepdims=True)
    small[1:2, :] += jnp.sum(r, axis=0, keepdims=True)
    small[2:3, :] += jnp.sum(dy.astype(F32), axis=0, keepdims=True)
    dwd[...] += mm(hid, dy, TN)
    dwu[...] += mm(nm, gp, TN)
    dot[...] = mm(wo[...], dy, NT).astype(BF)

    @pl.when(step == 1)
    def _():
        copies[3].wait_recv()
        copies[7].start()

    @pl.when(step == 2)
    def _():
        copies[4].wait_recv()
        copies[8].start()

    @pl.when(step == 3)
    def _():
        rows = dwu.shape[0] // 8
        keep = dn0.shape[1]
        for b in range(4):
            for ref, at in ((up_keep, 2 * b + i % 2), (up_send, 2 * b + 1 - i % 2)):
                at = pl.multiple_of(at * rows, rows)
                ref[b, :rows] = dwu[pl.ds(at, rows), :].astype(BF)
                ref[b, rows:] = dwd[pl.ds(at + keep, rows - keep), :].astype(BF)
            ref = (dn0, dn1, dn2, dn3)[b]
            for x in range(2):
                at = 2 * ((i // 2) ^ b) + x
                ref[x] = dwd[pl.ds(pl.multiple_of(at * rows, rows), keep), :].astype(BF)
        w_t[...] = wt[...]
        copies[10].wait_recv()
        p_own[...] = (parts[0].astype(F32) + near_in[...].astype(F32)).astype(BF)
        copies[11].wait_recv()
        p_far[lo] = (parts[2, lo].astype(F32) + far_in[lo].astype(F32)).astype(BF)
        copies[12].wait_recv()
        p_far[hi] = (parts[3, lo].astype(F32) + far_in[hi].astype(F32)).astype(BF)
        for c in copies:
            c.wait_send()


def head_stage(x, dy, w_up, w_down, w_qkv, w_out, ga, sa, gm, sm, bu, bq, lens, n, cid):
    own, d = x.shape
    tok = own * n
    w = d // n
    f = w_up.shape[1] // n
    row = lambda i: (i, 0)
    lane = lambda rows: pl.BlockSpec((rows, own), lambda i: (0, i))
    nat = lambda cols: pl.BlockSpec((own, cols), row)
    one = pl.Buffered(1)
    const = lambda shape: pl.BlockSpec(shape, lambda i: (0,) * len(shape), pipeline_mode=one)
    hbm = pl.BlockSpec(memory_space=pl.ANY)
    sds = jax.ShapeDtypeStruct
    return pl.pallas_call(
        functools.partial(head_kernel, w // HD),
        grid=(n,),
        in_specs=[hbm] * 6
        + [const(v.shape) for v in (ga, sa, gm, sm, bu, bq)]
        + [pl.BlockSpec(memory_space=pltpu.SMEM)],
        out_specs=[nat(d)] * 3
        + [lane(w)] * 4
        + [nat(w)] * 2
        + [lane(HALF)] * 2
        + [const((own, d))] * 2
        + [const((4, d // 8 + 3 * d // 64, d))] * 2
        + [const((2, 5 * d // 64, d))] * 4
        + [const((3 * w, d)), const((8, d)), const((8, f))],
        out_shape=tuple(
            [sds((tok, d), BF)] * 3
            + [sds((w, tok), BF)] * 4
            + [sds((tok, w), BF)] * 2
            + [sds((HALF, tok), F32)] * 2
            + [sds((own, d), BF)] * 2
            + [sds((4, d // 8 + 3 * d // 64, d), BF)] * 2
            + [sds((2, 5 * d // 64, d), BF)] * 4
            + [sds((3 * w, d), BF), sds((8, d), F32), sds((8, f), F32)]
        ),
        scratch_shapes=[
            pltpu.VMEM((4, own, d), BF),
            pltpu.VMEM((4, own, d), BF),
            pltpu.VMEM((d, f), BF),
            pltpu.VMEM((f, d), BF),
            pltpu.VMEM((d, 3 * w), BF),
            pltpu.VMEM((3 * w, d), BF),
            pltpu.VMEM((w, d), BF),
            pltpu.VMEM((3 * w, 128), F32),
            pltpu.VMEM((8, 4 * f), F32),
            pltpu.VMEM((8, f), F32),
            pltpu.VMEM((4, own, d), BF),
            pltpu.VMEM((own, d), BF),
            pltpu.VMEM((own, d), BF),
            pltpu.VMEM((d, f), F32),
            pltpu.VMEM((f, d), F32),
            pltpu.SemaphoreType.DMA((22,)),
            pltpu.SemaphoreType.DMA((13,)),
            pltpu.SemaphoreType.DMA((13,)),
        ],
        compiler_params=pltpu.CompilerParams(
            vmem_limit_bytes=VMEM_LIMIT, collective_id=cid, has_side_effects=True
        ),
        cost_estimate=pl.CostEstimate(
            flops=12 * tok * d * f + 10 * tok * d * w, bytes_accessed=12 * tok * d + 8 * d * f, transcendentals=2 * tok * f
        ),
        name="head_stage",
    )(x, dy, w_up, w_down, w_qkv, w_out, ga, sa, gm, sm, bu, bq, lens)


def attn_kernel(nh, tok, blk, per, halved, lens, rel, cos, sin, qt, kt, vt, dot, kn, vn,
                gt_ref, ctx_ref, exps, low_exps, dk, dv, oacc, dqacc, mpart, lpart, rowsc, qpad, dopad):
    nseq = lens.shape[0]
    nblk = tok // blk
    shift = rel[0]
    heads = range(nh)

    def place(b):
        chunk = (b // per) ^ shift
        half = b % per
        at = chunk * per + half
        if halved:
            at = jnp.where(chunk < 2, at, 4 + (chunk - 2) + 2 * half)
        return pl.multiple_of(at * blk, blk)

    def rows_of(h):
        return slice(h * HD, (h + 1) * HD)

    def pair_of(h):
        return slice((h // 2) * 128, (h // 2) * 128 + 128)

    def fold(v, op):
        return op(v.reshape(blk // 8, 8, blk), axis=0)

    def begin_of(at):
        begin = jnp.int32(0)
        total = jnp.int32(0)
        for s in range(nseq - 1):
            total = total + lens[s]
            begin = jnp.where(at >= total, total, begin)
        return begin

    dk[...] = jnp.zeros_like(dk)
    dv[...] = jnp.zeros_like(dv)
    qpad[...] = jnp.zeros_like(qpad)
    dopad[...] = jnp.zeros_like(dopad)
    rows_iota = lax.broadcasted_iota(jnp.int32, (blk, blk), 0)
    cols_iota = lax.broadcasted_iota(jnp.int32, (1, blk), 1)

    def one_block(i, carry):
        first_tok = i * blk
        count = i - begin_of(first_tok) // blk + 1
        last_begin = begin_of(first_tok + blk - 1)
        cols = pl.ds(place(i), blk)
        query_idx = cols_iota + first_tok
        start_row = begin_of(query_idx)
        for h in heads:
            half = (h % 2) * HD
            qpad[h, half : half + HD, :] = qt[rows_of(h), cols]

        krow = pl.ds(place(i), blk)
        kidx = rows_iota + first_tok
        allowed = (kidx >= start_row) & (kidx <= query_idx)
        for h in heads:
            s = jnp.where(allowed, mm(kn[krow, pair_of(h)], qpad[h]), -1e30)
            exps[h, 0] = s
            mpart[h] = fold(s, jnp.max)

        def scores(step, c):
            b = i - step
            krow = pl.ds(place(b), blk)
            edge = last_begin > b * blk

            @pl.when(edge)
            def _():
                allowed = (rows_iota + b * blk) >= start_row
                for h in heads:
                    s = jnp.where(allowed, mm(kn[krow, pair_of(h)], qpad[h]), -1e30)
                    exps[h, step] = s
                    mpart[h] = jnp.maximum(mpart[h], fold(s, jnp.max))

            @pl.when(jnp.logical_not(edge))
            def _():
                for h in heads:
                    s = mm(kn[krow, pair_of(h)], qpad[h])
                    exps[h, step] = s
                    mpart[h] = jnp.maximum(mpart[h], fold(s, jnp.max))

            return c

        lax.fori_loop(1, count, scores, 0)
        for h in heads:
            rowsc[h : h + 1, :] = jnp.max(mpart[h], axis=0, keepdims=True)
        lpart[...] = jnp.zeros_like(lpart)
        oacc[...] = jnp.zeros_like(oacc)

        def weights(step, c):
            kcols = pl.ds(place(i - step), blk)
            for h in heads:
                e = jnp.exp(exps[h, step] - rowsc[h : h + 1, :])
                exps[h, step] = e
                lpart[h] += fold(e, jnp.sum)
                low = e.astype(BF)
                low_exps[h, step] = low
                oacc[h] += mm(vt[rows_of(h), kcols], low)
            return c

        lax.fori_loop(0, count, weights, 0)
        for h in heads:
            half = (h % 2) * HD
            inv = 1.0 / jnp.sum(lpart[h], axis=0, keepdims=True)
            o = oacc[h] * inv
            ctx_ref[rows_of(h), cols] = o.astype(BF)
            scaled = (dot[rows_of(h), cols].astype(F32) * inv).astype(BF)
            dopad[h, half : half + HD, :] = scaled
            rowsc[h : h + 1, :] = jnp.sum(o * scaled.astype(F32), axis=0, keepdims=True)
        dqacc[...] = jnp.zeros_like(dqacc)

        def backward(step, c):
            kcols = pl.ds(place(i - step), blk)
            dps = [mm(vn[kcols, pair_of(h)], dopad[h]) for h in heads]
            dss = [(exps[h, step] * (dps[h] - rowsc[h : h + 1, :])).astype(BF) for h in heads]
            dvs = [mm(dopad[h, (h % 2) * HD : (h % 2) * HD + HD, :], low_exps[h, step], NT) for h in heads]
            dks = [mm(qt[rows_of(h), cols], dss[h], NT) for h in heads]
            dqs = [mm(kt[rows_of(h), kcols], dss[h]) for h in heads]
            for h in heads:
                dv[rows_of(h), kcols] += dvs[h]
                dk[rows_of(h), kcols] += dks[h]
                dqacc[rows_of(h), :] += dqs[h]
            return c

        lax.fori_loop(0, count, backward, 0)
        co = cos[:, cols]
        si = sin[:, cols]
        for h in heads:
            base = h * HD
            g = dqacc[base : base + HD, :] * (HD**-0.5)
            g1 = g[:HALF]
            g2 = g[HALF:ROT]
            gt_ref[base : base + HD, cols] = jnp.concatenate(
                [g1 * co + g2 * si, g2 * co - g1 * si, g[ROT:]], axis=0
            ).astype(BF)
        return carry

    lax.fori_loop(0, nblk, one_block, 0)

    def finish(i, carry):
        cols = pl.ds(pl.multiple_of(i * blk, blk), blk)
        co = cos[:, cols]
        si = sin[:, cols]
        for h in heads:
            base = h * HD
            g = dk[base : base + HD, cols]
            g1 = g[:HALF]
            g2 = g[HALF:ROT]
            gt_ref[nh * HD + base : nh * HD + base + HD, cols] = jnp.concatenate(
                [g1 * co + g2 * si, g2 * co - g1 * si, g[ROT:]], axis=0
            ).astype(BF)
        gt_ref[2 * nh * HD :, cols] = dv[:, cols].astype(BF)
        return carry

    lax.fori_loop(0, nblk, finish, 0)


def attention(lens, rel, cos, sin, qt, kt, vt, dot, kn, vn, chunk, maxlen, halved=False, blk=256):
    width, tok = qt.shape
    nh = width // HD
    wb = maxlen // blk + 1
    vm = pl.BlockSpec(memory_space=pltpu.VMEM)
    sm = pl.BlockSpec(memory_space=pltpu.SMEM)
    return pl.pallas_call(
        functools.partial(attn_kernel, nh, tok, blk, chunk // blk, halved),
        out_shape=(jax.ShapeDtypeStruct((3 * width, tok), BF), jax.ShapeDtypeStruct((width, tok), BF)),
        in_specs=[sm, sm] + [vm] * 8,
        out_specs=(vm, vm),
        scratch_shapes=[
            pltpu.VMEM((nh, wb, blk, blk), F32),
            pltpu.VMEM((nh, wb, blk, blk), BF),
            pltpu.VMEM((width, tok), F32),
            pltpu.VMEM((width, tok), F32),
            pltpu.VMEM((nh, HD, blk), F32),
            pltpu.VMEM((width, blk), F32),
            pltpu.VMEM((nh, 8, blk), F32),
            pltpu.VMEM((nh, 8, blk), F32),
            pltpu.VMEM((8, blk), F32),
            pltpu.VMEM((nh, 128, blk), BF),
            pltpu.VMEM((nh, 128, blk), BF),
        ],
        compiler_params=pltpu.CompilerParams(vmem_limit_bytes=VMEM_LIMIT),
        cost_estimate=pl.CostEstimate(
            flops=20 * width * tok * maxlen, bytes_accessed=20 * width * tok, transcendentals=nh * tok * maxlen
        ),
        name="attention",
    )(lens, rel, cos, sin, qt, kt, vt, dot, kn, vn)


def post_kernel(pos, gt_ref, na_ref, gm_ref, wq, wk, wv, gain, shift, g_ref, out_w, bias, small, dw):
    step = pl.program_id(0)

    @pl.when(step == 0)
    def _():
        dw[...] = jnp.zeros_like(dw)
        bias[...] = jnp.zeros_like(bias)
        small[...] = jnp.zeros_like(small)

    gt = gt_ref[...]
    na = na_ref[...]
    w = wq.shape[1]
    scale = gain[...].astype(F32)
    gn = gt.T
    r = mm(gn[:, :w], wq[...], NT) + mm(gn[:, w : 2 * w], wk[...], NT) + mm(gn[:, 2 * w :], wv[...], NT)
    g_ref[...] = (r * scale + gm_ref[...].astype(F32)).astype(BF)
    small[0:1, :] += jnp.sum(r * na.astype(F32), axis=0, keepdims=True)
    small[1:2, :] += jnp.sum(r, axis=0, keepdims=True)
    bias[0:1, :] += jnp.sum(gn.astype(F32), axis=0, keepdims=True)
    dw[...] += mm(gt, na)

    @pl.when(step == pl.num_programs(0) - 1)
    def _():
        for b in range(dw.shape[1] // 128):
            out_w[b] = dw[:, b * 128 : (b + 1) * 128].astype(BF)
        small[0:1, :] = (small[0:1, :] - shift[...].astype(F32) * small[1:2, :]) / scale


def post(pos, gt, na, gm, w_qkv, gain, shift, n, tt=512):
    tok, d = na.shape
    w = d // n
    row = lambda i, p: (i, 0)
    zero = lambda i, p: (0, 0)
    one = pl.Buffered(1)
    const = lambda shape: pl.BlockSpec(shape, zero, pipeline_mode=one)
    wspec = lambda k: pl.BlockSpec((d, w), lambda i, p: (0, k * n + p[0]), pipeline_mode=one)
    grid_spec = pltpu.PrefetchScalarGridSpec(
        num_scalar_prefetch=1,
        grid=(tok // tt,),
        in_specs=[
            pl.BlockSpec((3 * w, tt), lambda i, p: (0, i)),
            pl.BlockSpec((tt, d), row),
            pl.BlockSpec((tt, d), row),
            wspec(0),
            wspec(1),
            wspec(2),
            const((1, d)),
            const((1, d)),
        ],
        out_specs=[
            pl.BlockSpec((tt, d), row),
            pl.BlockSpec((d // 128, 3 * w, 128), lambda i, p: (0, 0, 0), pipeline_mode=one),
            const((8, 3 * w)),
            const((8, d)),
        ],
        scratch_shapes=[pltpu.VMEM((3 * w, d), F32)],
    )
    return pl.pallas_call(
        post_kernel,
        grid_spec=grid_spec,
        out_shape=(
            jax.ShapeDtypeStruct((tok, d), BF),
            jax.ShapeDtypeStruct((d // 128, 3 * w, 128), BF),
            jax.ShapeDtypeStruct((8, 3 * w), F32),
            jax.ShapeDtypeStruct((8, d), F32),
        ),
        compiler_params=pltpu.CompilerParams(vmem_limit_bytes=VMEM_LIMIT),
        cost_estimate=pl.CostEstimate(
            flops=12 * tok * d * w, bytes_accessed=8 * tok * d + 6 * tok * w + 18 * d * w, transcendentals=0
        ),
        name="post",
    )(pos, gt, na, gm, w_qkv, w_qkv, w_qkv, gain, shift)


def tail_kernel(gt_h, na_h, gm_h, ctx_h, dya_h, wt_h, wo_h, upk_h, upo_h, dn0_h, dn1_h, dn2_h, dn3_h, x_h, pown_h, py_h,
                gain, shift_ref, bo, bd, small, smallf,
                out_ref, g_ref, wup_ref, wdn_ref, wq_ref, wout_ref, sums_ref,
                gt, na, gm, ctx, dya, wt, wo, upk, upo, dn, xo, pown, py,
                ctx_in, up4, up_in, dn_in, dn2,
                dwq, qa_in, qb_in, qa4, qb4, qa_in2, qb_in2, qa2, qb2, qa_in3, qb_in3, qfin, q_own,
                dwo, wo_in, wo4, wo_in2, wo2, wo_in3, fin, piece2, own_in, owner_in2,
                far_in, near_in, far_sum, y_in, sm, sm_in, load, send, recv):
    i = lax.axis_index("dp")
    j = lax.axis_index("head")
    own, d = x_h.shape
    w = wt.shape[0] // 3
    half = own // 2
    bx = i % 2
    b0 = (i // 2) % 2
    b1 = i // 4
    z = i // 2
    mesh_id = pl.DeviceIdType.MESH
    core, across, diag = {"head": j ^ 1}, {"head": j ^ 2}, {"head": j ^ 3}
    px, p0, p1 = {"dp": i ^ 1}, {"dp": i ^ 2}, {"dp": i ^ 4}
    lo, hi = pl.ds(0, half), pl.ds(half, half)
    count = [0]
    started = []

    def remote(src, dst, to):
        k = count[0]
        count[0] += 1
        return pltpu.make_async_remote_copy(
            src_ref=src, dst_ref=dst, send_sem=send.at[k], recv_sem=recv.at[k], device_id=to, device_id_type=mesh_id)

    def go(*copies):
        for c in copies:
            c.start()
            started.append(c)

    def local(src, dst, k):
        return pltpu.make_async_copy(src, dst, load.at[k])

    loads = [
        local(upk_h, upk, 0), local(upo_h, upo, 1),
        local(dn0_h, dn.at[0], 2), local(dn1_h, dn.at[1], 3), local(dn2_h, dn.at[2], 4), local(dn3_h, dn.at[3], 5),
        local(gt_h, gt, 6), local(na_h, na, 7), local(wt_h, wt, 8), local(ctx_h, ctx, 9), local(dya_h, dya, 10),
        local(gm_h, gm, 11), local(wo_h, wo, 12), local(x_h, xo, 13), local(pown_h, pown, 14), local(py_h, py, 15),
    ]
    c_ctx = [
        remote(ctx_h.at[:, pl.ds(2 * own, half)], ctx_in.at[1, :, lo], across),
        remote(ctx_h.at[:, pl.ds(3 * own, half)], ctx_in.at[1, :, hi], across),
        remote(ctx_h.at[:, pl.ds(2 * own + half, half)], ctx_in.at[2, :, lo], diag),
        remote(ctx_h.at[:, pl.ds(3 * own + half, half)], ctx_in.at[2, :, hi], diag),
        remote(ctx_h.at[:, pl.ds(own, own)], ctx_in.at[0], core),
    ]
    c_up = [remote(up4.at[z ^ k], up_in.at[k - 1], {"dp": i ^ (2 * k)}) for k in (1, 2, 3)]
    c_dnx = remote(dn2.at[1 - bx], dn_in, px)
    rows = dwq.shape[3] // 2
    ra, rb = pl.ds(0, rows), pl.ds(rows, rows)
    c_qa = remote(dwq.at[:, :, 1 - bx, ra], qa_in, px)
    c_qb = remote(dwq.at[:, :, 1 - bx, rb], qb_in, px)
    c_qa0 = remote(qa4.at[:, 1 - b0], qa_in2, p0)
    c_qb0 = remote(qb4.at[:, 1 - b0], qb_in2, p0)
    c_qa1 = remote(qa2.at[1 - b1], qa_in3, p1)
    c_qb1 = remote(qb2.at[1 - b1], qb_in3, p1)
    c_wox = remote(dwo.at[:, :, 1 - bx], wo_in, px)
    c_wo0 = remote(wo4.at[:, 1 - b0], wo_in2, p0)
    c_wo1 = remote(wo2.at[1 - b1], wo_in3, p1)
    c_g = [
        remote(gm.at[pl.ds(2 * own + half, half)], far_in.at[lo], core),
        remote(gm.at[pl.ds(3 * own + half, half)], far_in.at[hi], core),
        remote(gm.at[pl.ds(own, own)], near_in, core),
    ]
    c_y = [remote(far_sum.at[lo], y_in.at[lo], across), remote(far_sum.at[hi], y_in.at[hi], across)]
    c_sm = [remote(sm.at[s], sm_in.at[s], to) for s, to in enumerate((core, across, px, p0, p1))]
    c_own = [remote(fin.at[j ^ r], own_in.at[j], {"head": j ^ r}) for r in (1, 2, 3)]
    dests = []
    c_own2 = []
    for r in range(4):
        di, dj = 2 * j + i // 4, (i % 4) ^ r
        dests.append((di, dj))
        cut = pl.ds(pl.multiple_of(dj * w, 128), w)
        c_own2.append(remote(piece2.at[:, cut], owner_in2.at[i % 4], {"dp": di, "head": dj}))
    c_q = []
    q_dst = []
    for t in range(3):
        dst = (t - j + 4) % 4
        q_dst.append(dst)
        c_q.append(remote(qfin.at[(3 * dst + t) // 4], q_own.at[t], {"head": dst}))

    barrier = pltpu.get_barrier_semaphore()
    for to in (core, across, diag, px, p0, p1, {"dp": i ^ 6}):
        pl.semaphore_signal(barrier, inc=1, device_id=to, device_id_type=mesh_id)
    for c in loads:
        c.start()
    for r in range(4):
        si, sj = 4 * (i % 2) + (j ^ r), i // 2

        @pl.when((si != i) | (sj != j))
        def _():
            pl.semaphore_signal(barrier, inc=1, device_id={"dp": si, "head": sj}, device_id_type=mesh_id)

    to_self = jnp.where(2 * j + i // 4 == i, 1, 0)
    pl.semaphore_wait(barrier, 11 - to_self)

    go(*c_ctx)

    def added(a, b):
        return a.astype(F32) + b.astype(F32)

    def ready(first, last):
        for k in range(first, last):
            loads[k].wait()

    ready(0, 2)
    up4[...] = added(upk[...], upo[...]).astype(BF)
    go(*c_up)
    ready(2, 6)
    dn2[...] = (added(dn[0], dn[1]) + added(dn[2], dn[3])).astype(BF)
    go(c_dnx)

    ready(6, 9)
    gains = [jnp.zeros((1, 256), F32)] * 4
    for part, c in ((ra, c_qa), (rb, c_qb)):
        left = gt[part, :]
        for k in range(4):
            t = mm(left, na[:, 256 * k : 256 * (k + 1)])
            gains[k] += jnp.sum(t * wt[part, 256 * k : 256 * (k + 1)].astype(F32), axis=0, keepdims=True)
            t = t.astype(BF)
            dwq[k // 2, k % 2, 0, part] = t[:, :128]
            dwq[k // 2, k % 2, 1, part] = t[:, 128:]
        if c is c_qa:
            go(c)
    s_bias = mm(jnp.ones((8, gt.shape[1]), BF), gt[...], NT)[0:1]
    high = s_bias.astype(BF)
    low = (s_bias - high.astype(F32)).astype(BF)
    s_shift = mm(jnp.broadcast_to(high, (8, 3 * w)), wt[...])[0:1] + mm(jnp.broadcast_to(low, (8, 3 * w)), wt[...])[0:1]
    s_gain = jnp.concatenate(gains, axis=1)
    scale = flat(gain[...])

    sm[0] = jnp.zeros((16, d), F32)
    sm[0, 0:1, :] = (s_gain - flat(shift_ref[...]) * s_shift) / scale
    sm[0, 1:2, :] = s_shift
    for k in range(3):
        sm[0, 2 + k : 3 + k, pl.ds(pl.multiple_of(j * w, 128), w)] = s_bias[:, k * w : (k + 1) * w]
    sm[0, 5:7, :] = small[0:2, :]
    sm[0, 7:8, :] = small[2:3, :] * 0.25
    part_u = d // 8
    for b in range(8):
        at = pl.multiple_of((b % 2) * 4 * part_u + j * part_u, 128)
        sm[0, 8 + b // 2 : 9 + b // 2, pl.ds(at, part_u)] = smallf[0:1, b * part_u : (b + 1) * part_u]
    go(c_sm[0])

    def small_step(s):
        c_sm[s].wait_recv()
        sm[s + 1] = sm[s] + sm_in[s]
        if s < 4:
            go(c_sm[s + 1])

    ready(9, 11)
    t = mm(ctx[...], dya[...]).astype(BF)
    for b in range(8):
        dwo[b // 4, (b // 2) % 2, b % 2] = t[32 * b : 32 * (b + 1)]
    small_step(0)

    ready(11, 12)

    def tile(at):
        ts = slice(at, at + own)
        r = mm(gt[:, ts].T, wt[...])
        gm[ts, :] = (r * scale + gm[ts, :].astype(F32)).astype(BF)

    tile(2 * own)
    go(c_g[0])
    tile(3 * own)
    go(c_g[1])
    c_g[0].wait_recv()
    far_sum[lo] = added(gm[2 * own : 2 * own + half], far_in[lo]).astype(BF)
    go(c_y[0])
    small_step(1)
    go(c_qb, c_wox)
    c_g[1].wait_recv()
    far_sum[hi] = added(gm[3 * own : 3 * own + half], far_in[hi]).astype(BF)
    go(c_y[1])
    tile(own)
    go(c_g[2])
    small_step(2)
    c_qa.wait_recv()
    qa4[...] = added(dwq[:, :, bx, ra], qa_in[...]).astype(BF)
    go(c_qa0)
    tile(0)
    small_step(3)

    ready(12, 16)
    attn = mm(ctx[:, :own], wo[pl.ds(pl.multiple_of(j * w, 128), w), :], TN)
    c_ctx[4].wait_recv()
    attn += mm(ctx_in[0], wo[pl.ds(pl.multiple_of((j ^ 1) * w, 128), w), :], TN)
    for k in range(4):
        c_ctx[k].wait_recv()
    attn += mm(ctx_in[1], wo[pl.ds(pl.multiple_of((j ^ 2) * w, 128), w), :], TN)
    attn += mm(ctx_in[2], wo[pl.ds(pl.multiple_of((j ^ 3) * w, 128), w), :], TN)
    out_ref[...] = (
        xo[...].astype(F32) + attn + added(pown[...], py[...]) + (flat(bo[...]) + flat(bd[...]))
    ).astype(BF)

    c_qa0.wait_recv()
    qa2[...] = added(qa4[:, b0], qa_in2[...]).astype(BF)
    go(c_qa1)
    c_qb.wait_recv()
    qb4[...] = added(dwq[:, :, bx, rb], qb_in[...]).astype(BF)
    go(c_qb0)
    for c in c_up:
        c.wait_recv()
    c_dnx.wait_recv()
    mine = up4[z].astype(F32) + up_in[0].astype(F32) + added(up_in[1], up_in[2])
    nu = wup_ref.shape[0]
    nd = dn2.shape[1]
    down = added(dn2[bx], dn_in[...])
    for a in range(4):
        cut = slice(a * w, (a + 1) * w)
        fin[a, :nu] = mine[:nu, cut].astype(BF)
        fin[a, nu : nu + nd] = down[:, cut].astype(BF)
        fin[a, nu + nd :] = mine[nu:, cut].astype(BF)
    go(*c_own)
    own_in[j] = fin[j]
    small_step(4)
    sums_ref[...] = sm[5]
    c_wox.wait_recv()
    wo4[...] = added(dwo[:, :, bx], wo_in[...]).astype(BF)
    go(c_wo0)
    c_qb0.wait_recv()
    qb2[...] = added(qb4[:, b0], qb_in2[...]).astype(BF)
    go(c_qb1)
    c_wo0.wait_recv()
    wo2[...] = added(wo4[:, b0], wo_in2[...]).astype(BF)
    go(c_wo1)
    c_qa1.wait_recv()
    c_qb1.wait_recv()
    done = jnp.concatenate([added(qa2[b1], qa_in3[...]), added(qb2[b1], qb_in3[...])], axis=0).astype(BF)
    for k in range(3):
        qfin[k] = done[k * w : (k + 1) * w]
    for t in range(3):

        @pl.when(q_dst[t] != j)
        def _():
            c_q[t].start()

        @pl.when(q_dst[t] == j)
        def _():
            q_own[t] = qfin[(3 * j + t) // 4]

    c_wo1.wait_recv()
    piece2[...] = added(wo2[b1], wo_in3[...]).astype(BF)
    for r in range(4):
        di, dj = dests[r]

        @pl.when((di != i) | (dj != j))
        def _():
            c_own2[r].start()

        @pl.when((di == i) & (dj == j))
        def _():
            owner_in2[i % 4] = piece2[:, pl.ds(pl.multiple_of(dj * w, 128), w)]


    c_g[2].wait_recv()
    c_y[0].wait_recv()
    g_ref[lo] = added(gm[lo], near_in[lo]) + y_in[lo].astype(F32)
    c_y[1].wait_recv()
    g_ref[hi] = added(gm[hi], near_in[hi]) + y_in[hi].astype(F32)

    for t in range(3):

        @pl.when(q_dst[t] != j)
        def _():
            c_q[t].wait_recv()

        wq_ref[:, t * w : (t + 1) * w] = q_own[t].astype(F32).T.astype(BF)
    for r in range(4):
        di, dj = dests[r]

        @pl.when((di != i) | (dj != j))
        def _():
            c_own2[r].wait_recv()

    for c in c_own:
        c.wait_recv()
    no = piece2.shape[0]
    for a in range(4):
        wup_ref[:, a * part_u : (a + 1) * part_u] = own_in[a, :nu, :part_u]
        wup_ref[:, (4 + a) * part_u : (5 + a) * part_u] = own_in[a, :nu, part_u:]
        wdn_ref[a * nu : (a + 1) * nu, :] = own_in[a, nu:]
        wout_ref[a * no : (a + 1) * no, :] = owner_in2[a]

    for c in started:
        c.wait_send()
    for t in range(3):

        @pl.when(q_dst[t] != j)
        def _():
            c_q[t].wait_send()

    for r in range(4):
        di, dj = dests[r]

        @pl.when((di != i) | (dj != j))
        def _():
            c_own2[r].wait_send()


def tail_stage(gt, na, gm, ctx, dya, wt, w_out, upk, upo, dn, x, pown, py, ga, sa, bo, bd, small, smallf, cid):
    own, d = x.shape
    tok = na.shape[0]
    w = d // 4
    vm = pl.BlockSpec(memory_space=pltpu.VMEM)
    hbm = pl.BlockSpec(memory_space=pl.ANY)
    sds = jax.ShapeDtypeStruct
    big = lambda *s: pltpu.VMEM(s, BF)
    nb = d // 8
    nu = upk.shape[1]
    nd = dn[0].shape[1]
    no = w // 8
    r2 = 3 * w // 2
    return pl.pallas_call(
        tail_kernel,
        in_specs=[hbm] * 16 + [vm] * 6,
        out_specs=[vm] * 7,
        out_shape=(
            sds((own, d), BF), sds((own, d), F32), sds((nb, d), BF), sds((4 * nb, w), BF),
            sds((nb, 3 * w), BF), sds((4 * no, w), BF), sds((16, d), F32),
        ),
        scratch_shapes=[
            big(3 * w, tok), big(tok, d), big(tok, d), big(w, tok), big(tok, d), big(3 * w, d), big(d, d),
            big(4, nu, d), big(4, nu, d), big(4, 2, nd, d),
            big(own, d), big(own, d), big(own, d),
            big(3, w, own), big(4, nu, d), big(3, nu, d), big(nd, d), big(2, nd, d),
            big(2, 2, 2, 3 * w, 128), big(2, 2, r2, 128), big(2, 2, r2, 128), big(2, 2, r2, 128), big(2, 2, r2, 128),
            big(2, r2, 128), big(2, r2, 128), big(2, r2, 128), big(2, r2, 128), big(r2, 128), big(r2, 128),
            big(3, w, 128), big(3, w, 128),
            big(2, 2, 2, no, d), big(2, 2, no, d), big(2, 2, no, d), big(2, no, d), big(2, no, d), big(no, d),
            big(4, 2 * nb, w), big(no, d), big(4, 2 * nb, w), big(4, no, w),
            big(own, d), big(own, d), big(own, d), big(own, d),
            pltpu.VMEM((6, 16, d), F32), pltpu.VMEM((5, 16, d), F32),
            pltpu.SemaphoreType.DMA((16,)), pltpu.SemaphoreType.DMA((40,)), pltpu.SemaphoreType.DMA((40,)),
        ],
        compiler_params=pltpu.CompilerParams(vmem_limit_bytes=VMEM_LIMIT, collective_id=cid, has_side_effects=True),
        cost_estimate=pl.CostEstimate(
            flops=14 * tok * d * w, bytes_accessed=10 * tok * d, transcendentals=0
        ),
        name="tail_stage",
    )(gt, na, gm, ctx, dya, wt, w_out, upk, upo, *dn, x, pown, py, ga, sa, bo, bd, small, smallf)


def final_kernel(out_t, g_ref, x_ref, dy_ref, wup, wdn, wq, wout, sums,
                 out, gin, ga, sa, gm, sm, dwq, bq, dwout, bo, dwup, bu, dwdn, bd):
    out[...] = out_t[...]
    normed, inv = norm_parts(x_ref[...])
    g = g_ref[...]
    gin[...] = dy_ref[...].astype(F32) + inv * (
        g - jnp.mean(g, axis=-1, keepdims=True) - normed * jnp.mean(g * normed, axis=-1, keepdims=True)
    )

    @pl.when(pl.program_id(0) == 0)
    def _():
        d = sums.shape[1]
        for ref, first, count in ((ga, 0, 1), (sa, 1, 1), (bq, 2, 3), (gm, 5, 1), (sm, 6, 1), (bo, 7, 1), (bd, 7, 1), (bu, 8, 4)):
            for k in range(count):
                ref[k * d : (k + 1) * d] = sums[first + k, :]
        dwup[...] = wup[...].astype(F32)
        dwdn[...] = wdn[...].astype(F32)
        dwq[...] = wq[...].astype(F32)
        dwout[...] = wout[...].astype(F32)


def final_stage(out_t, g, x, dy, wup, wdn, wq, wout, sums, steps=2):
    own, d = x.shape
    row = pl.BlockSpec((own // steps, d), lambda i: (i, 0))
    const = lambda v: pl.BlockSpec(v.shape, lambda i: (0,) * len(v.shape))
    sds = lambda *s: jax.ShapeDtypeStruct(s, F32)
    like = lambda v: sds(*v.shape)
    outs = (
        jax.ShapeDtypeStruct((own, d), BF), sds(own, d), sds(d), sds(d), sds(d), sds(d), like(wq), sds(3 * d),
        like(wout), sds(d), like(wup), sds(4 * d), like(wdn), sds(d),
    )
    return pl.pallas_call(
        final_kernel,
        grid=(steps,),
        in_specs=[row, row, row, row] + [const(v) for v in (wup, wdn, wq, wout, sums)],
        out_specs=[row, row] + [const(v) for v in outs[2:]],
        out_shape=outs,
        compiler_params=pltpu.CompilerParams(vmem_limit_bytes=VMEM_LIMIT),
        name="final_stage",
    )(out_t, g, x, dy, wup, wdn, wq, wout, sums)


def layout(seq_lens, index):
    ends = jnp.cumsum(seq_lens, dtype=jnp.int32)
    starts = ends - seq_lens
    first = jnp.zeros_like(index)
    for s in range(1, seq_lens.shape[0]):
        first = jnp.where(index >= starts[s], starts[s], first)
    return first, index - first


def head_perm(v, bit):
    return lax.ppermute(v, "head", [(k, k ^ bit) for k in range(4)])


def dp_perm(v, bit):
    return lax.ppermute(v, "dp", [(k, k ^ bit) for k in range(8)])


def fast_body(inputs, lengths, attn_gain, attn_shift, mlp_gain, mlp_shift, w_qkv, b_qkv, w_out, b_out,
              w_up, b_up, w_down, b_down, cotangent):
    own, d = inputs.shape
    n = 4
    tok = own * n
    w = d // n
    pos = lax.axis_index("head").astype(jnp.int32).reshape(1)
    lens = lengths[0]
    (g_mlp, na, dy_all, qt, kt, vt, dot, kn, vn, cos, sin, p_own, p_far, up_keep, up_send, *dn, wt, small,
     smallf) = head_stage(
        inputs, cotangent, w_up, w_down, w_qkv, w_out, attn_gain, attn_shift, mlp_gain, mlp_shift, b_up, b_qkv, lens, n, 0
    )
    up_other = dp_perm(up_send, 1)
    dn = [dn[0]] + [dp_perm(dn[k], 2 * k) for k in (1, 2, 3)]
    p_y = head_perm(p_far, 2)
    gt, ctx = attention(lens, pos, cos, sin, qt, kt, vt, dot, kn, vn, own, tok // 2, halved=True)
    out_t, g, wup, wdn, wq, wout, sums = tail_stage(
        gt, na, g_mlp, ctx, dy_all, wt, w_out, up_keep, up_other, dn, inputs, p_own, p_y,
        attn_gain, attn_shift, b_out, b_down, small, smallf, 1
    )
    return tuple(final_stage(out_t, g, inputs, cotangent, wup, wdn, wq, wout, sums))


def general_body(inputs, lengths, attn_gain, attn_shift, mlp_gain, mlp_shift, w_qkv, b_qkv, w_out, b_out,
                 w_up, b_up, w_down, b_down, cotangent):
    own, d = inputs.shape
    n = lax.axis_size("head")
    n_dp = lax.axis_size("dp")
    tok = own * n
    w = d // n
    f = w_up.shape[1] // n
    j = lax.axis_index("head")
    pos = j.astype(jnp.int32).reshape(1)
    rows = lambda v: v.reshape(1, -1)
    ga, sa, gm, sm = rows(attn_gain), rows(attn_shift), rows(mlp_gain), rows(mlp_shift)
    bq, bu = rows(b_qkv), rows(b_up)
    lens = lengths[0]
    gather = lambda v: lax.all_gather(v, "head", axis=0, tiled=True)
    over_dp = lambda v, axis: lax.psum_scatter(v, "dp", scatter_dimension=axis, tiled=True)
    over_head = lambda v: lax.psum_scatter(v, "head", scatter_dimension=0, tiled=True)
    x_all = gather(inputs)
    dy_all = gather(cotangent)
    first, position = layout(lens, jnp.arange(tok, dtype=jnp.int32))
    freqs = 10000.0 ** (-(2.0 * jnp.arange(HALF, dtype=F32)) / ROT)
    angle = freqs[:, None] * position.astype(F32)[None, :]
    cos, sin = jnp.cos(angle), jnp.sin(angle)
    part, g_mlp, dwu, dwd, small, smallf = mlp(pos, x_all, dy_all, w_up, w_down, bu, gm, sm, n)
    qt, kt, vt, dot, kn, vn, na = proj(pos, x_all, dy_all, w_qkv, bq, w_out, ga, sa, cos, sin, n, tok, 0)
    gt, ctx = attention(
        lens, jnp.zeros((1,), jnp.int32), cos, sin, qt, kt, vt, dot, kn, vn, own, tok // 2
    )
    total, dwq, bias_q, small_q = post(pos, gt, na, g_mlp, w_qkv, ga, sa, n)
    attn_part = mm(ctx, lax.dynamic_slice_in_dim(w_out, j * w, w, 0), TN)
    bias = b_out.astype(F32) + b_down.astype(F32)
    output = inputs.astype(F32) + over_head((attn_part + part.astype(F32)).astype(BF)).astype(F32) + bias
    g_sum = over_head(total).astype(F32)
    normed, inv = norm_parts(inputs)
    grad_inputs = cotangent.astype(F32) + inv * (
        g_sum - jnp.mean(g_sum, axis=-1, keepdims=True) - normed * jnp.mean(g_sum * normed, axis=-1, keepdims=True)
    )
    dw_out = mm(ctx, dy_all).astype(BF)
    spread = lambda v: lax.all_to_all(v, "head", split_axis=1, concat_axis=0, tiled=True)
    grad_w_up = over_dp(dwu, 0).astype(F32)
    grad_w_down = over_dp(spread(dwd), 0).astype(F32)
    grad_w_out = over_dp(spread(dw_out), 0).astype(F32)
    qkv = over_dp(jnp.transpose(dwq, (0, 2, 1)).reshape(d, 3 * w), 0)
    qkv = lax.all_gather(qkv.reshape(d // n_dp, 3, w), "head", axis=2, tiled=True).reshape(d // n_dp, 3 * d)
    grad_w_qkv = lax.dynamic_slice_in_dim(qkv, j * 3 * w, 3 * w, 1).astype(F32)
    slots = jnp.where(jnp.arange(n)[:, None] == j, smallf[0:1], 0.0).reshape(-1)
    slots_q = jnp.where(jnp.arange(n)[None, :, None] == j, bias_q[0].reshape(3, 1, w), 0.0).reshape(-1)
    sums = lax.psum((small_q[0], small_q[1], small[0], small[1], slots_q, small[2] / n, slots), ("dp", "head"))
    return (output.astype(BF), grad_inputs, sums[0], sums[1], sums[2], sums[3], grad_w_qkv, sums[4],
            grad_w_out, sums[5], grad_w_up, sums[6], grad_w_down, sums[5])


def solution(mesh):
    fast = mesh.shape["dp"] == 8 and mesh.shape["head"] == 4
    whole = P(("dp", "head"), None)
    weight = P("dp", "head")
    return jax.shard_map(
        fast_body if fast else general_body,
        mesh=mesh,
        in_specs=(whole, P("dp", None)) + (P(),) * 12 + (whole,),
        out_specs=(whole, whole, P(), P(), P(), P(), weight, P(), weight, P(), weight, P(), weight, P()),
        check_vma=False,
    )
```

```python
import functools

import jax
import jax.numpy as jnp
import numpy as np
from jax import lax
from jax.experimental import pallas as pl
from jax.experimental.pallas import tpu as pltpu
from jax.sharding import PartitionSpec as P

HD = 64
ROT = 16
HALF = ROT // 2
NN = (((1,), (0,)), ((), ()))
NT = (((1,), (1,)), ((), ()))
TN = (((0,), (0,)), ((), ()))
FREQS = (10000.0 ** (-(2.0 * np.arange(HALF)) / ROT)).astype(np.float32)
BF = jnp.bfloat16
F32 = jnp.float32
VMEM_LIMIT = 62 * 1024 * 1024


def mm(a, b, dims=NN):
    return lax.dot_general(a, b, dims, preferred_element_type=F32)


def flat(v):
    return v.astype(F32).reshape(1, v.shape[0])


def norm_parts(x):
    v = x.astype(F32)
    center = v - jnp.mean(v, axis=-1, keepdims=True)
    inv = lax.rsqrt(jnp.mean(center * center, axis=-1, keepdims=True) + 1e-5)
    return center * inv, inv


def mlp_kernel(prev, final, pos, *refs):
    x_ref, dy_ref, wu, wd, bu, gain, shift = refs[:7]
    refs = refs[7:]
    if prev:
        pwu, pwd, psmall, psmallf = refs[:4]
        refs = refs[4:]
    part_ref, g_ref, out_wu, out_wd, small, smallf = refs[:6]
    if final:
        dwu, dwd = refs[6:8]
    else:
        dwu, dwd = out_wu, out_wd
    step = pl.program_id(0)

    @pl.when(step == 0)
    def _():
        if prev:
            dwu[...] = pwu[...]
            dwd[...] = pwd[...]
            small[...] = psmall[...]
            smallf[...] = psmallf[...]
        else:
            dwu[...] = jnp.zeros_like(dwu)
            dwd[...] = jnp.zeros_like(dwd)
            small[...] = jnp.zeros_like(small)
            smallf[...] = jnp.zeros_like(smallf)

    normed, _unused = norm_parts(x_ref[...])
    scale = gain[...].astype(F32)
    nm = (normed * scale + shift[...].astype(F32)).astype(BF)
    dy = dy_ref[...]
    pre = mm(nm, wu[...]) + bu[...].astype(F32)
    cdf = 0.5 + 0.5 * lax.erf(pre * (0.5**0.5))
    hid = (pre * cdf).astype(BF)
    slope = cdf + pre * (jnp.exp(-0.5 * pre * pre) * 0.3989422804014327)
    gp = (mm(dy, wd[...], NT) * slope).astype(BF)
    part_ref[...] = mm(hid, wd[...]).astype(BF)
    r = mm(gp, wu[...], NT)
    g_ref[...] = (r * scale).astype(BF)
    smallf[0:1, :] += jnp.sum(gp.astype(F32), axis=0, keepdims=True)
    small[0:1, :] += jnp.sum(r * normed, axis=0, keepdims=True)
    small[1:2, :] += jnp.sum(r, axis=0, keepdims=True)
    small[2:3, :] += jnp.sum(dy.astype(F32), axis=0, keepdims=True)
    dwd[...] += mm(hid, dy, TN)
    dwu[...] += mm(nm, gp, TN)

    if final:

        @pl.when(step == pl.num_programs(0) - 1)
        def _():
            out_wu[...] = dwu[...].astype(BF)
            out_wd[...] = dwd[...].astype(BF)


def mlp(pos, x, dy, wu, wd, bu, gain, shift, n, prev=None, final=True, tt=512):
    tok, d = x.shape
    f = wu.shape[1] // n
    row = lambda i, p: (i, 0)
    zero = lambda i, p: (0, 0)
    one = pl.Buffered(1)
    const = lambda shape: pl.BlockSpec(shape, zero, pipeline_mode=one)
    accs = [const((d, f)), const((f, d)), const((8, d)), const((8, f))]
    kind = BF if final else F32
    grid_spec = pltpu.PrefetchScalarGridSpec(
        num_scalar_prefetch=1,
        grid=(tok // tt,),
        in_specs=[
            pl.BlockSpec((tt, d), row),
            pl.BlockSpec((tt, d), row),
            pl.BlockSpec((d, f), lambda i, p: (0, p[0]), pipeline_mode=one),
            pl.BlockSpec((f, d), lambda i, p: (p[0], 0), pipeline_mode=one),
            pl.BlockSpec((1, f), lambda i, p: (0, p[0])),
            const((1, d)),
            const((1, d)),
        ]
        + (accs if prev is not None else []),
        out_specs=[pl.BlockSpec((tt, d), row), pl.BlockSpec((tt, d), row)] + accs,
        scratch_shapes=[pltpu.VMEM((d, f), F32), pltpu.VMEM((f, d), F32)] if final else [],
    )
    return pl.pallas_call(
        functools.partial(mlp_kernel, prev is not None, final),
        grid_spec=grid_spec,
        out_shape=(
            jax.ShapeDtypeStruct((tok, d), BF),
            jax.ShapeDtypeStruct((tok, d), BF),
            jax.ShapeDtypeStruct((d, f), kind),
            jax.ShapeDtypeStruct((f, d), kind),
            jax.ShapeDtypeStruct((8, d), F32),
            jax.ShapeDtypeStruct((8, f), F32),
        ),
        compiler_params=pltpu.CompilerParams(vmem_limit_bytes=VMEM_LIMIT),
        cost_estimate=pl.CostEstimate(
            flops=12 * tok * d * f, bytes_accessed=8 * tok * d + 12 * d * f, transcendentals=2 * tok * f
        ),
        name="mlp",
    )(pos, x, dy, wu, wd, bu, gain, shift, *(prev or ()))


def proj_kernel(nh, prev, pos, *refs):
    x_ref, dy_ref, wq, wk, wv, bq, bk, bv, wo, gain, shift, cos, sin = refs[:13]
    qt, kt, vt, dot, kn, vn, na_ref = refs[13 + (7 if prev else 0) :]
    normed, _unused = norm_parts(x_ref[...])
    na = (normed * gain[...].astype(F32) + shift[...].astype(F32)).astype(BF)
    na_ref[...] = na
    co = cos[...]
    si = sin[...]

    def rotated(t, scale):
        rows = []
        for h in range(nh):
            u = t[h * HD : (h + 1) * HD]
            u1 = u[:HALF]
            u2 = u[HALF:ROT]
            rows += [u1 * co - u2 * si, u2 * co + u1 * si, u[ROT:]]
        out = jnp.concatenate(rows, axis=0).astype(BF)
        return out if scale is None else out * jnp.asarray(scale, BF)

    def triple(w, b):
        return (mm(na, w[...]) + b[...].astype(F32)).astype(BF)

    qt[...] = rotated(triple(wq, bq).astype(F32).T, HD**-0.5)
    keys = rotated(triple(wk, bk).astype(F32).T, None)
    kt[...] = keys
    kn[...] = keys.T
    values = triple(wv, bv)
    vn[...] = values
    vt[...] = values.T
    dot[...] = mm(wo[...], dy_ref[...], NT).astype(BF)


def proj(pos, x, dy, w_qkv, b_qkv, w_out, gain, shift, cos, sin, n, total, first, prev=None, tt=512):
    tok, d = x.shape
    w = d // n
    nh = w // HD
    off = first // tt
    row = lambda i, p: (i, 0)
    zero = lambda i, p: (0, 0)
    one = pl.Buffered(1)
    wspec = lambda k: pl.BlockSpec((d, w), lambda i, p: (0, k * n + p[0]), pipeline_mode=one)
    bspec = lambda k: pl.BlockSpec((1, w), lambda i, p: (0, k * n + p[0]))
    lane = lambda rows: pl.BlockSpec((rows, tt), lambda i, p: (0, off + i))
    nat = lambda cols: pl.BlockSpec((tt, cols), lambda i, p: (off + i, 0))
    shapes = [(w, total)] * 4 + [(total, w)] * 2 + [(total, d)]
    grid_spec = pltpu.PrefetchScalarGridSpec(
        num_scalar_prefetch=1,
        grid=(tok // tt,),
        in_specs=[pl.BlockSpec((tt, d), row), pl.BlockSpec((tt, d), row)]
        + [wspec(0), wspec(1), wspec(2), bspec(0), bspec(1), bspec(2)]
        + [pl.BlockSpec((w, d), lambda i, p: (p[0], 0), pipeline_mode=one)]
        + [pl.BlockSpec((1, d), zero), pl.BlockSpec((1, d), zero), lane(HALF), lane(HALF)]
        + ([pl.BlockSpec(memory_space=pl.ANY)] * 7 if prev is not None else []),
        out_specs=[lane(w)] * 4 + [nat(w)] * 2 + [nat(d)],
    )
    return pl.pallas_call(
        functools.partial(proj_kernel, nh, prev is not None),
        grid_spec=grid_spec,
        out_shape=tuple(jax.ShapeDtypeStruct(s, BF) for s in shapes),
        input_output_aliases={14 + k: k for k in range(7)} if prev is not None else {},
        compiler_params=pltpu.CompilerParams(vmem_limit_bytes=VMEM_LIMIT),
        cost_estimate=pl.CostEstimate(
            flops=8 * tok * d * w, bytes_accessed=6 * tok * d + 12 * tok * w + 8 * d * w, transcendentals=0
        ),
        name="proj",
    )(pos, x, dy, w_qkv, w_qkv, w_qkv, b_qkv, b_qkv, b_qkv, w_out, gain, shift, cos, sin, *(prev or ()))


def head_kernel(nh, x_hbm, dy_hbm, wu_hbm, wd_hbm, wqkv_hbm, wo_hbm, gain_a, shift_a, gain_m, shift_m, bu, bq, lens,
                g_out, na_out, dy_out, qt, kt, vt, dot, kn, vn, cos, sin, p_own, p_far, up_keep, up_send, dn0, dn1, dn2, dn3,
                w_t, small, smallf,
                xs, dys, wu, wd, wqkv, wt, wo, bias_t, bias_all, bias_u, parts, far_in, near_in, dwu, dwd, load, send, recv):
    step = pl.program_id(0)
    i = lax.axis_index("dp")
    j = lax.axis_index("head")
    own, d = x_hbm.shape
    f = wu.shape[1]
    w = wo.shape[0]
    half = own // 2
    core = {"head": j ^ 1}
    across = {"head": j ^ 2}

    def remote(src, dst, k, to):
        return pltpu.make_async_remote_copy(
            src_ref=src, dst_ref=dst, send_sem=send.at[k], recv_sem=recv.at[k], device_id=to,
            device_id_type=pl.DeviceIdType.MESH)

    lo, hi = pl.ds(0, half), pl.ds(half, half)
    copies = [
        remote(x_hbm, xs.at[1], 0, core),
        remote(dy_hbm, dys.at[1], 1, core),
        remote(x_hbm.at[lo], xs.at[2, lo], 2, across),
        remote(dy_hbm.at[lo], dys.at[2, lo], 3, across),
        remote(x_hbm.at[hi], xs.at[3, lo], 4, across),
        remote(dy_hbm.at[hi], dys.at[3, lo], 5, across),
        remote(xs.at[2, lo], xs.at[2, hi], 6, core),
        remote(dys.at[2, lo], dys.at[2, hi], 7, core),
        remote(xs.at[3, lo], xs.at[3, hi], 8, core),
        remote(dys.at[3, lo], dys.at[3, hi], 9, core),
        remote(parts.at[1], near_in, 10, core),
        remote(parts.at[2, hi], far_in.at[lo], 11, core),
        remote(parts.at[3, hi], far_in.at[hi], 12, core),
    ]
    locals_ = [
        pltpu.make_async_copy(x_hbm, xs.at[0], load.at[0]),
        pltpu.make_async_copy(dy_hbm, dys.at[0], load.at[1]),
        pltpu.make_async_copy(wo_hbm.at[pl.ds(j * w, w)], wo, load.at[2]),
    ] + [
        pltpu.make_async_copy(wqkv_hbm.at[:, pl.ds(k * d + j * w, w)], wqkv.at[:, pl.ds(k * w, w)], load.at[3 + k])
        for k in range(3)
    ]
    part = f // 8
    for k in range(8):
        there, here = pl.ds(4 * k * part + j * part, part), pl.ds(k * part, part)
        locals_.append(pltpu.make_async_copy(wu_hbm.at[:, there], wu.at[:, here], load.at[6 + k]))
        locals_.append(pltpu.make_async_copy(wd_hbm.at[there], wd.at[here], load.at[14 + k]))

    @pl.when(step == 0)
    def _():
        barrier = pltpu.get_barrier_semaphore()
        for to in (core, across):
            pl.semaphore_signal(barrier, inc=1, device_id=to, device_id_type=pl.DeviceIdType.MESH)
        for c in locals_:
            c.start()
        pl.semaphore_wait(barrier, 2)
        for c in copies[:6]:
            c.start()
        dwu[...] = jnp.zeros_like(dwu)
        dwd[...] = jnp.zeros_like(dwd)
        small[...] = jnp.zeros_like(small)
        smallf[...] = jnp.zeros_like(smallf)
        for c in locals_:
            c.wait()
        for k in range(3):
            wt[k * w : (k + 1) * w, :] = wqkv[:, k * w : (k + 1) * w].T
            row = flat(bq[pl.ds(pl.multiple_of(k * d + j * w, 256), w)])
            bias_t[k * w : (k + 1) * w, :] = jnp.broadcast_to(row, (128, w)).T
        bias_all[0:1, :] = flat(bu[...])
        for k in range(8):
            bias_u[0:1, k * part : (k + 1) * part] = bias_all[0:1, pl.ds(pl.multiple_of(4 * k * part + j * part, 128), part)]

    @pl.when(step == 1)
    def _():
        copies[0].wait_recv()

    @pl.when(step == 2)
    def _():
        copies[6].wait_recv()

    @pl.when(step == 3)
    def _():
        copies[8].wait_recv()

    normed, _unused = norm_parts(xs[step])
    scale = flat(gain_m[...])
    nm = (normed * scale + flat(shift_m[...])).astype(BF)
    na = (normed * flat(gain_a[...]) + flat(shift_a[...])).astype(BF)
    na_out[...] = na
    pre = mm(nm, wu[...]) + bias_u[0:1, :]
    cdf = 0.5 + 0.5 * lax.erf(pre * (0.5**0.5))
    hid = (pre * cdf).astype(BF)
    slope = cdf + pre * (jnp.exp(-0.5 * pre * pre) * 0.3989422804014327)
    parts[step] = mm(hid, wd[...]).astype(BF)

    lane = lax.broadcasted_iota(jnp.int32, (1, own), 1)
    far = jnp.where(lane < half, j ^ 2, j ^ 3) * own + (step - 2) * half + lane % half
    index = jnp.where(step == 0, j * own + lane, jnp.where(step == 1, (j ^ 1) * own + lane, far))
    begin = jnp.zeros_like(index)
    total = jnp.int32(0)
    for s in range(lens.shape[0] - 1):
        total = total + lens[s]
        begin = jnp.where(index >= total, total, begin)
    sub = lax.broadcasted_iota(jnp.int32, (HALF, own), 0)
    freqs = jnp.zeros((HALF, own), F32)
    for k in range(HALF):
        freqs = jnp.where(sub == k, float(FREQS[k]), freqs)
    angle = freqs * (index - begin).astype(F32)
    co = jnp.cos(angle)
    si = jnp.sin(angle)
    cos[...] = co
    sin[...] = si

    def projected(k):
        b = bias_t[k * w : (k + 1) * w, :]
        t = mm(wt[k * w : (k + 1) * w, :], na, NT)
        return (t + jnp.concatenate([b] * (own // 128), axis=1)).astype(BF)

    def rotated(t, factor):
        rows = []
        for h in range(nh):
            u = t[h * HD : (h + 1) * HD].astype(F32)
            u1 = u[:HALF]
            u2 = u[HALF:ROT]
            rows += [u1 * co - u2 * si, u2 * co + u1 * si, u[ROT:]]
        out = jnp.concatenate(rows, axis=0)
        return (out if factor is None else out * factor).astype(BF)

    qt[...] = rotated(projected(0), HD**-0.5)
    keys = rotated(projected(1), None)
    kt[...] = keys
    kn[...] = keys.T
    values = projected(2)
    vt[...] = values
    vn[...] = values.T

    @pl.when(step == 1)
    def _():
        copies[1].wait_recv()
        copies[10].start()
        copies[2].wait_recv()
        copies[6].start()

    @pl.when(step == 2)
    def _():
        copies[7].wait_recv()
        copies[11].start()

    @pl.when(step == 3)
    def _():
        copies[12].start()
        copies[5].wait_recv()
        copies[9].start()
        copies[9].wait_recv()

    dy = dys[step]
    dy_out[...] = dy
    gp = (mm(dy, wd[...], NT) * slope).astype(BF)
    r = mm(gp, wu[...], NT)
    g_out[...] = (r * scale).astype(BF)
    smallf[0:1, :] += jnp.sum(gp.astype(F32), axis=0, keepdims=True)
    small[0:1, :] += jnp.sum(r * normed, axis=0, keepdims=True)
    small[1:2, :] += jnp.sum(r, axis=0, keepdims=True)
    small[2:3, :] += jnp.sum(dy.astype(F32), axis=0, keepdims=True)
    dwd[...] += mm(hid, dy, TN)
    dwu[...] += mm(nm, gp, TN)
    dot[...] = mm(wo[...], dy, NT).astype(BF)

    @pl.when(step == 1)
    def _():
        copies[3].wait_recv()
        copies[7].start()

    @pl.when(step == 2)
    def _():
        copies[4].wait_recv()
        copies[8].start()

    @pl.when(step == 3)
    def _():
        rows = dwu.shape[0] // 8
        keep = dn0.shape[1]
        for b in range(4):
            for ref, at in ((up_keep, 2 * b + i % 2), (up_send, 2 * b + 1 - i % 2)):
                at = pl.multiple_of(at * rows, rows)
                ref[b, :rows] = dwu[pl.ds(at, rows), :].astype(BF)
                ref[b, rows:] = dwd[pl.ds(at + keep, rows - keep), :].astype(BF)
            ref = (dn0, dn1, dn2, dn3)[b]
            for x in range(2):
                at = 2 * ((i // 2) ^ b) + x
                ref[x] = dwd[pl.ds(pl.multiple_of(at * rows, rows), keep), :].astype(BF)
        w_t[...] = wt[...]
        copies[10].wait_recv()
        p_own[...] = (parts[0].astype(F32) + near_in[...].astype(F32)).astype(BF)
        copies[11].wait_recv()
        p_far[lo] = (parts[2, lo].astype(F32) + far_in[lo].astype(F32)).astype(BF)
        copies[12].wait_recv()
        p_far[hi] = (parts[3, lo].astype(F32) + far_in[hi].astype(F32)).astype(BF)
        for c in copies:
            c.wait_send()


def head_stage(x, dy, w_up, w_down, w_qkv, w_out, ga, sa, gm, sm, bu, bq, lens, n, cid):
    own, d = x.shape
    tok = own * n
    w = d // n
    f = w_up.shape[1] // n
    row = lambda i: (i, 0)
    lane = lambda rows: pl.BlockSpec((rows, own), lambda i: (0, i))
    nat = lambda cols: pl.BlockSpec((own, cols), row)
    one = pl.Buffered(1)
    const = lambda shape: pl.BlockSpec(shape, lambda i: (0,) * len(shape), pipeline_mode=one)
    hbm = pl.BlockSpec(memory_space=pl.ANY)
    sds = jax.ShapeDtypeStruct
    return pl.pallas_call(
        functools.partial(head_kernel, w // HD),
        grid=(n,),
        in_specs=[hbm] * 6
        + [const(v.shape) for v in (ga, sa, gm, sm, bu, bq)]
        + [pl.BlockSpec(memory_space=pltpu.SMEM)],
        out_specs=[nat(d)] * 3
        + [lane(w)] * 4
        + [nat(w)] * 2
        + [lane(HALF)] * 2
        + [const((own, d))] * 2
        + [const((4, d // 8 + d // 32, d))] * 2
        + [const((2, 3 * d // 32, d))] * 4
        + [const((3 * w, d)), const((8, d)), const((8, f))],
        out_shape=tuple(
            [sds((tok, d), BF)] * 3
            + [sds((w, tok), BF)] * 4
            + [sds((tok, w), BF)] * 2
            + [sds((HALF, tok), F32)] * 2
            + [sds((own, d), BF)] * 2
            + [sds((4, d // 8 + d // 32, d), BF)] * 2
            + [sds((2, 3 * d // 32, d), BF)] * 4
            + [sds((3 * w, d), BF), sds((8, d), F32), sds((8, f), F32)]
        ),
        scratch_shapes=[
            pltpu.VMEM((4, own, d), BF),
            pltpu.VMEM((4, own, d), BF),
            pltpu.VMEM((d, f), BF),
            pltpu.VMEM((f, d), BF),
            pltpu.VMEM((d, 3 * w), BF),
            pltpu.VMEM((3 * w, d), BF),
            pltpu.VMEM((w, d), BF),
            pltpu.VMEM((3 * w, 128), F32),
            pltpu.VMEM((8, 4 * f), F32),
            pltpu.VMEM((8, f), F32),
            pltpu.VMEM((4, own, d), BF),
            pltpu.VMEM((own, d), BF),
            pltpu.VMEM((own, d), BF),
            pltpu.VMEM((d, f), F32),
            pltpu.VMEM((f, d), F32),
            pltpu.SemaphoreType.DMA((22,)),
            pltpu.SemaphoreType.DMA((13,)),
            pltpu.SemaphoreType.DMA((13,)),
        ],
        compiler_params=pltpu.CompilerParams(
            vmem_limit_bytes=VMEM_LIMIT, collective_id=cid, has_side_effects=True
        ),
        cost_estimate=pl.CostEstimate(
            flops=12 * tok * d * f + 10 * tok * d * w, bytes_accessed=12 * tok * d + 8 * d * f, transcendentals=2 * tok * f
        ),
        name="head_stage",
    )(x, dy, w_up, w_down, w_qkv, w_out, ga, sa, gm, sm, bu, bq, lens)


def attn_kernel(nh, tok, blk, per, halved, lens, rel, cos, sin, qt, kt, vt, dot, kn, vn,
                gt_ref, ctx_ref, exps, low_exps, dk, dv, oacc, dqacc, mpart, lpart, rowsc, qpad, dopad):
    nseq = lens.shape[0]
    nblk = tok // blk
    shift = rel[0]
    heads = range(nh)

    def place(b):
        chunk = (b // per) ^ shift
        half = b % per
        at = chunk * per + half
        if halved:
            at = jnp.where(chunk < 2, at, 4 + (chunk - 2) + 2 * half)
        return pl.multiple_of(at * blk, blk)

    def rows_of(h):
        return slice(h * HD, (h + 1) * HD)

    def pair_of(h):
        return slice((h // 2) * 128, (h // 2) * 128 + 128)

    def fold(v, op):
        return op(v.reshape(blk // 8, 8, blk), axis=0)

    def begin_of(at):
        begin = jnp.int32(0)
        total = jnp.int32(0)
        for s in range(nseq - 1):
            total = total + lens[s]
            begin = jnp.where(at >= total, total, begin)
        return begin

    dk[...] = jnp.zeros_like(dk)
    dv[...] = jnp.zeros_like(dv)
    qpad[...] = jnp.zeros_like(qpad)
    dopad[...] = jnp.zeros_like(dopad)
    rows_iota = lax.broadcasted_iota(jnp.int32, (blk, blk), 0)
    cols_iota = lax.broadcasted_iota(jnp.int32, (1, blk), 1)

    def one_block(i, carry):
        first_tok = i * blk
        count = i - begin_of(first_tok) // blk + 1
        last_begin = begin_of(first_tok + blk - 1)
        cols = pl.ds(place(i), blk)
        query_idx = cols_iota + first_tok
        start_row = begin_of(query_idx)
        for h in heads:
            half = (h % 2) * HD
            qpad[h, half : half + HD, :] = qt[rows_of(h), cols]

        krow = pl.ds(place(i), blk)
        kidx = rows_iota + first_tok
        allowed = (kidx >= start_row) & (kidx <= query_idx)
        for h in heads:
            s = jnp.where(allowed, mm(kn[krow, pair_of(h)], qpad[h]), -1e30)
            exps[h, 0] = s
            mpart[h] = fold(s, jnp.max)

        def scores(step, c):
            b = i - step
            krow = pl.ds(place(b), blk)
            edge = last_begin > b * blk

            @pl.when(edge)
            def _():
                allowed = (rows_iota + b * blk) >= start_row
                for h in heads:
                    s = jnp.where(allowed, mm(kn[krow, pair_of(h)], qpad[h]), -1e30)
                    exps[h, step] = s
                    mpart[h] = jnp.maximum(mpart[h], fold(s, jnp.max))

            @pl.when(jnp.logical_not(edge))
            def _():
                for h in heads:
                    s = mm(kn[krow, pair_of(h)], qpad[h])
                    exps[h, step] = s
                    mpart[h] = jnp.maximum(mpart[h], fold(s, jnp.max))

            return c

        lax.fori_loop(1, count, scores, 0)
        for h in heads:
            rowsc[h : h + 1, :] = jnp.max(mpart[h], axis=0, keepdims=True)
        lpart[...] = jnp.zeros_like(lpart)
        oacc[...] = jnp.zeros_like(oacc)

        def weights(step, c):
            kcols = pl.ds(place(i - step), blk)
            for h in heads:
                e = jnp.exp(exps[h, step] - rowsc[h : h + 1, :])
                exps[h, step] = e
                lpart[h] += fold(e, jnp.sum)
                low = e.astype(BF)
                low_exps[h, step] = low
                oacc[h] += mm(vt[rows_of(h), kcols], low)
            return c

        lax.fori_loop(0, count, weights, 0)
        for h in heads:
            half = (h % 2) * HD
            inv = 1.0 / jnp.sum(lpart[h], axis=0, keepdims=True)
            o = oacc[h] * inv
            ctx_ref[rows_of(h), cols] = o.astype(BF)
            scaled = (dot[rows_of(h), cols].astype(F32) * inv).astype(BF)
            dopad[h, half : half + HD, :] = scaled
            rowsc[h : h + 1, :] = jnp.sum(o * scaled.astype(F32), axis=0, keepdims=True)
        dqacc[...] = jnp.zeros_like(dqacc)

        def backward(step, c):
            kcols = pl.ds(place(i - step), blk)
            dps = [mm(vn[kcols, pair_of(h)], dopad[h]) for h in heads]
            dss = [(exps[h, step] * (dps[h] - rowsc[h : h + 1, :])).astype(BF) for h in heads]
            dvs = [mm(dopad[h, (h % 2) * HD : (h % 2) * HD + HD, :], low_exps[h, step], NT) for h in heads]
            dks = [mm(qt[rows_of(h), cols], dss[h], NT) for h in heads]
            dqs = [mm(kt[rows_of(h), kcols], dss[h]) for h in heads]
            for h in heads:
                dv[rows_of(h), kcols] += dvs[h]
                dk[rows_of(h), kcols] += dks[h]
                dqacc[rows_of(h), :] += dqs[h]
            return c

        lax.fori_loop(0, count, backward, 0)
        co = cos[:, cols]
        si = sin[:, cols]
        for h in heads:
            base = h * HD
            g = dqacc[base : base + HD, :] * (HD**-0.5)
            g1 = g[:HALF]
            g2 = g[HALF:ROT]
            gt_ref[base : base + HD, cols] = jnp.concatenate(
                [g1 * co + g2 * si, g2 * co - g1 * si, g[ROT:]], axis=0
            ).astype(BF)
        return carry

    lax.fori_loop(0, nblk, one_block, 0)

    def finish(i, carry):
        cols = pl.ds(pl.multiple_of(i * blk, blk), blk)
        co = cos[:, cols]
        si = sin[:, cols]
        for h in heads:
            base = h * HD
            g = dk[base : base + HD, cols]
            g1 = g[:HALF]
            g2 = g[HALF:ROT]
            gt_ref[nh * HD + base : nh * HD + base + HD, cols] = jnp.concatenate(
                [g1 * co + g2 * si, g2 * co - g1 * si, g[ROT:]], axis=0
            ).astype(BF)
        gt_ref[2 * nh * HD :, cols] = dv[:, cols].astype(BF)
        return carry

    lax.fori_loop(0, nblk, finish, 0)


def attention(lens, rel, cos, sin, qt, kt, vt, dot, kn, vn, chunk, maxlen, halved=False, blk=256):
    width, tok = qt.shape
    nh = width // HD
    wb = maxlen // blk + 1
    vm = pl.BlockSpec(memory_space=pltpu.VMEM)
    sm = pl.BlockSpec(memory_space=pltpu.SMEM)
    return pl.pallas_call(
        functools.partial(attn_kernel, nh, tok, blk, chunk // blk, halved),
        out_shape=(jax.ShapeDtypeStruct((3 * width, tok), BF), jax.ShapeDtypeStruct((width, tok), BF)),
        in_specs=[sm, sm] + [vm] * 8,
        out_specs=(vm, vm),
        scratch_shapes=[
            pltpu.VMEM((nh, wb, blk, blk), F32),
            pltpu.VMEM((nh, wb, blk, blk), BF),
            pltpu.VMEM((width, tok), F32),
            pltpu.VMEM((width, tok), F32),
            pltpu.VMEM((nh, HD, blk), F32),
            pltpu.VMEM((width, blk), F32),
            pltpu.VMEM((nh, 8, blk), F32),
            pltpu.VMEM((nh, 8, blk), F32),
            pltpu.VMEM((8, blk), F32),
            pltpu.VMEM((nh, 128, blk), BF),
            pltpu.VMEM((nh, 128, blk), BF),
        ],
        compiler_params=pltpu.CompilerParams(vmem_limit_bytes=VMEM_LIMIT),
        cost_estimate=pl.CostEstimate(
            flops=20 * width * tok * maxlen, bytes_accessed=20 * width * tok, transcendentals=nh * tok * maxlen
        ),
        name="attention",
    )(lens, rel, cos, sin, qt, kt, vt, dot, kn, vn)


def post_kernel(pos, gt_ref, na_ref, gm_ref, wq, wk, wv, gain, shift, g_ref, out_w, bias, small, dw):
    step = pl.program_id(0)

    @pl.when(step == 0)
    def _():
        dw[...] = jnp.zeros_like(dw)
        bias[...] = jnp.zeros_like(bias)
        small[...] = jnp.zeros_like(small)

    gt = gt_ref[...]
    na = na_ref[...]
    w = wq.shape[1]
    scale = gain[...].astype(F32)
    gn = gt.T
    r = mm(gn[:, :w], wq[...], NT) + mm(gn[:, w : 2 * w], wk[...], NT) + mm(gn[:, 2 * w :], wv[...], NT)
    g_ref[...] = (r * scale + gm_ref[...].astype(F32)).astype(BF)
    small[0:1, :] += jnp.sum(r * na.astype(F32), axis=0, keepdims=True)
    small[1:2, :] += jnp.sum(r, axis=0, keepdims=True)
    bias[0:1, :] += jnp.sum(gn.astype(F32), axis=0, keepdims=True)
    dw[...] += mm(gt, na)

    @pl.when(step == pl.num_programs(0) - 1)
    def _():
        for b in range(dw.shape[1] // 128):
            out_w[b] = dw[:, b * 128 : (b + 1) * 128].astype(BF)
        small[0:1, :] = (small[0:1, :] - shift[...].astype(F32) * small[1:2, :]) / scale


def post(pos, gt, na, gm, w_qkv, gain, shift, n, tt=512):
    tok, d = na.shape
    w = d // n
    row = lambda i, p: (i, 0)
    zero = lambda i, p: (0, 0)
    one = pl.Buffered(1)
    const = lambda shape: pl.BlockSpec(shape, zero, pipeline_mode=one)
    wspec = lambda k: pl.BlockSpec((d, w), lambda i, p: (0, k * n + p[0]), pipeline_mode=one)
    grid_spec = pltpu.PrefetchScalarGridSpec(
        num_scalar_prefetch=1,
        grid=(tok // tt,),
        in_specs=[
            pl.BlockSpec((3 * w, tt), lambda i, p: (0, i)),
            pl.BlockSpec((tt, d), row),
            pl.BlockSpec((tt, d), row),
            wspec(0),
            wspec(1),
            wspec(2),
            const((1, d)),
            const((1, d)),
        ],
        out_specs=[
            pl.BlockSpec((tt, d), row),
            pl.BlockSpec((d // 128, 3 * w, 128), lambda i, p: (0, 0, 0), pipeline_mode=one),
            const((8, 3 * w)),
            const((8, d)),
        ],
        scratch_shapes=[pltpu.VMEM((3 * w, d), F32)],
    )
    return pl.pallas_call(
        post_kernel,
        grid_spec=grid_spec,
        out_shape=(
            jax.ShapeDtypeStruct((tok, d), BF),
            jax.ShapeDtypeStruct((d // 128, 3 * w, 128), BF),
            jax.ShapeDtypeStruct((8, 3 * w), F32),
            jax.ShapeDtypeStruct((8, d), F32),
        ),
        compiler_params=pltpu.CompilerParams(vmem_limit_bytes=VMEM_LIMIT),
        cost_estimate=pl.CostEstimate(
            flops=12 * tok * d * w, bytes_accessed=8 * tok * d + 6 * tok * w + 18 * d * w, transcendentals=0
        ),
        name="post",
    )(pos, gt, na, gm, w_qkv, w_qkv, w_qkv, gain, shift)


def tail_kernel(gt_h, na_h, gm_h, ctx_h, dya_h, wt_h, wo_h, upk_h, upo_h, dn0_h, dn1_h, dn2_h, dn3_h, x_h, pown_h, py_h,
                gain, shift_ref, bo, bd, small, smallf,
                out_ref, g_ref, wup_ref, wdn_ref, wq_ref, wout_ref, sums_ref,
                gt, na, gm, ctx, dya, wt, wo, upk, upo, dn, xo, pown, py,
                ctx_in, up4, up_in, dn_in, dn2,
                dwq, qa_in, qb_in, qa4, qb4, qa_in2, qb_in2, qa2, qb2, qa_in3, qb_in3, qfin, q_own,
                dwo, wo_in, wo4, wo_in2, wo2, wo_in3, fin, piece2, own_in, owner_in2,
                far_in, near_in, far_sum, y_in, sm, sm_in, load, send, recv):
    i = lax.axis_index("dp")
    j = lax.axis_index("head")
    own, d = x_h.shape
    w = wt.shape[0] // 3
    half = own // 2
    bx = i % 2
    b0 = (i // 2) % 2
    b1 = i // 4
    z = i // 2
    mesh_id = pl.DeviceIdType.MESH
    core, across, diag = {"head": j ^ 1}, {"head": j ^ 2}, {"head": j ^ 3}
    px, p0, p1 = {"dp": i ^ 1}, {"dp": i ^ 2}, {"dp": i ^ 4}
    lo, hi = pl.ds(0, half), pl.ds(half, half)
    count = [0]
    started = []

    def remote(src, dst, to):
        k = count[0]
        count[0] += 1
        return pltpu.make_async_remote_copy(
            src_ref=src, dst_ref=dst, send_sem=send.at[k], recv_sem=recv.at[k], device_id=to, device_id_type=mesh_id)

    def go(*copies):
        for c in copies:
            c.start()
            started.append(c)

    def local(src, dst, k):
        return pltpu.make_async_copy(src, dst, load.at[k])

    loads = [
        local(upk_h, upk, 0), local(upo_h, upo, 1),
        local(dn0_h, dn.at[0], 2), local(dn1_h, dn.at[1], 3), local(dn2_h, dn.at[2], 4), local(dn3_h, dn.at[3], 5),
        local(gt_h, gt, 6), local(na_h, na, 7), local(wt_h, wt, 8), local(ctx_h, ctx, 9), local(dya_h, dya, 10),
        local(gm_h, gm, 11), local(wo_h, wo, 12), local(x_h, xo, 13), local(pown_h, pown, 14), local(py_h, py, 15),
    ]
    c_ctx = [
        remote(ctx_h.at[:, pl.ds(2 * own, half)], ctx_in.at[1, :, lo], across),
        remote(ctx_h.at[:, pl.ds(3 * own, half)], ctx_in.at[1, :, hi], across),
        remote(ctx_h.at[:, pl.ds(2 * own + half, half)], ctx_in.at[2, :, lo], diag),
        remote(ctx_h.at[:, pl.ds(3 * own + half, half)], ctx_in.at[2, :, hi], diag),
        remote(ctx_h.at[:, pl.ds(own, own)], ctx_in.at[0], core),
    ]
    c_up = [remote(up4.at[z ^ k], up_in.at[k - 1], {"dp": i ^ (2 * k)}) for k in (1, 2, 3)]
    c_dnx = remote(dn2.at[1 - bx], dn_in, px)
    rows = dwq.shape[3] // 2
    ra, rb = pl.ds(0, rows), pl.ds(rows, rows)
    c_qa = remote(dwq.at[:, :, 1 - bx, ra], qa_in, px)
    c_qb = remote(dwq.at[:, :, 1 - bx, rb], qb_in, px)
    c_qa0 = remote(qa4.at[:, 1 - b0], qa_in2, p0)
    c_qb0 = remote(qb4.at[:, 1 - b0], qb_in2, p0)
    c_qa1 = remote(qa2.at[1 - b1], qa_in3, p1)
    c_qb1 = remote(qb2.at[1 - b1], qb_in3, p1)
    c_wox = remote(dwo.at[:, :, 1 - bx], wo_in, px)
    c_wo0 = remote(wo4.at[:, 1 - b0], wo_in2, p0)
    c_wo1 = remote(wo2.at[1 - b1], wo_in3, p1)
    c_g = [
        remote(gm.at[pl.ds(2 * own + half, half)], far_in.at[lo], core),
        remote(gm.at[pl.ds(3 * own + half, half)], far_in.at[hi], core),
        remote(gm.at[pl.ds(own, own)], near_in, core),
    ]
    c_y = [remote(far_sum.at[lo], y_in.at[lo], across), remote(far_sum.at[hi], y_in.at[hi], across)]
    c_sm = [remote(sm.at[s], sm_in.at[s], to) for s, to in enumerate((core, across, px, p0, p1))]
    c_own = [remote(fin.at[j ^ r], own_in.at[j], {"head": j ^ r}) for r in (1, 2, 3)]
    dests = []
    c_own2 = []
    for r in range(4):
        di, dj = 2 * j + i // 4, (i % 4) ^ r
        dests.append((di, dj))
        cut = pl.ds(pl.multiple_of(dj * w, 128), w)
        c_own2.append(remote(piece2.at[:, cut], owner_in2.at[i % 4], {"dp": di, "head": dj}))
    c_q = []
    q_dst = []
    for t in range(3):
        dst = (t - j + 4) % 4
        q_dst.append(dst)
        c_q.append(remote(qfin.at[(3 * dst + t) // 4], q_own.at[t], {"head": dst}))

    barrier = pltpu.get_barrier_semaphore()
    for to in (core, across, diag, px, p0, p1, {"dp": i ^ 6}):
        pl.semaphore_signal(barrier, inc=1, device_id=to, device_id_type=mesh_id)
    for c in loads:
        c.start()
    for r in range(4):
        si, sj = 4 * (i % 2) + (j ^ r), i // 2

        @pl.when((si != i) | (sj != j))
        def _():
            pl.semaphore_signal(barrier, inc=1, device_id={"dp": si, "head": sj}, device_id_type=mesh_id)

    to_self = jnp.where(2 * j + i // 4 == i, 1, 0)
    pl.semaphore_wait(barrier, 11 - to_self)

    go(*c_ctx)

    def added(a, b):
        return a.astype(F32) + b.astype(F32)

    def ready(first, last):
        for k in range(first, last):
            loads[k].wait()

    ready(0, 2)
    up4[...] = added(upk[...], upo[...]).astype(BF)
    go(*c_up)
    ready(2, 6)
    dn2[...] = (added(dn[0], dn[1]) + added(dn[2], dn[3])).astype(BF)
    go(c_dnx)

    ready(6, 9)
    gains = [jnp.zeros((1, 256), F32)] * 4
    for part, c in ((ra, c_qa), (rb, c_qb)):
        left = gt[part, :]
        for k in range(4):
            t = mm(left, na[:, 256 * k : 256 * (k + 1)])
            gains[k] += jnp.sum(t * wt[part, 256 * k : 256 * (k + 1)].astype(F32), axis=0, keepdims=True)
            t = t.astype(BF)
            dwq[k // 2, k % 2, 0, part] = t[:, :128]
            dwq[k // 2, k % 2, 1, part] = t[:, 128:]
        if c is c_qa:
            go(c)
    s_bias = mm(jnp.ones((8, gt.shape[1]), BF), gt[...], NT)[0:1]
    high = s_bias.astype(BF)
    low = (s_bias - high.astype(F32)).astype(BF)
    s_shift = mm(jnp.broadcast_to(high, (8, 3 * w)), wt[...])[0:1] + mm(jnp.broadcast_to(low, (8, 3 * w)), wt[...])[0:1]
    s_gain = jnp.concatenate(gains, axis=1)
    scale = flat(gain[...])

    sm[0] = jnp.zeros((16, d), F32)
    sm[0, 0:1, :] = (s_gain - flat(shift_ref[...]) * s_shift) / scale
    sm[0, 1:2, :] = s_shift
    for k in range(3):
        sm[0, 2 + k : 3 + k, pl.ds(pl.multiple_of(j * w, 128), w)] = s_bias[:, k * w : (k + 1) * w]
    sm[0, 5:7, :] = small[0:2, :]
    sm[0, 7:8, :] = small[2:3, :] * 0.25
    part_u = d // 8
    for b in range(8):
        at = pl.multiple_of((b % 2) * 4 * part_u + j * part_u, 128)
        sm[0, 8 + b // 2 : 9 + b // 2, pl.ds(at, part_u)] = smallf[0:1, b * part_u : (b + 1) * part_u]
    go(c_sm[0])

    def small_step(s):
        c_sm[s].wait_recv()
        sm[s + 1] = sm[s] + sm_in[s]
        if s < 4:
            go(c_sm[s + 1])

    ready(9, 11)
    t = mm(ctx[...], dya[...]).astype(BF)
    for b in range(8):
        dwo[b // 4, (b // 2) % 2, b % 2] = t[32 * b : 32 * (b + 1)]
    small_step(0)

    ready(11, 12)

    def tile(at):
        ts = slice(at, at + own)
        r = mm(gt[:, ts].T, wt[...])
        gm[ts, :] = (r * scale + gm[ts, :].astype(F32)).astype(BF)

    tile(2 * own)
    go(c_g[0])
    tile(3 * own)
    go(c_g[1])
    c_g[0].wait_recv()
    far_sum[lo] = added(gm[2 * own : 2 * own + half], far_in[lo]).astype(BF)
    go(c_y[0])
    small_step(1)
    go(c_qb, c_wox)
    c_g[1].wait_recv()
    far_sum[hi] = added(gm[3 * own : 3 * own + half], far_in[hi]).astype(BF)
    go(c_y[1])
    tile(own)
    go(c_g[2])
    small_step(2)
    c_qa.wait_recv()
    qa4[...] = added(dwq[:, :, bx, ra], qa_in[...]).astype(BF)
    go(c_qa0)
    tile(0)
    small_step(3)

    ready(12, 16)
    attn = mm(ctx[:, :own], wo[pl.ds(pl.multiple_of(j * w, 128), w), :], TN)
    c_ctx[4].wait_recv()
    attn += mm(ctx_in[0], wo[pl.ds(pl.multiple_of((j ^ 1) * w, 128), w), :], TN)
    for k in range(4):
        c_ctx[k].wait_recv()
    attn += mm(ctx_in[1], wo[pl.ds(pl.multiple_of((j ^ 2) * w, 128), w), :], TN)
    attn += mm(ctx_in[2], wo[pl.ds(pl.multiple_of((j ^ 3) * w, 128), w), :], TN)
    out_ref[...] = (
        xo[...].astype(F32) + attn + added(pown[...], py[...]) + (flat(bo[...]) + flat(bd[...]))
    ).astype(BF)

    c_qa0.wait_recv()
    qa2[...] = added(qa4[:, b0], qa_in2[...]).astype(BF)
    go(c_qa1)
    c_qb.wait_recv()
    qb4[...] = added(dwq[:, :, bx, rb], qb_in[...]).astype(BF)
    go(c_qb0)
    for c in c_up:
        c.wait_recv()
    c_dnx.wait_recv()
    mine = up4[z].astype(F32) + up_in[0].astype(F32) + added(up_in[1], up_in[2])
    nu = wup_ref.shape[0]
    nd = dn2.shape[1]
    down = added(dn2[bx], dn_in[...])
    for a in range(4):
        cut = slice(a * w, (a + 1) * w)
        fin[a, :nu] = mine[:nu, cut].astype(BF)
        fin[a, nu : nu + nd] = down[:, cut].astype(BF)
        fin[a, nu + nd :] = mine[nu:, cut].astype(BF)
    go(*c_own)
    own_in[j] = fin[j]
    small_step(4)
    sums_ref[...] = sm[5]
    c_wox.wait_recv()
    wo4[...] = added(dwo[:, :, bx], wo_in[...]).astype(BF)
    go(c_wo0)
    c_qb0.wait_recv()
    qb2[...] = added(qb4[:, b0], qb_in2[...]).astype(BF)
    go(c_qb1)
    c_wo0.wait_recv()
    wo2[...] = added(wo4[:, b0], wo_in2[...]).astype(BF)
    go(c_wo1)
    c_qa1.wait_recv()
    c_qb1.wait_recv()
    done = jnp.concatenate([added(qa2[b1], qa_in3[...]), added(qb2[b1], qb_in3[...])], axis=0).astype(BF)
    for k in range(3):
        qfin[k] = done[k * w : (k + 1) * w]
    for t in range(3):

        @pl.when(q_dst[t] != j)
        def _():
            c_q[t].start()

        @pl.when(q_dst[t] == j)
        def _():
            q_own[t] = qfin[(3 * j + t) // 4]

    c_wo1.wait_recv()
    piece2[...] = added(wo2[b1], wo_in3[...]).astype(BF)
    for r in range(4):
        di, dj = dests[r]

        @pl.when((di != i) | (dj != j))
        def _():
            c_own2[r].start()

        @pl.when((di == i) & (dj == j))
        def _():
            owner_in2[i % 4] = piece2[:, pl.ds(pl.multiple_of(dj * w, 128), w)]


    c_g[2].wait_recv()
    c_y[0].wait_recv()
    g_ref[lo] = added(gm[lo], near_in[lo]) + y_in[lo].astype(F32)
    c_y[1].wait_recv()
    g_ref[hi] = added(gm[hi], near_in[hi]) + y_in[hi].astype(F32)

    for t in range(3):

        @pl.when(q_dst[t] != j)
        def _():
            c_q[t].wait_recv()

        wq_ref[:, t * w : (t + 1) * w] = q_own[t].astype(F32).T.astype(BF)
    for r in range(4):
        di, dj = dests[r]

        @pl.when((di != i) | (dj != j))
        def _():
            c_own2[r].wait_recv()

    for c in c_own:
        c.wait_recv()
    no = piece2.shape[0]
    for a in range(4):
        wup_ref[:, a * part_u : (a + 1) * part_u] = own_in[a, :nu, :part_u]
        wup_ref[:, (4 + a) * part_u : (5 + a) * part_u] = own_in[a, :nu, part_u:]
        wdn_ref[a * nu : (a + 1) * nu, :] = own_in[a, nu:]
        wout_ref[a * no : (a + 1) * no, :] = owner_in2[a]

    for c in started:
        c.wait_send()
    for t in range(3):

        @pl.when(q_dst[t] != j)
        def _():
            c_q[t].wait_send()

    for r in range(4):
        di, dj = dests[r]

        @pl.when((di != i) | (dj != j))
        def _():
            c_own2[r].wait_send()


def tail_stage(gt, na, gm, ctx, dya, wt, w_out, upk, upo, dn, x, pown, py, ga, sa, bo, bd, small, smallf, cid):
    own, d = x.shape
    tok = na.shape[0]
    w = d // 4
    vm = pl.BlockSpec(memory_space=pltpu.VMEM)
    hbm = pl.BlockSpec(memory_space=pl.ANY)
    sds = jax.ShapeDtypeStruct
    big = lambda *s: pltpu.VMEM(s, BF)
    nb = d // 8
    nu = upk.shape[1]
    nd = dn[0].shape[1]
    no = w // 8
    r2 = 3 * w // 2
    return pl.pallas_call(
        tail_kernel,
        in_specs=[hbm] * 16 + [vm] * 6,
        out_specs=[vm] * 7,
        out_shape=(
            sds((own, d), BF), sds((own, d), F32), sds((nb, d), BF), sds((4 * nb, w), BF),
            sds((nb, 3 * w), BF), sds((4 * no, w), BF), sds((16, d), F32),
        ),
        scratch_shapes=[
            big(3 * w, tok), big(tok, d), big(tok, d), big(w, tok), big(tok, d), big(3 * w, d), big(d, d),
            big(4, nu, d), big(4, nu, d), big(4, 2, nd, d),
            big(own, d), big(own, d), big(own, d),
            big(3, w, own), big(4, nu, d), big(3, nu, d), big(nd, d), big(2, nd, d),
            big(2, 2, 2, 3 * w, 128), big(2, 2, r2, 128), big(2, 2, r2, 128), big(2, 2, r2, 128), big(2, 2, r2, 128),
            big(2, r2, 128), big(2, r2, 128), big(2, r2, 128), big(2, r2, 128), big(r2, 128), big(r2, 128),
            big(3, w, 128), big(3, w, 128),
            big(2, 2, 2, no, d), big(2, 2, no, d), big(2, 2, no, d), big(2, no, d), big(2, no, d), big(no, d),
            big(4, 2 * nb, w), big(no, d), big(4, 2 * nb, w), big(4, no, w),
            big(own, d), big(own, d), big(own, d), big(own, d),
            pltpu.VMEM((6, 16, d), F32), pltpu.VMEM((5, 16, d), F32),
            pltpu.SemaphoreType.DMA((16,)), pltpu.SemaphoreType.DMA((40,)), pltpu.SemaphoreType.DMA((40,)),
        ],
        compiler_params=pltpu.CompilerParams(vmem_limit_bytes=VMEM_LIMIT, collective_id=cid, has_side_effects=True),
        cost_estimate=pl.CostEstimate(
            flops=14 * tok * d * w, bytes_accessed=10 * tok * d, transcendentals=0
        ),
        name="tail_stage",
    )(gt, na, gm, ctx, dya, wt, w_out, upk, upo, *dn, x, pown, py, ga, sa, bo, bd, small, smallf)


def final_kernel(out_t, g_ref, x_ref, dy_ref, wup, wdn, wq, wout, sums,
                 out, gin, ga, sa, gm, sm, dwq, bq, dwout, bo, dwup, bu, dwdn, bd):
    out[...] = out_t[...]
    normed, inv = norm_parts(x_ref[...])
    g = g_ref[...]
    gin[...] = dy_ref[...].astype(F32) + inv * (
        g - jnp.mean(g, axis=-1, keepdims=True) - normed * jnp.mean(g * normed, axis=-1, keepdims=True)
    )

    @pl.when(pl.program_id(0) == 0)
    def _():
        d = sums.shape[1]
        for ref, first, count in ((ga, 0, 1), (sa, 1, 1), (bq, 2, 3), (gm, 5, 1), (sm, 6, 1), (bo, 7, 1), (bd, 7, 1), (bu, 8, 4)):
            for k in range(count):
                ref[k * d : (k + 1) * d] = sums[first + k, :]
        dwup[...] = wup[...].astype(F32)
        dwdn[...] = wdn[...].astype(F32)
        dwq[...] = wq[...].astype(F32)
        dwout[...] = wout[...].astype(F32)


def final_stage(out_t, g, x, dy, wup, wdn, wq, wout, sums, steps=2):
    own, d = x.shape
    row = pl.BlockSpec((own // steps, d), lambda i: (i, 0))
    const = lambda v: pl.BlockSpec(v.shape, lambda i: (0,) * len(v.shape))
    sds = lambda *s: jax.ShapeDtypeStruct(s, F32)
    like = lambda v: sds(*v.shape)
    outs = (
        jax.ShapeDtypeStruct((own, d), BF), sds(own, d), sds(d), sds(d), sds(d), sds(d), like(wq), sds(3 * d),
        like(wout), sds(d), like(wup), sds(4 * d), like(wdn), sds(d),
    )
    return pl.pallas_call(
        final_kernel,
        grid=(steps,),
        in_specs=[row, row, row, row] + [const(v) for v in (wup, wdn, wq, wout, sums)],
        out_specs=[row, row] + [const(v) for v in outs[2:]],
        out_shape=outs,
        compiler_params=pltpu.CompilerParams(vmem_limit_bytes=VMEM_LIMIT),
        name="final_stage",
    )(out_t, g, x, dy, wup, wdn, wq, wout, sums)


def layout(seq_lens, index):
    ends = jnp.cumsum(seq_lens, dtype=jnp.int32)
    starts = ends - seq_lens
    first = jnp.zeros_like(index)
    for s in range(1, seq_lens.shape[0]):
        first = jnp.where(index >= starts[s], starts[s], first)
    return first, index - first


def head_perm(v, bit):
    return lax.ppermute(v, "head", [(k, k ^ bit) for k in range(4)])


def dp_perm(v, bit):
    return lax.ppermute(v, "dp", [(k, k ^ bit) for k in range(8)])


def fast_body(inputs, lengths, attn_gain, attn_shift, mlp_gain, mlp_shift, w_qkv, b_qkv, w_out, b_out,
              w_up, b_up, w_down, b_down, cotangent):
    own, d = inputs.shape
    n = 4
    tok = own * n
    w = d // n
    pos = lax.axis_index("head").astype(jnp.int32).reshape(1)
    lens = lengths[0]
    (g_mlp, na, dy_all, qt, kt, vt, dot, kn, vn, cos, sin, p_own, p_far, up_keep, up_send, *dn, wt, small,
     smallf) = head_stage(
        inputs, cotangent, w_up, w_down, w_qkv, w_out, attn_gain, attn_shift, mlp_gain, mlp_shift, b_up, b_qkv, lens, n, 0
    )
    up_other = dp_perm(up_send, 1)
    dn = [dn[0]] + [dp_perm(dn[k], 2 * k) for k in (1, 2, 3)]
    p_y = head_perm(p_far, 2)
    gt, ctx = attention(lens, pos, cos, sin, qt, kt, vt, dot, kn, vn, own, tok // 2, halved=True)
    out_t, g, wup, wdn, wq, wout, sums = tail_stage(
        gt, na, g_mlp, ctx, dy_all, wt, w_out, up_keep, up_other, dn, inputs, p_own, p_y,
        attn_gain, attn_shift, b_out, b_down, small, smallf, 1
    )
    return tuple(final_stage(out_t, g, inputs, cotangent, wup, wdn, wq, wout, sums))


def general_body(inputs, lengths, attn_gain, attn_shift, mlp_gain, mlp_shift, w_qkv, b_qkv, w_out, b_out,
                 w_up, b_up, w_down, b_down, cotangent):
    own, d = inputs.shape
    n = lax.axis_size("head")
    n_dp = lax.axis_size("dp")
    tok = own * n
    w = d // n
    f = w_up.shape[1] // n
    j = lax.axis_index("head")
    pos = j.astype(jnp.int32).reshape(1)
    rows = lambda v: v.reshape(1, -1)
    ga, sa, gm, sm = rows(attn_gain), rows(attn_shift), rows(mlp_gain), rows(mlp_shift)
    bq, bu = rows(b_qkv), rows(b_up)
    lens = lengths[0]
    gather = lambda v: lax.all_gather(v, "head", axis=0, tiled=True)
    over_dp = lambda v, axis: lax.psum_scatter(v, "dp", scatter_dimension=axis, tiled=True)
    over_head = lambda v: lax.psum_scatter(v, "head", scatter_dimension=0, tiled=True)
    x_all = gather(inputs)
    dy_all = gather(cotangent)
    first, position = layout(lens, jnp.arange(tok, dtype=jnp.int32))
    freqs = 10000.0 ** (-(2.0 * jnp.arange(HALF, dtype=F32)) / ROT)
    angle = freqs[:, None] * position.astype(F32)[None, :]
    cos, sin = jnp.cos(angle), jnp.sin(angle)
    part, g_mlp, dwu, dwd, small, smallf = mlp(pos, x_all, dy_all, w_up, w_down, bu, gm, sm, n)
    qt, kt, vt, dot, kn, vn, na = proj(pos, x_all, dy_all, w_qkv, bq, w_out, ga, sa, cos, sin, n, tok, 0)
    gt, ctx = attention(
        lens, jnp.zeros((1,), jnp.int32), cos, sin, qt, kt, vt, dot, kn, vn, own, tok // 2
    )
    total, dwq, bias_q, small_q = post(pos, gt, na, g_mlp, w_qkv, ga, sa, n)
    attn_part = mm(ctx, lax.dynamic_slice_in_dim(w_out, j * w, w, 0), TN)
    bias = b_out.astype(F32) + b_down.astype(F32)
    output = inputs.astype(F32) + over_head((attn_part + part.astype(F32)).astype(BF)).astype(F32) + bias
    g_sum = over_head(total).astype(F32)
    normed, inv = norm_parts(inputs)
    grad_inputs = cotangent.astype(F32) + inv * (
        g_sum - jnp.mean(g_sum, axis=-1, keepdims=True) - normed * jnp.mean(g_sum * normed, axis=-1, keepdims=True)
    )
    dw_out = mm(ctx, dy_all).astype(BF)
    spread = lambda v: lax.all_to_all(v, "head", split_axis=1, concat_axis=0, tiled=True)
    grad_w_up = over_dp(dwu, 0).astype(F32)
    grad_w_down = over_dp(spread(dwd), 0).astype(F32)
    grad_w_out = over_dp(spread(dw_out), 0).astype(F32)
    qkv = over_dp(jnp.transpose(dwq, (0, 2, 1)).reshape(d, 3 * w), 0)
    qkv = lax.all_gather(qkv.reshape(d // n_dp, 3, w), "head", axis=2, tiled=True).reshape(d // n_dp, 3 * d)
    grad_w_qkv = lax.dynamic_slice_in_dim(qkv, j * 3 * w, 3 * w, 1).astype(F32)
    slots = jnp.where(jnp.arange(n)[:, None] == j, smallf[0:1], 0.0).reshape(-1)
    slots_q = jnp.where(jnp.arange(n)[None, :, None] == j, bias_q[0].reshape(3, 1, w), 0.0).reshape(-1)
    sums = lax.psum((small_q[0], small_q[1], small[0], small[1], slots_q, small[2] / n, slots), ("dp", "head"))
    return (output.astype(BF), grad_inputs, sums[0], sums[1], sums[2], sums[3], grad_w_qkv, sums[4],
            grad_w_out, sums[5], grad_w_up, sums[6], grad_w_down, sums[5])


def solution(mesh):
    fast = mesh.shape["dp"] == 8 and mesh.shape["head"] == 4
    whole = P(("dp", "head"), None)
    weight = P("dp", "head")
    return jax.shard_map(
        fast_body if fast else general_body,
        mesh=mesh,
        in_specs=(whole, P("dp", None)) + (P(),) * 12 + (whole,),
        out_specs=(whole, whole, P(), P(), P(), P(), weight, P(), weight, P(), weight, P(), weight, P()),
        check_vma=False,
    )
```
